256 devices in a mesh: section: 4 (over y), pix: 64 (over x, z, core).
Axes of the slice: x: 4, y: 4, z: 8, core: 2. Of those that a mesh axis runs over, the one named last changes fastest.
Arguments:
- slc: float32 [2, 200, 16384], P(None, 'section', 'pix'), may hold values from -6 to 6
- neighbours: int32 [15, 16384], P(None, 'pix'), may hold values from 0 to 16383, as said below
- reference_pixel: int32 [1], replicated, may hold values from 0 to 16383
Outputs:
- phases: float32 [2, 200, 16384], P(None, 'section', 'pix')
- compressed: float32 [2, 4, 16384], P(None, 'section', 'pix')
The draws below stay inside these ranges and needn't reach their ends.
Inputs may be any that keep to these rules, and one draw needn't show every extreme that they name: neighbours[0, p] = p; every entry lies within 256 of its column's pixel p, and that distance is reached.
All inputs are finite; a program needn't handle non-finite values.
Results may differ from the reference program's by a relative error of at most 0.0003.
Values sent between devices are 32-bit elements; how exact they have to be, the bound alone decides.
A program may use at most 64 MiB of HBM per device.

```python
import math
import jax
import jax.numpy as jnp
from jax import lax

M = 50
NEIGHBOURS = 15
ITERS = 16
STACK = 51
DATES = 200
PIXELS = 16384
REACH = 256
N_SECTION = 4


def draw_neighbours(key, part):
    offsets = jax.random.randint(key, (NEIGHBOURS, PIXELS), -REACH, REACH + 1)
    offsets = offsets.at[0].set(0)
    middle = PIXELS // 2
    offsets = offsets.at[1, middle].set(REACH)
    offsets = offsets.at[1, middle + 1].set(-REACH)
    places = jnp.arange(PIXELS, dtype=jnp.int32)[None, :]
    return jnp.clip(places + offsets, 0, PIXELS - 1).astype(jnp.int32)


def levels(stream_key, extent, cuts, least, largest):
    factor_of, own = 1.0, jax.random.fold_in(stream_key, 6)
    for axis_at, shards_of in cuts:
        heights = jnp.exp(jax.random.uniform(jax.random.fold_in(own, axis_at), (shards_of,), jnp.float32, least / len(cuts), largest / len(cuts)))
        factor_of = factor_of * jnp.repeat(heights, extent[axis_at] // shards_of).reshape([-1 if axis == axis_at else 1 for axis in range(len(extent))])
    return factor_of


def noise(stream_key, extent, spread, bound, split=(), kind=jnp.bfloat16):
    values = jax.random.normal(stream_key, extent, jnp.float32) * spread
    if len(split) > 0:
        values = levels(stream_key, extent, split, -0.22, 0.18) * values
    return jnp.clip(values, min=-bound, max=bound).astype(kind)


def setup_inputs(seed: int = 0) -> dict:
    key_list = jax.random.split(jax.random.key(seed), 4)
    return {
        "slc": noise(key_list[0], (2, DATES, PIXELS), 1.0, 6.0, ((1, 4), (2, 64)), jnp.float32),
        "neighbours": draw_neighbours(jax.random.fold_in(key_list[3], 71), 0),
        "reference_pixel": jax.random.randint(key_list[2], (1,), 0, PIXELS).astype(jnp.int32),
    }


FLOOR = 0.05

def unit(real, imag):
    scale = 1.0 / jnp.maximum(jnp.sqrt(real * real + imag * imag), FLOOR)
    return (real * scale, imag * scale)

def solve_block(ext_re, ext_im, index, own_re, own_im):
    near_re = ext_re[:, index]
    near_im = ext_im[:, index]
    power = lax.optimization_barrier(jnp.sum(near_re * near_re + near_im * near_im, axis=1))
    scale = 1.0 / jnp.sqrt(jnp.maximum(power, 1.0))
    z_re = near_re * scale[:, None, :]
    z_im = near_im * scale[:, None, :]
    count = own_re.shape[0]
    start_re = jnp.full(own_re.shape, 1.0 / math.sqrt(count), jnp.float32)
    start_im = jnp.zeros(own_re.shape, jnp.float32)

    def turn(step, carry):
        vec_re, vec_im = carry
        c_re = lax.optimization_barrier(jnp.sum(z_re * vec_re[:, None, :] + z_im * vec_im[:, None, :], axis=0))
        c_im = lax.optimization_barrier(jnp.sum(z_re * vec_im[:, None, :] - z_im * vec_re[:, None, :], axis=0))
        u_re = vec_re + lax.optimization_barrier(jnp.sum(z_re * c_re[None] - z_im * c_im[None], axis=1))
        u_im = vec_im + lax.optimization_barrier(jnp.sum(z_re * c_im[None] + z_im * c_re[None], axis=1))
        norm = jnp.sqrt(lax.optimization_barrier(jnp.sum(u_re * u_re + u_im * u_im, axis=0)))
        return (u_re / norm, u_im / norm)
    vec_re, vec_im = lax.fori_loop(0, ITERS, turn, (start_re, start_im))
    comp_re = lax.optimization_barrier(jnp.sum(vec_re * own_re + vec_im * own_im, axis=0))
    comp_im = lax.optimization_barrier(jnp.sum(vec_re * own_im - vec_im * own_re, axis=0))
    return (vec_re, vec_im, comp_re, comp_im)

def reference(slc, neighbours, reference_pixel):
    width = math.gcd(PIXELS, 2048)
    blocks = PIXELS // width
    virtual = jnp.zeros((2, PIXELS), jnp.float32)
    vectors = []
    packed = []
    for section in range(N_SECTION):
        stack = jnp.concatenate([virtual[:, None, :], slc[:, section * M:(section + 1) * M, :]], axis=1)

        def one(block):
            start = (block * width).astype(jnp.int32)
            index = lax.dynamic_slice_in_dim(neighbours, start, width, 1)
            own = lax.dynamic_slice_in_dim(stack, start, width, 2)
            return solve_block(stack[0], stack[1], index, own[0], own[1])
        vr, vi, cr, ci = lax.map(one, jnp.arange(blocks, dtype=jnp.int32))
        vec_re = jnp.transpose(vr, (1, 0, 2)).reshape(STACK, PIXELS)
        vec_im = jnp.transpose(vi, (1, 0, 2)).reshape(STACK, PIXELS)
        virtual = jnp.stack([cr.reshape(PIXELS), ci.reshape(PIXELS)])
        vectors.append((vec_re, vec_im))
        packed.append(virtual)
    datum_re = jnp.ones((PIXELS,), jnp.float32)
    datum_im = jnp.zeros((PIXELS,), jnp.float32)
    pieces = [None] * N_SECTION
    for section in range(N_SECTION - 1, -1, -1):
        vec_re, vec_im = vectors[section]
        s_re = vec_re[1:] * datum_re - vec_im[1:] * datum_im
        s_im = vec_re[1:] * datum_im + vec_im[1:] * datum_re
        pieces[section] = (s_re, s_im)
        f_re, f_im = unit(vec_re[0], vec_im[0])
        datum_re, datum_im = (datum_re * f_re - datum_im * f_im, datum_re * f_im + datum_im * f_re)
    series_re = jnp.concatenate([p[0] for p in pieces], axis=0)
    series_im = jnp.concatenate([p[1] for p in pieces], axis=0)
    ref_re = lax.dynamic_index_in_dim(series_re, reference_pixel[0], 1, False)
    ref_im = lax.dynamic_index_in_dim(series_im, reference_pixel[0], 1, False)
    u_re, u_im = unit(ref_re, ref_im)
    gain = math.sqrt(STACK)
    out_re = gain * (series_re * u_re[:, None] + series_im * u_im[:, None])
    out_im = gain * (series_im * u_re[:, None] - series_re * u_im[:, None])
    return (jnp.stack([out_re, out_im]), jnp.stack(packed, axis=1))
```

```python
import math

import jax
import jax.numpy as jnp
from jax import lax
from jax.experimental import pallas as pl
from jax.experimental.pallas import tpu as pltpu
from jax.sharding import PartitionSpec as P

ITERS = 16
FLOOR = 0.05
REACH = 256
NB = 15
ROWS = 50
PAD = 56
GROUPS = PAD // 8
TILES = 2
SPAN = 5
SCALE = 2.0**-45
START = 1.0 / math.sqrt(ROWS + 1)
GAIN = math.sqrt(ROWS + 1)
SECTIONS = 4
PIX = 64
MESH = pl.DeviceIdType.MESH
F32 = jnp.float32


def bcast(row):
    return jnp.broadcast_to(row, (8, 128))


def pick(sources, lane, tile):
    out = jnp.zeros((8, 128), F32)
    for m, source in enumerate(sources):
        got = jnp.take_along_axis(source, lane, axis=1, mode="promise_in_bounds")
        out = jnp.where(tile == m, got, out)
    return out


def column_sum(x):
    return jnp.sum(x, axis=0, keepdims=True)


def unit(re, im):
    scale = 1.0 / jnp.maximum(jnp.sqrt(re * re + im * im), FLOOR)
    return re * scale, im * scale


def remote(src, dst, send, recv, device):
    return pltpu.make_async_remote_copy(
        src_ref=src, dst_ref=dst, send_sem=send, recv_sem=recv, device_id=device, device_id_type=MESH
    )


def kernel(
    slc_hbm, nbr, ref, phases, comp,
    slc, left, right, ext, lanes, tiles, zs, kre, kim, cvec, bvec, xsum, zbuf, sbuf,
    vbuf, msg, fmsg, fbuf, series, rmsg, rbuf1, rmsg2, rbuf2,
    load_sem, halo_send, halo_recv, v_send, v_recv, f_send, f_recv, r_send, r_recv,
):
    sec = lax.axis_index("section")
    pix = lax.axis_index("pix")
    before = lax.rem(pix + (PIX - 1), PIX)
    after = lax.rem(pix + 1, PIX)
    near = (before, pix, after)
    sec_up = lax.rem(sec + 1, SECTIONS)
    sec_down = lax.rem(sec + (SECTIONS - 1), SECTIONS)
    x = pix // 16
    z = lax.rem(pix // 2, 8)
    core = lax.rem(pix, 2)
    group = x * 2 + core
    first = []
    second = []
    for d in range(1, 8):
        g = lax.rem(group + d, 8)
        first.append((g // 2) * 16 + z * 2 + lax.rem(g, 2))
        second.append(x * 16 + lax.rem(z + d, 8) * 2 + core)

    load = pltpu.make_async_copy(slc_hbm, slc, load_sem)
    load.start()
    barrier = pltpu.get_barrier_semaphore()
    peers = [(sec, before), (sec, after), (lax.rem(sec + 2, SECTIONS), pix)]
    peers += [(s, p) for s in (sec_up, sec_down) for p in near]
    peers += [(sec, p) for p in first + second]
    for peer in peers:
        pl.semaphore_signal(barrier, inc=1, device_id=peer, device_id_type=MESH)
    load.wait()
    pl.semaphore_wait(barrier, len(peers))

    to_left = remote(slc, right, halo_send.at[0], halo_recv.at[0], (sec, before))
    to_right = remote(slc, left, halo_send.at[1], halo_recv.at[1], (sec, after))
    to_left.start()
    to_right.start()

    base = pix * (TILES * 128) - REACH
    for t in range(TILES):
        rel = nbr[:, t * 128 : (t + 1) * 128] - (base + t * 128)
        lanes[t, 0:NB, :] = jnp.bitwise_and(rel, 127)
        tiles[t, 0:NB, :] = jnp.right_shift(rel, 7)
        lanes[t, NB : NB + 1, :] = jnp.zeros((1, 128), jnp.int32)
        tiles[t, NB : NB + 1, :] = jnp.full((1, 128), SPAN, jnp.int32)
    for c in range(2):
        for m in range(6):
            ext[c, m, PAD - 8 : PAD, :] = jnp.zeros((8, 128), F32)
        for m in range(2):
            ext[c, 2 + m, 0:ROWS, :] = slc[c, :, m * 128 : (m + 1) * 128]
    kre[...] = jnp.zeros_like(kre)
    kim[...] = jnp.zeros_like(kim)
    for t in range(TILES):
        for c in range(2):
            own = ext[c, 2 + t, 0:8, :]
            for g in range(1, GROUPS):
                own = own + ext[c, 2 + t, g * 8 : (g + 1) * 8, :]
            xsum[t, c : c + 1, :] = column_sum(own)

    to_left.wait()
    to_right.wait()
    for c in range(2):
        for m in range(2):
            ext[c, m, 0:ROWS, :] = left[c, :, m * 128 : (m + 1) * 128]
            ext[c, 4 + m, 0:ROWS, :] = right[c, :, m * 128 : (m + 1) * 128]

    for t in range(TILES):

        @pl.loop(0, GROUPS)
        def _(g):
            rows = pl.ds(pl.multiple_of(g * 8, 8), 8)
            src = [[ext[c, t + m, rows, :] for m in range(SPAN)] for c in range(2)]
            got = []
            power = jnp.zeros((8, 128), F32)
            for k in range(NB):
                if k == 0:
                    re, im = src[0][2], src[1][2]
                else:
                    lane = bcast(lanes[t, k : k + 1, :])
                    tile = bcast(tiles[t, k : k + 1, :])
                    re = pick(src[0], lane, tile)
                    im = pick(src[1], lane, tile)
                power = power + (re * re + im * im)
                zs[t, k, 0, rows, :] = re
                zs[t, k, 1, rows, :] = im
            w = lax.rsqrt(jnp.maximum(power, 1.0))
            for k in range(NB):
                zs[t, k, 0, rows, :] = zs[t, k, 0, rows, :] * w
                zs[t, k, 1, rows, :] = zs[t, k, 1, rows, :] * w
            zs[t, NB, 0, rows, :] = src[0][2]
            zs[t, NB, 1, rows, :] = src[1][2]

    for t in range(TILES):
        for kg in range(2):
            count = 8 if kg == 0 else NB - 8

            @pl.loop(8 * kg, NB + 1)
            def _(l):
                acc_re = [jnp.zeros((8, 128), F32) for _ in range(count)]
                acc_im = [jnp.zeros((8, 128), F32) for _ in range(count)]
                for g in range(GROUPS):
                    rows = slice(g * 8, (g + 1) * 8)
                    lr = zs[t, l, 0, rows, :]
                    li = zs[t, l, 1, rows, :]
                    for i in range(count):
                        kr = zs[t, 8 * kg + i, 0, rows, :]
                        ki = zs[t, 8 * kg + i, 1, rows, :]
                        acc_re[i] = acc_re[i] + (kr * lr + ki * li)
                        acc_im[i] = acc_im[i] + (kr * li - ki * lr)
                for i in range(count):
                    kre[t, l, 8 * kg + i : 8 * kg + i + 1, :] = column_sum(acc_re[i])
                    kim[t, l, 8 * kg + i : 8 * kg + i + 1, :] = column_sum(acc_im[i])

        for l in range(8):
            for k in range(8, NB):
                kre[t, l, k : k + 1, :] = kre[t, k, l : l + 1, :]
                kim[t, l, k : k + 1, :] = -kim[t, k, l : l + 1, :]

        bvec[t, 0] = kre[t, NB]
        bvec[t, 1] = kim[t, NB]
        cvec[t, 0, NB : NB + 1, :] = jnp.zeros((1, 128), F32)
        cvec[t, 1, NB : NB + 1, :] = jnp.zeros((1, 128), F32)

        @pl.loop(0, NB)
        def _(k):
            sr = zs[t, k, 0, 0:8, :]
            si = zs[t, k, 1, 0:8, :]
            for g in range(1, GROUPS):
                sr = sr + zs[t, k, 0, g * 8 : (g + 1) * 8, :]
                si = si + zs[t, k, 1, g * 8 : (g + 1) * 8, :]
            cvec[t, 0, pl.ds(k, 1), :] = START * column_sum(sr)
            cvec[t, 1, pl.ds(k, 1), :] = -START * column_sum(si)

    @pl.when(sec == 0)
    def _():
        zbuf[...] = jnp.zeros_like(zbuf)

    @pl.when(sec > 0)
    def _():
        for i in range(3):
            remote(msg, vbuf.at[i], v_send.at[i], v_recv.at[i], (sec_down, near[i])).wait_recv()
        for t in range(TILES):
            z0 = []
            for kg in range(2):
                rows = slice(8 * kg, 8 * kg + 8)
                lane = lanes[t, rows, :]
                tile = tiles[t, rows, :]
                pair = []
                for c in range(2):
                    src = []
                    for m in range(SPAN):
                        at = t + m
                        src.append(bcast(vbuf[at // 2, c : c + 1, (at % 2) * 128 : (at % 2) * 128 + 128]))
                    pair.append(pick(src, lane, tile))
                z0.append(pair)
            power = column_sum(z0[0][0] * z0[0][0] + z0[0][1] * z0[0][1] + (z0[1][0] * z0[1][0] + z0[1][1] * z0[1][1]))
            w = lax.rsqrt(jnp.maximum(power, 1.0))
            vr = vbuf[1, 0:1, t * 128 : (t + 1) * 128]
            vi = vbuf[1, 1:2, t * 128 : (t + 1) * 128]
            xsum[t, 0:1, :] = xsum[t, 0:1, :] + vr
            xsum[t, 1:2, :] = xsum[t, 1:2, :] + vi
            for kg in range(2):
                rows = slice(8 * kg, 8 * kg + 8)
                zr, zi = z0[kg][0] * w, z0[kg][1] * w
                z0[kg] = (zr, zi)
                zbuf[t, 0, rows, :] = zr
                zbuf[t, 1, rows, :] = zi
                cvec[t, 0, rows, :] = cvec[t, 0, rows, :] + START * zr
                cvec[t, 1, rows, :] = cvec[t, 1, rows, :] - START * zi
                bvec[t, 0, rows, :] = bvec[t, 0, rows, :] + (zr * vr + zi * vi)
                bvec[t, 1, rows, :] = bvec[t, 1, rows, :] + (zr * vi - zi * vr)
            for l in range(NB):
                lr = bcast(zbuf[t, 0, l : l + 1, :])
                li = bcast(zbuf[t, 1, l : l + 1, :])
                for kg in range(2):
                    rows = slice(8 * kg, 8 * kg + 8)
                    zr, zi = z0[kg]
                    kre[t, l, rows, :] = kre[t, l, rows, :] + (zr * lr + zi * li)
                    kim[t, l, rows, :] = kim[t, l, rows, :] + (zr * li - zi * lr)

    def product(state):
        for i, (t, c, kg) in enumerate((t, c, kg) for t in range(TILES) for c in range(2) for kg in range(2)):
            sbuf[t, c, 8 * kg : 8 * kg + 8, :] = state[i]
        out = []
        for t in range(TILES):
            y = [[None, None], [None, None]]
            for l in range(NB):
                lr = bcast(sbuf[t, 0, l : l + 1, :])
                li = bcast(sbuf[t, 1, l : l + 1, :])
                for kg in range(2):
                    rows = slice(8 * kg, 8 * kg + 8)
                    ar, ai = kre[t, l, rows, :], kim[t, l, rows, :]
                    re = ar * lr - ai * li
                    im = ar * li + ai * lr
                    y[0][kg] = re if l == 0 else y[0][kg] + re
                    y[1][kg] = im if l == 0 else y[1][kg] + im
            out += [y[0][0], y[0][1], y[1][0], y[1][1]]
        return out

    places = [(t, c, kg) for t in range(TILES) for c in range(2) for kg in range(2)]

    def c0(i):
        t, c, kg = places[i]
        return cvec[t, c, 8 * kg : 8 * kg + 8, :]

    def turn(_, state):
        return tuple(a + y + c0(i) for i, (a, y) in enumerate(zip(state, product(state))))

    state = lax.fori_loop(0, ITERS - 1, turn, tuple(c0(i) for i in range(8)))
    state = [a * SCALE for a in state]
    ks = product(state)
    norms = []
    for t in range(TILES):
        s = state[4 * t : 4 * t + 4]
        y = ks[4 * t : 4 * t + 4]
        total = None
        for i in range(4):
            term = s[i] * (y[i] + (2.0 * SCALE) * c0(4 * t + i))
            total = term if total is None else total + term
        norm = lax.rsqrt(column_sum(total) + SCALE * SCALE)
        norms.append(norm)
        cr = ci = fr = fi = None
        for kg in range(2):
            rows = slice(8 * kg, 8 * kg + 8)
            sr, si = s[kg], s[2 + kg]
            br, bi = bvec[t, 0, rows, :], bvec[t, 1, rows, :]
            zr, zi = zbuf[t, 0, rows, :], zbuf[t, 1, rows, :]
            a, b = sr * br + si * bi, sr * bi - si * br
            e, f = zr * sr - zi * si, zr * si + zi * sr
            cr = a if kg == 0 else column_sum(cr + a)
            ci = b if kg == 0 else column_sum(ci + b)
            fr = e if kg == 0 else column_sum(fr + e)
            fi = f if kg == 0 else column_sum(fi + f)
        cols = slice(t * 128, (t + 1) * 128)
        msg[0:1, cols] = (cr + (SCALE * START) * xsum[t, 0:1, :]) * norm
        msg[1:2, cols] = (ci + (SCALE * START) * xsum[t, 1:2, :]) * norm
        fr, fi = unit((fr + SCALE * START) * norm, fi * norm)
        fmsg[0:1, cols] = fr
        fmsg[1:2, cols] = fi

    @pl.when(sec < SECTIONS - 1)
    def _():
        for i in range(3):
            remote(msg, vbuf.at[2 - i], v_send.at[i], v_recv.at[2 - i], (sec_up, near[i])).start()

    for s in range(1, SECTIONS):

        @pl.when(sec == s)
        def _():
            for j in range(s):
                remote(fmsg, fbuf.at[s - 1], f_send.at[j], f_recv.at[s - 1], (j, pix)).start()

    comp[0, 0:1, :] = msg[0:1, :]
    comp[1, 0:1, :] = msg[1:2, :]

    for i, (t, c, kg) in enumerate(places):
        sbuf[t, c, 8 * kg : 8 * kg + 8, :] = state[i] * norms[t]
    for t in range(TILES):

        @pl.loop(0, GROUPS)
        def _(g):
            rows = pl.ds(pl.multiple_of(g * 8, 8), 8)
            re = bcast((SCALE * START) * norms[t])
            im = jnp.zeros((8, 128), F32)
            for k in range(NB):
                sr = bcast(sbuf[t, 0, k : k + 1, :])
                si = bcast(sbuf[t, 1, k : k + 1, :])
                zr, zi = zs[t, k, 0, rows, :], zs[t, k, 1, rows, :]
                re = re + (zr * sr - zi * si)
                im = im + (zr * si + zi * sr)
            series[t, 0, rows, :] = re
            series[t, 1, rows, :] = im

    for s in range(SECTIONS - 1, 0, -1):

        @pl.when(sec < s)
        def _():
            remote(fmsg, fbuf.at[s - 1], f_send.at[0], f_recv.at[s - 1], (s, pix)).wait_recv()
            for t in range(TILES):
                fr = fbuf[s - 1, 0:1, t * 128 : (t + 1) * 128]
                fi = fbuf[s - 1, 1:2, t * 128 : (t + 1) * 128]
                re, im = series[t, 0], series[t, 1]
                series[t, 0] = re * fr - im * fi
                series[t, 1] = re * fi + im * fr

    want = ref[0] - pix * (TILES * 128)
    lane = lax.broadcasted_iota(jnp.int32, (PAD, 128), 1)
    diag = lane == lax.broadcasted_iota(jnp.int32, (PAD, 128), 0)
    for c in range(2):
        column = jnp.zeros((PAD, 128), F32)
        for t in range(TILES):
            column = column + jnp.where(lane == want - t * 128, series[t, c], 0.0)
        column = jnp.sum(column, axis=1, keepdims=True)
        rmsg[c : c + 1, :] = column_sum(jnp.where(diag, column, 0.0))
    copies = []
    for d in range(1, 8):
        copies.append(remote(rmsg, rbuf1.at[d - 1], r_send.at[d - 1], r_recv.at[d - 1], (sec, first[d - 1])))
        copies[-1].start()
    for copy in copies:
        copy.wait_recv()
    total = rmsg[...]
    for d in range(1, 8):
        total = total + rbuf1[d - 1]
    rmsg2[...] = total
    for d in range(1, 8):
        copies.append(remote(rmsg2, rbuf2.at[d - 1], r_send.at[6 + d], r_recv.at[6 + d], (sec, second[d - 1])))
        copies[-1].start()
    for copy in copies[7:]:
        copy.wait_recv()
    for d in range(1, 8):
        total = total + rbuf2[d - 1]
    u = []
    for c in range(2):
        u.append(jnp.sum(jnp.where(diag, jnp.broadcast_to(total[c : c + 1, :], (PAD, 128)), 0.0), axis=1, keepdims=True))
    ur, ui = unit(u[0], u[1])
    ur, ui = GAIN * ur, GAIN * ui
    for t in range(TILES):
        re, im = series[t, 0], series[t, 1]
        cols = slice(t * 128, (t + 1) * 128)
        phases[0, :, cols] = (re * ur + im * ui)[0:ROWS]
        phases[1, :, cols] = (im * ur - re * ui)[0:ROWS]

    for copy in copies:
        copy.wait_send()

    @pl.when(sec < SECTIONS - 1)
    def _():
        for i in range(3):
            remote(msg, vbuf.at[2 - i], v_send.at[i], v_recv.at[2 - i], (sec_up, near[i])).wait_send()

    for s in range(1, SECTIONS):

        @pl.when(sec == s)
        def _():
            for j in range(s):
                remote(fmsg, fbuf.at[s - 1], f_send.at[j], f_recv.at[s - 1], (j, pix)).wait_send()


def on_device(slc, neighbours, reference_pixel):
    vmem = pl.BlockSpec(memory_space=pltpu.VMEM)
    pixels = slc.shape[2]
    dma = pltpu.SemaphoreType.DMA
    return pl.pallas_call(
        kernel,
        out_shape=(
            jax.ShapeDtypeStruct((2, ROWS, pixels), F32),
            jax.ShapeDtypeStruct((2, 1, pixels), F32),
        ),
        in_specs=[pl.BlockSpec(memory_space=pl.ANY), vmem, pl.BlockSpec(memory_space=pltpu.SMEM)],
        out_specs=(vmem, vmem),
        scratch_shapes=[
            pltpu.VMEM((2, ROWS, pixels), F32),
            pltpu.VMEM((2, ROWS, pixels), F32),
            pltpu.VMEM((2, ROWS, pixels), F32),
            pltpu.VMEM((2, 6, PAD, 128), F32),
            pltpu.VMEM((TILES, 16, 128), jnp.int32),
            pltpu.VMEM((TILES, 16, 128), jnp.int32),
            pltpu.VMEM((TILES, 16, 2, PAD, 128), F32),
            pltpu.VMEM((TILES, 16, 16, 128), F32),
            pltpu.VMEM((TILES, 16, 16, 128), F32),
            pltpu.VMEM((TILES, 2, 16, 128), F32),
            pltpu.VMEM((TILES, 2, 16, 128), F32),
            pltpu.VMEM((TILES, 2, 128), F32),
            pltpu.VMEM((TILES, 2, 16, 128), F32),
            pltpu.VMEM((TILES, 2, 16, 128), F32),
            pltpu.VMEM((3, 2, pixels), F32),
            pltpu.VMEM((2, pixels), F32),
            pltpu.VMEM((2, pixels), F32),
            pltpu.VMEM((3, 2, pixels), F32),
            pltpu.VMEM((TILES, 2, PAD, 128), F32),
            pltpu.VMEM((2, 128), F32),
            pltpu.VMEM((7, 2, 128), F32),
            pltpu.VMEM((2, 128), F32),
            pltpu.VMEM((7, 2, 128), F32),
            dma(()),
            dma((2,)),
            dma((2,)),
            dma((3,)),
            dma((3,)),
            dma((3,)),
            dma((3,)),
            dma((14,)),
            dma((14,)),
        ],
        compiler_params=pltpu.CompilerParams(collective_id=0, has_side_effects=True),
        cost_estimate=pl.CostEstimate(flops=100_000_000, bytes_accessed=1_000_000, transcendentals=0),
    )(slc, neighbours, reference_pixel)


def solution(mesh):
    return jax.shard_map(
        on_device,
        mesh=mesh,
        in_specs=(P(None, "section", "pix"), P(None, "pix"), P()),
        out_specs=(P(None, "section", "pix"), P(None, "section", "pix")),
        check_vma=False,
    )
```

```python
import math

import jax
import jax.numpy as jnp
from jax import lax
from jax.experimental import pallas as pl
from jax.experimental.pallas import tpu as pltpu
from jax.sharding import PartitionSpec as P

ITERS = 16
FLOOR = 0.05
REACH = 256
NB = 15
ROWS = 50
PAD = 56
GROUPS = PAD // 8
FLAT = 4 * ROWS
TILES = 2
SPAN = 5
SCALE = 2.0**-45
START = 1.0 / math.sqrt(ROWS + 1)
GAIN = math.sqrt(ROWS + 1)
SECTIONS = 4
PIX = 64
MESH = pl.DeviceIdType.MESH
F32 = jnp.float32


def bcast(row):
    return jnp.broadcast_to(row, (8, 128))


def pick(sources, lane, tile):
    out = jnp.zeros((8, 128), F32)
    for m, source in enumerate(sources):
        out = jnp.where(tile == m, take(source, lane), out)
    return out


def take(source, lane):
    return jnp.take_along_axis(source, lane, axis=1, mode="promise_in_bounds")


def column_sum(x):
    return jnp.sum(x, axis=0, keepdims=True)


def unit(re, im):
    scale = 1.0 / jnp.maximum(jnp.sqrt(re * re + im * im), FLOOR)
    return re * scale, im * scale


def remote(src, dst, send, recv, device):
    return pltpu.make_async_remote_copy(
        src_ref=src, dst_ref=dst, send_sem=send, recv_sem=recv, device_id=device, device_id_type=MESH
    )


def kernel(
    slc_hbm, nbr_hbm, ref_hbm, phases, comp,
    nbr, ref, blocks, ext, lanes, tiles, zs, wbuf, red, kre, kim, cvec, bvec, xsum, zbuf, sbuf,
    vbuf, msg, fmsg, fbuf, series, rmsg, rbuf1, rmsg2, rbuf2,
    load_sem, halo_send, halo_recv, v_send, v_recv, f_send, f_recv, r_send, r_recv,
):
    sec = lax.axis_index("section")
    pix = lax.axis_index("pix")
    before = lax.rem(pix + (PIX - 1), PIX)
    after = lax.rem(pix + 1, PIX)
    near = (before, pix, after)
    present = (pix > 0, pix >= 0, pix < PIX - 1)
    sec_up = lax.rem(sec + 1, SECTIONS)
    sec_down = lax.rem(sec + (SECTIONS - 1), SECTIONS)
    x = pix // 16
    z = lax.rem(pix // 2, 8)
    core = lax.rem(pix, 2)
    group = x * 2 + core
    first = []
    second = []
    for d in range(1, 8):
        g = lax.rem(group + d, 8)
        first.append((g // 2) * 16 + z * 2 + lax.rem(g, 2))
        second.append(x * 16 + lax.rem(z + d, 8) * 2 + core)

    own_rows = pl.ds(0, FLAT)
    loads = [
        pltpu.make_async_copy(slc_hbm, blocks.at[1, own_rows], load_sem.at[0]),
        pltpu.make_async_copy(nbr_hbm, nbr, load_sem.at[1]),
        pltpu.make_async_copy(ref_hbm, ref, load_sem.at[2]),
    ]
    for load in loads:
        load.start()
    barrier = pltpu.get_barrier_semaphore()
    peers = [(sec, before), (sec, after), (lax.rem(sec + 2, SECTIONS), pix)]
    peers += [(s, p) for s in (sec_up, sec_down) for p in near]
    peers += [(sec, p) for p in first + second]
    for peer in peers:
        pl.semaphore_signal(barrier, inc=1, device_id=peer, device_id_type=MESH)
    for i in range(3):
        blocks[i, FLAT:, :] = jnp.zeros((32 * GROUPS - FLAT, 128), F32)
    kre[...] = jnp.zeros_like(kre)
    kim[...] = jnp.zeros_like(kim)
    red[...] = jnp.zeros_like(red)
    cvec[...] = jnp.zeros_like(cvec)
    bvec[...] = jnp.zeros_like(bvec)
    for i in (0, 2):

        @pl.when(jnp.logical_not(present[i]))
        def _():
            blocks[i] = jnp.zeros((32 * GROUPS, 128), F32)
            vbuf[i] = jnp.zeros_like(vbuf[i])

    pl.semaphore_wait(barrier, len(peers))

    halos = [
        remote(slc_hbm, blocks.at[2 - i, own_rows], halo_send.at[i // 2], halo_recv.at[i // 2], (sec, near[i]))
        for i in (0, 2)
    ]
    for i, halo in zip((0, 2), halos):
        pl.when(present[i])(halo.start)

    for load in loads:
        load.wait()

    base = pix * (TILES * 128) - REACH
    for t in range(TILES):
        rel = nbr[:, t * 128 : (t + 1) * 128] - (base + t * 128)
        lanes[t, 0:NB, :] = jnp.bitwise_and(rel, 127)
        tiles[t, 0:NB, :] = jnp.right_shift(rel, 7)
        lanes[t, NB : NB + 1, :] = jnp.zeros((1, 128), jnp.int32)
        tiles[t, NB : NB + 1, :] = jnp.full((1, 128), SPAN, jnp.int32)

    def spread(i):
        for g in range(GROUPS):
            for m in range(2):
                for c in range(2):
                    ext[2 * i + m, c, g * 8 : (g + 1) * 8, :] = blocks[i, pl.ds(g * 32 + m * 2 + c, 8, stride=4), :]

    spread(1)
    for t in range(TILES):
        for c in range(2):
            total = None
            for g in range(GROUPS):
                own = ext[2 + t, c, g * 8 : (g + 1) * 8, :]
                zs[t, 0, c, g * 8 : (g + 1) * 8, :] = own
                total = own if total is None else total + own
            xsum[t, c : c + 1, :] = column_sum(total)
        zs[t, 0, 2] = zs[t, 0, 0] - zs[t, 0, 1]

    for i, halo in zip((0, 2), halos):
        pl.when(present[i])(halo.wait_send)
        pl.when(present[2 - i])(halo.wait_recv)
    spread(0)
    spread(2)

    @pl.loop(0, 2 * TILES)
    def _(step):
        t = step // 2
        for i in range(NB // 2):
            k = 1 + lax.rem(step, 2) * (NB // 2) + i
            lane = bcast(lanes[t, pl.ds(k, 1), :])
            tile = bcast(tiles[t, pl.ds(k, 1), :])
            here = [tile == m for m in range(SPAN)]
            for g in range(GROUPS):
                rows = slice(g * 8, (g + 1) * 8)
                pair = []
                for c in range(2):
                    out = take(ext[t, c, rows, :], lane)
                    for m in range(1, SPAN):
                        out = jnp.where(here[m], take(ext[t + m, c, rows, :], lane), out)
                    zs[t, k, c, rows, :] = out
                    pair.append(out)
                zs[t, k, 2, rows, :] = pair[0] - pair[1]

    @pl.loop(0, TILES)
    def _(t):
        for g in range(GROUPS):
            rows = slice(g * 8, (g + 1) * 8)
            power = None
            for k in range(NB):
                re, im = zs[t, k, 0, rows, :], zs[t, k, 1, rows, :]
                term = re * re + im * im
                power = term if power is None else power + term
            wbuf[t, rows, :] = lax.rsqrt(jnp.maximum(power, 1.0))

        def fold(slot, parts):
            for i, part in enumerate(parts):
                red[slot, i * 8 : (i + 1) * 8, :] = part
            total = None
            for i in range(8):
                row = red[slot, pl.ds(i, 8, stride=8), :]
                total = row if total is None else total + row
            return total

        slot = 0
        for l in range(NB + 1):
            for kg in range(2):
                low, high = 8 * kg, min(8 * kg + 8, l + 1, NB)
                if high <= low:
                    continue
                count = high - low
                p, q, r = [None] * count, [None] * count, [None] * count
                cr, ci = [None] * count, [None] * count

                def put(box, i, value):
                    box[i] = value if box[i] is None else box[i] + value

                for g in range(GROUPS):
                    rows = slice(g * 8, (g + 1) * 8)
                    w = wbuf[t, rows, :]
                    if l < NB:
                        w2 = w * w
                        lr, li = zs[t, l, 0, rows, :] * w2, zs[t, l, 1, rows, :] * w2
                    else:
                        lr, li = zs[t, 0, 0, rows, :] * w, zs[t, 0, 1, rows, :] * w
                    le = lr + li
                    for i in range(count):
                        k = low + i
                        kr, ki = zs[t, k, 0, rows, :], zs[t, k, 1, rows, :]
                        put(p, i, kr * lr)
                        put(q, i, ki * li)
                        if k != l:
                            put(r, i, zs[t, k, 2, rows, :] * le)
                        if l == NB:
                            put(cr, i, kr * w)
                            put(ci, i, ki * w)
                re = fold(4 * kg + slot, [a + b for a, b in zip(p, q)])
                im = fold(4 * kg + slot + 1, [jnp.zeros((8, 128), F32) if c is None else c + (b - a) for a, b, c in zip(p, q, r)])
                rows = slice(low, low + 8)
                if l < NB:
                    kre[t, l, rows, :] = re
                    kim[t, l, rows, :] = im
                    for i in range(count):
                        k = low + i
                        if k != l:
                            kre[t, k, l : l + 1, :] = re[i : i + 1, :]
                            kim[t, k, l : l + 1, :] = -im[i : i + 1, :]
                else:
                    bvec[t, 0, rows, :] = re
                    bvec[t, 1, rows, :] = im
                    slot = 2 - slot
                    cvec[t, 0, rows, :] = START * fold(4 * kg + slot, cr)
                    cvec[t, 1, rows, :] = -START * fold(4 * kg + slot + 1, ci)
                slot = 2 - slot

    @pl.when(sec == 0)
    def _():
        zbuf[...] = jnp.zeros_like(zbuf)

    @pl.when(sec > 0)
    def _():
        for i in range(3):
            pl.when(present[i])(remote(msg, vbuf.at[i], v_send.at[i], v_recv.at[i], (sec_down, near[i])).wait_recv)
        for t in range(TILES):
            z0 = []
            for kg in range(2):
                rows = slice(8 * kg, 8 * kg + 8)
                lane = lanes[t, rows, :]
                tile = tiles[t, rows, :]
                pair = []
                for c in range(2):
                    src = []
                    for m in range(SPAN):
                        at = t + m
                        src.append(bcast(vbuf[at // 2, c : c + 1, (at % 2) * 128 : (at % 2) * 128 + 128]))
                    pair.append(pick(src, lane, tile))
                z0.append(pair)
            power = column_sum(z0[0][0] * z0[0][0] + z0[0][1] * z0[0][1] + (z0[1][0] * z0[1][0] + z0[1][1] * z0[1][1]))
            w = lax.rsqrt(jnp.maximum(power, 1.0))
            vr = vbuf[1, 0:1, t * 128 : (t + 1) * 128]
            vi = vbuf[1, 1:2, t * 128 : (t + 1) * 128]
            xsum[t, 0:1, :] = xsum[t, 0:1, :] + vr
            xsum[t, 1:2, :] = xsum[t, 1:2, :] + vi
            for kg in range(2):
                rows = slice(8 * kg, 8 * kg + 8)
                zr, zi = z0[kg][0] * w, z0[kg][1] * w
                z0[kg] = (zr, zi)
                zbuf[t, 0, rows, :] = zr
                zbuf[t, 1, rows, :] = zi
                cvec[t, 0, rows, :] = cvec[t, 0, rows, :] + START * zr
                cvec[t, 1, rows, :] = cvec[t, 1, rows, :] - START * zi
                bvec[t, 0, rows, :] = bvec[t, 0, rows, :] + (zr * vr + zi * vi)
                bvec[t, 1, rows, :] = bvec[t, 1, rows, :] + (zr * vi - zi * vr)
            for l in range(NB):
                lr = bcast(zbuf[t, 0, l : l + 1, :])
                li = bcast(zbuf[t, 1, l : l + 1, :])
                for kg in range(2):
                    rows = slice(8 * kg, 8 * kg + 8)
                    zr, zi = z0[kg]
                    kre[t, l, rows, :] = kre[t, l, rows, :] + (zr * lr + zi * li)
                    kim[t, l, rows, :] = kim[t, l, rows, :] + (zr * li - zi * lr)

    def product(state):
        for i, (t, c, kg) in enumerate((t, c, kg) for t in range(TILES) for c in range(2) for kg in range(2)):
            sbuf[t, c, 8 * kg : 8 * kg + 8, :] = state[i]
        out = []
        for t in range(TILES):
            y = [[None, None], [None, None]]
            for l in range(NB):
                lr = bcast(sbuf[t, 0, l : l + 1, :])
                li = bcast(sbuf[t, 1, l : l + 1, :])
                for kg in range(2):
                    rows = slice(8 * kg, 8 * kg + 8)
                    ar, ai = kre[t, l, rows, :], kim[t, l, rows, :]
                    re = ar * lr - ai * li
                    im = ar * li + ai * lr
                    y[0][kg] = re if l == 0 else y[0][kg] + re
                    y[1][kg] = im if l == 0 else y[1][kg] + im
            out += [y[0][0], y[0][1], y[1][0], y[1][1]]
        return out

    places = [(t, c, kg) for t in range(TILES) for c in range(2) for kg in range(2)]

    def c0(i):
        t, c, kg = places[i]
        return cvec[t, c, 8 * kg : 8 * kg + 8, :]

    def turn(_, state):
        return tuple(a + y + c0(i) for i, (a, y) in enumerate(zip(state, product(state))))

    state = lax.fori_loop(0, ITERS - 1, turn, tuple(c0(i) for i in range(8)))
    state = [a * SCALE for a in state]
    ks = product(state)
    norms = []
    for t in range(TILES):
        s = state[4 * t : 4 * t + 4]
        y = ks[4 * t : 4 * t + 4]
        total = None
        for i in range(4):
            term = s[i] * (y[i] + (2.0 * SCALE) * c0(4 * t + i))
            total = term if total is None else total + term
        norm = lax.rsqrt(column_sum(total) + SCALE * SCALE)
        norms.append(norm)
        cr = ci = fr = fi = None
        for kg in range(2):
            rows = slice(8 * kg, 8 * kg + 8)
            sr, si = s[kg], s[2 + kg]
            br, bi = bvec[t, 0, rows, :], bvec[t, 1, rows, :]
            zr, zi = zbuf[t, 0, rows, :], zbuf[t, 1, rows, :]
            a, b = sr * br + si * bi, sr * bi - si * br
            e, f = zr * sr - zi * si, zr * si + zi * sr
            cr = a if kg == 0 else column_sum(cr + a)
            ci = b if kg == 0 else column_sum(ci + b)
            fr = e if kg == 0 else column_sum(fr + e)
            fi = f if kg == 0 else column_sum(fi + f)
        cols = slice(t * 128, (t + 1) * 128)
        msg[0:1, cols] = (cr + (SCALE * START) * xsum[t, 0:1, :]) * norm
        msg[1:2, cols] = (ci + (SCALE * START) * xsum[t, 1:2, :]) * norm
        fr, fi = unit((fr + SCALE * START) * norm, fi * norm)
        fmsg[0:1, cols] = fr
        fmsg[1:2, cols] = fi

    @pl.when(sec < SECTIONS - 1)
    def _():
        for i in range(3):
            pl.when(present[i])(remote(msg, vbuf.at[2 - i], v_send.at[i], v_recv.at[2 - i], (sec_up, near[i])).start)

    for s in range(1, SECTIONS):

        @pl.when(sec == s)
        def _():
            for j in range(s):
                remote(fmsg, fbuf.at[s - 1], f_send.at[j], f_recv.at[s - 1], (j, pix)).start()

    comp[0, 0:1, :] = msg[0:1, :]
    comp[1, 0:1, :] = msg[1:2, :]

    for i, (t, c, kg) in enumerate(places):
        sbuf[t, c, 8 * kg : 8 * kg + 8, :] = state[i] * norms[t]
    for t in range(TILES):

        @pl.loop(0, GROUPS)
        def _(g):
            rows = pl.ds(pl.multiple_of(g * 8, 8), 8)
            re = im = None
            for k in range(NB):
                sr = bcast(sbuf[t, 0, k : k + 1, :])
                si = bcast(sbuf[t, 1, k : k + 1, :])
                zr, zi = zs[t, k, 0, rows, :], zs[t, k, 1, rows, :]
                a, b = zr * sr - zi * si, zr * si + zi * sr
                re = a if re is None else re + a
                im = b if im is None else im + b
            w = wbuf[t, rows, :]
            series[t, 0, rows, :] = bcast((SCALE * START) * norms[t]) + w * re
            series[t, 1, rows, :] = w * im

    for s in range(SECTIONS - 1, 0, -1):

        @pl.when(sec < s)
        def _():
            remote(fmsg, fbuf.at[s - 1], f_send.at[0], f_recv.at[s - 1], (s, pix)).wait_recv()
            for t in range(TILES):
                fr = fbuf[s - 1, 0:1, t * 128 : (t + 1) * 128]
                fi = fbuf[s - 1, 1:2, t * 128 : (t + 1) * 128]
                re, im = series[t, 0], series[t, 1]
                series[t, 0] = re * fr - im * fi
                series[t, 1] = re * fi + im * fr

    want = ref[0] - pix * (TILES * 128)
    lane = lax.broadcasted_iota(jnp.int32, (PAD, 128), 1)
    diag = lane == lax.broadcasted_iota(jnp.int32, (PAD, 128), 0)
    for c in range(2):
        column = jnp.zeros((PAD, 128), F32)
        for t in range(TILES):
            column = column + jnp.where(lane == want - t * 128, series[t, c], 0.0)
        column = jnp.sum(column, axis=1, keepdims=True)
        rmsg[c : c + 1, :] = column_sum(jnp.where(diag, column, 0.0))
    copies = []
    for d in range(1, 8):
        copies.append(remote(rmsg, rbuf1.at[d - 1], r_send.at[d - 1], r_recv.at[d - 1], (sec, first[d - 1])))
        copies[-1].start()
    for copy in copies:
        copy.wait_recv()
    total = rmsg[...]
    for d in range(1, 8):
        total = total + rbuf1[d - 1]
    rmsg2[...] = total
    for d in range(1, 8):
        copies.append(remote(rmsg2, rbuf2.at[d - 1], r_send.at[6 + d], r_recv.at[6 + d], (sec, second[d - 1])))
        copies[-1].start()
    for copy in copies[7:]:
        copy.wait_recv()
    for d in range(1, 8):
        total = total + rbuf2[d - 1]
    u = []
    for c in range(2):
        u.append(jnp.sum(jnp.where(diag, jnp.broadcast_to(total[c : c + 1, :], (PAD, 128)), 0.0), axis=1, keepdims=True))
    ur, ui = unit(u[0], u[1])
    ur, ui = GAIN * ur, GAIN * ui
    for t in range(TILES):
        re, im = series[t, 0], series[t, 1]
        for c, part in enumerate((re * ur + im * ui, im * ur - re * ui)):
            for g in range(GROUPS):
                count = min(8, ROWS - g * 8)
                phases[pl.ds(g * 32 + t * 2 + c, count, stride=4), :] = part[g * 8 : g * 8 + count]

    for copy in copies:
        copy.wait_send()

    @pl.when(sec < SECTIONS - 1)
    def _():
        for i in range(3):
            pl.when(present[i])(remote(msg, vbuf.at[2 - i], v_send.at[i], v_recv.at[2 - i], (sec_up, near[i])).wait_send)

    for s in range(1, SECTIONS):

        @pl.when(sec == s)
        def _():
            for j in range(s):
                remote(fmsg, fbuf.at[s - 1], f_send.at[j], f_recv.at[s - 1], (j, pix)).wait_send()


def on_device(slc, neighbours, reference_pixel):
    vmem = pl.BlockSpec(memory_space=pltpu.VMEM)
    any_space = pl.BlockSpec(memory_space=pl.ANY)
    pixels = slc.shape[2]
    dma = pltpu.SemaphoreType.DMA
    flat = slc.reshape(2, ROWS, TILES, 128).transpose(1, 2, 0, 3).reshape(FLAT, 128)
    phases, comp = pl.pallas_call(
        kernel,
        out_shape=(
            jax.ShapeDtypeStruct((FLAT, 128), F32),
            jax.ShapeDtypeStruct((2, 1, pixels), F32),
        ),
        in_specs=[any_space, any_space, any_space],
        out_specs=(vmem, vmem),
        scratch_shapes=[
            pltpu.VMEM((NB, pixels), jnp.int32),
            pltpu.SMEM((1,), jnp.int32),
            pltpu.VMEM((3, 32 * GROUPS, 128), F32),
            pltpu.VMEM((6, 2, PAD, 128), F32),
            pltpu.VMEM((TILES, 16, 128), jnp.int32),
            pltpu.VMEM((TILES, 16, 128), jnp.int32),
            pltpu.VMEM((TILES, NB, 3, PAD, 128), F32),
            pltpu.VMEM((TILES, PAD, 128), F32),
            pltpu.VMEM((8, 64, 128), F32),
            pltpu.VMEM((TILES, 16, 16, 128), F32),
            pltpu.VMEM((TILES, 16, 16, 128), F32),
            pltpu.VMEM((TILES, 2, 16, 128), F32),
            pltpu.VMEM((TILES, 2, 16, 128), F32),
            pltpu.VMEM((TILES, 2, 128), F32),
            pltpu.VMEM((TILES, 2, 16, 128), F32),
            pltpu.VMEM((TILES, 2, 16, 128), F32),
            pltpu.VMEM((3, 2, pixels), F32),
            pltpu.VMEM((2, pixels), F32),
            pltpu.VMEM((2, pixels), F32),
            pltpu.VMEM((3, 2, pixels), F32),
            pltpu.VMEM((TILES, 2, PAD, 128), F32),
            pltpu.VMEM((2, 128), F32),
            pltpu.VMEM((7, 2, 128), F32),
            pltpu.VMEM((2, 128), F32),
            pltpu.VMEM((7, 2, 128), F32),
            dma((3,)),
            dma((2,)),
            dma((2,)),
            dma((3,)),
            dma((3,)),
            dma((3,)),
            dma((3,)),
            dma((14,)),
            dma((14,)),
        ],
        compiler_params=pltpu.CompilerParams(
            collective_id=0, has_side_effects=True, vmem_limit_bytes=16 * 2**20
        ),
        cost_estimate=pl.CostEstimate(flops=100_000_000, bytes_accessed=1_000_000, transcendentals=0),
    )(flat, neighbours, reference_pixel)
    return phases.reshape(ROWS, TILES, 2, 128).transpose(2, 0, 1, 3).reshape(2, ROWS, pixels), comp


def solution(mesh):
    return jax.shard_map(
        on_device,
        mesh=mesh,
        in_specs=(P(None, "section", "pix"), P(None, "pix"), P()),
        out_specs=(P(None, "section", "pix"), P(None, "section", "pix")),
        check_vma=False,
    )
```

```python
import math

import jax
import jax.numpy as jnp
from jax import lax
from jax.experimental import pallas as pl
from jax.experimental.pallas import tpu as pltpu
from jax.sharding import PartitionSpec as P

ITERS = 16
FLOOR = 0.05
REACH = 256
NB = 15
ROWS = 50
PAD = 56
GROUPS = PAD // 8
FLAT = 4 * ROWS
TILES = 2
SPAN = 5
SCALE = 2.0**-45
START = 1.0 / math.sqrt(ROWS + 1)
GAIN = math.sqrt(ROWS + 1)
SECTIONS = 4
PIX = 64
MESH = pl.DeviceIdType.MESH
F32 = jnp.float32


def bcast(row):
    return jnp.broadcast_to(row, (8, 128))


def pick(sources, lane, tile):
    out = jnp.zeros((8, 128), F32)
    for m, source in enumerate(sources):
        out = jnp.where(tile == m, take(source, lane), out)
    return out


def take(source, lane):
    return jnp.take_along_axis(source, lane, axis=1, mode="promise_in_bounds")


def column_sum(x):
    return jnp.sum(x, axis=0, keepdims=True)


def unit(re, im):
    scale = 1.0 / jnp.maximum(jnp.sqrt(re * re + im * im), FLOOR)
    return re * scale, im * scale


def remote(src, dst, send, recv, device):
    return pltpu.make_async_remote_copy(
        src_ref=src, dst_ref=dst, send_sem=send, recv_sem=recv, device_id=device, device_id_type=MESH
    )


def kernel(
    slc_hbm, nbr_hbm, ref_hbm, phases, comp,
    nbr, ref, blocks, ext, lanes, tiles, zs, wbuf, red, kre, kim, cvec, bvec, xsum, zbuf, sbuf,
    vbuf, msg, fmsg, fbuf, series, rmsg, rbuf1, rmsg2, rbuf2,
    load_sem, halo_send, halo_recv, v_send, v_recv, f_send, f_recv, r_send, r_recv, ready,
):
    sec = lax.axis_index("section")
    pix = lax.axis_index("pix")
    before = lax.rem(pix + (PIX - 1), PIX)
    after = lax.rem(pix + 1, PIX)
    near = (before, pix, after)
    present = (pix > 0, pix >= 0, pix < PIX - 1)
    sec_up = lax.rem(sec + 1, SECTIONS)
    sec_down = lax.rem(sec + (SECTIONS - 1), SECTIONS)
    x = pix // 16
    z = lax.rem(pix // 2, 8)
    core = lax.rem(pix, 2)
    group = x * 2 + core
    first = []
    second = []
    for d in range(1, 8):
        g = lax.rem(group + d, 8)
        first.append((g // 2) * 16 + z * 2 + lax.rem(g, 2))
        second.append(x * 16 + lax.rem(z + d, 8) * 2 + core)

    own_rows = pl.ds(0, FLAT)
    loads = [
        pltpu.make_async_copy(slc_hbm, blocks.at[1, own_rows], load_sem.at[0]),
        pltpu.make_async_copy(nbr_hbm, nbr, load_sem.at[1]),
        pltpu.make_async_copy(ref_hbm, ref, load_sem.at[2]),
    ]
    for load in loads:
        load.start()
    barrier = pltpu.get_barrier_semaphore()
    peers = [(sec, before), (sec, after), (sec_up, pix), (sec_down, pix)]
    peers += [(sec, x * 16 + lax.rem(z + d, 8) * 2 + core) for d in (1, 7)]
    peers += [(sec, lax.rem(x + d, 4) * 16 + z * 2 + core) for d in (1, 3)]

    def tell(sem):
        for peer in peers:
            pl.semaphore_signal(sem, inc=1, device_id=peer, device_id_type=MESH)

    def hear(sem):
        pl.semaphore_wait(sem, len(peers))

    tell(barrier)
    for i in range(3):
        blocks[i, FLAT:, :] = jnp.zeros((32 * GROUPS - FLAT, 128), F32)
    kre[...] = jnp.zeros_like(kre)
    kim[...] = jnp.zeros_like(kim)
    red[...] = jnp.zeros_like(red)
    cvec[...] = jnp.zeros_like(cvec)
    bvec[...] = jnp.zeros_like(bvec)
    for i in (0, 2):

        @pl.when(jnp.logical_not(present[i]))
        def _():
            blocks[i] = jnp.zeros((32 * GROUPS, 128), F32)
            vbuf[i] = jnp.zeros_like(vbuf[i])

    hear(barrier)
    tell(ready.at[0])

    loads[0].wait()
    halos = [
        remote(blocks.at[1, own_rows], blocks.at[2 - i, own_rows], halo_send.at[i // 2], halo_recv.at[i // 2], (sec, near[i]))
        for i in (0, 2)
    ]
    for i, halo in zip((0, 2), halos):
        pl.when(present[i])(halo.start)

    for load in loads[1:]:
        load.wait()

    base = pix * (TILES * 128) - REACH
    for t in range(TILES):
        rel = nbr[:, t * 128 : (t + 1) * 128] - (base + t * 128)
        lanes[t, 0:NB, :] = jnp.bitwise_and(rel, 127)
        tiles[t, 0:NB, :] = jnp.right_shift(rel, 7)
        lanes[t, NB : NB + 1, :] = jnp.zeros((1, 128), jnp.int32)
        tiles[t, NB : NB + 1, :] = jnp.full((1, 128), SPAN, jnp.int32)

    def spread(i):
        for g in range(GROUPS):
            for m in range(2):
                for c in range(2):
                    ext[2 * i + m, c, g * 8 : (g + 1) * 8, :] = blocks[i, pl.ds(g * 32 + m * 2 + c, 8, stride=4), :]

    spread(1)
    for t in range(TILES):
        for c in range(2):
            total = None
            for g in range(GROUPS):
                own = ext[2 + t, c, g * 8 : (g + 1) * 8, :]
                zs[t, 0, c, g * 8 : (g + 1) * 8, :] = own
                total = own if total is None else total + own
            xsum[t, c : c + 1, :] = column_sum(total)
        zs[t, 0, 2] = zs[t, 0, 0] - zs[t, 0, 1]

    def gather(t, mine, theirs, begin):
        @pl.loop(0, 2)
        def _(half):
            for i in range(NB // 2):
                k = 1 + half * (NB // 2) + i
                lane = bcast(lanes[t, pl.ds(k, 1), :])
                tile = bcast(tiles[t, pl.ds(k, 1), :])
                here = [tile == m for m in theirs]
                for g in range(GROUPS):
                    rows = slice(g * 8, (g + 1) * 8)
                    pair = []
                    for c in range(2):
                        out = take(ext[t + mine, c, rows, :], lane) if begin else zs[t, k, c, rows, :]
                        for there, m in zip(here, theirs):
                            out = jnp.where(there, take(ext[t + m, c, rows, :], lane), out)
                        zs[t, k, c, rows, :] = out
                        pair.append(out)
                    if not begin:
                        zs[t, k, 2, rows, :] = pair[0] - pair[1]

    for t in range(TILES):
        gather(t, 2 - t, (3 - t,), True)

    for i, halo in zip((0, 2), halos):
        pl.when(present[i])(halo.wait_send)
        pl.when(present[2 - i])(halo.wait_recv)
    spread(0)
    spread(2)

    for t in range(TILES):
        gather(t, None, tuple(m for m in range(SPAN) if t + m not in (2, 3)), False)
    hear(ready.at[0])
    tell(ready.at[1])

    @pl.loop(0, TILES)
    def _(t):
        for g in range(GROUPS):
            rows = slice(g * 8, (g + 1) * 8)
            power = None
            for k in range(NB):
                re, im = zs[t, k, 0, rows, :], zs[t, k, 1, rows, :]
                term = re * re + im * im
                power = term if power is None else power + term
            wbuf[t, rows, :] = lax.rsqrt(jnp.maximum(power, 1.0))

        def fold(slot, parts):
            for i, part in enumerate(parts):
                red[slot, i * 8 : (i + 1) * 8, :] = part
            total = None
            for i in range(8):
                row = red[slot, pl.ds(i, 8, stride=8), :]
                total = row if total is None else total + row
            return total

        slot = 0
        for l in range(NB + 1):
            for kg in range(2):
                low, high = 8 * kg, min(8 * kg + 8, l + 1, NB)
                if high <= low:
                    continue
                count = high - low
                p, q, r = [None] * count, [None] * count, [None] * count
                cr, ci = [None] * count, [None] * count

                def put(box, i, value):
                    box[i] = value if box[i] is None else box[i] + value

                for g in range(GROUPS):
                    rows = slice(g * 8, (g + 1) * 8)
                    w = wbuf[t, rows, :]
                    if l < NB:
                        w2 = w * w
                        lr, li = zs[t, l, 0, rows, :] * w2, zs[t, l, 1, rows, :] * w2
                    else:
                        lr, li = zs[t, 0, 0, rows, :] * w, zs[t, 0, 1, rows, :] * w
                    le = lr + li
                    for i in range(count):
                        k = low + i
                        kr, ki = zs[t, k, 0, rows, :], zs[t, k, 1, rows, :]
                        put(p, i, kr * lr)
                        put(q, i, ki * li)
                        if k != l:
                            put(r, i, zs[t, k, 2, rows, :] * le)
                        if l == NB:
                            put(cr, i, kr * w)
                            put(ci, i, ki * w)
                re = fold(4 * kg + slot, [a + b for a, b in zip(p, q)])
                im = fold(4 * kg + slot + 1, [jnp.zeros((8, 128), F32) if c is None else c + (b - a) for a, b, c in zip(p, q, r)])
                rows = slice(low, low + 8)
                if l < NB:
                    kre[t, l, rows, :] = re
                    kim[t, l, rows, :] = im
                    for i in range(count):
                        k = low + i
                        if k != l:
                            kre[t, k, l : l + 1, :] = re[i : i + 1, :]
                            kim[t, k, l : l + 1, :] = -im[i : i + 1, :]
                else:
                    bvec[t, 0, rows, :] = re
                    bvec[t, 1, rows, :] = im
                    slot = 2 - slot
                    cvec[t, 0, rows, :] = START * fold(4 * kg + slot, cr)
                    cvec[t, 1, rows, :] = -START * fold(4 * kg + slot + 1, ci)
                slot = 2 - slot

    hear(ready.at[1])
    tell(ready.at[2])

    @pl.when(sec == 0)
    def _():
        zbuf[...] = jnp.zeros_like(zbuf)

    @pl.when(sec > 0)
    def _():
        for i in range(3):
            pl.when(present[i])(remote(msg, vbuf.at[i], v_send.at[i], v_recv.at[i], (sec_down, near[i])).wait_recv)
        for t in range(TILES):
            z0 = []
            for kg in range(2):
                rows = slice(8 * kg, 8 * kg + 8)
                lane = lanes[t, rows, :]
                tile = tiles[t, rows, :]
                pair = []
                for c in range(2):
                    src = []
                    for m in range(SPAN):
                        at = t + m
                        src.append(bcast(vbuf[at // 2, c : c + 1, (at % 2) * 128 : (at % 2) * 128 + 128]))
                    pair.append(pick(src, lane, tile))
                z0.append(pair)
            power = column_sum(z0[0][0] * z0[0][0] + z0[0][1] * z0[0][1] + (z0[1][0] * z0[1][0] + z0[1][1] * z0[1][1]))
            w = lax.rsqrt(jnp.maximum(power, 1.0))
            vr = vbuf[1, 0:1, t * 128 : (t + 1) * 128]
            vi = vbuf[1, 1:2, t * 128 : (t + 1) * 128]
            xsum[t, 0:1, :] = xsum[t, 0:1, :] + vr
            xsum[t, 1:2, :] = xsum[t, 1:2, :] + vi
            for kg in range(2):
                rows = slice(8 * kg, 8 * kg + 8)
                zr, zi = z0[kg][0] * w, z0[kg][1] * w
                z0[kg] = (zr, zi)
                zbuf[t, 0, rows, :] = zr
                zbuf[t, 1, rows, :] = zi
                cvec[t, 0, rows, :] = cvec[t, 0, rows, :] + START * zr
                cvec[t, 1, rows, :] = cvec[t, 1, rows, :] - START * zi
                bvec[t, 0, rows, :] = bvec[t, 0, rows, :] + (zr * vr + zi * vi)
                bvec[t, 1, rows, :] = bvec[t, 1, rows, :] + (zr * vi - zi * vr)
            for l in range(NB):
                lr = bcast(zbuf[t, 0, l : l + 1, :])
                li = bcast(zbuf[t, 1, l : l + 1, :])
                for kg in range(2):
                    rows = slice(8 * kg, 8 * kg + 8)
                    zr, zi = z0[kg]
                    kre[t, l, rows, :] = kre[t, l, rows, :] + (zr * lr + zi * li)
                    kim[t, l, rows, :] = kim[t, l, rows, :] + (zr * li - zi * lr)

    def product(state):
        for i, (t, c, kg) in enumerate((t, c, kg) for t in range(TILES) for c in range(2) for kg in range(2)):
            sbuf[t, c, 8 * kg : 8 * kg + 8, :] = state[i]
        out = []
        for t in range(TILES):
            y = [[None, None], [None, None]]
            for l in range(NB):
                lr = bcast(sbuf[t, 0, l : l + 1, :])
                li = bcast(sbuf[t, 1, l : l + 1, :])
                for kg in range(2):
                    rows = slice(8 * kg, 8 * kg + 8)
                    ar, ai = kre[t, l, rows, :], kim[t, l, rows, :]
                    re = ar * lr - ai * li
                    im = ar * li + ai * lr
                    y[0][kg] = re if l == 0 else y[0][kg] + re
                    y[1][kg] = im if l == 0 else y[1][kg] + im
            out += [y[0][0], y[0][1], y[1][0], y[1][1]]
        return out

    places = [(t, c, kg) for t in range(TILES) for c in range(2) for kg in range(2)]

    def c0(i):
        t, c, kg = places[i]
        return cvec[t, c, 8 * kg : 8 * kg + 8, :]

    def turn(_, state):
        return tuple(a + y + c0(i) for i, (a, y) in enumerate(zip(state, product(state))))

    state = lax.fori_loop(0, ITERS - 1, turn, tuple(c0(i) for i in range(8)))
    state = [a * SCALE for a in state]
    ks = product(state)
    norms = []
    for t in range(TILES):
        s = state[4 * t : 4 * t + 4]
        y = ks[4 * t : 4 * t + 4]
        total = None
        for i in range(4):
            term = s[i] * (y[i] + (2.0 * SCALE) * c0(4 * t + i))
            total = term if total is None else total + term
        norm = lax.rsqrt(column_sum(total) + SCALE * SCALE)
        norms.append(norm)
        cr = ci = fr = fi = None
        for kg in range(2):
            rows = slice(8 * kg, 8 * kg + 8)
            sr, si = s[kg], s[2 + kg]
            br, bi = bvec[t, 0, rows, :], bvec[t, 1, rows, :]
            zr, zi = zbuf[t, 0, rows, :], zbuf[t, 1, rows, :]
            a, b = sr * br + si * bi, sr * bi - si * br
            e, f = zr * sr - zi * si, zr * si + zi * sr
            cr = a if kg == 0 else column_sum(cr + a)
            ci = b if kg == 0 else column_sum(ci + b)
            fr = e if kg == 0 else column_sum(fr + e)
            fi = f if kg == 0 else column_sum(fi + f)
        cols = slice(t * 128, (t + 1) * 128)
        msg[0:1, cols] = (cr + (SCALE * START) * xsum[t, 0:1, :]) * norm
        msg[1:2, cols] = (ci + (SCALE * START) * xsum[t, 1:2, :]) * norm
        fr, fi = unit((fr + SCALE * START) * norm, fi * norm)
        fmsg[0:1, cols] = fr
        fmsg[1:2, cols] = fi

    @pl.when(sec < SECTIONS - 1)
    def _():
        for i in range(3):
            pl.when(present[i])(remote(msg, vbuf.at[2 - i], v_send.at[i], v_recv.at[2 - i], (sec_up, near[i])).start)

    for s in range(1, SECTIONS):

        @pl.when(sec == s)
        def _():
            for j in range(s):
                remote(fmsg, fbuf.at[s - 1], f_send.at[j], f_recv.at[s - 1], (j, pix)).start()

    hear(ready.at[2])
    comp[0, 0:1, :] = msg[0:1, :]
    comp[1, 0:1, :] = msg[1:2, :]

    for i, (t, c, kg) in enumerate(places):
        sbuf[t, c, 8 * kg : 8 * kg + 8, :] = state[i] * norms[t]
    for t in range(TILES):

        @pl.loop(0, GROUPS)
        def _(g):
            rows = pl.ds(pl.multiple_of(g * 8, 8), 8)
            re = im = None
            for k in range(NB):
                sr = bcast(sbuf[t, 0, k : k + 1, :])
                si = bcast(sbuf[t, 1, k : k + 1, :])
                zr, zi = zs[t, k, 0, rows, :], zs[t, k, 1, rows, :]
                a, b = zr * sr - zi * si, zr * si + zi * sr
                re = a if re is None else re + a
                im = b if im is None else im + b
            w = wbuf[t, rows, :]
            series[t, 0, rows, :] = bcast((SCALE * START) * norms[t]) + w * re
            series[t, 1, rows, :] = w * im

    for s in range(SECTIONS - 1, 0, -1):

        @pl.when(sec < s)
        def _():
            remote(fmsg, fbuf.at[s - 1], f_send.at[0], f_recv.at[s - 1], (s, pix)).wait_recv()
            for t in range(TILES):
                fr = fbuf[s - 1, 0:1, t * 128 : (t + 1) * 128]
                fi = fbuf[s - 1, 1:2, t * 128 : (t + 1) * 128]
                re, im = series[t, 0], series[t, 1]
                series[t, 0] = re * fr - im * fi
                series[t, 1] = re * fi + im * fr

    want = ref[0] - pix * (TILES * 128)
    lane = lax.broadcasted_iota(jnp.int32, (PAD, 128), 1)
    diag = lane == lax.broadcasted_iota(jnp.int32, (PAD, 128), 0)
    for c in range(2):
        column = jnp.zeros((PAD, 128), F32)
        for t in range(TILES):
            column = column + jnp.where(lane == want - t * 128, series[t, c], 0.0)
        column = jnp.sum(column, axis=1, keepdims=True)
        rmsg[c : c + 1, :] = column_sum(jnp.where(diag, column, 0.0))
    copies = []
    for d in range(1, 8):
        copies.append(remote(rmsg, rbuf1.at[d - 1], r_send.at[d - 1], r_recv.at[d - 1], (sec, first[d - 1])))
        copies[-1].start()
    for copy in copies:
        copy.wait_recv()
    total = rmsg[...]
    for d in range(1, 8):
        total = total + rbuf1[d - 1]
    rmsg2[...] = total
    for d in range(1, 8):
        copies.append(remote(rmsg2, rbuf2.at[d - 1], r_send.at[6 + d], r_recv.at[6 + d], (sec, second[d - 1])))
        copies[-1].start()
    for copy in copies[7:]:
        copy.wait_recv()
    for d in range(1, 8):
        total = total + rbuf2[d - 1]
    u = []
    for c in range(2):
        u.append(jnp.sum(jnp.where(diag, jnp.broadcast_to(total[c : c + 1, :], (PAD, 128)), 0.0), axis=1, keepdims=True))
    ur, ui = unit(u[0], u[1])
    ur, ui = GAIN * ur, GAIN * ui
    for t in range(TILES):
        re, im = series[t, 0], series[t, 1]
        for c, part in enumerate((re * ur + im * ui, im * ur - re * ui)):
            for g in range(GROUPS):
                count = min(8, ROWS - g * 8)
                phases[pl.ds(g * 32 + t * 2 + c, count, stride=4), :] = part[g * 8 : g * 8 + count]

    for copy in copies:
        copy.wait_send()

    @pl.when(sec < SECTIONS - 1)
    def _():
        for i in range(3):
            pl.when(present[i])(remote(msg, vbuf.at[2 - i], v_send.at[i], v_recv.at[2 - i], (sec_up, near[i])).wait_send)

    for s in range(1, SECTIONS):

        @pl.when(sec == s)
        def _():
            for j in range(s):
                remote(fmsg, fbuf.at[s - 1], f_send.at[j], f_recv.at[s - 1], (j, pix)).wait_send()


def on_device(slc, neighbours, reference_pixel):
    vmem = pl.BlockSpec(memory_space=pltpu.VMEM)
    hbm = pl.BlockSpec(memory_space=pltpu.HBM)
    pixels = slc.shape[2]
    dma = pltpu.SemaphoreType.DMA
    flat = slc.reshape(2, ROWS, TILES, 128).transpose(1, 2, 0, 3).reshape(FLAT, 128)
    phases, comp = pl.pallas_call(
        kernel,
        out_shape=(
            jax.ShapeDtypeStruct((FLAT, 128), F32),
            jax.ShapeDtypeStruct((2, 1, pixels), F32),
        ),
        in_specs=[hbm, hbm, hbm],
        out_specs=(vmem, vmem),
        scratch_shapes=[
            pltpu.VMEM((NB, pixels), jnp.int32),
            pltpu.SMEM((1,), jnp.int32),
            pltpu.VMEM((3, 32 * GROUPS, 128), F32),
            pltpu.VMEM((6, 2, PAD, 128), F32),
            pltpu.VMEM((TILES, 16, 128), jnp.int32),
            pltpu.VMEM((TILES, 16, 128), jnp.int32),
            pltpu.VMEM((TILES, NB, 3, PAD, 128), F32),
            pltpu.VMEM((TILES, PAD, 128), F32),
            pltpu.VMEM((8, 64, 128), F32),
            pltpu.VMEM((TILES, 16, 16, 128), F32),
            pltpu.VMEM((TILES, 16, 16, 128), F32),
            pltpu.VMEM((TILES, 2, 16, 128), F32),
            pltpu.VMEM((TILES, 2, 16, 128), F32),
            pltpu.VMEM((TILES, 2, 128), F32),
            pltpu.VMEM((TILES, 2, 16, 128), F32),
            pltpu.VMEM((TILES, 2, 16, 128), F32),
            pltpu.VMEM((3, 2, pixels), F32),
            pltpu.VMEM((2, pixels), F32),
            pltpu.VMEM((2, pixels), F32),
            pltpu.VMEM((3, 2, pixels), F32),
            pltpu.VMEM((TILES, 2, PAD, 128), F32),
            pltpu.VMEM((2, 128), F32),
            pltpu.VMEM((7, 2, 128), F32),
            pltpu.VMEM((2, 128), F32),
            pltpu.VMEM((7, 2, 128), F32),
            dma((3,)),
            dma((2,)),
            dma((2,)),
            dma((3,)),
            dma((3,)),
            dma((3,)),
            dma((3,)),
            dma((14,)),
            dma((14,)),
            pltpu.SemaphoreType.REGULAR((3,)),
        ],
        compiler_params=pltpu.CompilerParams(
            collective_id=0, has_side_effects=True, vmem_limit_bytes=16 * 2**20
        ),
        cost_estimate=pl.CostEstimate(flops=100_000_000, bytes_accessed=1_000_000, transcendentals=0),
    )(flat, neighbours, reference_pixel)
    return phases.reshape(ROWS, TILES, 2, 128).transpose(2, 0, 1, 3).reshape(2, ROWS, pixels), comp


def solution(mesh):
    return jax.shard_map(
        on_device,
        mesh=mesh,
        in_specs=(P(None, "section", "pix"), P(None, "pix"), P()),
        out_specs=(P(None, "section", "pix"), P(None, "section", "pix")),
        check_vma=False,
    )
```

```python
import math

import jax
import jax.numpy as jnp
from jax import lax
from jax.experimental import pallas as pl
from jax.experimental.pallas import tpu as pltpu
from jax.sharding import PartitionSpec as P

ITERS = 16
FLOOR = 0.05
REACH = 256
NB = 15
ROWS = 50
PAD = 56
GROUPS = PAD // 8
FLAT = 4 * ROWS
TILES = 2
SPAN = 5
SCALE = 2.0**-45
START = 1.0 / math.sqrt(ROWS + 1)
GAIN = math.sqrt(ROWS + 1)
SECTIONS = 4
PIX = 64
MESH = pl.DeviceIdType.MESH
F32 = jnp.float32


def bcast(row):
    return jnp.broadcast_to(row, (8, 128))


def pick(sources, lane, tile):
    out = jnp.zeros((8, 128), F32)
    for m, source in enumerate(sources):
        out = jnp.where(tile == m, take(source, lane), out)
    return out


def take(source, lane):
    return jnp.take_along_axis(source, lane, axis=1, mode="promise_in_bounds")


def column_sum(x):
    return jnp.sum(x, axis=0, keepdims=True)


def unit(re, im):
    scale = 1.0 / jnp.maximum(jnp.sqrt(re * re + im * im), FLOOR)
    return re * scale, im * scale


def remote(src, dst, send, recv, device):
    return pltpu.make_async_remote_copy(
        src_ref=src, dst_ref=dst, send_sem=send, recv_sem=recv, device_id=device, device_id_type=MESH
    )


def kernel(
    slc_hbm, nbr_hbm, ref, phases, comp,
    nbr, blocks, ext, lanes, tiles, zs, wbuf, red, kre, kim, cvec, bvec, xsum, zbuf, sbuf,
    vbuf, msg, fmsg, fbuf, series, rmsg, rbuf1, rmsg2, rbuf2,
    load_sem, halo_send, halo_recv, v_send, v_recv, f_send, f_recv, r_send, r_recv, ready,
):
    sec = lax.axis_index("section")
    pix = lax.axis_index("pix")
    before = lax.rem(pix + (PIX - 1), PIX)
    after = lax.rem(pix + 1, PIX)
    near = (before, pix, after)
    present = (pix > 0, pix >= 0, pix < PIX - 1)
    sec_up = lax.rem(sec + 1, SECTIONS)
    sec_down = lax.rem(sec + (SECTIONS - 1), SECTIONS)
    x = pix // 16
    z = lax.rem(pix // 2, 8)
    core = lax.rem(pix, 2)
    group = x * 2 + core
    first = []
    second = []
    for d in range(1, 8):
        g = lax.rem(group + d, 8)
        first.append((g // 2) * 16 + z * 2 + lax.rem(g, 2))
        second.append(x * 16 + lax.rem(z + d, 8) * 2 + core)

    own_rows = pl.ds(0, FLAT)
    loads = [
        pltpu.make_async_copy(slc_hbm, blocks.at[1, own_rows], load_sem.at[0]),
        pltpu.make_async_copy(nbr_hbm, nbr, load_sem.at[1]),
    ]
    for load in loads:
        load.start()
    barrier = pltpu.get_barrier_semaphore()
    peers = [(sec, before), (sec, after), (sec_up, pix), (sec_down, pix)]
    peers += [(sec, x * 16 + lax.rem(z + d, 8) * 2 + core) for d in (1, 7)]
    peers += [(sec, lax.rem(x + d, 4) * 16 + z * 2 + core) for d in (1, 3)]

    def tell(sem):
        for peer in peers:
            pl.semaphore_signal(sem, inc=1, device_id=peer, device_id_type=MESH)

    def hear(sem):
        pl.semaphore_wait(sem, len(peers))

    tell(barrier)
    for i in range(3):
        blocks[i, FLAT:, :] = jnp.zeros((32 * GROUPS - FLAT, 128), F32)
    kre[...] = jnp.zeros_like(kre)
    kim[...] = jnp.zeros_like(kim)
    red[...] = jnp.zeros_like(red)
    cvec[...] = jnp.zeros_like(cvec)
    bvec[...] = jnp.zeros_like(bvec)
    for i in (0, 2):

        @pl.when(jnp.logical_not(present[i]))
        def _():
            blocks[i] = jnp.zeros((32 * GROUPS, 128), F32)
            vbuf[i] = jnp.zeros_like(vbuf[i])

    hear(barrier)
    tell(ready.at[0])

    loads[0].wait()
    halos = [
        remote(blocks.at[1, own_rows], blocks.at[2 - i, own_rows], halo_send.at[i // 2], halo_recv.at[i // 2], (sec, near[i]))
        for i in (0, 2)
    ]
    for i, halo in zip((0, 2), halos):
        pl.when(present[i])(halo.start)

    for load in loads[1:]:
        load.wait()

    base = pix * (TILES * 128) - REACH
    for t in range(TILES):
        rel = nbr[:, t * 128 : (t + 1) * 128] - (base + t * 128)
        lanes[t, 0:NB, :] = jnp.bitwise_and(rel, 127)
        tiles[t, 0:NB, :] = jnp.right_shift(rel, 7)
        lanes[t, NB : NB + 1, :] = jnp.zeros((1, 128), jnp.int32)
        tiles[t, NB : NB + 1, :] = jnp.full((1, 128), SPAN, jnp.int32)

    def spread(i):
        for g in range(GROUPS):
            for m in range(2):
                for c in range(2):
                    ext[2 * i + m, c, g * 8 : (g + 1) * 8, :] = blocks[i, pl.ds(g * 32 + m * 2 + c, 8, stride=4), :]

    spread(1)
    for t in range(TILES):
        for c in range(2):
            total = None
            for g in range(GROUPS):
                own = ext[2 + t, c, g * 8 : (g + 1) * 8, :]
                zs[t, 0, c, g * 8 : (g + 1) * 8, :] = own
                total = own if total is None else total + own
            xsum[t, c : c + 1, :] = column_sum(total)
        zs[t, 0, 2] = zs[t, 0, 0] - zs[t, 0, 1]

    def gather(t, mine, theirs, begin):
        @pl.loop(0, 2)
        def _(half):
            for i in range(NB // 2):
                k = 1 + half * (NB // 2) + i
                lane = bcast(lanes[t, pl.ds(k, 1), :])
                tile = bcast(tiles[t, pl.ds(k, 1), :])
                here = [tile == m for m in theirs]
                for g in range(GROUPS):
                    rows = slice(g * 8, (g + 1) * 8)
                    pair = []
                    for c in range(2):
                        out = take(ext[t + mine, c, rows, :], lane) if begin else zs[t, k, c, rows, :]
                        for there, m in zip(here, theirs):
                            out = jnp.where(there, take(ext[t + m, c, rows, :], lane), out)
                        zs[t, k, c, rows, :] = out
                        pair.append(out)
                    if not begin:
                        zs[t, k, 2, rows, :] = pair[0] - pair[1]

    for t in range(TILES):
        gather(t, 2 - t, (3 - t,), True)

    for i, halo in zip((0, 2), halos):
        pl.when(present[i])(halo.wait_send)
        pl.when(present[2 - i])(halo.wait_recv)
    spread(0)
    spread(2)

    for t in range(TILES):
        gather(t, None, tuple(m for m in range(SPAN) if t + m not in (2, 3)), False)
    hear(ready.at[0])
    tell(ready.at[1])

    @pl.loop(0, TILES)
    def _(t):
        for g in range(GROUPS):
            rows = slice(g * 8, (g + 1) * 8)
            power = None
            for k in range(NB):
                re, im = zs[t, k, 0, rows, :], zs[t, k, 1, rows, :]
                term = re * re + im * im
                power = term if power is None else power + term
            wbuf[t, rows, :] = lax.rsqrt(jnp.maximum(power, 1.0))

        def fold(slot, parts):
            for i, part in enumerate(parts):
                red[slot, i * 8 : (i + 1) * 8, :] = part
            total = None
            for i in range(8):
                row = red[slot, pl.ds(i, 8, stride=8), :]
                total = row if total is None else total + row
            return total

        slot = 0
        for l in range(NB + 1):
            for kg in range(2):
                low, high = 8 * kg, min(8 * kg + 8, l + 1, NB)
                if high <= low:
                    continue
                count = high - low
                p, q, r = [None] * count, [None] * count, [None] * count
                cr, ci = [None] * count, [None] * count

                def put(box, i, value):
                    box[i] = value if box[i] is None else box[i] + value

                for g in range(GROUPS):
                    rows = slice(g * 8, (g + 1) * 8)
                    w = wbuf[t, rows, :]
                    if l < NB:
                        w2 = w * w
                        lr, li = zs[t, l, 0, rows, :] * w2, zs[t, l, 1, rows, :] * w2
                    else:
                        lr, li = zs[t, 0, 0, rows, :] * w, zs[t, 0, 1, rows, :] * w
                    le = lr + li
                    for i in range(count):
                        k = low + i
                        kr, ki = zs[t, k, 0, rows, :], zs[t, k, 1, rows, :]
                        put(p, i, kr * lr)
                        put(q, i, ki * li)
                        if k != l:
                            put(r, i, zs[t, k, 2, rows, :] * le)
                        if l == NB:
                            put(cr, i, kr * w)
                            put(ci, i, ki * w)
                re = fold(4 * kg + slot, [a + b for a, b in zip(p, q)])
                im = fold(4 * kg + slot + 1, [jnp.zeros((8, 128), F32) if c is None else c + (b - a) for a, b, c in zip(p, q, r)])
                rows = slice(low, low + 8)
                if l < NB:
                    kre[t, l, rows, :] = re
                    kim[t, l, rows, :] = im
                    for i in range(count):
                        k = low + i
                        if k != l:
                            kre[t, k, l : l + 1, :] = re[i : i + 1, :]
                            kim[t, k, l : l + 1, :] = -im[i : i + 1, :]
                else:
                    bvec[t, 0, rows, :] = re
                    bvec[t, 1, rows, :] = im
                    slot = 2 - slot
                    cvec[t, 0, rows, :] = START * fold(4 * kg + slot, cr)
                    cvec[t, 1, rows, :] = -START * fold(4 * kg + slot + 1, ci)
                slot = 2 - slot

    hear(ready.at[1])
    tell(ready.at[2])

    @pl.when(sec == 0)
    def _():
        zbuf[...] = jnp.zeros_like(zbuf)

    @pl.when(sec > 0)
    def _():
        for i in range(3):
            pl.when(present[i])(remote(msg, vbuf.at[i], v_send.at[i], v_recv.at[i], (sec_down, near[i])).wait_recv)
        for t in range(TILES):
            z0 = []
            for kg in range(2):
                rows = slice(8 * kg, 8 * kg + 8)
                lane = lanes[t, rows, :]
                tile = tiles[t, rows, :]
                pair = []
                for c in range(2):
                    src = []
                    for m in range(SPAN):
                        at = t + m
                        src.append(bcast(vbuf[at // 2, c : c + 1, (at % 2) * 128 : (at % 2) * 128 + 128]))
                    pair.append(pick(src, lane, tile))
                z0.append(pair)
            power = column_sum(z0[0][0] * z0[0][0] + z0[0][1] * z0[0][1] + (z0[1][0] * z0[1][0] + z0[1][1] * z0[1][1]))
            w = lax.rsqrt(jnp.maximum(power, 1.0))
            vr = vbuf[1, 0:1, t * 128 : (t + 1) * 128]
            vi = vbuf[1, 1:2, t * 128 : (t + 1) * 128]
            xsum[t, 0:1, :] = xsum[t, 0:1, :] + vr
            xsum[t, 1:2, :] = xsum[t, 1:2, :] + vi
            for kg in range(2):
                rows = slice(8 * kg, 8 * kg + 8)
                zr, zi = z0[kg][0] * w, z0[kg][1] * w
                z0[kg] = (zr, zi)
                zbuf[t, 0, rows, :] = zr
                zbuf[t, 1, rows, :] = zi
                cvec[t, 0, rows, :] = cvec[t, 0, rows, :] + START * zr
                cvec[t, 1, rows, :] = cvec[t, 1, rows, :] - START * zi
                bvec[t, 0, rows, :] = bvec[t, 0, rows, :] + (zr * vr + zi * vi)
                bvec[t, 1, rows, :] = bvec[t, 1, rows, :] + (zr * vi - zi * vr)
            for l in range(NB):
                lr = bcast(zbuf[t, 0, l : l + 1, :])
                li = bcast(zbuf[t, 1, l : l + 1, :])
                for kg in range(2):
                    rows = slice(8 * kg, 8 * kg + 8)
                    zr, zi = z0[kg]
                    kre[t, l, rows, :] = kre[t, l, rows, :] + (zr * lr + zi * li)
                    kim[t, l, rows, :] = kim[t, l, rows, :] + (zr * li - zi * lr)

    def product(state):
        for i, (t, c, kg) in enumerate((t, c, kg) for t in range(TILES) for c in range(2) for kg in range(2)):
            sbuf[t, c, 8 * kg : 8 * kg + 8, :] = state[i]
        out = []
        for t in range(TILES):
            y = [[None, None], [None, None]]
            for l in range(NB):
                lr = bcast(sbuf[t, 0, l : l + 1, :])
                li = bcast(sbuf[t, 1, l : l + 1, :])
                for kg in range(2):
                    rows = slice(8 * kg, 8 * kg + 8)
                    ar, ai = kre[t, l, rows, :], kim[t, l, rows, :]
                    re = ar * lr - ai * li
                    im = ar * li + ai * lr
                    y[0][kg] = re if l == 0 else y[0][kg] + re
                    y[1][kg] = im if l == 0 else y[1][kg] + im
            out += [y[0][0], y[0][1], y[1][0], y[1][1]]
        return out

    places = [(t, c, kg) for t in range(TILES) for c in range(2) for kg in range(2)]

    def c0(i):
        t, c, kg = places[i]
        return cvec[t, c, 8 * kg : 8 * kg + 8, :]

    def turn(_, state):
        return tuple(a + y + c0(i) for i, (a, y) in enumerate(zip(state, product(state))))

    state = lax.fori_loop(0, ITERS - 1, turn, tuple(c0(i) for i in range(8)))
    state = [a * SCALE for a in state]
    ks = product(state)
    norms = []
    for t in range(TILES):
        s = state[4 * t : 4 * t + 4]
        y = ks[4 * t : 4 * t + 4]
        total = None
        for i in range(4):
            term = s[i] * (y[i] + (2.0 * SCALE) * c0(4 * t + i))
            total = term if total is None else total + term
        norm = lax.rsqrt(column_sum(total) + SCALE * SCALE)
        norms.append(norm)
        cr = ci = fr = fi = None
        for kg in range(2):
            rows = slice(8 * kg, 8 * kg + 8)
            sr, si = s[kg], s[2 + kg]
            br, bi = bvec[t, 0, rows, :], bvec[t, 1, rows, :]
            zr, zi = zbuf[t, 0, rows, :], zbuf[t, 1, rows, :]
            a, b = sr * br + si * bi, sr * bi - si * br
            e, f = zr * sr - zi * si, zr * si + zi * sr
            cr = a if kg == 0 else column_sum(cr + a)
            ci = b if kg == 0 else column_sum(ci + b)
            fr = e if kg == 0 else column_sum(fr + e)
            fi = f if kg == 0 else column_sum(fi + f)
        cols = slice(t * 128, (t + 1) * 128)
        msg[0:1, cols] = (cr + (SCALE * START) * xsum[t, 0:1, :]) * norm
        msg[1:2, cols] = (ci + (SCALE * START) * xsum[t, 1:2, :]) * norm
        fr, fi = unit((fr + SCALE * START) * norm, fi * norm)
        fmsg[0:1, cols] = fr
        fmsg[1:2, cols] = fi

    @pl.when(sec < SECTIONS - 1)
    def _():
        for i in range(3):
            pl.when(present[i])(remote(msg, vbuf.at[2 - i], v_send.at[i], v_recv.at[2 - i], (sec_up, near[i])).start)

    for s in range(1, SECTIONS):

        @pl.when(sec == s)
        def _():
            for j in range(s):
                remote(fmsg, fbuf.at[s - 1], f_send.at[j], f_recv.at[s - 1], (j, pix)).start()

    hear(ready.at[2])
    comp[0, 0:1, :] = msg[0:1, :]
    comp[1, 0:1, :] = msg[1:2, :]

    for i, (t, c, kg) in enumerate(places):
        sbuf[t, c, 8 * kg : 8 * kg + 8, :] = state[i] * norms[t]
    for t in range(TILES):

        @pl.loop(0, GROUPS)
        def _(g):
            rows = pl.ds(pl.multiple_of(g * 8, 8), 8)
            re = im = None
            for k in range(NB):
                sr = bcast(sbuf[t, 0, k : k + 1, :])
                si = bcast(sbuf[t, 1, k : k + 1, :])
                zr, zi = zs[t, k, 0, rows, :], zs[t, k, 1, rows, :]
                a, b = zr * sr - zi * si, zr * si + zi * sr
                re = a if re is None else re + a
                im = b if im is None else im + b
            w = wbuf[t, rows, :]
            series[t, 0, rows, :] = bcast((SCALE * START) * norms[t]) + w * re
            series[t, 1, rows, :] = w * im

    for s in range(SECTIONS - 1, 0, -1):

        @pl.when(sec < s)
        def _():
            remote(fmsg, fbuf.at[s - 1], f_send.at[0], f_recv.at[s - 1], (s, pix)).wait_recv()
            for t in range(TILES):
                fr = fbuf[s - 1, 0:1, t * 128 : (t + 1) * 128]
                fi = fbuf[s - 1, 1:2, t * 128 : (t + 1) * 128]
                re, im = series[t, 0], series[t, 1]
                series[t, 0] = re * fr - im * fi
                series[t, 1] = re * fi + im * fr

    want = ref[0] - pix * (TILES * 128)
    lane = lax.broadcasted_iota(jnp.int32, (PAD, 128), 1)
    diag = lane == lax.broadcasted_iota(jnp.int32, (PAD, 128), 0)
    for c in range(2):
        column = jnp.zeros((PAD, 128), F32)
        for t in range(TILES):
            column = column + jnp.where(lane == want - t * 128, series[t, c], 0.0)
        column = jnp.sum(column, axis=1, keepdims=True)
        rmsg[c : c + 1, :] = column_sum(jnp.where(diag, column, 0.0))
    copies = []
    for d in range(1, 8):
        copies.append(remote(rmsg, rbuf1.at[d - 1], r_send.at[d - 1], r_recv.at[d - 1], (sec, first[d - 1])))
        copies[-1].start()
    for copy in copies:
        copy.wait_recv()
    total = rmsg[...]
    for d in range(1, 8):
        total = total + rbuf1[d - 1]
    rmsg2[...] = total
    for d in range(1, 8):
        copies.append(remote(rmsg2, rbuf2.at[d - 1], r_send.at[6 + d], r_recv.at[6 + d], (sec, second[d - 1])))
        copies[-1].start()
    for copy in copies[7:]:
        copy.wait_recv()
    for d in range(1, 8):
        total = total + rbuf2[d - 1]
    u = []
    for c in range(2):
        u.append(jnp.sum(jnp.where(diag, jnp.broadcast_to(total[c : c + 1, :], (PAD, 128)), 0.0), axis=1, keepdims=True))
    ur, ui = unit(u[0], u[1])
    ur, ui = GAIN * ur, GAIN * ui
    for t in range(TILES):
        re, im = series[t, 0], series[t, 1]
        for c, part in enumerate((re * ur + im * ui, im * ur - re * ui)):
            for g in range(GROUPS):
                count = min(8, ROWS - g * 8)
                phases[pl.ds(g * 32 + t * 2 + c, count, stride=4), :] = part[g * 8 : g * 8 + count]

    for copy in copies:
        copy.wait_send()

    @pl.when(sec < SECTIONS - 1)
    def _():
        for i in range(3):
            pl.when(present[i])(remote(msg, vbuf.at[2 - i], v_send.at[i], v_recv.at[2 - i], (sec_up, near[i])).wait_send)

    for s in range(1, SECTIONS):

        @pl.when(sec == s)
        def _():
            for j in range(s):
                remote(fmsg, fbuf.at[s - 1], f_send.at[j], f_recv.at[s - 1], (j, pix)).wait_send()


def on_device(slc, neighbours, reference_pixel):
    vmem = pl.BlockSpec(memory_space=pltpu.VMEM)
    hbm = pl.BlockSpec(memory_space=pltpu.HBM)
    pixels = slc.shape[2]
    dma = pltpu.SemaphoreType.DMA
    flat = slc.reshape(2, ROWS, TILES, 128).transpose(1, 2, 0, 3).reshape(FLAT, 128)
    phases, comp = pl.pallas_call(
        kernel,
        out_shape=(
            jax.ShapeDtypeStruct((FLAT, 128), F32),
            jax.ShapeDtypeStruct((2, 1, pixels), F32),
        ),
        in_specs=[hbm, hbm, pl.BlockSpec(memory_space=pltpu.SMEM)],
        out_specs=(vmem, vmem),
        scratch_shapes=[
            pltpu.VMEM((NB, pixels), jnp.int32),
            pltpu.VMEM((3, 32 * GROUPS, 128), F32),
            pltpu.VMEM((6, 2, PAD, 128), F32),
            pltpu.VMEM((TILES, 16, 128), jnp.int32),
            pltpu.VMEM((TILES, 16, 128), jnp.int32),
            pltpu.VMEM((TILES, NB, 3, PAD, 128), F32),
            pltpu.VMEM((TILES, PAD, 128), F32),
            pltpu.VMEM((8, 64, 128), F32),
            pltpu.VMEM((TILES, 16, 16, 128), F32),
            pltpu.VMEM((TILES, 16, 16, 128), F32),
            pltpu.VMEM((TILES, 2, 16, 128), F32),
            pltpu.VMEM((TILES, 2, 16, 128), F32),
            pltpu.VMEM((TILES, 2, 128), F32),
            pltpu.VMEM((TILES, 2, 16, 128), F32),
            pltpu.VMEM((TILES, 2, 16, 128), F32),
            pltpu.VMEM((3, 2, pixels), F32),
            pltpu.VMEM((2, pixels), F32),
            pltpu.VMEM((2, pixels), F32),
            pltpu.VMEM((3, 2, pixels), F32),
            pltpu.VMEM((TILES, 2, PAD, 128), F32),
            pltpu.VMEM((2, 128), F32),
            pltpu.VMEM((7, 2, 128), F32),
            pltpu.VMEM((2, 128), F32),
            pltpu.VMEM((7, 2, 128), F32),
            dma((2,)),
            dma((2,)),
            dma((2,)),
            dma((3,)),
            dma((3,)),
            dma((3,)),
            dma((3,)),
            dma((14,)),
            dma((14,)),
            pltpu.SemaphoreType.REGULAR((3,)),
        ],
        compiler_params=pltpu.CompilerParams(
            collective_id=0, has_side_effects=True, vmem_limit_bytes=16 * 2**20
        ),
        cost_estimate=pl.CostEstimate(flops=100_000_000, bytes_accessed=1_000_000, transcendentals=0),
    )(*(pltpu.with_memory_space_constraint(a, pltpu.HBM) for a in (flat, neighbours)), reference_pixel)
    return phases.reshape(ROWS, TILES, 2, 128).transpose(2, 0, 1, 3).reshape(2, ROWS, pixels), comp


def solution(mesh):
    return jax.shard_map(
        on_device,
        mesh=mesh,
        in_specs=(P(None, "section", "pix"), P(None, "pix"), P()),
        out_specs=(P(None, "section", "pix"), P(None, "section", "pix")),
        check_vma=False,
    )
```

```python
import math

import jax
import jax.numpy as jnp
from jax import lax
from jax.experimental import pallas as pl
from jax.experimental.pallas import tpu as pltpu
from jax.sharding import PartitionSpec as P

ITERS = 16
FLOOR = 0.05
REACH = 256
NB = 15
ROWS = 50
PAD = 56
GROUPS = PAD // 8
FLAT = 4 * ROWS
TILES = 2
SPAN = 5
SCALE = 2.0**-45
START = 1.0 / math.sqrt(ROWS + 1)
GAIN = math.sqrt(ROWS + 1)
SECTIONS = 4
PIX = 64
MESH = pl.DeviceIdType.MESH
F32 = jnp.float32


def bcast(row):
    return jnp.broadcast_to(row, (8, 128))


def pick(sources, lane, tile):
    out = jnp.zeros((8, 128), F32)
    for m, source in enumerate(sources):
        out = jnp.where(tile == m, take(source, lane), out)
    return out


def take(source, lane):
    return jnp.take_along_axis(source, lane, axis=1, mode="promise_in_bounds")


def column_sum(x):
    return jnp.sum(x, axis=0, keepdims=True)


def eye(count, shift=0):
    lane = lax.broadcasted_iota(jnp.int32, (count, 128), 1)
    return lane == lax.broadcasted_iota(jnp.int32, (count, 128), 0) + shift


def to_row(column, shift=0):
    return column_sum(jnp.where(eye(column.shape[0], shift), column, 0.0))


def to_column(row, count):
    spread = jnp.broadcast_to(row, (count, 128))
    return jnp.sum(jnp.where(eye(count), spread, 0.0), axis=1, keepdims=True)


def unit(re, im):
    scale = 1.0 / jnp.maximum(jnp.sqrt(re * re + im * im), FLOOR)
    return re * scale, im * scale


def remote(src, dst, send, recv, device):
    return pltpu.make_async_remote_copy(
        src_ref=src, dst_ref=dst, send_sem=send, recv_sem=recv, device_id=device, device_id_type=MESH
    )


def kernel(
    slc_hbm, nbr_hbm, ref, phases, comp,
    nbr, blocks, ext, lanes, tiles, zs, wbuf, red, kre, kim, cvec, bvec, xsum, zbuf, sbuf,
    vbuf, msg, fmsg, fbuf, series, datum,
    nmsg, nbuf1, nmsg2, nbuf2, ncol, emsg, ebuf1, emsg2, ebuf2, eall, gmsg, gbuf, rmsg, rbuf1, bmsg, bbuf,
    kref, kimf, cref, zref, sref,
    load_sem, halo_send, halo_recv, v_send, v_recv, f_send, f_recv, n_send, n_recv, e_send, e_recv,
    y_send, y_recv, g_send, g_recv, r_send, r_recv, b_send, b_recv, ready,
):
    sec = lax.axis_index("section")
    pix = lax.axis_index("pix")
    before = lax.rem(pix + (PIX - 1), PIX)
    after = lax.rem(pix + 1, PIX)
    near = (before, pix, after)
    present = (pix > 0, pix >= 0, pix < PIX - 1)
    sec_up = lax.rem(sec + 1, SECTIONS)
    sec_down = lax.rem(sec + (SECTIONS - 1), SECTIONS)
    x = pix // 16
    z = lax.rem(pix // 2, 8)
    core = lax.rem(pix, 2)
    group = x * 2 + core
    first = []
    second = []
    for d in range(1, 8):
        g = lax.rem(group + d, 8)
        first.append((g // 2) * 16 + z * 2 + lax.rem(g, 2))
        second.append(x * 16 + lax.rem(z + d, 8) * 2 + core)

    want = ref[0] - pix * (TILES * 128)

    def at_ref(parts):
        total = None
        for t, part in enumerate(parts):
            lane = lax.broadcasted_iota(jnp.int32, part.shape, 1)
            part = jnp.where(lane == want - t * 128, part, 0.0)
            total = part if total is None else total + part
        return jnp.sum(total, axis=1, keepdims=True)

    def copies(src, dst, send, recv, devices, base=0):
        return [
            remote(src, dst.at[i], send.at[base + i], recv.at[base + i], (sec, device))
            for i, device in enumerate(devices)
        ]

    def start(made):
        for copy in made:
            copy.start()

    def finish(made):
        for copy in made:
            copy.wait_send()
            copy.wait_recv()

    def sum_of(own, buffers):
        total = own[...]
        for i in range(7):
            total = total + buffers[i]
        return total

    steps_n = copies(nmsg, nbuf1, n_send, n_recv, first), copies(nmsg2, nbuf2, n_send, n_recv, second, 7)
    steps_e = copies(emsg, ebuf1, e_send, e_recv, first), copies(emsg2, ebuf2, e_send, e_recv, second, 7)
    steps_r = copies(rmsg, rbuf1, r_send, r_recv, first)
    steps_b = copies(bmsg, bbuf, b_send, b_recv, second)

    own_rows = pl.ds(0, FLAT)
    loads = [
        pltpu.make_async_copy(slc_hbm, blocks.at[1, own_rows], load_sem.at[0]),
        pltpu.make_async_copy(nbr_hbm, nbr, load_sem.at[1]),
    ]
    for load in loads:
        load.start()
    barrier = pltpu.get_barrier_semaphore()
    peers = [(sec, before), (sec, after), (sec_up, pix), (sec_down, pix)]
    peers += [(sec, x * 16 + lax.rem(z + d, 8) * 2 + core) for d in (1, 7)]
    peers += [(sec, lax.rem(x + d, 4) * 16 + z * 2 + core) for d in (1, 3)]

    def tell(sem):
        for peer in peers:
            pl.semaphore_signal(sem, inc=1, device_id=peer, device_id_type=MESH)

    def hear(sem):
        pl.semaphore_wait(sem, len(peers))

    tell(barrier)
    for i in range(3):
        blocks[i, FLAT:, :] = jnp.zeros((32 * GROUPS - FLAT, 128), F32)
    kre[...] = jnp.zeros_like(kre)
    kim[...] = jnp.zeros_like(kim)
    red[...] = jnp.zeros_like(red)
    cvec[...] = jnp.zeros_like(cvec)
    bvec[...] = jnp.zeros_like(bvec)
    for i in (0, 2):

        @pl.when(jnp.logical_not(present[i]))
        def _():
            blocks[i] = jnp.zeros((32 * GROUPS, 128), F32)
            vbuf[i] = jnp.zeros_like(vbuf[i])

    hear(barrier)
    tell(ready.at[0])

    loads[0].wait()
    halos = [
        remote(blocks.at[1, own_rows], blocks.at[2 - i, own_rows], halo_send.at[i // 2], halo_recv.at[i // 2], (sec, near[i]))
        for i in (0, 2)
    ]
    for i, halo in zip((0, 2), halos):
        pl.when(present[i])(halo.start)

    for load in loads[1:]:
        load.wait()

    base = pix * (TILES * 128) - REACH
    for t in range(TILES):
        rel = nbr[:, t * 128 : (t + 1) * 128] - (base + t * 128)
        lanes[t, 0:NB, :] = jnp.bitwise_and(rel, 127)
        tiles[t, 0:NB, :] = jnp.right_shift(rel, 7)
        lanes[t, NB : NB + 1, :] = jnp.zeros((1, 128), jnp.int32)
        tiles[t, NB : NB + 1, :] = jnp.full((1, 128), SPAN, jnp.int32)

    def spread(i):
        for g in range(GROUPS):
            for m in range(2):
                for c in range(2):
                    ext[2 * i + m, c, g * 8 : (g + 1) * 8, :] = blocks[i, pl.ds(g * 32 + m * 2 + c, 8, stride=4), :]

    spread(1)
    for t in range(TILES):
        for c in range(2):
            total = None
            for g in range(GROUPS):
                own = ext[2 + t, c, g * 8 : (g + 1) * 8, :]
                zs[t, 0, c, g * 8 : (g + 1) * 8, :] = own
                total = own if total is None else total + own
            xsum[t, c : c + 1, :] = column_sum(total)
        zs[t, 0, 2] = zs[t, 0, 0] - zs[t, 0, 1]

    def gather(t, mine, theirs, begin):
        @pl.loop(0, 2)
        def _(half):
            for i in range(NB // 2):
                k = 1 + half * (NB // 2) + i
                lane = bcast(lanes[t, pl.ds(k, 1), :])
                tile = bcast(tiles[t, pl.ds(k, 1), :])
                here = [tile == m for m in theirs]
                for g in range(GROUPS):
                    rows = slice(g * 8, (g + 1) * 8)
                    pair = []
                    for c in range(2):
                        out = take(ext[t + mine, c, rows, :], lane) if begin else zs[t, k, c, rows, :]
                        for there, m in zip(here, theirs):
                            out = jnp.where(there, take(ext[t + m, c, rows, :], lane), out)
                        zs[t, k, c, rows, :] = out
                        pair.append(out)
                    if not begin:
                        zs[t, k, 2, rows, :] = pair[0] - pair[1]

    for t in range(TILES):
        gather(t, 2 - t, (3 - t,), True)
    hear(ready.at[0])
    tell(ready.at[1])

    for i, halo in zip((0, 2), halos):
        pl.when(present[i])(halo.wait_send)
        pl.when(present[2 - i])(halo.wait_recv)
    spread(0)
    spread(2)

    for t in range(TILES):
        gather(t, None, tuple(m for m in range(SPAN) if t + m not in (2, 3)), False)
    hear(ready.at[1])
    tell(ready.at[2])

    @pl.when(sec == 2)
    def _():
        column = at_ref([nbr[:, t * 128 : (t + 1) * 128].astype(F32) for t in range(TILES)])
        nmsg[...] = to_row(column)
        start(steps_n[0])

    @pl.loop(0, TILES)
    def _(t):
        for g in range(GROUPS):
            rows = slice(g * 8, (g + 1) * 8)
            power = None
            for k in range(NB):
                re, im = zs[t, k, 0, rows, :], zs[t, k, 1, rows, :]
                term = re * re + im * im
                power = term if power is None else power + term
            wbuf[t, rows, :] = lax.rsqrt(jnp.maximum(power, 1.0))

        def fold(slot, parts):
            for i, part in enumerate(parts):
                red[slot, i * 8 : (i + 1) * 8, :] = part
            total = None
            for i in range(8):
                row = red[slot, pl.ds(i, 8, stride=8), :]
                total = row if total is None else total + row
            return total

        slot = 0
        for l in range(NB + 1):
            for kg in range(2):
                low, high = 8 * kg, min(8 * kg + 8, l + 1, NB)
                if high <= low:
                    continue
                count = high - low
                p, q, r = [None] * count, [None] * count, [None] * count
                cr, ci = [None] * count, [None] * count

                def put(box, i, value):
                    box[i] = value if box[i] is None else box[i] + value

                for g in range(GROUPS):
                    rows = slice(g * 8, (g + 1) * 8)
                    w = wbuf[t, rows, :]
                    if l < NB:
                        w2 = w * w
                        lr, li = zs[t, l, 0, rows, :] * w2, zs[t, l, 1, rows, :] * w2
                    else:
                        lr, li = zs[t, 0, 0, rows, :] * w, zs[t, 0, 1, rows, :] * w
                    le = lr + li
                    for i in range(count):
                        k = low + i
                        kr, ki = zs[t, k, 0, rows, :], zs[t, k, 1, rows, :]
                        put(p, i, kr * lr)
                        put(q, i, ki * li)
                        if k != l:
                            put(r, i, zs[t, k, 2, rows, :] * le)
                        if l == NB:
                            put(cr, i, kr * w)
                            put(ci, i, ki * w)
                re = fold(4 * kg + slot, [a + b for a, b in zip(p, q)])
                im = fold(4 * kg + slot + 1, [jnp.zeros((8, 128), F32) if c is None else c + (b - a) for a, b, c in zip(p, q, r)])
                rows = slice(low, low + 8)
                if l < NB:
                    kre[t, l, rows, :] = re
                    kim[t, l, rows, :] = im
                    for i in range(count):
                        k = low + i
                        if k != l:
                            kre[t, k, l : l + 1, :] = re[i : i + 1, :]
                            kim[t, k, l : l + 1, :] = -im[i : i + 1, :]
                else:
                    bvec[t, 0, rows, :] = re
                    bvec[t, 1, rows, :] = im
                    slot = 2 - slot
                    cvec[t, 0, rows, :] = START * fold(4 * kg + slot, cr)
                    cvec[t, 1, rows, :] = -START * fold(4 * kg + slot + 1, ci)
                slot = 2 - slot

    @pl.when(sec >= 2)
    def _():
        hear(ready.at[2])
        tell(ready.at[3])

    @pl.when(sec == 2)
    def _():
        finish(steps_n[0])
        nmsg2[...] = sum_of(nmsg, nbuf1)
        start(steps_n[1])

    def expand():
        for l in range(NB):
            kref[0, l] = jnp.broadcast_to(eall[0:16, l : l + 1], (16, 128))
            kimf[0, l] = jnp.broadcast_to(eall[0:16, 16 + l : 17 + l], (16, 128))
        for c in range(2):
            cref[0, c] = jnp.broadcast_to(eall[0:16, 32 + c : 33 + c], (16, 128))

    @pl.when(sec == SECTIONS - 1)
    def _():
        lane = lax.broadcasted_iota(jnp.int32, (16, 128), 1)
        emsg[16:32, :] = jnp.zeros((16, 128), F32)
        acc = jnp.zeros((16, 128), F32)
        for c in range(2):
            acc = jnp.where(lane == 32 + c, at_ref([cvec[t, c] for t in range(TILES)]), acc)
        emsg[0:16, :] = acc

        @pl.loop(0, NB)
        def _(k):
            acc = emsg[0:16, :]
            acc = jnp.where(lane == k, at_ref([kre[t, k] for t in range(TILES)]), acc)
            emsg[0:16, :] = jnp.where(lane == 16 + k, at_ref([kim[t, k] for t in range(TILES)]), acc)
            parts = [at_ref([zs[t, k, c] * wbuf[t] for t in range(TILES)]) for c in range(2)]
            emsg[pl.ds(16 + k, 1), :] = to_row(parts[0]) + to_row(parts[1], 64)

        start(steps_e[0])
        finish(steps_e[0])
        emsg2[...] = sum_of(emsg, ebuf1)
        start(steps_e[1])
        finish(steps_e[1])
        eall[...] = sum_of(emsg2, ebuf2)
        for j in range(SECTIONS - 1):
            remote(eall.at[pl.ds(0, 16)], eall.at[pl.ds(0, 16)], y_send.at[j], y_recv, (j, pix)).start()
        expand()

    @pl.when(sec == 2)
    def _():
        finish(steps_n[1])
        column = to_column(sum_of(nmsg2, nbuf2), 16)
        row = lax.broadcasted_iota(jnp.int32, (16, 128), 0)
        ncol[...] = jnp.where(row == NB, ref[0].astype(F32), column) - (pix * (TILES * 128)).astype(F32)

    def add_date(kr, ki, zb, t, z0):
        for l in range(NB):
            lr = bcast(zb[t, 0, l : l + 1, :])
            li = bcast(zb[t, 1, l : l + 1, :])
            for kg in range(2):
                rows = slice(8 * kg, 8 * kg + 8)
                zr, zi = z0[kg]
                kr[t, l, rows, :] = kr[t, l, rows, :] + (zr * lr + zi * li)
                ki[t, l, rows, :] = ki[t, l, rows, :] + (zr * li - zi * lr)

    @pl.when(sec == 0)
    def _():
        zbuf[...] = jnp.zeros_like(zbuf)

    @pl.when(sec > 0)
    def _():
        for i in range(3):
            pl.when(present[i])(remote(msg, vbuf.at[i], v_send.at[i], v_recv.at[i], (sec_down, near[i])).wait_recv)
        for t in range(TILES):
            z0 = []
            for kg in range(2):
                rows = slice(8 * kg, 8 * kg + 8)
                lane = lanes[t, rows, :]
                tile = tiles[t, rows, :]
                pair = []
                for c in range(2):
                    src = []
                    for m in range(SPAN):
                        at = t + m
                        src.append(bcast(vbuf[at // 2, c : c + 1, (at % 2) * 128 : (at % 2) * 128 + 128]))
                    pair.append(pick(src, lane, tile))
                z0.append(pair)
            power = column_sum(z0[0][0] * z0[0][0] + z0[0][1] * z0[0][1] + (z0[1][0] * z0[1][0] + z0[1][1] * z0[1][1]))
            w = lax.rsqrt(jnp.maximum(power, 1.0))
            vr = vbuf[1, 0:1, t * 128 : (t + 1) * 128]
            vi = vbuf[1, 1:2, t * 128 : (t + 1) * 128]
            xsum[t, 0:1, :] = xsum[t, 0:1, :] + vr
            xsum[t, 1:2, :] = xsum[t, 1:2, :] + vi
            for kg in range(2):
                rows = slice(8 * kg, 8 * kg + 8)
                zr, zi = z0[kg][0] * w, z0[kg][1] * w
                z0[kg] = (zr, zi)
                zbuf[t, 0, rows, :] = zr
                zbuf[t, 1, rows, :] = zi
                cvec[t, 0, rows, :] = cvec[t, 0, rows, :] + START * zr
                cvec[t, 1, rows, :] = cvec[t, 1, rows, :] - START * zi
                bvec[t, 0, rows, :] = bvec[t, 0, rows, :] + (zr * vr + zi * vi)
                bvec[t, 1, rows, :] = bvec[t, 1, rows, :] + (zr * vi - zi * vr)
            add_date(kre, kim, zbuf, t, z0)

    def solve(kr, ki, cv, sb, count):
        places = [(t, c, kg) for t in range(count) for c in range(2) for kg in range(2)]

        def product(state):
            for i, (t, c, kg) in enumerate(places):
                sb[t, c, 8 * kg : 8 * kg + 8, :] = state[i]
            out = []
            for t in range(count):
                y = [[None, None], [None, None]]
                for l in range(NB):
                    lr = bcast(sb[t, 0, l : l + 1, :])
                    li = bcast(sb[t, 1, l : l + 1, :])
                    for kg in range(2):
                        rows = slice(8 * kg, 8 * kg + 8)
                        ar, ai = kr[t, l, rows, :], ki[t, l, rows, :]
                        re = ar * lr - ai * li
                        im = ar * li + ai * lr
                        y[0][kg] = re if l == 0 else y[0][kg] + re
                        y[1][kg] = im if l == 0 else y[1][kg] + im
                out += [y[0][0], y[0][1], y[1][0], y[1][1]]
            return out

        def c0(i):
            t, c, kg = places[i]
            return cv[t, c, 8 * kg : 8 * kg + 8, :]

        def turn(_, state):
            return tuple(a + y + c0(i) for i, (a, y) in enumerate(zip(state, product(state))))

        state = lax.fori_loop(0, ITERS - 1, turn, tuple(c0(i) for i in range(len(places))))
        state = [a * SCALE for a in state]
        ks = product(state)
        norms = []
        for t in range(count):
            total = None
            for i in range(4 * t, 4 * t + 4):
                term = state[i] * (ks[i] + (2.0 * SCALE) * c0(i))
                total = term if total is None else total + term
            norms.append(lax.rsqrt(column_sum(total) + SCALE * SCALE))
        return state, norms

    state, norms = solve(kre, kim, cvec, sbuf, TILES)
    for t in range(TILES):
        s = state[4 * t : 4 * t + 4]
        norm = norms[t]
        cr = ci = fr = fi = None
        for kg in range(2):
            rows = slice(8 * kg, 8 * kg + 8)
            sr, si = s[kg], s[2 + kg]
            br, bi = bvec[t, 0, rows, :], bvec[t, 1, rows, :]
            zr, zi = zbuf[t, 0, rows, :], zbuf[t, 1, rows, :]
            a, b = sr * br + si * bi, sr * bi - si * br
            e, f = zr * sr - zi * si, zr * si + zi * sr
            cr = a if kg == 0 else column_sum(cr + a)
            ci = b if kg == 0 else column_sum(ci + b)
            fr = e if kg == 0 else column_sum(fr + e)
            fi = f if kg == 0 else column_sum(fi + f)
        cols = slice(t * 128, (t + 1) * 128)
        msg[0:1, cols] = (cr + (SCALE * START) * xsum[t, 0:1, :]) * norm
        msg[1:2, cols] = (ci + (SCALE * START) * xsum[t, 1:2, :]) * norm
        fr, fi = unit((fr + SCALE * START) * norm, fi * norm)
        fmsg[0:1, cols] = fr
        fmsg[1:2, cols] = fi

    @pl.when(sec < SECTIONS - 1)
    def _():
        for i in range(3):
            pl.when(present[i])(remote(msg, vbuf.at[2 - i], v_send.at[i], v_recv.at[2 - i], (sec_up, near[i])).start)

    for s in range(1, SECTIONS):

        @pl.when(sec == s)
        def _():
            for j in range(s):
                remote(fmsg, fbuf.at[s - 1], f_send.at[j], f_recv.at[s - 1], (j, pix)).start()

    steps_g = [
        (s, d, remote(gmsg, gbuf.at[d], g_send.at[8 * s + d], g_recv.at[d], (s, pix if d == 0 else first[d - 1])))
        for s in range(SECTIONS)
        for d in range(8)
        if (s, d) != (2, 0)
    ]

    @pl.when(sec < 2)
    def _():
        hear(ready.at[2])
        tell(ready.at[3])

    hear(ready.at[3])

    @pl.when(sec == 2)
    def _():
        lane = lax.broadcasted_iota(jnp.int32, (16, 128), 1).astype(F32)
        row = lax.broadcasted_iota(jnp.int32, (16, 128), 0)
        for c in range(2):
            total = None
            for t in range(TILES):
                cols = slice(t * 128, (t + 1) * 128)
                value = jnp.where(
                    row == NB,
                    jnp.broadcast_to(fmsg[c : c + 1, cols], (16, 128)),
                    jnp.broadcast_to(msg[c : c + 1, cols], (16, 128)),
                )
                value = jnp.where(ncol[...] - t * 128.0 == lane, value, 0.0)
                total = value if total is None else total + value
            gmsg[c : c + 1, :] = to_row(jnp.sum(total, axis=1, keepdims=True))
        for _, _, copy in steps_g:
            copy.start()
        gbuf[0] = gmsg[...]

    comp[0, 0:1, :] = msg[0:1, :]
    comp[1, 0:1, :] = msg[1:2, :]

    for i, (t, c, kg) in enumerate((t, c, kg) for t in range(TILES) for c in range(2) for kg in range(2)):
        sbuf[t, c, 8 * kg : 8 * kg + 8, :] = state[i] * norms[t]
    for t in range(TILES):

        @pl.loop(0, GROUPS)
        def _(g):
            rows = pl.ds(pl.multiple_of(g * 8, 8), 8)
            re = im = None
            for k in range(NB):
                sr = bcast(sbuf[t, 0, k : k + 1, :])
                si = bcast(sbuf[t, 1, k : k + 1, :])
                zr, zi = zs[t, k, 0, rows, :], zs[t, k, 1, rows, :]
                a, b = zr * sr - zi * si, zr * si + zi * sr
                re = a if re is None else re + a
                im = b if im is None else im + b
            w = wbuf[t, rows, :]
            series[t, 0, rows, :] = bcast((SCALE * START) * norms[t]) + w * re
            series[t, 1, rows, :] = w * im

    def take_f(j):
        remote(fmsg, fbuf.at[j - 1], f_send.at[0], f_recv.at[j - 1], (j, pix)).wait_recv()

    @pl.when(sec == 0)
    def _():
        take_f(1)
        for t in range(TILES):
            fr = fbuf[0, 0:1, t * 128 : (t + 1) * 128]
            fi = fbuf[0, 1:2, t * 128 : (t + 1) * 128]
            re, im = series[t, 0], series[t, 1]
            series[t, 0] = re * fr - im * fi
            series[t, 1] = re * fi + im * fr

    @pl.when(sec < SECTIONS - 1)
    def _():
        for c in range(2):
            rmsg[c : c + 1, :] = to_row(at_ref([series[t, c] for t in range(TILES)]))
        start(steps_r)
        remote(eall.at[pl.ds(0, 16)], eall.at[pl.ds(0, 16)], y_send.at[0], y_recv, (SECTIONS - 1, pix)).wait_recv()
        expand()

    for s, d, copy in steps_g:
        if s == 0:
            if d == 0:
                pl.when(sec != 2)(copy.wait_recv)
            else:
                copy.wait_recv()
    total = gbuf[0]
    for d in range(1, 8):
        total = total + gbuf[d]
    bmsg[2:4, :] = total

    @pl.when(sec < SECTIONS - 1)
    def _():
        finish(steps_r)
        bmsg[0:2, :] = sum_of(rmsg, rbuf1)

    @pl.when(sec == SECTIONS - 1)
    def _():
        bmsg[0:2, :] = jnp.zeros((2, 128), F32)

    start(steps_b)
    finish(steps_b)
    total = sum_of(bmsg, bbuf)

    values = [to_column(total[2 + c : 3 + c, :], 16) for c in range(2)]
    f2r, f2i = values[0][NB:16], values[1][NB:16]
    row = lax.broadcasted_iota(jnp.int32, (16, 128), 0)
    zr, zi = (jnp.where(row < NB, value, 0.0) for value in values)
    w = lax.rsqrt(jnp.maximum(column_sum(zr * zr + zi * zi), 1.0))
    zr, zi = zr * w, zi * w
    zref[0, 0] = zr
    zref[0, 1] = zi
    cref[0, 0] = cref[0, 0] + START * zr
    cref[0, 1] = cref[0, 1] - START * zi
    add_date(kref, kimf, zref, 0, [(zr[0:8], zi[0:8]), (zr[8:16], zi[8:16])])
    state_ref, norm_ref = solve(kref, kimf, cref, sref, 1)
    sr = jnp.concatenate(state_ref[0:2], axis=0)
    si = jnp.concatenate(state_ref[2:4], axis=0)
    norm = norm_ref[0]
    f3r = column_sum(zr * sr - zi * si)
    f3i = column_sum(zr * si + zi * sr)
    f3r, f3i = unit((f3r + SCALE * START) * norm, f3i * norm)
    fr = jnp.where(sec < 2, f3r * f2r - f3i * f2i, f3r)
    fi = jnp.where(sec < 2, f3r * f2i + f3i * f2r, f3i)
    vr, vi = total[0:1, :], total[1:2, :]
    rmsg[0:1, :] = vr * fr - vi * fi
    rmsg[1:2, :] = vr * fi + vi * fr

    @pl.when(sec == SECTIONS - 1)
    def _():
        z = eall[16:32, :]
        a = bcast(column_sum(z * sr))
        b = bcast(column_sum(z * si))
        re = a - pltpu.roll(b, 64, 1)
        im = b + pltpu.roll(a, 64, 1)
        rmsg[0:1, :] = (re[0:1] + SCALE * START) * norm
        rmsg[1:2, :] = im[0:1] * norm

    ur, ui = unit(rmsg[0:1, :], rmsg[1:2, :])
    ur, ui = GAIN * to_column(ur, PAD), GAIN * to_column(ui, PAD)

    datum[0:1, :] = jnp.ones((1, TILES * 128), F32)
    datum[1:2, :] = jnp.zeros((1, TILES * 128), F32)

    @pl.when(sec < SECTIONS - 1)
    def _():
        take_f(3)
        datum[...] = fbuf[2]

    @pl.when(sec < 2)
    def _():
        take_f(2)
        dr, di = datum[0:1, :], datum[1:2, :]
        fr, fi = fbuf[1, 0:1, :], fbuf[1, 1:2, :]
        datum[0:1, :] = dr * fr - di * fi
        datum[1:2, :] = dr * fi + di * fr

    for t in range(TILES):
        dr, di = datum[0:1, t * 128 : (t + 1) * 128], datum[1:2, t * 128 : (t + 1) * 128]
        re, im = series[t, 0], series[t, 1]
        re, im = re * dr - im * di, re * di + im * dr
        for c, part in enumerate((re * ur + im * ui, im * ur - re * ui)):
            for g in range(GROUPS):
                count = min(8, ROWS - g * 8)
                phases[pl.ds(g * 32 + t * 2 + c, count, stride=4), :] = part[g * 8 : g * 8 + count]

    @pl.when(sec == 2)
    def _():
        for _, _, copy in steps_g:
            copy.wait_send()

    @pl.when(sec == SECTIONS - 1)
    def _():
        for j in range(SECTIONS - 1):
            remote(eall.at[pl.ds(0, 16)], eall.at[pl.ds(0, 16)], y_send.at[j], y_recv, (j, pix)).wait_send()

    @pl.when(sec < SECTIONS - 1)
    def _():
        for i in range(3):
            pl.when(present[i])(remote(msg, vbuf.at[2 - i], v_send.at[i], v_recv.at[2 - i], (sec_up, near[i])).wait_send)

    for s in range(1, SECTIONS):

        @pl.when(sec == s)
        def _():
            for j in range(s):
                remote(fmsg, fbuf.at[s - 1], f_send.at[j], f_recv.at[s - 1], (j, pix)).wait_send()


def on_device(slc, neighbours, reference_pixel):
    vmem = pl.BlockSpec(memory_space=pltpu.VMEM)
    hbm = pl.BlockSpec(memory_space=pltpu.HBM)
    pixels = slc.shape[2]
    dma = pltpu.SemaphoreType.DMA
    flat = slc.reshape(2, ROWS, TILES, 128).transpose(1, 2, 0, 3).reshape(FLAT, 128)
    phases, comp = pl.pallas_call(
        kernel,
        out_shape=(
            jax.ShapeDtypeStruct((FLAT, 128), F32),
            jax.ShapeDtypeStruct((2, 1, pixels), F32),
        ),
        in_specs=[hbm, hbm, pl.BlockSpec(memory_space=pltpu.SMEM)],
        out_specs=(vmem, vmem),
        scratch_shapes=[
            pltpu.VMEM((NB, pixels), jnp.int32),
            pltpu.VMEM((3, 32 * GROUPS, 128), F32),
            pltpu.VMEM((6, 2, PAD, 128), F32),
            pltpu.VMEM((TILES, 16, 128), jnp.int32),
            pltpu.VMEM((TILES, 16, 128), jnp.int32),
            pltpu.VMEM((TILES, NB, 3, PAD, 128), F32),
            pltpu.VMEM((TILES, PAD, 128), F32),
            pltpu.VMEM((8, 64, 128), F32),
            pltpu.VMEM((TILES, 16, 16, 128), F32),
            pltpu.VMEM((TILES, 16, 16, 128), F32),
            pltpu.VMEM((TILES, 2, 16, 128), F32),
            pltpu.VMEM((TILES, 2, 16, 128), F32),
            pltpu.VMEM((TILES, 2, 128), F32),
            pltpu.VMEM((TILES, 2, 16, 128), F32),
            pltpu.VMEM((TILES, 2, 16, 128), F32),
            pltpu.VMEM((3, 2, pixels), F32),
            pltpu.VMEM((2, pixels), F32),
            pltpu.VMEM((2, pixels), F32),
            pltpu.VMEM((3, 2, pixels), F32),
            pltpu.VMEM((TILES, 2, PAD, 128), F32),
            pltpu.VMEM((2, pixels), F32),
            pltpu.VMEM((1, 128), F32),
            pltpu.VMEM((7, 1, 128), F32),
            pltpu.VMEM((1, 128), F32),
            pltpu.VMEM((7, 1, 128), F32),
            pltpu.VMEM((16, 128), F32),
            pltpu.VMEM((32, 128), F32),
            pltpu.VMEM((7, 32, 128), F32),
            pltpu.VMEM((32, 128), F32),
            pltpu.VMEM((7, 32, 128), F32),
            pltpu.VMEM((32, 128), F32),
            pltpu.VMEM((2, 128), F32),
            pltpu.VMEM((8, 2, 128), F32),
            pltpu.VMEM((2, 128), F32),
            pltpu.VMEM((7, 2, 128), F32),
            pltpu.VMEM((4, 128), F32),
            pltpu.VMEM((7, 4, 128), F32),
            pltpu.VMEM((1, 16, 16, 128), F32),
            pltpu.VMEM((1, 16, 16, 128), F32),
            pltpu.VMEM((1, 2, 16, 128), F32),
            pltpu.VMEM((1, 2, 16, 128), F32),
            pltpu.VMEM((1, 2, 16, 128), F32),
            dma((2,)),
            dma((2,)),
            dma((2,)),
            dma((3,)),
            dma((3,)),
            dma((3,)),
            dma((3,)),
            dma((14,)),
            dma((14,)),
            dma((14,)),
            dma((14,)),
            dma((3,)),
            dma(()),
            dma((32,)),
            dma((8,)),
            dma((7,)),
            dma((7,)),
            dma((7,)),
            dma((7,)),
            pltpu.SemaphoreType.REGULAR((4,)),
        ],
        compiler_params=pltpu.CompilerParams(
            collective_id=0, has_side_effects=True, vmem_limit_bytes=16 * 2**20
        ),
        cost_estimate=pl.CostEstimate(flops=100_000_000, bytes_accessed=1_000_000, transcendentals=0),
    )(*(pltpu.with_memory_space_constraint(a, pltpu.HBM) for a in (flat, neighbours)), reference_pixel)
    return phases.reshape(ROWS, TILES, 2, 128).transpose(2, 0, 1, 3).reshape(2, ROWS, pixels), comp


def solution(mesh):
    return jax.shard_map(
        on_device,
        mesh=mesh,
        in_specs=(P(None, "section", "pix"), P(None, "pix"), P()),
        out_specs=(P(None, "section", "pix"), P(None, "section", "pix")),
        check_vma=False,
    )
```

```python
import math

import jax
import jax.numpy as jnp
from jax import lax
from jax.experimental import pallas as pl
from jax.experimental.pallas import tpu as pltpu
from jax.sharding import PartitionSpec as P

ITERS = 16
FLOOR = 0.05
REACH = 256
NB = 15
ROWS = 50
PAD = 56
GROUPS = PAD // 8
FLAT = 4 * ROWS
TILES = 2
SPAN = 5
SCALE = 2.0**-45
START = 1.0 / math.sqrt(ROWS + 1)
GAIN = math.sqrt(ROWS + 1)
SECTIONS = 4
PIX = 64
MESH = pl.DeviceIdType.MESH
F32 = jnp.float32


def bcast(row):
    return jnp.broadcast_to(row, (8, 128))


def pick(sources, lane, tile):
    out = jnp.zeros((8, 128), F32)
    for m, source in enumerate(sources):
        out = jnp.where(tile == m, take(source, lane), out)
    return out


def take(source, lane):
    return jnp.take_along_axis(source, lane, axis=1, mode="promise_in_bounds")


def column_sum(x):
    return jnp.sum(x, axis=0, keepdims=True)


def eye(count, shift=0):
    lane = lax.broadcasted_iota(jnp.int32, (count, 128), 1)
    return lane == lax.broadcasted_iota(jnp.int32, (count, 128), 0) + shift


def to_row(column, shift=0):
    return column_sum(jnp.where(eye(column.shape[0], shift), column, 0.0))


def to_column(row, count):
    spread = jnp.broadcast_to(row, (count, 128))
    return jnp.sum(jnp.where(eye(count), spread, 0.0), axis=1, keepdims=True)


def unit(re, im):
    scale = 1.0 / jnp.maximum(jnp.sqrt(re * re + im * im), FLOOR)
    return re * scale, im * scale


def remote(src, dst, send, recv, device):
    return pltpu.make_async_remote_copy(
        src_ref=src, dst_ref=dst, send_sem=send, recv_sem=recv, device_id=device, device_id_type=MESH
    )


def kernel(
    slc_hbm, nbr_hbm, ref, phases, comp,
    nbr, blocks, ext, lanes, tiles, zs, wbuf, red, kre, kim, cvec, bvec, xsum, zbuf, sbuf,
    vbuf, msg, fmsg, fbuf, series, datum,
    nmsg, nbuf1, nmsg2, nbuf2, ncol, emsg, ebuf1, emsg2, ebuf2, eall, gmsg, gbuf, rmsg, rbuf1, bmsg, bbuf,
    kref, kimf, cref, zref, sref,
    load_sem, halo_send, halo_recv, v_send, v_recv, f_send, f_recv, early_sem,
    y_send, y_recv, g_send, g_recv, r_sem, b_sem, ready,
):
    sec = lax.axis_index("section")
    pix = lax.axis_index("pix")
    before = lax.rem(pix + (PIX - 1), PIX)
    after = lax.rem(pix + 1, PIX)
    near = (before, pix, after)
    present = (pix > 0, pix >= 0, pix < PIX - 1)
    inner = jnp.logical_and(present[0], present[2])
    sec_up = lax.rem(sec + 1, SECTIONS)
    sec_down = lax.rem(sec + (SECTIONS - 1), SECTIONS)
    x = pix // 16
    z = lax.rem(pix // 2, 8)
    core = lax.rem(pix, 2)
    group = x * 2 + core
    first = []
    second = []
    for d in range(1, 8):
        g = lax.rem(group + d, 8)
        first.append((g // 2) * 16 + z * 2 + lax.rem(g, 2))
        second.append(x * 16 + lax.rem(z + d, 8) * 2 + core)

    want = ref[0] - pix * (TILES * 128)

    def at_ref(parts):
        total = None
        for t, part in enumerate(parts):
            lane = lax.broadcasted_iota(jnp.int32, part.shape, 1)
            part = jnp.where(lane == want - t * 128, part, 0.0)
            total = part if total is None else total + part
        return jnp.sum(total, axis=1, keepdims=True)

    def arrived(ref, sem):
        pltpu.make_async_copy(ref, ref, sem).wait()

    def start(src, dst, sem, devices):
        for i, device in enumerate(devices):
            remote(src, dst.at[i], sem.at[0], sem.at[1], (sec, device)).start()

    def finish(src, dst, sem, devices):
        arrived(dst, sem.at[0])
        arrived(dst, sem.at[1])

    def sum_of(own, buffers):
        total = own[...]
        for i in range(7):
            total = total + buffers[i]
        return total

    steps_n = (nmsg, nbuf1, early_sem.at[0], first), (nmsg2, nbuf2, early_sem.at[1], second)
    steps_e = (emsg, ebuf1, early_sem.at[0], first), (emsg2, ebuf2, early_sem.at[1], second)
    steps_r = (rmsg, rbuf1, r_sem, first)
    steps_b = (bmsg, bbuf, b_sem, second)

    chunks = [(0, 3), (3, GROUPS)]
    spans = [pl.ds(32 * low, min(32 * high, FLAT) - 32 * low) for low, high in chunks]
    loads = [
        pltpu.make_async_copy(slc_hbm.at[span], blocks.at[1, span], load_sem.at[i]) for i, span in enumerate(spans)
    ]
    loads.append(pltpu.make_async_copy(nbr_hbm, nbr, load_sem.at[2]))
    for load in loads:
        load.start()
    barrier = pltpu.get_barrier_semaphore()
    peers = [(sec, before), (sec, after), (sec_up, pix), (sec_down, pix)]
    peers += [(sec, x * 16 + lax.rem(z + d, 8) * 2 + core) for d in (1, 7)]
    peers += [(sec, lax.rem(x + d, 4) * 16 + z * 2 + core) for d in (1, 3)]

    def tell(sem):
        for peer in peers:
            pl.semaphore_signal(sem, inc=1, device_id=peer, device_id_type=MESH)

    def hear(sem):
        pl.semaphore_wait(sem, len(peers))

    tell(barrier)
    hear(barrier)
    tell(ready.at[0])

    def halo(i, n):
        part = blocks.at[1, spans[n]]
        return remote(part, blocks.at[2 - i, spans[n]], halo_send.at[i // 2], halo_recv.at[i // 2, n], (sec, near[i]))

    for n in range(len(chunks)):
        loads[n].wait()
        for i in (0, 2):
            pl.when(present[i])(halo(i, n).start)

    for i in range(3):
        blocks[i, FLAT:, :] = jnp.zeros((32 * GROUPS - FLAT, 128), F32)
    kre[...] = jnp.zeros_like(kre)
    kim[...] = jnp.zeros_like(kim)
    red[...] = jnp.zeros_like(red)
    cvec[...] = jnp.zeros_like(cvec)
    bvec[...] = jnp.zeros_like(bvec)
    for i in (0, 2):

        @pl.when(jnp.logical_not(present[i]))
        def _():
            blocks[i] = jnp.zeros((32 * GROUPS, 128), F32)
            vbuf[i] = jnp.zeros_like(vbuf[i])

    loads[2].wait()

    base = pix * (TILES * 128) - REACH
    for t in range(TILES):
        rel = nbr[:, t * 128 : (t + 1) * 128] - (base + t * 128)
        lanes[t, 0:NB, :] = jnp.bitwise_and(rel, 127)
        tiles[t, 0:NB, :] = jnp.right_shift(rel, 7)
        lanes[t, NB : NB + 1, :] = jnp.zeros((1, 128), jnp.int32)
        tiles[t, NB : NB + 1, :] = jnp.full((1, 128), SPAN, jnp.int32)

    def spread(i, groups=range(GROUPS)):
        for g in groups:
            for m in range(2):
                for c in range(2):
                    ext[2 * i + m, c, g * 8 : (g + 1) * 8, :] = blocks[i, pl.ds(g * 32 + m * 2 + c, 8, stride=4), :]

    spread(1)
    for t in range(TILES):
        for c in range(2):
            total = None
            for g in range(GROUPS):
                own = ext[2 + t, c, g * 8 : (g + 1) * 8, :]
                zs[t, 0, c, g * 8 : (g + 1) * 8, :] = own
                total = own if total is None else total + own
            xsum[t, c : c + 1, :] = column_sum(total)
        zs[t, 0, 2] = zs[t, 0, 0] - zs[t, 0, 1]

    def gather(t, mine, theirs, begin, groups=range(GROUPS)):
        @pl.loop(0, 2)
        def _(half):
            for i in range(NB // 2):
                k = 1 + half * (NB // 2) + i
                lane = bcast(lanes[t, pl.ds(k, 1), :])
                tile = bcast(tiles[t, pl.ds(k, 1), :])
                here = [tile == m for m in theirs]
                for g in groups:
                    rows = slice(g * 8, (g + 1) * 8)
                    pair = []
                    for c in range(2):
                        out = take(ext[t + mine, c, rows, :], lane) if begin else zs[t, k, c, rows, :]
                        for there, m in zip(here, theirs):
                            out = jnp.where(there, take(ext[t + m, c, rows, :], lane), out)
                        zs[t, k, c, rows, :] = out
                        pair.append(out)
                    if not begin:
                        zs[t, k, 2, rows, :] = pair[0] - pair[1]

    for t in range(TILES):
        gather(t, 2 - t, (3 - t,), True)
    hear(ready.at[0])
    tell(ready.at[1])

    for n, (low, high) in enumerate(chunks):
        for i in (0, 2):
            pl.when(present[2 - i])(halo(i, n).wait_recv)
        for i in (0, 2):
            spread(i, range(low, high))
        for t in range(TILES):
            gather(t, None, tuple(m for m in range(SPAN) if t + m not in (2, 3)), False, range(low, high))
    hear(ready.at[1])
    tell(ready.at[2])

    @pl.when(sec == 2)
    def _():
        column = at_ref([nbr[:, t * 128 : (t + 1) * 128].astype(F32) for t in range(TILES)])
        nmsg[...] = to_row(column)
        start(*steps_n[0])

    @pl.loop(0, TILES)
    def _(t):
        for g in range(GROUPS):
            rows = slice(g * 8, (g + 1) * 8)
            power = None
            for k in range(NB):
                re, im = zs[t, k, 0, rows, :], zs[t, k, 1, rows, :]
                term = re * re + im * im
                power = term if power is None else power + term
            wbuf[t, rows, :] = lax.rsqrt(jnp.maximum(power, 1.0))

        def fold(slot, parts):
            for i, part in enumerate(parts):
                red[slot, i * 8 : (i + 1) * 8, :] = part
            total = None
            for i in range(8):
                row = red[slot, pl.ds(i, 8, stride=8), :]
                total = row if total is None else total + row
            return total

        slot = 0
        for l in range(NB + 1):
            for kg in range(2):
                low, high = 8 * kg, min(8 * kg + 8, l + 1, NB)
                if high <= low:
                    continue
                count = high - low
                p, q, r = [None] * count, [None] * count, [None] * count
                cr, ci = [None] * count, [None] * count

                def put(box, i, value):
                    box[i] = value if box[i] is None else box[i] + value

                for g in range(GROUPS):
                    rows = slice(g * 8, (g + 1) * 8)
                    w = wbuf[t, rows, :]
                    if l < NB:
                        w2 = w * w
                        lr, li = zs[t, l, 0, rows, :] * w2, zs[t, l, 1, rows, :] * w2
                    else:
                        lr, li = zs[t, 0, 0, rows, :] * w, zs[t, 0, 1, rows, :] * w
                    le = lr + li
                    for i in range(count):
                        k = low + i
                        kr, ki = zs[t, k, 0, rows, :], zs[t, k, 1, rows, :]
                        put(p, i, kr * lr)
                        put(q, i, ki * li)
                        if k != l:
                            put(r, i, zs[t, k, 2, rows, :] * le)
                        if l == NB:
                            put(cr, i, kr * w)
                            put(ci, i, ki * w)
                re = fold(4 * kg + slot, [a + b for a, b in zip(p, q)])
                im = fold(4 * kg + slot + 1, [jnp.zeros((8, 128), F32) if c is None else c + (b - a) for a, b, c in zip(p, q, r)])
                rows = slice(low, low + 8)
                if l < NB:
                    kre[t, l, rows, :] = re
                    kim[t, l, rows, :] = im
                    for i in range(count):
                        k = low + i
                        if k != l:
                            kre[t, k, l : l + 1, :] = re[i : i + 1, :]
                            kim[t, k, l : l + 1, :] = -im[i : i + 1, :]
                else:
                    bvec[t, 0, rows, :] = re
                    bvec[t, 1, rows, :] = im
                    slot = 2 - slot
                    cvec[t, 0, rows, :] = START * fold(4 * kg + slot, cr)
                    cvec[t, 1, rows, :] = -START * fold(4 * kg + slot + 1, ci)
                slot = 2 - slot

    @pl.when(sec >= 2)
    def _():
        hear(ready.at[2])
        tell(ready.at[3])

    @pl.when(sec == 2)
    def _():
        finish(*steps_n[0])
        nmsg2[...] = sum_of(nmsg, nbuf1)
        start(*steps_n[1])

    def expand():
        for l in range(NB):
            kref[0, l] = jnp.broadcast_to(eall[0:16, l : l + 1], (16, 128))
            kimf[0, l] = jnp.broadcast_to(eall[0:16, 16 + l : 17 + l], (16, 128))
        for c in range(2):
            cref[0, c] = jnp.broadcast_to(eall[0:16, 32 + c : 33 + c], (16, 128))

    @pl.when(sec == SECTIONS - 1)
    def _():
        lane = lax.broadcasted_iota(jnp.int32, (16, 128), 1)
        emsg[16:32, :] = jnp.zeros((16, 128), F32)
        acc = jnp.zeros((16, 128), F32)
        for c in range(2):
            acc = jnp.where(lane == 32 + c, at_ref([cvec[t, c] for t in range(TILES)]), acc)
        emsg[0:16, :] = acc

        @pl.loop(0, NB)
        def _(k):
            acc = emsg[0:16, :]
            acc = jnp.where(lane == k, at_ref([kre[t, k] for t in range(TILES)]), acc)
            emsg[0:16, :] = jnp.where(lane == 16 + k, at_ref([kim[t, k] for t in range(TILES)]), acc)
            parts = [at_ref([zs[t, k, c] * wbuf[t] for t in range(TILES)]) for c in range(2)]
            emsg[pl.ds(16 + k, 1), :] = to_row(parts[0]) + to_row(parts[1], 64)

        start(*steps_e[0])
        finish(*steps_e[0])
        emsg2[...] = sum_of(emsg, ebuf1)
        start(*steps_e[1])
        finish(*steps_e[1])
        eall[...] = sum_of(emsg2, ebuf2)
        for j in range(SECTIONS - 1):
            remote(eall.at[pl.ds(0, 16)], eall.at[pl.ds(0, 16)], y_send, y_recv, (j, pix)).start()
        expand()

    @pl.when(sec == 2)
    def _():
        finish(*steps_n[1])
        column = to_column(sum_of(nmsg2, nbuf2), 16)
        row = lax.broadcasted_iota(jnp.int32, (16, 128), 0)
        ncol[...] = jnp.where(row == NB, ref[0].astype(F32), column) - (pix * (TILES * 128)).astype(F32)

    def add_date(kr, ki, zb, t, z0):
        for l in range(NB):
            lr = bcast(zb[t, 0, l : l + 1, :])
            li = bcast(zb[t, 1, l : l + 1, :])
            for kg in range(2):
                rows = slice(8 * kg, 8 * kg + 8)
                zr, zi = z0[kg]
                kr[t, l, rows, :] = kr[t, l, rows, :] + (zr * lr + zi * li)
                ki[t, l, rows, :] = ki[t, l, rows, :] + (zr * li - zi * lr)

    @pl.when(sec == 0)
    def _():
        zbuf[...] = jnp.zeros_like(zbuf)

    @pl.when(sec > 0)
    def _():
        pl.when(inner)(lambda: arrived(vbuf, v_recv))
        pl.when(jnp.logical_not(inner))(lambda: arrived(vbuf.at[0:2], v_recv))
        for t in range(TILES):
            z0 = []
            for kg in range(2):
                rows = slice(8 * kg, 8 * kg + 8)
                lane = lanes[t, rows, :]
                tile = tiles[t, rows, :]
                pair = []
                for c in range(2):
                    src = []
                    for m in range(SPAN):
                        at = t + m
                        src.append(bcast(vbuf[at // 2, c : c + 1, (at % 2) * 128 : (at % 2) * 128 + 128]))
                    pair.append(pick(src, lane, tile))
                z0.append(pair)
            power = column_sum(z0[0][0] * z0[0][0] + z0[0][1] * z0[0][1] + (z0[1][0] * z0[1][0] + z0[1][1] * z0[1][1]))
            w = lax.rsqrt(jnp.maximum(power, 1.0))
            vr = vbuf[1, 0:1, t * 128 : (t + 1) * 128]
            vi = vbuf[1, 1:2, t * 128 : (t + 1) * 128]
            xsum[t, 0:1, :] = xsum[t, 0:1, :] + vr
            xsum[t, 1:2, :] = xsum[t, 1:2, :] + vi
            for kg in range(2):
                rows = slice(8 * kg, 8 * kg + 8)
                zr, zi = z0[kg][0] * w, z0[kg][1] * w
                z0[kg] = (zr, zi)
                zbuf[t, 0, rows, :] = zr
                zbuf[t, 1, rows, :] = zi
                cvec[t, 0, rows, :] = cvec[t, 0, rows, :] + START * zr
                cvec[t, 1, rows, :] = cvec[t, 1, rows, :] - START * zi
                bvec[t, 0, rows, :] = bvec[t, 0, rows, :] + (zr * vr + zi * vi)
                bvec[t, 1, rows, :] = bvec[t, 1, rows, :] + (zr * vi - zi * vr)
            add_date(kre, kim, zbuf, t, z0)

    def solve(kr, ki, cv, sb, count):
        places = [(t, c, kg) for t in range(count) for c in range(2) for kg in range(2)]

        def product(state):
            for i, (t, c, kg) in enumerate(places):
                sb[t, c, 8 * kg : 8 * kg + 8, :] = state[i]
            out = []
            for t in range(count):
                y = [[None, None], [None, None]]
                for l in range(NB):
                    lr = bcast(sb[t, 0, l : l + 1, :])
                    li = bcast(sb[t, 1, l : l + 1, :])
                    for kg in range(2):
                        rows = slice(8 * kg, 8 * kg + 8)
                        ar, ai = kr[t, l, rows, :], ki[t, l, rows, :]
                        re = ar * lr - ai * li
                        im = ar * li + ai * lr
                        y[0][kg] = re if l == 0 else y[0][kg] + re
                        y[1][kg] = im if l == 0 else y[1][kg] + im
                out += [y[0][0], y[0][1], y[1][0], y[1][1]]
            return out

        def c0(i):
            t, c, kg = places[i]
            return cv[t, c, 8 * kg : 8 * kg + 8, :]

        def turn(_, state):
            return tuple(a + y + c0(i) for i, (a, y) in enumerate(zip(state, product(state))))

        state = lax.fori_loop(0, ITERS - 1, turn, tuple(c0(i) for i in range(len(places))))
        state = [a * SCALE for a in state]
        ks = product(state)
        norms = []
        for t in range(count):
            total = None
            for i in range(4 * t, 4 * t + 4):
                term = state[i] * (ks[i] + (2.0 * SCALE) * c0(i))
                total = term if total is None else total + term
            norms.append(lax.rsqrt(column_sum(total) + SCALE * SCALE))
        return state, norms

    state, norms = solve(kre, kim, cvec, sbuf, TILES)
    for t in range(TILES):
        s = state[4 * t : 4 * t + 4]
        norm = norms[t]
        cr = ci = fr = fi = None
        for kg in range(2):
            rows = slice(8 * kg, 8 * kg + 8)
            sr, si = s[kg], s[2 + kg]
            br, bi = bvec[t, 0, rows, :], bvec[t, 1, rows, :]
            zr, zi = zbuf[t, 0, rows, :], zbuf[t, 1, rows, :]
            a, b = sr * br + si * bi, sr * bi - si * br
            e, f = zr * sr - zi * si, zr * si + zi * sr
            cr = a if kg == 0 else column_sum(cr + a)
            ci = b if kg == 0 else column_sum(ci + b)
            fr = e if kg == 0 else column_sum(fr + e)
            fi = f if kg == 0 else column_sum(fi + f)
        cols = slice(t * 128, (t + 1) * 128)
        msg[0:1, cols] = (cr + (SCALE * START) * xsum[t, 0:1, :]) * norm
        msg[1:2, cols] = (ci + (SCALE * START) * xsum[t, 1:2, :]) * norm
        fr, fi = unit((fr + SCALE * START) * norm, fi * norm)
        fmsg[0:1, cols] = fr
        fmsg[1:2, cols] = fi

    @pl.when(sec < SECTIONS - 1)
    def _():
        for i in range(3):
            pl.when(present[i])(remote(msg, vbuf.at[2 - i], v_send, v_recv, (sec_up, near[i])).start)

    for s in range(1, SECTIONS):

        @pl.when(sec == s)
        def _():
            for j in range(s):
                remote(fmsg, fbuf.at[s - 1], f_send, f_recv.at[s - 1], (j, pix)).start()

    steps_g = [
        remote(gmsg, gbuf.at[d], g_send, g_recv, (s, pix if d == 0 else first[d - 1]))
        for s in range(SECTIONS)
        for d in range(8)
        if (s, d) != (2, 0)
    ]

    @pl.when(sec < 2)
    def _():
        hear(ready.at[2])
        tell(ready.at[3])

    hear(ready.at[3])

    @pl.when(sec == 2)
    def _():
        lane = lax.broadcasted_iota(jnp.int32, (16, 128), 1).astype(F32)
        row = lax.broadcasted_iota(jnp.int32, (16, 128), 0)
        for c in range(2):
            total = None
            for t in range(TILES):
                cols = slice(t * 128, (t + 1) * 128)
                value = jnp.where(
                    row == NB,
                    jnp.broadcast_to(fmsg[c : c + 1, cols], (16, 128)),
                    jnp.broadcast_to(msg[c : c + 1, cols], (16, 128)),
                )
                value = jnp.where(ncol[...] - t * 128.0 == lane, value, 0.0)
                total = value if total is None else total + value
            gmsg[c : c + 1, :] = to_row(jnp.sum(total, axis=1, keepdims=True))
        for copy in steps_g:
            copy.start()
        gbuf[0] = gmsg[...]

    comp[0, 0:1, :] = msg[0:1, :]
    comp[1, 0:1, :] = msg[1:2, :]

    for i, (t, c, kg) in enumerate((t, c, kg) for t in range(TILES) for c in range(2) for kg in range(2)):
        sbuf[t, c, 8 * kg : 8 * kg + 8, :] = state[i] * norms[t]
    for t in range(TILES):

        @pl.loop(0, GROUPS)
        def _(g):
            rows = pl.ds(pl.multiple_of(g * 8, 8), 8)
            re = im = None
            for k in range(NB):
                sr = bcast(sbuf[t, 0, k : k + 1, :])
                si = bcast(sbuf[t, 1, k : k + 1, :])
                zr, zi = zs[t, k, 0, rows, :], zs[t, k, 1, rows, :]
                a, b = zr * sr - zi * si, zr * si + zi * sr
                re = a if re is None else re + a
                im = b if im is None else im + b
            w = wbuf[t, rows, :]
            series[t, 0, rows, :] = bcast((SCALE * START) * norms[t]) + w * re
            series[t, 1, rows, :] = w * im

    def take_f(j):
        arrived(fbuf.at[j - 1], f_recv.at[j - 1])

    @pl.when(sec == 0)
    def _():
        take_f(1)
        for t in range(TILES):
            fr = fbuf[0, 0:1, t * 128 : (t + 1) * 128]
            fi = fbuf[0, 1:2, t * 128 : (t + 1) * 128]
            re, im = series[t, 0], series[t, 1]
            series[t, 0] = re * fr - im * fi
            series[t, 1] = re * fi + im * fr

    @pl.when(sec < SECTIONS - 1)
    def _():
        for c in range(2):
            rmsg[c : c + 1, :] = to_row(at_ref([series[t, c] for t in range(TILES)]))
        start(*steps_r)
        remote(eall.at[pl.ds(0, 16)], eall.at[pl.ds(0, 16)], y_send, y_recv, (SECTIONS - 1, pix)).wait_recv()
        expand()

    @pl.when(sec == 2)
    def _():
        arrived(gbuf.at[1:8], g_recv)

    @pl.when(sec != 2)
    def _():
        arrived(gbuf.at[0:8], g_recv)

    total = gbuf[0]
    for d in range(1, 8):
        total = total + gbuf[d]
    bmsg[2:4, :] = total

    @pl.when(sec < SECTIONS - 1)
    def _():
        finish(*steps_r)
        bmsg[0:2, :] = sum_of(rmsg, rbuf1)

    @pl.when(sec == SECTIONS - 1)
    def _():
        bmsg[0:2, :] = jnp.zeros((2, 128), F32)

    start(*steps_b)
    finish(*steps_b)
    total = sum_of(bmsg, bbuf)

    values = [to_column(total[2 + c : 3 + c, :], 16) for c in range(2)]
    f2r, f2i = values[0][NB:16], values[1][NB:16]
    row = lax.broadcasted_iota(jnp.int32, (16, 128), 0)
    zr, zi = (jnp.where(row < NB, value, 0.0) for value in values)
    w = lax.rsqrt(jnp.maximum(column_sum(zr * zr + zi * zi), 1.0))
    zr, zi = zr * w, zi * w
    zref[0, 0] = zr
    zref[0, 1] = zi
    cref[0, 0] = cref[0, 0] + START * zr
    cref[0, 1] = cref[0, 1] - START * zi
    add_date(kref, kimf, zref, 0, [(zr[0:8], zi[0:8]), (zr[8:16], zi[8:16])])
    state_ref, norm_ref = solve(kref, kimf, cref, sref, 1)
    sr = jnp.concatenate(state_ref[0:2], axis=0)
    si = jnp.concatenate(state_ref[2:4], axis=0)
    norm = norm_ref[0]
    f3r = column_sum(zr * sr - zi * si)
    f3i = column_sum(zr * si + zi * sr)
    f3r, f3i = unit((f3r + SCALE * START) * norm, f3i * norm)
    fr = jnp.where(sec < 2, f3r * f2r - f3i * f2i, f3r)
    fi = jnp.where(sec < 2, f3r * f2i + f3i * f2r, f3i)
    vr, vi = total[0:1, :], total[1:2, :]
    rmsg[0:1, :] = vr * fr - vi * fi
    rmsg[1:2, :] = vr * fi + vi * fr

    @pl.when(sec == SECTIONS - 1)
    def _():
        z = eall[16:32, :]
        a = bcast(column_sum(z * sr))
        b = bcast(column_sum(z * si))
        re = a - pltpu.roll(b, 64, 1)
        im = b + pltpu.roll(a, 64, 1)
        rmsg[0:1, :] = (re[0:1] + SCALE * START) * norm
        rmsg[1:2, :] = im[0:1] * norm

    ur, ui = unit(rmsg[0:1, :], rmsg[1:2, :])
    ur, ui = GAIN * to_column(ur, PAD), GAIN * to_column(ui, PAD)

    datum[0:1, :] = jnp.ones((1, TILES * 128), F32)
    datum[1:2, :] = jnp.zeros((1, TILES * 128), F32)

    @pl.when(sec < SECTIONS - 1)
    def _():
        take_f(3)
        datum[...] = fbuf[2]

    @pl.when(sec < 2)
    def _():
        take_f(2)
        dr, di = datum[0:1, :], datum[1:2, :]
        fr, fi = fbuf[1, 0:1, :], fbuf[1, 1:2, :]
        datum[0:1, :] = dr * fr - di * fi
        datum[1:2, :] = dr * fi + di * fr

    for t in range(TILES):
        dr, di = datum[0:1, t * 128 : (t + 1) * 128], datum[1:2, t * 128 : (t + 1) * 128]
        re, im = series[t, 0], series[t, 1]
        re, im = re * dr - im * di, re * di + im * dr
        for c, part in enumerate((re * ur + im * ui, im * ur - re * ui)):
            for g in range(GROUPS):
                count = min(8, ROWS - g * 8)
                phases[pl.ds(g * 32 + t * 2 + c, count, stride=4), :] = part[g * 8 : g * 8 + count]

    for i in (0, 2):
        pl.when(present[i])(lambda i=i: arrived(blocks.at[1, pl.ds(0, FLAT)], halo_send.at[i // 2]))
    @pl.when(sec == 2)
    def _():
        arrived(gbuf, g_send)

    @pl.when(sec == SECTIONS - 1)
    def _():
        arrived(ebuf1.at[0:3, 0:16], y_send)

    @pl.when(sec < SECTIONS - 1)
    def _():
        pl.when(inner)(lambda: arrived(vbuf, v_send))
        pl.when(jnp.logical_not(inner))(lambda: arrived(vbuf.at[0:2], v_send))

    for s in range(1, SECTIONS):

        @pl.when(sec == s)
        def _():
            arrived(fbuf.at[0:s], f_send)


def hand_out(phases_in, comp_in, phases, comp, sem):
    copies = [
        pltpu.make_async_copy(phases_in, phases, sem.at[0]),
        pltpu.make_async_copy(comp_in, comp, sem.at[1]),
    ]
    for copy in copies:
        copy.start()
    for copy in copies:
        copy.wait()


def on_device(slc, neighbours, reference_pixel):
    vmem = pl.BlockSpec(memory_space=pltpu.VMEM)
    hbm = pl.BlockSpec(memory_space=pltpu.HBM)
    pixels = slc.shape[2]
    dma = pltpu.SemaphoreType.DMA
    flat = slc.reshape(2, ROWS, TILES, 128).transpose(1, 2, 0, 3).reshape(FLAT, 128)
    phases, comp = pl.pallas_call(
        kernel,
        out_shape=(
            jax.ShapeDtypeStruct((FLAT, 128), F32),
            jax.ShapeDtypeStruct((2, 1, pixels), F32),
        ),
        in_specs=[hbm, hbm, pl.BlockSpec(memory_space=pltpu.SMEM)],
        out_specs=(vmem, vmem),
        scratch_shapes=[
            pltpu.VMEM((NB, pixels), jnp.int32),
            pltpu.VMEM((3, 32 * GROUPS, 128), F32),
            pltpu.VMEM((6, 2, PAD, 128), F32),
            pltpu.VMEM((TILES, 16, 128), jnp.int32),
            pltpu.VMEM((TILES, 16, 128), jnp.int32),
            pltpu.VMEM((TILES, NB, 3, PAD, 128), F32),
            pltpu.VMEM((TILES, PAD, 128), F32),
            pltpu.VMEM((8, 64, 128), F32),
            pltpu.VMEM((TILES, 16, 16, 128), F32),
            pltpu.VMEM((TILES, 16, 16, 128), F32),
            pltpu.VMEM((TILES, 2, 16, 128), F32),
            pltpu.VMEM((TILES, 2, 16, 128), F32),
            pltpu.VMEM((TILES, 2, 128), F32),
            pltpu.VMEM((TILES, 2, 16, 128), F32),
            pltpu.VMEM((TILES, 2, 16, 128), F32),
            pltpu.VMEM((3, 2, pixels), F32),
            pltpu.VMEM((2, pixels), F32),
            pltpu.VMEM((2, pixels), F32),
            pltpu.VMEM((3, 2, pixels), F32),
            pltpu.VMEM((TILES, 2, PAD, 128), F32),
            pltpu.VMEM((2, pixels), F32),
            pltpu.VMEM((1, 128), F32),
            pltpu.VMEM((7, 1, 128), F32),
            pltpu.VMEM((1, 128), F32),
            pltpu.VMEM((7, 1, 128), F32),
            pltpu.VMEM((16, 128), F32),
            pltpu.VMEM((32, 128), F32),
            pltpu.VMEM((7, 32, 128), F32),
            pltpu.VMEM((32, 128), F32),
            pltpu.VMEM((7, 32, 128), F32),
            pltpu.VMEM((32, 128), F32),
            pltpu.VMEM((2, 128), F32),
            pltpu.VMEM((31, 2, 128), F32),
            pltpu.VMEM((2, 128), F32),
            pltpu.VMEM((7, 2, 128), F32),
            pltpu.VMEM((4, 128), F32),
            pltpu.VMEM((7, 4, 128), F32),
            pltpu.VMEM((1, 16, 16, 128), F32),
            pltpu.VMEM((1, 16, 16, 128), F32),
            pltpu.VMEM((1, 2, 16, 128), F32),
            pltpu.VMEM((1, 2, 16, 128), F32),
            pltpu.VMEM((1, 2, 16, 128), F32),
            dma((3,)),
            dma((2,)),
            dma((2, 2)),
            dma(()),
            dma(()),
            dma(()),
            dma((3,)),
            dma((2, 2)),
            dma(()),
            dma(()),
            dma(()),
            dma(()),
            dma((2,)),
            dma((2,)),
            pltpu.SemaphoreType.REGULAR((4,)),
        ],
        compiler_params=pltpu.CompilerParams(
            collective_id=0, has_side_effects=True, vmem_limit_bytes=16 * 2**20
        ),
        cost_estimate=pl.CostEstimate(flops=100_000_000, bytes_accessed=1_000_000, transcendentals=0),
    )(*(pltpu.with_memory_space_constraint(a, pltpu.HBM) for a in (flat, neighbours)), reference_pixel)
    phases, comp = pl.pallas_call(
        hand_out,
        out_shape=(
            jax.ShapeDtypeStruct((FLAT, 128), F32),
            jax.ShapeDtypeStruct((2, 1, pixels), F32),
        ),
        in_specs=[pl.BlockSpec(memory_space=pl.ANY)] * 2,
        out_specs=(hbm, hbm),
        scratch_shapes=[dma((2,))],
        compiler_params=pltpu.CompilerParams(vmem_limit_bytes=2**20),
    )(phases, comp)
    return phases.reshape(ROWS, TILES, 2, 128).transpose(2, 0, 1, 3).reshape(2, ROWS, pixels), comp


def solution(mesh):
    return jax.shard_map(
        on_device,
        mesh=mesh,
        in_specs=(P(None, "section", "pix"), P(None, "pix"), P()),
        out_specs=(P(None, "section", "pix"), P(None, "section", "pix")),
        check_vma=False,
    )
```

```python
import math

import jax
import jax.numpy as jnp
from jax import lax
from jax.experimental import pallas as pl
from jax.experimental.pallas import tpu as pltpu
from jax.sharding import PartitionSpec as P

ITERS = 16
FLOOR = 0.05
REACH = 256
NB = 15
ROWS = 50
PAD = 56
GROUPS = PAD // 8
FLAT = 4 * ROWS
TILES = 2
SPAN = 5
SCALE = 2.0**-45
START = 1.0 / math.sqrt(ROWS + 1)
GAIN = math.sqrt(ROWS + 1)
SECTIONS = 4
PIX = 64
MESH = pl.DeviceIdType.MESH
F32 = jnp.float32


def bcast(row):
    return jnp.broadcast_to(row, (8, 128))


def pick(sources, lane, tile):
    out = jnp.zeros((8, 128), F32)
    for m, source in enumerate(sources):
        out = jnp.where(tile == m, take(source, lane), out)
    return out


def take(source, lane):
    return jnp.take_along_axis(source, lane, axis=1, mode="promise_in_bounds")


def column_sum(x):
    return jnp.sum(x, axis=0, keepdims=True)


def eye(count, shift=0):
    lane = lax.broadcasted_iota(jnp.int32, (count, 128), 1)
    return lane == lax.broadcasted_iota(jnp.int32, (count, 128), 0) + shift


def to_row(column, shift=0):
    return column_sum(jnp.where(eye(column.shape[0], shift), column, 0.0))


def to_column(row, count):
    spread = jnp.broadcast_to(row, (count, 128))
    return jnp.sum(jnp.where(eye(count), spread, 0.0), axis=1, keepdims=True)


def unit(re, im):
    scale = 1.0 / jnp.maximum(jnp.sqrt(re * re + im * im), FLOOR)
    return re * scale, im * scale


def remote(src, dst, send, recv, device):
    return pltpu.make_async_remote_copy(
        src_ref=src, dst_ref=dst, send_sem=send, recv_sem=recv, device_id=device, device_id_type=MESH
    )


def kernel(
    slc_hbm, nbr_hbm, ref, phases, comp,
    nbr, blocks, ext, lanes, tiles, zs, wbuf, red, kre, kim, cvec, bvec, xsum, zbuf, sbuf,
    vbuf, msg, fmsg, fbuf, series, datum,
    nmsg, nbuf1, nmsg2, nbuf2, ncol, emsg, ebuf1, emsg2, ebuf2, eall, gmsg, gbuf, rmsg, rbuf1, bmsg, bbuf,
    kref, kimf, cref, zref, sref,
    load_sem, halo_send, halo_recv, v_send, v_recv, f_send, f_recv, early_sem,
    y_send, y_recv, g_send, g_recv, r_sem, b_sem, ready,
):
    sec = lax.axis_index("section")
    pix = lax.axis_index("pix")
    before = lax.rem(pix + (PIX - 1), PIX)
    after = lax.rem(pix + 1, PIX)
    near = (before, pix, after)
    present = (pix > 0, pix >= 0, pix < PIX - 1)
    inner = jnp.logical_and(present[0], present[2])
    sec_up = lax.rem(sec + 1, SECTIONS)
    sec_down = lax.rem(sec + (SECTIONS - 1), SECTIONS)
    x = pix // 16
    z = lax.rem(pix // 2, 8)
    core = lax.rem(pix, 2)
    group = x * 2 + core
    first = []
    second = []
    for d in range(1, 8):
        g = lax.rem(group + d, 8)
        first.append((g // 2) * 16 + z * 2 + lax.rem(g, 2))
        second.append(x * 16 + lax.rem(z + d, 8) * 2 + core)

    want = ref[0] - pix * (TILES * 128)

    def at_ref(parts):
        total = None
        for t, part in enumerate(parts):
            lane = lax.broadcasted_iota(jnp.int32, part.shape, 1)
            part = jnp.where(lane == want - t * 128, part, 0.0)
            total = part if total is None else total + part
        return jnp.sum(total, axis=1, keepdims=True)

    def arrived(ref, sem):
        pltpu.make_async_copy(ref, ref, sem).wait()

    def start(src, dst, sem, devices):
        for i, device in enumerate(devices):
            remote(src, dst.at[i], sem.at[0], sem.at[1], (sec, device)).start()

    def finish(src, dst, sem, devices):
        arrived(dst, sem.at[0])
        arrived(dst, sem.at[1])

    def sum_of(own, buffers):
        total = own[...]
        for i in range(7):
            total = total + buffers[i]
        return total

    steps_n = (nmsg, nbuf1, early_sem.at[0], first), (nmsg2, nbuf2, early_sem.at[1], second)
    steps_e = (emsg, ebuf1, early_sem.at[0], first), (emsg2, ebuf2, early_sem.at[1], second)
    steps_r = (rmsg, rbuf1, r_sem, first)
    steps_b = (bmsg, bbuf, b_sem, second)

    chunks = [(0, 3), (3, GROUPS)]
    spans = [pl.ds(32 * low, min(32 * high, FLAT) - 32 * low) for low, high in chunks]
    loads = [
        pltpu.make_async_copy(slc_hbm.at[span], blocks.at[1, span], load_sem.at[i]) for i, span in enumerate(spans)
    ]
    loads.append(pltpu.make_async_copy(nbr_hbm, nbr, load_sem.at[2]))
    for load in loads:
        load.start()
    barrier = pltpu.get_barrier_semaphore()
    peers = [(sec, before), (sec, after), (sec_up, pix), (sec_down, pix)]
    peers += [(sec, x * 16 + lax.rem(z + d, 8) * 2 + core) for d in (1, 7)]
    peers += [(sec, lax.rem(x + d, 4) * 16 + z * 2 + core) for d in (1, 3)]

    def tell(sem):
        for peer in peers:
            pl.semaphore_signal(sem, inc=1, device_id=peer, device_id_type=MESH)

    def hear(sem):
        pl.semaphore_wait(sem, len(peers))

    tell(barrier)
    hear(barrier)
    tell(ready.at[0])

    def halo(i, n):
        part = blocks.at[1, spans[n]]
        return remote(part, blocks.at[2 - i, spans[n]], halo_send.at[i // 2], halo_recv.at[i // 2, n], (sec, near[i]))

    for n in range(len(chunks)):
        loads[n].wait()
        for i in (0, 2):
            pl.when(present[i])(halo(i, n).start)

    for i in range(3):
        blocks[i, FLAT:, :] = jnp.zeros((32 * GROUPS - FLAT, 128), F32)
    kre[...] = jnp.zeros_like(kre)
    kim[...] = jnp.zeros_like(kim)
    red[...] = jnp.zeros_like(red)
    cvec[...] = jnp.zeros_like(cvec)
    bvec[...] = jnp.zeros_like(bvec)
    for i in (0, 2):

        @pl.when(jnp.logical_not(present[i]))
        def _():
            blocks[i] = jnp.zeros((32 * GROUPS, 128), F32)
            vbuf[i] = jnp.zeros_like(vbuf[i])

    loads[2].wait()

    base = pix * (TILES * 128) - REACH
    for t in range(TILES):
        rel = nbr[:, t * 128 : (t + 1) * 128] - (base + t * 128)
        lanes[t, 0:NB, :] = jnp.bitwise_and(rel, 127)
        tiles[t, 0:NB, :] = jnp.right_shift(rel, 7)
        lanes[t, NB : NB + 1, :] = jnp.zeros((1, 128), jnp.int32)
        tiles[t, NB : NB + 1, :] = jnp.full((1, 128), SPAN, jnp.int32)

    def spread(i, groups=range(GROUPS)):
        for g in groups:
            for m in range(2):
                for c in range(2):
                    ext[2 * i + m, c, g * 8 : (g + 1) * 8, :] = blocks[i, pl.ds(g * 32 + m * 2 + c, 8, stride=4), :]

    spread(1)
    for t in range(TILES):
        for c in range(2):
            total = None
            for g in range(GROUPS):
                own = ext[2 + t, c, g * 8 : (g + 1) * 8, :]
                zs[t, 0, c, g * 8 : (g + 1) * 8, :] = own
                total = own if total is None else total + own
            xsum[t, c : c + 1, :] = column_sum(total)

    def gather(t, offsets, begin, groups=range(GROUPS), halves=None):
        def some(half):
            for i in range(NB // 2):
                k = 1 + half * (NB // 2) + i
                lane = bcast(lanes[t, pl.ds(k, 1), :])
                tile = bcast(tiles[t, pl.ds(k, 1), :])
                for g in groups:
                    rows = slice(g * 8, (g + 1) * 8)
                    for c in range(2):
                        out = None if begin else zs[t, k, c, rows, :]
                        for m in offsets:
                            got = take(ext[t + m, c, rows, :], lane)
                            out = got if out is None else jnp.where(tile == m, got, out)
                        zs[t, k, c, rows, :] = out

        if halves is None:
            pl.loop(0, 2)(some)
        else:
            for half in halves:
                some(half)

    for t in range(TILES):
        gather(t, (2 - t, 3 - t), True)
    hear(ready.at[0])
    tell(ready.at[1])

    def side(s, groups, halves=None):
        spread(2 * s, groups)
        close, distant = 1 + 3 * s, 5 * s
        gather(s, (close - s, distant - s), False, groups, halves)
        gather(1 - s, (close - (1 - s),), False, groups, halves)

    def both(soon):
        late = 1 - soon
        for n in range(len(chunks)):
            arrived(blocks.at[2 * soon, spans[n]], halo_recv.at[1 - soon, n])
        side(soon, range(GROUPS))
        for n, (low, high) in enumerate(chunks):
            pl.when(inner)(lambda n=n: arrived(blocks.at[2 * late, spans[n]], halo_recv.at[1 - late, n]))
            side(late, range(low, high), range(2))

    pl.when(core == 0)(lambda: both(1))
    pl.when(core == 1)(lambda: both(0))

    hear(ready.at[1])
    tell(ready.at[2])

    @pl.when(sec == 2)
    def _():
        column = at_ref([nbr[:, t * 128 : (t + 1) * 128].astype(F32) for t in range(TILES)])
        nmsg[...] = to_row(column)
        start(*steps_n[0])

    @pl.loop(0, TILES)
    def _(t):
        for g in range(GROUPS):
            rows = slice(g * 8, (g + 1) * 8)
            power = None
            for k in range(NB):
                re, im = zs[t, k, 0, rows, :], zs[t, k, 1, rows, :]
                zs[t, k, 2, rows, :] = re - im
                term = re * re + im * im
                power = term if power is None else power + term
            wbuf[t, rows, :] = lax.rsqrt(jnp.maximum(power, 1.0))

        def fold(slot, parts):
            for i, part in enumerate(parts):
                red[slot, i * 8 : (i + 1) * 8, :] = part
            total = None
            for i in range(8):
                row = red[slot, pl.ds(i, 8, stride=8), :]
                total = row if total is None else total + row
            return total

        slot = 0
        for l in range(NB + 1):
            for kg in range(2):
                low, high = 8 * kg, min(8 * kg + 8, l + 1, NB)
                if high <= low:
                    continue
                count = high - low
                p, q, r = [None] * count, [None] * count, [None] * count
                cr, ci = [None] * count, [None] * count

                def put(box, i, value):
                    box[i] = value if box[i] is None else box[i] + value

                for g in range(GROUPS):
                    rows = slice(g * 8, (g + 1) * 8)
                    w = wbuf[t, rows, :]
                    if l < NB:
                        w2 = w * w
                        lr, li = zs[t, l, 0, rows, :] * w2, zs[t, l, 1, rows, :] * w2
                    else:
                        lr, li = zs[t, 0, 0, rows, :] * w, zs[t, 0, 1, rows, :] * w
                    le = lr + li
                    for i in range(count):
                        k = low + i
                        kr, ki = zs[t, k, 0, rows, :], zs[t, k, 1, rows, :]
                        put(p, i, kr * lr)
                        put(q, i, ki * li)
                        if k != l:
                            put(r, i, zs[t, k, 2, rows, :] * le)
                        if l == NB:
                            put(cr, i, kr * w)
                            put(ci, i, ki * w)
                re = fold(4 * kg + slot, [a + b for a, b in zip(p, q)])
                im = fold(4 * kg + slot + 1, [jnp.zeros((8, 128), F32) if c is None else c + (b - a) for a, b, c in zip(p, q, r)])
                rows = slice(low, low + 8)
                if l < NB:
                    kre[t, l, rows, :] = re
                    kim[t, l, rows, :] = im
                    for i in range(count):
                        k = low + i
                        if k != l:
                            kre[t, k, l : l + 1, :] = re[i : i + 1, :]
                            kim[t, k, l : l + 1, :] = -im[i : i + 1, :]
                else:
                    bvec[t, 0, rows, :] = re
                    bvec[t, 1, rows, :] = im
                    slot = 2 - slot
                    cvec[t, 0, rows, :] = START * fold(4 * kg + slot, cr)
                    cvec[t, 1, rows, :] = -START * fold(4 * kg + slot + 1, ci)
                slot = 2 - slot

    @pl.when(sec >= 2)
    def _():
        hear(ready.at[2])
        tell(ready.at[3])

    @pl.when(sec == 2)
    def _():
        finish(*steps_n[0])
        nmsg2[...] = sum_of(nmsg, nbuf1)
        start(*steps_n[1])

    def expand():
        for l in range(NB):
            kref[0, l] = jnp.broadcast_to(eall[0:16, l : l + 1], (16, 128))
            kimf[0, l] = jnp.broadcast_to(eall[0:16, 16 + l : 17 + l], (16, 128))
        for c in range(2):
            cref[0, c] = jnp.broadcast_to(eall[0:16, 32 + c : 33 + c], (16, 128))

    @pl.when(sec == SECTIONS - 1)
    def _():
        lane = lax.broadcasted_iota(jnp.int32, (16, 128), 1)
        emsg[16:32, :] = jnp.zeros((16, 128), F32)
        acc = jnp.zeros((16, 128), F32)
        for c in range(2):
            acc = jnp.where(lane == 32 + c, at_ref([cvec[t, c] for t in range(TILES)]), acc)
        emsg[0:16, :] = acc

        @pl.loop(0, NB)
        def _(k):
            acc = emsg[0:16, :]
            acc = jnp.where(lane == k, at_ref([kre[t, k] for t in range(TILES)]), acc)
            emsg[0:16, :] = jnp.where(lane == 16 + k, at_ref([kim[t, k] for t in range(TILES)]), acc)
            parts = [at_ref([zs[t, k, c] * wbuf[t] for t in range(TILES)]) for c in range(2)]
            emsg[pl.ds(16 + k, 1), :] = to_row(parts[0]) + to_row(parts[1], 64)

        start(*steps_e[0])
        finish(*steps_e[0])
        emsg2[...] = sum_of(emsg, ebuf1)
        start(*steps_e[1])
        finish(*steps_e[1])
        eall[...] = sum_of(emsg2, ebuf2)
        for j in range(SECTIONS - 1):
            remote(eall.at[pl.ds(0, 16)], eall.at[pl.ds(0, 16)], y_send, y_recv, (j, pix)).start()
        expand()

    @pl.when(sec == 2)
    def _():
        finish(*steps_n[1])
        column = to_column(sum_of(nmsg2, nbuf2), 16)
        row = lax.broadcasted_iota(jnp.int32, (16, 128), 0)
        ncol[...] = jnp.where(row == NB, ref[0].astype(F32), column) - (pix * (TILES * 128)).astype(F32)

    def add_date(kr, ki, zb, t, z0):
        for l in range(NB):
            lr = bcast(zb[t, 0, l : l + 1, :])
            li = bcast(zb[t, 1, l : l + 1, :])
            for kg in range(2):
                rows = slice(8 * kg, 8 * kg + 8)
                zr, zi = z0[kg]
                kr[t, l, rows, :] = kr[t, l, rows, :] + (zr * lr + zi * li)
                ki[t, l, rows, :] = ki[t, l, rows, :] + (zr * li - zi * lr)

    @pl.when(sec == 0)
    def _():
        zbuf[...] = jnp.zeros_like(zbuf)

    @pl.when(sec > 0)
    def _():
        pl.when(inner)(lambda: arrived(vbuf, v_recv))
        pl.when(jnp.logical_not(inner))(lambda: arrived(vbuf.at[0:2], v_recv))
        for t in range(TILES):
            z0 = []
            for kg in range(2):
                rows = slice(8 * kg, 8 * kg + 8)
                lane = lanes[t, rows, :]
                tile = tiles[t, rows, :]
                pair = []
                for c in range(2):
                    src = []
                    for m in range(SPAN):
                        at = t + m
                        src.append(bcast(vbuf[at // 2, c : c + 1, (at % 2) * 128 : (at % 2) * 128 + 128]))
                    pair.append(pick(src, lane, tile))
                z0.append(pair)
            power = column_sum(z0[0][0] * z0[0][0] + z0[0][1] * z0[0][1] + (z0[1][0] * z0[1][0] + z0[1][1] * z0[1][1]))
            w = lax.rsqrt(jnp.maximum(power, 1.0))
            vr = vbuf[1, 0:1, t * 128 : (t + 1) * 128]
            vi = vbuf[1, 1:2, t * 128 : (t + 1) * 128]
            xsum[t, 0:1, :] = xsum[t, 0:1, :] + vr
            xsum[t, 1:2, :] = xsum[t, 1:2, :] + vi
            for kg in range(2):
                rows = slice(8 * kg, 8 * kg + 8)
                zr, zi = z0[kg][0] * w, z0[kg][1] * w
                z0[kg] = (zr, zi)
                zbuf[t, 0, rows, :] = zr
                zbuf[t, 1, rows, :] = zi
                cvec[t, 0, rows, :] = cvec[t, 0, rows, :] + START * zr
                cvec[t, 1, rows, :] = cvec[t, 1, rows, :] - START * zi
                bvec[t, 0, rows, :] = bvec[t, 0, rows, :] + (zr * vr + zi * vi)
                bvec[t, 1, rows, :] = bvec[t, 1, rows, :] + (zr * vi - zi * vr)
            add_date(kre, kim, zbuf, t, z0)

    def solve(kr, ki, cv, sb, count):
        places = [(t, c, kg) for t in range(count) for c in range(2) for kg in range(2)]

        def product(state):
            for i, (t, c, kg) in enumerate(places):
                sb[t, c, 8 * kg : 8 * kg + 8, :] = state[i]
            out = []
            for t in range(count):
                y = [[None, None], [None, None]]
                for l in range(NB):
                    lr = bcast(sb[t, 0, l : l + 1, :])
                    li = bcast(sb[t, 1, l : l + 1, :])
                    for kg in range(2):
                        rows = slice(8 * kg, 8 * kg + 8)
                        ar, ai = kr[t, l, rows, :], ki[t, l, rows, :]
                        re = ar * lr - ai * li
                        im = ar * li + ai * lr
                        y[0][kg] = re if l == 0 else y[0][kg] + re
                        y[1][kg] = im if l == 0 else y[1][kg] + im
                out += [y[0][0], y[0][1], y[1][0], y[1][1]]
            return out

        def c0(i):
            t, c, kg = places[i]
            return cv[t, c, 8 * kg : 8 * kg + 8, :]

        def turn(_, state):
            return tuple(a + y + c0(i) for i, (a, y) in enumerate(zip(state, product(state))))

        state = lax.fori_loop(0, ITERS - 1, turn, tuple(c0(i) for i in range(len(places))))
        state = [a * SCALE for a in state]
        ks = product(state)
        norms = []
        for t in range(count):
            total = None
            for i in range(4 * t, 4 * t + 4):
                term = state[i] * (ks[i] + (2.0 * SCALE) * c0(i))
                total = term if total is None else total + term
            norms.append(lax.rsqrt(column_sum(total) + SCALE * SCALE))
        return state, norms

    state, norms = solve(kre, kim, cvec, sbuf, TILES)
    for t in range(TILES):
        s = state[4 * t : 4 * t + 4]
        norm = norms[t]
        cr = ci = fr = fi = None
        for kg in range(2):
            rows = slice(8 * kg, 8 * kg + 8)
            sr, si = s[kg], s[2 + kg]
            br, bi = bvec[t, 0, rows, :], bvec[t, 1, rows, :]
            zr, zi = zbuf[t, 0, rows, :], zbuf[t, 1, rows, :]
            a, b = sr * br + si * bi, sr * bi - si * br
            e, f = zr * sr - zi * si, zr * si + zi * sr
            cr = a if kg == 0 else column_sum(cr + a)
            ci = b if kg == 0 else column_sum(ci + b)
            fr = e if kg == 0 else column_sum(fr + e)
            fi = f if kg == 0 else column_sum(fi + f)
        cols = slice(t * 128, (t + 1) * 128)
        msg[0:1, cols] = (cr + (SCALE * START) * xsum[t, 0:1, :]) * norm
        msg[1:2, cols] = (ci + (SCALE * START) * xsum[t, 1:2, :]) * norm
        fr, fi = unit((fr + SCALE * START) * norm, fi * norm)
        fmsg[0:1, cols] = fr
        fmsg[1:2, cols] = fi

    steps_g = [
        remote(gmsg, gbuf.at[d], g_send, g_recv, (s, pix if d == 0 else first[d - 1]))
        for s in range(SECTIONS)
        for d in range(8)
        if (s, d) != (2, 0)
    ]

    @pl.when(sec == 2)
    def _():
        hear(ready.at[3])
        lane = lax.broadcasted_iota(jnp.int32, (16, 128), 1).astype(F32)
        row = lax.broadcasted_iota(jnp.int32, (16, 128), 0)
        for c in range(2):
            total = None
            for t in range(TILES):
                cols = slice(t * 128, (t + 1) * 128)
                value = jnp.where(
                    row == NB,
                    jnp.broadcast_to(fmsg[c : c + 1, cols], (16, 128)),
                    jnp.broadcast_to(msg[c : c + 1, cols], (16, 128)),
                )
                value = jnp.where(ncol[...] - t * 128.0 == lane, value, 0.0)
                total = value if total is None else total + value
            gmsg[c : c + 1, :] = to_row(jnp.sum(total, axis=1, keepdims=True))
        for copy in steps_g:
            copy.start()
        gbuf[0] = gmsg[...]

    @pl.when(sec < SECTIONS - 1)
    def _():
        for i in range(3):
            pl.when(present[i])(remote(msg, vbuf.at[2 - i], v_send, v_recv, (sec_up, near[i])).start)

    for s in range(1, SECTIONS):

        @pl.when(sec == s)
        def _():
            for j in range(s):
                remote(fmsg, fbuf.at[s - 1], f_send, f_recv.at[s - 1], (j, pix)).start()

    @pl.when(sec < 2)
    def _():
        hear(ready.at[2])
        tell(ready.at[3])

    pl.when(sec != 2)(lambda: hear(ready.at[3]))
    comp[0, 0:1, :] = msg[0:1, :]
    comp[1, 0:1, :] = msg[1:2, :]

    def vector():
        for i, (t, c, kg) in enumerate((t, c, kg) for t in range(TILES) for c in range(2) for kg in range(2)):
            sbuf[t, c, 8 * kg : 8 * kg + 8, :] = state[i] * norms[t]
        for t in range(TILES):

            @pl.loop(0, GROUPS)
            def _(g):
                rows = pl.ds(pl.multiple_of(g * 8, 8), 8)
                re = im = None
                for k in range(NB):
                    sr = bcast(sbuf[t, 0, k : k + 1, :])
                    si = bcast(sbuf[t, 1, k : k + 1, :])
                    zr, zi = zs[t, k, 0, rows, :], zs[t, k, 1, rows, :]
                    a, b = zr * sr - zi * si, zr * si + zi * sr
                    re = a if re is None else re + a
                    im = b if im is None else im + b
                w = wbuf[t, rows, :]
                series[t, 0, rows, :] = bcast((SCALE * START) * norms[t]) + w * re
                series[t, 1, rows, :] = w * im

    pl.when(sec < SECTIONS - 1)(vector)

    def take_f(j):
        arrived(fbuf.at[j - 1], f_recv.at[j - 1])

    @pl.when(sec == 0)
    def _():
        take_f(1)
        for t in range(TILES):
            fr = fbuf[0, 0:1, t * 128 : (t + 1) * 128]
            fi = fbuf[0, 1:2, t * 128 : (t + 1) * 128]
            re, im = series[t, 0], series[t, 1]
            series[t, 0] = re * fr - im * fi
            series[t, 1] = re * fi + im * fr

    @pl.when(sec < SECTIONS - 1)
    def _():
        for c in range(2):
            rmsg[c : c + 1, :] = to_row(at_ref([series[t, c] for t in range(TILES)]))
        start(*steps_r)
        remote(eall.at[pl.ds(0, 16)], eall.at[pl.ds(0, 16)], y_send, y_recv, (SECTIONS - 1, pix)).wait_recv()
        expand()

    @pl.when(sec == 2)
    def _():
        arrived(gbuf.at[1:8], g_recv)

    @pl.when(sec != 2)
    def _():
        arrived(gbuf.at[0:8], g_recv)

    total = gbuf[0]
    for d in range(1, 8):
        total = total + gbuf[d]
    bmsg[2:4, :] = total

    @pl.when(sec < SECTIONS - 1)
    def _():
        finish(*steps_r)
        bmsg[0:2, :] = sum_of(rmsg, rbuf1)

    @pl.when(sec == SECTIONS - 1)
    def _():
        bmsg[0:2, :] = jnp.zeros((2, 128), F32)

    start(*steps_b)
    pl.when(sec == SECTIONS - 1)(vector)
    finish(*steps_b)
    total = sum_of(bmsg, bbuf)

    values = [to_column(total[2 + c : 3 + c, :], 16) for c in range(2)]
    f2r, f2i = values[0][NB:16], values[1][NB:16]
    row = lax.broadcasted_iota(jnp.int32, (16, 128), 0)
    zr, zi = (jnp.where(row < NB, value, 0.0) for value in values)
    w = lax.rsqrt(jnp.maximum(column_sum(zr * zr + zi * zi), 1.0))
    zr, zi = zr * w, zi * w
    zref[0, 0] = zr
    zref[0, 1] = zi
    cref[0, 0] = cref[0, 0] + START * zr
    cref[0, 1] = cref[0, 1] - START * zi
    add_date(kref, kimf, zref, 0, [(zr[0:8], zi[0:8]), (zr[8:16], zi[8:16])])
    state_ref, norm_ref = solve(kref, kimf, cref, sref, 1)
    sr = jnp.concatenate(state_ref[0:2], axis=0)
    si = jnp.concatenate(state_ref[2:4], axis=0)
    norm = norm_ref[0]
    f3r = column_sum(zr * sr - zi * si)
    f3i = column_sum(zr * si + zi * sr)
    f3r, f3i = unit((f3r + SCALE * START) * norm, f3i * norm)
    fr = jnp.where(sec < 2, f3r * f2r - f3i * f2i, f3r)
    fi = jnp.where(sec < 2, f3r * f2i + f3i * f2r, f3i)
    vr, vi = total[0:1, :], total[1:2, :]
    rmsg[0:1, :] = vr * fr - vi * fi
    rmsg[1:2, :] = vr * fi + vi * fr

    @pl.when(sec == SECTIONS - 1)
    def _():
        z = eall[16:32, :]
        a = bcast(column_sum(z * sr))
        b = bcast(column_sum(z * si))
        re = a - pltpu.roll(b, 64, 1)
        im = b + pltpu.roll(a, 64, 1)
        rmsg[0:1, :] = (re[0:1] + SCALE * START) * norm
        rmsg[1:2, :] = im[0:1] * norm

    ur, ui = unit(rmsg[0:1, :], rmsg[1:2, :])
    ur, ui = GAIN * to_column(ur, PAD), GAIN * to_column(ui, PAD)

    datum[0:1, :] = jnp.ones((1, TILES * 128), F32)
    datum[1:2, :] = jnp.zeros((1, TILES * 128), F32)

    @pl.when(sec < SECTIONS - 1)
    def _():
        take_f(3)
        datum[...] = fbuf[2]

    @pl.when(sec < 2)
    def _():
        take_f(2)
        dr, di = datum[0:1, :], datum[1:2, :]
        fr, fi = fbuf[1, 0:1, :], fbuf[1, 1:2, :]
        datum[0:1, :] = dr * fr - di * fi
        datum[1:2, :] = dr * fi + di * fr

    for t in range(TILES):
        dr, di = datum[0:1, t * 128 : (t + 1) * 128], datum[1:2, t * 128 : (t + 1) * 128]
        re, im = series[t, 0], series[t, 1]
        re, im = re * dr - im * di, re * di + im * dr
        for c, part in enumerate((re * ur + im * ui, im * ur - re * ui)):
            for g in range(GROUPS):
                count = min(8, ROWS - g * 8)
                phases[pl.ds(g * 32 + t * 2 + c, count, stride=4), :] = part[g * 8 : g * 8 + count]

    for i in (0, 2):
        pl.when(present[i])(lambda i=i: arrived(blocks.at[1, pl.ds(0, FLAT)], halo_send.at[i // 2]))
    @pl.when(sec == 2)
    def _():
        arrived(gbuf, g_send)

    @pl.when(sec == SECTIONS - 1)
    def _():
        arrived(ebuf1.at[0:3, 0:16], y_send)

    @pl.when(sec < SECTIONS - 1)
    def _():
        pl.when(inner)(lambda: arrived(vbuf, v_send))
        pl.when(jnp.logical_not(inner))(lambda: arrived(vbuf.at[0:2], v_send))

    for s in range(1, SECTIONS):

        @pl.when(sec == s)
        def _():
            arrived(fbuf.at[0:s], f_send)


def hand_out(phases_in, comp_in, phases, comp, sem):
    copies = [
        pltpu.make_async_copy(phases_in, phases, sem.at[0]),
        pltpu.make_async_copy(comp_in, comp, sem.at[1]),
    ]
    for copy in copies:
        copy.start()
    for copy in copies:
        copy.wait()


def on_device(slc, neighbours, reference_pixel):
    vmem = pl.BlockSpec(memory_space=pltpu.VMEM)
    hbm = pl.BlockSpec(memory_space=pltpu.HBM)
    pixels = slc.shape[2]
    dma = pltpu.SemaphoreType.DMA
    flat = slc.reshape(2, ROWS, TILES, 128).transpose(1, 2, 0, 3).reshape(FLAT, 128)
    phases, comp = pl.pallas_call(
        kernel,
        out_shape=(
            jax.ShapeDtypeStruct((FLAT, 128), F32),
            jax.ShapeDtypeStruct((2, 1, pixels), F32),
        ),
        in_specs=[hbm, hbm, pl.BlockSpec(memory_space=pltpu.SMEM)],
        out_specs=(vmem, vmem),
        scratch_shapes=[
            pltpu.VMEM((NB, pixels), jnp.int32),
            pltpu.VMEM((3, 32 * GROUPS, 128), F32),
            pltpu.VMEM((6, 2, PAD, 128), F32),
            pltpu.VMEM((TILES, 16, 128), jnp.int32),
            pltpu.VMEM((TILES, 16, 128), jnp.int32),
            pltpu.VMEM((TILES, NB, 3, PAD, 128), F32),
            pltpu.VMEM((TILES, PAD, 128), F32),
            pltpu.VMEM((8, 64, 128), F32),
            pltpu.VMEM((TILES, 16, 16, 128), F32),
            pltpu.VMEM((TILES, 16, 16, 128), F32),
            pltpu.VMEM((TILES, 2, 16, 128), F32),
            pltpu.VMEM((TILES, 2, 16, 128), F32),
            pltpu.VMEM((TILES, 2, 128), F32),
            pltpu.VMEM((TILES, 2, 16, 128), F32),
            pltpu.VMEM((TILES, 2, 16, 128), F32),
            pltpu.VMEM((3, 2, pixels), F32),
            pltpu.VMEM((2, pixels), F32),
            pltpu.VMEM((2, pixels), F32),
            pltpu.VMEM((3, 2, pixels), F32),
            pltpu.VMEM((TILES, 2, PAD, 128), F32),
            pltpu.VMEM((2, pixels), F32),
            pltpu.VMEM((1, 128), F32),
            pltpu.VMEM((7, 1, 128), F32),
            pltpu.VMEM((1, 128), F32),
            pltpu.VMEM((7, 1, 128), F32),
            pltpu.VMEM((16, 128), F32),
            pltpu.VMEM((32, 128), F32),
            pltpu.VMEM((7, 32, 128), F32),
            pltpu.VMEM((32, 128), F32),
            pltpu.VMEM((7, 32, 128), F32),
            pltpu.VMEM((32, 128), F32),
            pltpu.VMEM((2, 128), F32),
            pltpu.VMEM((31, 2, 128), F32),
            pltpu.VMEM((2, 128), F32),
            pltpu.VMEM((7, 2, 128), F32),
            pltpu.VMEM((4, 128), F32),
            pltpu.VMEM((7, 4, 128), F32),
            pltpu.VMEM((1, 16, 16, 128), F32),
            pltpu.VMEM((1, 16, 16, 128), F32),
            pltpu.VMEM((1, 2, 16, 128), F32),
            pltpu.VMEM((1, 2, 16, 128), F32),
            pltpu.VMEM((1, 2, 16, 128), F32),
            dma((3,)),
            dma((2,)),
            dma((2, 2)),
            dma(()),
            dma(()),
            dma(()),
            dma((3,)),
            dma((2, 2)),
            dma(()),
            dma(()),
            dma(()),
            dma(()),
            dma((2,)),
            dma((2,)),
            pltpu.SemaphoreType.REGULAR((4,)),
        ],
        compiler_params=pltpu.CompilerParams(
            collective_id=0, has_side_effects=True, vmem_limit_bytes=16 * 2**20
        ),
        cost_estimate=pl.CostEstimate(flops=100_000_000, bytes_accessed=1_000_000, transcendentals=0),
    )(*(pltpu.with_memory_space_constraint(a, pltpu.HBM) for a in (flat, neighbours)), reference_pixel)
    phases, comp = pl.pallas_call(
        hand_out,
        out_shape=(
            jax.ShapeDtypeStruct((FLAT, 128), F32),
            jax.ShapeDtypeStruct((2, 1, pixels), F32),
        ),
        in_specs=[pl.BlockSpec(memory_space=pl.ANY)] * 2,
        out_specs=(hbm, hbm),
        scratch_shapes=[dma((2,))],
        compiler_params=pltpu.CompilerParams(vmem_limit_bytes=2**20),
    )(phases, comp)
    return phases.reshape(ROWS, TILES, 2, 128).transpose(2, 0, 1, 3).reshape(2, ROWS, pixels), comp


def solution(mesh):
    return jax.shard_map(
        on_device,
        mesh=mesh,
        in_specs=(P(None, "section", "pix"), P(None, "pix"), P()),
        out_specs=(P(None, "section", "pix"), P(None, "section", "pix")),
        check_vma=False,
    )
```

```python
import math

import jax
import jax.numpy as jnp
from jax import lax
from jax.experimental import pallas as pl
from jax.experimental.pallas import tpu as pltpu
from jax.sharding import PartitionSpec as P

ITERS = 16
FLOOR = 0.05
REACH = 256
NB = 15
ROWS = 50
PAD = 56
GROUPS = PAD // 8
FLAT = 4 * ROWS
TILES = 2
SPAN = 5
SCALE = 2.0**-45
START = 1.0 / math.sqrt(ROWS + 1)
GAIN = math.sqrt(ROWS + 1)
SECTIONS = 4
PIX = 64
MESH = pl.DeviceIdType.MESH
F32 = jnp.float32


def bcast(row):
    return jnp.broadcast_to(row, (8, 128))


def pick(sources, lane, tile):
    out = jnp.zeros((8, 128), F32)
    for m, source in enumerate(sources):
        out = jnp.where(tile == m, take(source, lane), out)
    return out


def take(source, lane):
    return jnp.take_along_axis(source, lane, axis=1, mode="promise_in_bounds")


def column_sum(x):
    return jnp.sum(x, axis=0, keepdims=True)


def eye(count, shift=0):
    lane = lax.broadcasted_iota(jnp.int32, (count, 128), 1)
    return lane == lax.broadcasted_iota(jnp.int32, (count, 128), 0) + shift


def to_row(column, shift=0):
    return column_sum(jnp.where(eye(column.shape[0], shift), column, 0.0))


def to_column(row, count):
    spread = jnp.broadcast_to(row, (count, 128))
    return jnp.sum(jnp.where(eye(count), spread, 0.0), axis=1, keepdims=True)


def unit(re, im):
    scale = 1.0 / jnp.maximum(jnp.sqrt(re * re + im * im), FLOOR)
    return re * scale, im * scale


def remote(src, dst, send, recv, device):
    return pltpu.make_async_remote_copy(
        src_ref=src, dst_ref=dst, send_sem=send, recv_sem=recv, device_id=device, device_id_type=MESH
    )


def kernel(
    slc_hbm, nbr_hbm, ref, phases, comp,
    nbr, blocks, ext, lanes, tiles, zs, wbuf, red, kre, kim, cvec, bvec, xsum, zbuf, sbuf,
    vbuf, msg, fmsg, fbuf, series, datum,
    nmsg, nbuf1, nmsg2, nbuf2, ncol, emsg, ebuf1, emsg2, ebuf2, eall, gmsg, gbuf, rmsg, rbuf1, bmsg, bbuf,
    kref, kimf, cref, zref, sref, kre2, kim2, qvec, gvec, result, inverse, kref2, kimf2, qref, gref,
    load_sem, halo_send, halo_recv, v_send, v_recv, f_send, f_recv, early_sem,
    y_send, y_recv, g_send, g_recv, r_sem, b_sem, ready,
):
    sec = lax.axis_index("section")
    pix = lax.axis_index("pix")
    before = lax.rem(pix + (PIX - 1), PIX)
    after = lax.rem(pix + 1, PIX)
    near = (before, pix, after)
    present = (pix > 0, pix >= 0, pix < PIX - 1)
    inner = jnp.logical_and(present[0], present[2])
    sec_up = lax.rem(sec + 1, SECTIONS)
    sec_down = lax.rem(sec + (SECTIONS - 1), SECTIONS)
    x = pix // 16
    z = lax.rem(pix // 2, 8)
    core = lax.rem(pix, 2)
    group = x * 2 + core
    first = []
    second = []
    for d in range(1, 8):
        g = lax.rem(group + d, 8)
        first.append((g // 2) * 16 + z * 2 + lax.rem(g, 2))
        second.append(x * 16 + lax.rem(z + d, 8) * 2 + core)

    want = ref[0] - pix * (TILES * 128)

    def at_ref(parts):
        total = None
        for t, part in enumerate(parts):
            lane = lax.broadcasted_iota(jnp.int32, part.shape, 1)
            part = jnp.where(lane == want - t * 128, part, 0.0)
            total = part if total is None else total + part
        return jnp.sum(total, axis=1, keepdims=True)

    def arrived(ref, sem):
        pltpu.make_async_copy(ref, ref, sem).wait()

    def start(src, dst, sem, devices):
        for i, device in enumerate(devices):
            remote(src, dst.at[i], sem.at[0], sem.at[1], (sec, device)).start()

    def finish(src, dst, sem, devices):
        arrived(dst, sem.at[0])
        arrived(dst, sem.at[1])

    def sum_of(own, buffers):
        total = own[...]
        for i in range(7):
            total = total + buffers[i]
        return total

    steps_n = (nmsg, nbuf1, early_sem.at[0], first), (nmsg2, nbuf2, early_sem.at[1], second)
    steps_e = (emsg, ebuf1, early_sem.at[0], first), (emsg2, ebuf2, early_sem.at[1], second)
    steps_r = (rmsg, rbuf1, r_sem, first)
    steps_b = (bmsg, bbuf, b_sem, second)

    chunks = [(0, 3), (3, GROUPS)]
    spans = [pl.ds(32 * low, min(32 * high, FLAT) - 32 * low) for low, high in chunks]
    loads = [
        pltpu.make_async_copy(slc_hbm.at[span], blocks.at[1, span], load_sem.at[i]) for i, span in enumerate(spans)
    ]
    loads.append(pltpu.make_async_copy(nbr_hbm, nbr, load_sem.at[2]))
    for load in loads:
        load.start()
    barrier = pltpu.get_barrier_semaphore()
    peers = [(sec, before), (sec, after), (sec_up, pix), (sec_down, pix)]
    peers += [(sec, x * 16 + lax.rem(z + d, 8) * 2 + core) for d in (1, 7)]
    peers += [(sec, lax.rem(x + d, 4) * 16 + z * 2 + core) for d in (1, 3)]

    def tell(sem):
        for peer in peers:
            pl.semaphore_signal(sem, inc=1, device_id=peer, device_id_type=MESH)

    def hear(sem):
        pl.semaphore_wait(sem, len(peers))

    tell(barrier)
    hear(barrier)
    tell(ready.at[0])

    def halo(i, n):
        part = blocks.at[1, spans[n]]
        return remote(part, blocks.at[2 - i, spans[n]], halo_send.at[i // 2], halo_recv.at[i // 2, n], (sec, near[i]))

    for n in range(len(chunks)):
        loads[n].wait()
        for i in (0, 2):
            pl.when(present[i])(halo(i, n).start)

    for i in range(3):
        blocks[i, FLAT:, :] = jnp.zeros((32 * GROUPS - FLAT, 128), F32)
    kre[...] = jnp.zeros_like(kre)
    kim[...] = jnp.zeros_like(kim)
    red[...] = jnp.zeros_like(red)
    cvec[...] = jnp.zeros_like(cvec)
    bvec[...] = jnp.zeros_like(bvec)
    for i in (0, 2):

        @pl.when(jnp.logical_not(present[i]))
        def _():
            blocks[i] = jnp.zeros((32 * GROUPS, 128), F32)
            vbuf[i] = jnp.zeros_like(vbuf[i])

    loads[2].wait()

    base = pix * (TILES * 128) - REACH
    for t in range(TILES):
        rel = nbr[:, t * 128 : (t + 1) * 128] - (base + t * 128)
        lanes[t, 0:NB, :] = jnp.bitwise_and(rel, 127)
        tiles[t, 0:NB, :] = jnp.right_shift(rel, 7)
        lanes[t, NB : NB + 1, :] = jnp.zeros((1, 128), jnp.int32)
        tiles[t, NB : NB + 1, :] = jnp.full((1, 128), SPAN, jnp.int32)

    def spread(i, groups=range(GROUPS)):
        for g in groups:
            for m in range(2):
                for c in range(2):
                    ext[2 * i + m, c, g * 8 : (g + 1) * 8, :] = blocks[i, pl.ds(g * 32 + m * 2 + c, 8, stride=4), :]

    spread(1)
    for t in range(TILES):
        for c in range(2):
            total = None
            for g in range(GROUPS):
                own = ext[2 + t, c, g * 8 : (g + 1) * 8, :]
                zs[t, 0, c, g * 8 : (g + 1) * 8, :] = own
                total = own if total is None else total + own
            xsum[t, c : c + 1, :] = column_sum(total)

    def gather(t, offsets, begin, groups=range(GROUPS), halves=None):
        def some(half):
            for i in range(NB // 2):
                k = 1 + half * (NB // 2) + i
                lane = bcast(lanes[t, pl.ds(k, 1), :])
                tile = bcast(tiles[t, pl.ds(k, 1), :])
                for g in groups:
                    rows = slice(g * 8, (g + 1) * 8)
                    for c in range(2):
                        out = None if begin else zs[t, k, c, rows, :]
                        for m in offsets:
                            got = take(ext[t + m, c, rows, :], lane)
                            out = got if out is None else jnp.where(tile == m, got, out)
                        zs[t, k, c, rows, :] = out

        if halves is None:
            pl.loop(0, 2)(some)
        else:
            for half in halves:
                some(half)

    for t in range(TILES):
        gather(t, (2 - t, 3 - t), True)
    hear(ready.at[0])
    tell(ready.at[1])

    def side(s, groups, halves=None):
        spread(2 * s, groups)
        close, distant = 1 + 3 * s, 5 * s
        gather(s, (close - s, distant - s), False, groups, halves)
        gather(1 - s, (close - (1 - s),), False, groups, halves)

    def both(soon):
        late = 1 - soon
        for n in range(len(chunks)):
            arrived(blocks.at[2 * soon, spans[n]], halo_recv.at[1 - soon, n])
        side(soon, range(GROUPS))
        for n, (low, high) in enumerate(chunks):
            pl.when(inner)(lambda n=n: arrived(blocks.at[2 * late, spans[n]], halo_recv.at[1 - late, n]))
            side(late, range(low, high), range(2))

    pl.when(core == 0)(lambda: both(1))
    pl.when(core == 1)(lambda: both(0))

    hear(ready.at[1])
    tell(ready.at[2])

    @pl.when(sec == 2)
    def _():
        column = at_ref([nbr[:, t * 128 : (t + 1) * 128].astype(F32) for t in range(TILES)])
        nmsg[...] = to_row(column)
        start(*steps_n[0])

    @pl.loop(0, TILES)
    def _(t):
        for g in range(GROUPS):
            rows = slice(g * 8, (g + 1) * 8)
            power = None
            for k in range(NB):
                re, im = zs[t, k, 0, rows, :], zs[t, k, 1, rows, :]
                zs[t, k, 2, rows, :] = re - im
                term = re * re + im * im
                power = term if power is None else power + term
            wbuf[t, rows, :] = lax.rsqrt(jnp.maximum(power, 1.0))

        def fold(slot, parts):
            for i, part in enumerate(parts):
                red[slot, i * 8 : (i + 1) * 8, :] = part
            total = None
            for i in range(8):
                row = red[slot, pl.ds(i, 8, stride=8), :]
                total = row if total is None else total + row
            return total

        slot = 0
        for l in range(NB + 1):
            for kg in range(2):
                low, high = 8 * kg, min(8 * kg + 8, l + 1, NB)
                if high <= low:
                    continue
                count = high - low
                p, q, r = [None] * count, [None] * count, [None] * count
                cr, ci = [None] * count, [None] * count

                def put(box, i, value):
                    box[i] = value if box[i] is None else box[i] + value

                for g in range(GROUPS):
                    rows = slice(g * 8, (g + 1) * 8)
                    w = wbuf[t, rows, :]
                    if l < NB:
                        w2 = w * w
                        lr, li = zs[t, l, 0, rows, :] * w2, zs[t, l, 1, rows, :] * w2
                    else:
                        lr, li = zs[t, 0, 0, rows, :] * w, zs[t, 0, 1, rows, :] * w
                    le = lr + li
                    for i in range(count):
                        k = low + i
                        kr, ki = zs[t, k, 0, rows, :], zs[t, k, 1, rows, :]
                        put(p, i, kr * lr)
                        put(q, i, ki * li)
                        if k != l:
                            put(r, i, zs[t, k, 2, rows, :] * le)
                        if l == NB:
                            put(cr, i, kr * w)
                            put(ci, i, ki * w)
                re = fold(4 * kg + slot, [a + b for a, b in zip(p, q)])
                im = fold(4 * kg + slot + 1, [jnp.zeros((8, 128), F32) if c is None else c + (b - a) for a, b, c in zip(p, q, r)])
                rows = slice(low, low + 8)
                if l < NB:
                    kre[t, l, rows, :] = re
                    kim[t, l, rows, :] = im
                    for i in range(count):
                        k = low + i
                        if k != l:
                            kre[t, k, l : l + 1, :] = re[i : i + 1, :]
                            kim[t, k, l : l + 1, :] = -im[i : i + 1, :]
                else:
                    bvec[t, 0, rows, :] = re
                    bvec[t, 1, rows, :] = im
                    slot = 2 - slot
                    cvec[t, 0, rows, :] = START * fold(4 * kg + slot, cr)
                    cvec[t, 1, rows, :] = -START * fold(4 * kg + slot + 1, ci)
                slot = 2 - slot

    def pieces(count):
        return [(t, c, kg) for t in range(count) for c in range(2) for kg in range(2)]

    def load(ref, count):
        return [ref[t, c, 8 * kg : 8 * kg + 8, :] for t, c, kg in pieces(count)]

    def save(ref, value):
        for (t, c, kg), part in zip(pieces(len(value) // 4), value):
            ref[t, c, 8 * kg : 8 * kg + 8, :] = part

    def plus(*values):
        return [sum(parts[1:], parts[0]) for parts in zip(*values)]

    def times(factor, value):
        return [factor * part for part in value]

    def product(mr, mi, box, value):
        save(box, value)
        out = []
        for t in range(len(value) // 4):
            y = [[None, None], [None, None]]
            for l in range(NB):
                lr = bcast(box[t, 0, l : l + 1, :])
                li = bcast(box[t, 1, l : l + 1, :])
                for kg in range(2):
                    rows = slice(8 * kg, 8 * kg + 8)
                    ar, ai = mr[t, l, rows, :], mi[t, l, rows, :]
                    re = ar * lr - ai * li
                    im = ar * li + ai * lr
                    y[0][kg] = re if l == 0 else y[0][kg] + re
                    y[1][kg] = im if l == 0 else y[1][kg] + im
            out += [y[0][0], y[0][1], y[1][0], y[1][1]]
        return out

    def prepare(mr, mi, sr, si, cv, qv, box, count):
        for t in range(count):

            @pl.loop(0, NB)
            def _(l):
                for kg in range(2):
                    rows = slice(8 * kg, 8 * kg + 8)
                    re, im = 2.0 * mr[t, l, rows, :], 2.0 * mi[t, l, rows, :]
                    for m in range(NB):
                        lr = bcast(mr[t, l, m : m + 1, :])
                        li = bcast(mi[t, l, m : m + 1, :])
                        ar, ai = mr[t, m, rows, :], mi[t, m, rows, :]
                        re = re + (ar * lr - ai * li)
                        im = im + (ar * li + ai * lr)
                    sr[t, l, rows, :] = re
                    si[t, l, rows, :] = im

        save(qv, product(mr, mi, box, load(cv, count)))

    def joined(z, value):
        out = []
        for t in range(len(value) // 4):
            zr, zi = z[4 * t : 4 * t + 2], z[4 * t + 2 : 4 * t + 4]
            vr, vi = value[4 * t : 4 * t + 2], value[4 * t + 2 : 4 * t + 4]
            ar = column_sum(zr[0] * vr[0] - zi[0] * vi[0] + (zr[1] * vr[1] - zi[1] * vi[1]))
            ai = column_sum(zr[0] * vi[0] + zi[0] * vr[0] + (zr[1] * vi[1] + zi[1] * vr[1]))
            out += [zr[i] * ar + zi[i] * ai for i in range(2)] + [zr[i] * ai - zi[i] * ar for i in range(2)]
        return out

    def conj(value):
        return [part if (i // 2) % 2 == 0 else -part for i, part in enumerate(value)]

    def norms_of(value, image, start):
        out = []
        for t in range(len(value) // 4):
            total = None
            for i in range(4 * t, 4 * t + 4):
                term = value[i] * (image[i] + (2.0 * SCALE) * start[i])
                total = term if total is None else total + term
            out.append(lax.rsqrt(column_sum(total) + SCALE * SCALE))
        return out

    def solve(mr, mi, cv, box, count):
        def turn(_, value):
            return tuple(plus(value, product(mr, mi, box, value), load(cv, count)))

        value = lax.fori_loop(0, ITERS - 1, turn, tuple(load(cv, count)))
        value = times(SCALE, value)
        return value, norms_of(value, product(mr, mi, box, value), load(cv, count))

    def solve_joined(mr, mi, sr, si, cv, qv, zv, box, gbox, count):
        z = load(zv, count)
        r = conj(z)
        kr = product(mr, mi, box, r)
        c = plus(load(cv, count), times(START, r))
        save(cv, c)
        g = plus(r, kr)
        for t in range(count):
            squares = [z[4 * t + i] * z[4 * t + i] for i in range(4)]
            half = 0.5 * column_sum(squares[0] + squares[1] + (squares[2] + squares[3]))
            for i in range(4 * t, 4 * t + 4):
                g[i] = g[i] + half * r[i]
        save(gbox, g)
        for t in range(count):
            for l in range(NB):
                zr, zi = bcast(zv[t, 0, l : l + 1, :]), bcast(zv[t, 1, l : l + 1, :])
                gr, gi = bcast(gbox[t, 0, l : l + 1, :]), bcast(gbox[t, 1, l : l + 1, :])
                for kg in range(2):
                    rows = slice(8 * kg, 8 * kg + 8)
                    hr, hi = g[4 * t + kg], g[4 * t + 2 + kg]
                    xr, xi = z[4 * t + kg], z[4 * t + 2 + kg]
                    sr[t, l, rows, :] = sr[t, l, rows, :] + (hr * zr - hi * zi + (xr * gr - xi * gi))
                    si[t, l, rows, :] = si[t, l, rows, :] + (hr * zi + hi * zr - (xr * gi + xi * gr))

        def square(value):
            return plus(value, product(sr, si, box, value))

        value = plus(c, c, load(qv, count), times(START, kr), joined(z, c))
        value = plus(value, square(value))
        value = plus(value, square(square(value)))

        last = lax.fori_loop(0, 4, lambda _, v: tuple(square(v)), tuple(value))
        value = times(SCALE, plus(value, last))
        image = plus(product(mr, mi, box, value), joined(z, value))
        return value, norms_of(value, image, c)

    @pl.when(sec >= 2)
    def _():
        hear(ready.at[2])
        tell(ready.at[3])

    def prepare_own():
        prepare(kre, kim, kre2, kim2, cvec, qvec, sbuf, TILES)

    pl.when(jnp.logical_or(sec == 1, sec == 2))(prepare_own)

    @pl.when(sec == 2)
    def _():
        finish(*steps_n[0])
        nmsg2[...] = sum_of(nmsg, nbuf1)
        start(*steps_n[1])

    def expand():
        for l in range(NB):
            kref[0, l] = jnp.broadcast_to(eall[0:16, l : l + 1], (16, 128))
            kimf[0, l] = jnp.broadcast_to(eall[0:16, 16 + l : 17 + l], (16, 128))
        for c in range(2):
            cref[0, c] = jnp.broadcast_to(eall[0:16, 32 + c : 33 + c], (16, 128))
        prepare(kref, kimf, kref2, kimf2, cref, qref, sref, 1)

    @pl.when(sec == SECTIONS - 1)
    def _():
        lane = lax.broadcasted_iota(jnp.int32, (16, 128), 1)
        emsg[16:32, :] = jnp.zeros((16, 128), F32)
        acc = jnp.zeros((16, 128), F32)
        for c in range(2):
            acc = jnp.where(lane == 32 + c, at_ref([cvec[t, c] for t in range(TILES)]), acc)
        emsg[0:16, :] = acc

        @pl.loop(0, NB)
        def _(k):
            acc = emsg[0:16, :]
            acc = jnp.where(lane == k, at_ref([kre[t, k] for t in range(TILES)]), acc)
            emsg[0:16, :] = jnp.where(lane == 16 + k, at_ref([kim[t, k] for t in range(TILES)]), acc)
            parts = [at_ref([zs[t, k, c] * wbuf[t] for t in range(TILES)]) for c in range(2)]
            emsg[pl.ds(16 + k, 1), :] = to_row(parts[0]) + to_row(parts[1], 64)

        start(*steps_e[0])
        prepare_own()
        finish(*steps_e[0])
        emsg2[...] = sum_of(emsg, ebuf1)
        start(*steps_e[1])
        finish(*steps_e[1])
        eall[...] = sum_of(emsg2, ebuf2)
        for j in range(SECTIONS - 1):
            remote(eall.at[pl.ds(0, 16)], eall.at[pl.ds(0, 16)], y_send, y_recv, (j, pix)).start()
        expand()

    @pl.when(sec == 2)
    def _():
        finish(*steps_n[1])
        column = to_column(sum_of(nmsg2, nbuf2), 16)
        row = lax.broadcasted_iota(jnp.int32, (16, 128), 0)
        ncol[...] = jnp.where(row == NB, ref[0].astype(F32), column) - (pix * (TILES * 128)).astype(F32)

    def step_one():
        @pl.when(sec == 2)
        def _():
            arrived(gbuf.at[1:8], g_recv)

        @pl.when(sec != 2)
        def _():
            arrived(gbuf.at[0:8], g_recv)

        total = gbuf[0]
        for d in range(1, 8):
            total = total + gbuf[d]
        bmsg[2:4, :] = total
        bmsg[0:2, :] = jnp.zeros((2, 128), F32)

        @pl.when(sec < SECTIONS - 1)
        def _():
            finish(*steps_r)
            bmsg[0:2, :] = sum_of(rmsg, rbuf1)

        start(*steps_b)

    pl.when(sec == SECTIONS - 1)(step_one)

    @pl.when(sec == 0)
    def _():
        zbuf[...] = jnp.zeros_like(zbuf)

    @pl.when(sec > 0)
    def _():
        pl.when(inner)(lambda: arrived(vbuf, v_recv))
        pl.when(jnp.logical_not(inner))(lambda: arrived(vbuf.at[0:2], v_recv))
        for t in range(TILES):
            z0 = []
            for kg in range(2):
                rows = slice(8 * kg, 8 * kg + 8)
                lane = lanes[t, rows, :]
                tile = tiles[t, rows, :]
                pair = []
                for c in range(2):
                    src = []
                    for m in range(SPAN):
                        at = t + m
                        src.append(bcast(vbuf[at // 2, c : c + 1, (at % 2) * 128 : (at % 2) * 128 + 128]))
                    pair.append(pick(src, lane, tile))
                z0.append(pair)
            power = column_sum(z0[0][0] * z0[0][0] + z0[0][1] * z0[0][1] + (z0[1][0] * z0[1][0] + z0[1][1] * z0[1][1]))
            w = lax.rsqrt(jnp.maximum(power, 1.0))
            vr = vbuf[1, 0:1, t * 128 : (t + 1) * 128]
            vi = vbuf[1, 1:2, t * 128 : (t + 1) * 128]
            xsum[t, 0:1, :] = xsum[t, 0:1, :] + vr
            xsum[t, 1:2, :] = xsum[t, 1:2, :] + vi
            for kg in range(2):
                rows = slice(8 * kg, 8 * kg + 8)
                zr, zi = z0[kg][0] * w, z0[kg][1] * w
                zbuf[t, 0, rows, :] = zr
                zbuf[t, 1, rows, :] = zi
                bvec[t, 0, rows, :] = bvec[t, 0, rows, :] + (zr * vr + zi * vi)
                bvec[t, 1, rows, :] = bvec[t, 1, rows, :] + (zr * vi - zi * vr)

    def keep(solved):
        value, norms = solved
        save(result, value)
        for t, norm in enumerate(norms):
            inverse[t] = norm

    pl.when(sec == 0)(lambda: keep(solve(kre, kim, cvec, sbuf, TILES)))
    pl.when(sec > 0)(lambda: keep(solve_joined(kre, kim, kre2, kim2, cvec, qvec, zbuf, sbuf, gvec, TILES)))

    state = load(result, TILES)
    norms = [inverse[t] for t in range(TILES)]
    for t in range(TILES):
        s = state[4 * t : 4 * t + 4]
        norm = norms[t]
        cr = ci = fr = fi = None
        for kg in range(2):
            rows = slice(8 * kg, 8 * kg + 8)
            sr, si = s[kg], s[2 + kg]
            br, bi = bvec[t, 0, rows, :], bvec[t, 1, rows, :]
            zr, zi = zbuf[t, 0, rows, :], zbuf[t, 1, rows, :]
            a, b = sr * br + si * bi, sr * bi - si * br
            e, f = zr * sr - zi * si, zr * si + zi * sr
            cr = a if kg == 0 else column_sum(cr + a)
            ci = b if kg == 0 else column_sum(ci + b)
            fr = e if kg == 0 else column_sum(fr + e)
            fi = f if kg == 0 else column_sum(fi + f)
        cols = slice(t * 128, (t + 1) * 128)
        msg[0:1, cols] = (cr + (SCALE * START) * xsum[t, 0:1, :]) * norm
        msg[1:2, cols] = (ci + (SCALE * START) * xsum[t, 1:2, :]) * norm
        fr, fi = unit((fr + SCALE * START) * norm, fi * norm)
        fmsg[0:1, cols] = fr
        fmsg[1:2, cols] = fi

    steps_g = [
        remote(gmsg, gbuf.at[d], g_send, g_recv, (s, pix if d == 0 else first[d - 1]))
        for s in range(SECTIONS)
        for d in range(8)
        if (s, d) != (2, 0)
    ]

    @pl.when(sec == 2)
    def _():
        hear(ready.at[3])
        lane = lax.broadcasted_iota(jnp.int32, (16, 128), 1).astype(F32)
        row = lax.broadcasted_iota(jnp.int32, (16, 128), 0)
        for c in range(2):
            total = None
            for t in range(TILES):
                cols = slice(t * 128, (t + 1) * 128)
                value = jnp.where(
                    row == NB,
                    jnp.broadcast_to(fmsg[c : c + 1, cols], (16, 128)),
                    jnp.broadcast_to(msg[c : c + 1, cols], (16, 128)),
                )
                value = jnp.where(ncol[...] - t * 128.0 == lane, value, 0.0)
                total = value if total is None else total + value
            gmsg[c : c + 1, :] = to_row(jnp.sum(total, axis=1, keepdims=True))
        for copy in steps_g:
            copy.start()
        gbuf[0] = gmsg[...]

    @pl.when(sec < SECTIONS - 1)
    def _():
        for i in range(3):
            pl.when(present[i])(remote(msg, vbuf.at[2 - i], v_send, v_recv, (sec_up, near[i])).start)

    for s in range(1, SECTIONS):

        @pl.when(sec == s)
        def _():
            for j in range(s):
                remote(fmsg, fbuf.at[s - 1], f_send, f_recv.at[s - 1], (j, pix)).start()

    @pl.when(sec < 2)
    def _():
        hear(ready.at[2])
        tell(ready.at[3])

    pl.when(sec != 2)(lambda: hear(ready.at[3]))
    comp[0, 0:1, :] = msg[0:1, :]
    comp[1, 0:1, :] = msg[1:2, :]

    def vector():
        for i, (t, c, kg) in enumerate((t, c, kg) for t in range(TILES) for c in range(2) for kg in range(2)):
            sbuf[t, c, 8 * kg : 8 * kg + 8, :] = result[t, c, 8 * kg : 8 * kg + 8, :] * inverse[t]
        for t in range(TILES):

            @pl.loop(0, GROUPS)
            def _(g):
                rows = pl.ds(pl.multiple_of(g * 8, 8), 8)
                re = im = None
                for k in range(NB):
                    sr = bcast(sbuf[t, 0, k : k + 1, :])
                    si = bcast(sbuf[t, 1, k : k + 1, :])
                    zr, zi = zs[t, k, 0, rows, :], zs[t, k, 1, rows, :]
                    a, b = zr * sr - zi * si, zr * si + zi * sr
                    re = a if re is None else re + a
                    im = b if im is None else im + b
                w = wbuf[t, rows, :]
                series[t, 0, rows, :] = bcast((SCALE * START) * inverse[t]) + w * re
                series[t, 1, rows, :] = w * im

    pl.when(sec < SECTIONS - 1)(vector)

    def take_f(j):
        arrived(fbuf.at[j - 1], f_recv.at[j - 1])

    @pl.when(sec == 0)
    def _():
        take_f(1)
        for t in range(TILES):
            fr = fbuf[0, 0:1, t * 128 : (t + 1) * 128]
            fi = fbuf[0, 1:2, t * 128 : (t + 1) * 128]
            re, im = series[t, 0], series[t, 1]
            series[t, 0] = re * fr - im * fi
            series[t, 1] = re * fi + im * fr

    @pl.when(sec < SECTIONS - 1)
    def _():
        for c in range(2):
            rmsg[c : c + 1, :] = to_row(at_ref([series[t, c] for t in range(TILES)]))
        start(*steps_r)

    pl.when(sec < SECTIONS - 1)(step_one)

    pl.when(sec == SECTIONS - 1)(vector)

    @pl.when(sec < SECTIONS - 1)
    def _():
        remote(eall.at[pl.ds(0, 16)], eall.at[pl.ds(0, 16)], y_send, y_recv, (SECTIONS - 1, pix)).wait_recv()
        expand()

    finish(*steps_b)
    total = sum_of(bmsg, bbuf)

    values = [to_column(total[2 + c : 3 + c, :], 16) for c in range(2)]
    f2r, f2i = values[0][NB:16], values[1][NB:16]
    row = lax.broadcasted_iota(jnp.int32, (16, 128), 0)
    zr, zi = (jnp.where(row < NB, value, 0.0) for value in values)
    w = lax.rsqrt(jnp.maximum(column_sum(zr * zr + zi * zi), 1.0))
    zr, zi = zr * w, zi * w
    zref[0, 0] = zr
    zref[0, 1] = zi
    state_ref, norm_ref = solve_joined(kref, kimf, kref2, kimf2, cref, qref, zref, sref, gref, 1)
    sr = jnp.concatenate(state_ref[0:2], axis=0)
    si = jnp.concatenate(state_ref[2:4], axis=0)
    norm = norm_ref[0]
    f3r = column_sum(zr * sr - zi * si)
    f3i = column_sum(zr * si + zi * sr)
    f3r, f3i = unit((f3r + SCALE * START) * norm, f3i * norm)
    fr = jnp.where(sec < 2, f3r * f2r - f3i * f2i, f3r)
    fi = jnp.where(sec < 2, f3r * f2i + f3i * f2r, f3i)
    vr, vi = total[0:1, :], total[1:2, :]
    rmsg[0:1, :] = vr * fr - vi * fi
    rmsg[1:2, :] = vr * fi + vi * fr

    @pl.when(sec == SECTIONS - 1)
    def _():
        z = eall[16:32, :]
        a = bcast(column_sum(z * sr))
        b = bcast(column_sum(z * si))
        re = a - pltpu.roll(b, 64, 1)
        im = b + pltpu.roll(a, 64, 1)
        rmsg[0:1, :] = (re[0:1] + SCALE * START) * norm
        rmsg[1:2, :] = im[0:1] * norm

    ur, ui = unit(rmsg[0:1, :], rmsg[1:2, :])
    ur, ui = GAIN * to_column(ur, PAD), GAIN * to_column(ui, PAD)

    datum[0:1, :] = jnp.ones((1, TILES * 128), F32)
    datum[1:2, :] = jnp.zeros((1, TILES * 128), F32)

    @pl.when(sec < SECTIONS - 1)
    def _():
        take_f(3)
        datum[...] = fbuf[2]

    @pl.when(sec < 2)
    def _():
        take_f(2)
        dr, di = datum[0:1, :], datum[1:2, :]
        fr, fi = fbuf[1, 0:1, :], fbuf[1, 1:2, :]
        datum[0:1, :] = dr * fr - di * fi
        datum[1:2, :] = dr * fi + di * fr

    for t in range(TILES):
        dr, di = datum[0:1, t * 128 : (t + 1) * 128], datum[1:2, t * 128 : (t + 1) * 128]
        re, im = series[t, 0], series[t, 1]
        re, im = re * dr - im * di, re * di + im * dr
        for c, part in enumerate((re * ur + im * ui, im * ur - re * ui)):
            for g in range(GROUPS):
                count = min(8, ROWS - g * 8)
                phases[pl.ds(g * 32 + t * 2 + c, count, stride=4), :] = part[g * 8 : g * 8 + count]

    for i in (0, 2):
        pl.when(present[i])(lambda i=i: arrived(blocks.at[1, pl.ds(0, FLAT)], halo_send.at[i // 2]))
    @pl.when(sec == 2)
    def _():
        arrived(gbuf, g_send)

    @pl.when(sec == SECTIONS - 1)
    def _():
        arrived(ebuf1.at[0:3, 0:16], y_send)

    @pl.when(sec < SECTIONS - 1)
    def _():
        pl.when(inner)(lambda: arrived(vbuf, v_send))
        pl.when(jnp.logical_not(inner))(lambda: arrived(vbuf.at[0:2], v_send))

    for s in range(1, SECTIONS):

        @pl.when(sec == s)
        def _():
            arrived(fbuf.at[0:s], f_send)


def hand_out(phases_in, comp_in, phases, comp, sem):
    copies = [
        pltpu.make_async_copy(phases_in, phases, sem.at[0]),
        pltpu.make_async_copy(comp_in, comp, sem.at[1]),
    ]
    for copy in copies:
        copy.start()
    for copy in copies:
        copy.wait()


def on_device(slc, neighbours, reference_pixel):
    vmem = pl.BlockSpec(memory_space=pltpu.VMEM)
    hbm = pl.BlockSpec(memory_space=pltpu.HBM)
    pixels = slc.shape[2]
    dma = pltpu.SemaphoreType.DMA
    flat = slc.reshape(2, ROWS, TILES, 128).transpose(1, 2, 0, 3).reshape(FLAT, 128)
    phases, comp = pl.pallas_call(
        kernel,
        out_shape=(
            jax.ShapeDtypeStruct((FLAT, 128), F32),
            jax.ShapeDtypeStruct((2, 1, pixels), F32),
        ),
        in_specs=[hbm, hbm, pl.BlockSpec(memory_space=pltpu.SMEM)],
        out_specs=(vmem, vmem),
        scratch_shapes=[
            pltpu.VMEM((NB, pixels), jnp.int32),
            pltpu.VMEM((3, 32 * GROUPS, 128), F32),
            pltpu.VMEM((6, 2, PAD, 128), F32),
            pltpu.VMEM((TILES, 16, 128), jnp.int32),
            pltpu.VMEM((TILES, 16, 128), jnp.int32),
            pltpu.VMEM((TILES, NB, 3, PAD, 128), F32),
            pltpu.VMEM((TILES, PAD, 128), F32),
            pltpu.VMEM((8, 64, 128), F32),
            pltpu.VMEM((TILES, 16, 16, 128), F32),
            pltpu.VMEM((TILES, 16, 16, 128), F32),
            pltpu.VMEM((TILES, 2, 16, 128), F32),
            pltpu.VMEM((TILES, 2, 16, 128), F32),
            pltpu.VMEM((TILES, 2, 128), F32),
            pltpu.VMEM((TILES, 2, 16, 128), F32),
            pltpu.VMEM((TILES, 2, 16, 128), F32),
            pltpu.VMEM((3, 2, pixels), F32),
            pltpu.VMEM((2, pixels), F32),
            pltpu.VMEM((2, pixels), F32),
            pltpu.VMEM((3, 2, pixels), F32),
            pltpu.VMEM((TILES, 2, PAD, 128), F32),
            pltpu.VMEM((2, pixels), F32),
            pltpu.VMEM((1, 128), F32),
            pltpu.VMEM((7, 1, 128), F32),
            pltpu.VMEM((1, 128), F32),
            pltpu.VMEM((7, 1, 128), F32),
            pltpu.VMEM((16, 128), F32),
            pltpu.VMEM((32, 128), F32),
            pltpu.VMEM((7, 32, 128), F32),
            pltpu.VMEM((32, 128), F32),
            pltpu.VMEM((7, 32, 128), F32),
            pltpu.VMEM((32, 128), F32),
            pltpu.VMEM((2, 128), F32),
            pltpu.VMEM((31, 2, 128), F32),
            pltpu.VMEM((2, 128), F32),
            pltpu.VMEM((7, 2, 128), F32),
            pltpu.VMEM((4, 128), F32),
            pltpu.VMEM((7, 4, 128), F32),
            pltpu.VMEM((1, 16, 16, 128), F32),
            pltpu.VMEM((1, 16, 16, 128), F32),
            pltpu.VMEM((1, 2, 16, 128), F32),
            pltpu.VMEM((1, 2, 16, 128), F32),
            pltpu.VMEM((1, 2, 16, 128), F32),
            pltpu.VMEM((TILES, 16, 16, 128), F32),
            pltpu.VMEM((TILES, 16, 16, 128), F32),
            pltpu.VMEM((TILES, 2, 16, 128), F32),
            pltpu.VMEM((TILES, 2, 16, 128), F32),
            pltpu.VMEM((TILES, 2, 16, 128), F32),
            pltpu.VMEM((TILES, 1, 128), F32),
            pltpu.VMEM((1, 16, 16, 128), F32),
            pltpu.VMEM((1, 16, 16, 128), F32),
            pltpu.VMEM((1, 2, 16, 128), F32),
            pltpu.VMEM((1, 2, 16, 128), F32),
            dma((3,)),
            dma((2,)),
            dma((2, 2)),
            dma(()),
            dma(()),
            dma(()),
            dma((3,)),
            dma((2, 2)),
            dma(()),
            dma(()),
            dma(()),
            dma(()),
            dma((2,)),
            dma((2,)),
            pltpu.SemaphoreType.REGULAR((4,)),
        ],
        compiler_params=pltpu.CompilerParams(
            collective_id=0, has_side_effects=True, vmem_limit_bytes=16 * 2**20
        ),
        cost_estimate=pl.CostEstimate(flops=100_000_000, bytes_accessed=1_000_000, transcendentals=0),
    )(*(pltpu.with_memory_space_constraint(a, pltpu.HBM) for a in (flat, neighbours)), reference_pixel)
    phases, comp = pl.pallas_call(
        hand_out,
        out_shape=(
            jax.ShapeDtypeStruct((FLAT, 128), F32),
            jax.ShapeDtypeStruct((2, 1, pixels), F32),
        ),
        in_specs=[pl.BlockSpec(memory_space=pl.ANY)] * 2,
        out_specs=(hbm, hbm),
        scratch_shapes=[dma((2,))],
        compiler_params=pltpu.CompilerParams(vmem_limit_bytes=2**20),
    )(phases, comp)
    return phases.reshape(ROWS, TILES, 2, 128).transpose(2, 0, 1, 3).reshape(2, ROWS, pixels), comp


def solution(mesh):
    return jax.shard_map(
        on_device,
        mesh=mesh,
        in_specs=(P(None, "section", "pix"), P(None, "pix"), P()),
        out_specs=(P(None, "section", "pix"), P(None, "section", "pix")),
        check_vma=False,
    )
```

```python
import math

import jax
import jax.numpy as jnp
from jax import lax
from jax.experimental import pallas as pl
from jax.experimental.pallas import tpu as pltpu
from jax.sharding import PartitionSpec as P

ITERS = 16
FLOOR = 0.05
REACH = 256
NB = 15
ROWS = 50
PAD = 56
GROUPS = PAD // 8
FLAT = 4 * ROWS
TILES = 2
SPAN = 5
SCALE = 2.0**-45
START = 1.0 / math.sqrt(ROWS + 1)
GAIN = math.sqrt(ROWS + 1)
SECTIONS = 4
PIX = 64
MESH = pl.DeviceIdType.MESH
F32 = jnp.float32


def bcast(row):
    return jnp.broadcast_to(row, (8, 128))


def pick(sources, lane, tile):
    out = jnp.zeros((8, 128), F32)
    for m, source in enumerate(sources):
        out = jnp.where(tile == m, take(source, lane), out)
    return out


def take(source, lane):
    return jnp.take_along_axis(source, lane, axis=1, mode="promise_in_bounds")


def column_sum(x):
    return jnp.sum(x, axis=0, keepdims=True)


def eye(count, shift=0):
    lane = lax.broadcasted_iota(jnp.int32, (count, 128), 1)
    return lane == lax.broadcasted_iota(jnp.int32, (count, 128), 0) + shift


def to_row(column, shift=0):
    return column_sum(jnp.where(eye(column.shape[0], shift), column, 0.0))


def to_column(row, count):
    spread = jnp.broadcast_to(row, (count, 128))
    return jnp.sum(jnp.where(eye(count), spread, 0.0), axis=1, keepdims=True)


def unit(re, im):
    scale = 1.0 / jnp.maximum(jnp.sqrt(re * re + im * im), FLOOR)
    return re * scale, im * scale


def remote(src, dst, send, recv, device):
    return pltpu.make_async_remote_copy(
        src_ref=src, dst_ref=dst, send_sem=send, recv_sem=recv, device_id=device, device_id_type=MESH
    )


def kernel(
    slc_hbm, nbr_hbm, ref, phases, comp,
    nbr, blocks, ext, lanes, tiles, zs, wbuf, red, kre, kim, cvec, bvec, xsum, zbuf, sbuf,
    vbuf, msg, fmsg, fbuf, series, datum,
    nmsg, nbuf1, nmsg2, nbuf2, ncol, emsg, ebuf1, emsg2, ebuf2, eall, gmsg, gbuf, rmsg, rbuf1, bmsg, bbuf,
    kref, kimf, cref, zref, sref, kre2, kim2, qvec, gvec, result, inverse, kref2, kimf2, qref, gref,
    ksum, ksum2, ksumf, ksumf2,
    load_sem, halo_send, halo_recv, v_send, v_recv, f_send, f_recv, early_sem,
    y_send, y_recv, g_send, g_recv, r_sem, b_sem, ready,
):
    sec = lax.axis_index("section")
    pix = lax.axis_index("pix")
    before = lax.rem(pix + (PIX - 1), PIX)
    after = lax.rem(pix + 1, PIX)
    near = (before, pix, after)
    present = (pix > 0, pix >= 0, pix < PIX - 1)
    inner = jnp.logical_and(present[0], present[2])
    sec_up = lax.rem(sec + 1, SECTIONS)
    sec_down = lax.rem(sec + (SECTIONS - 1), SECTIONS)
    x = pix // 16
    z = lax.rem(pix // 2, 8)
    core = lax.rem(pix, 2)
    group = x * 2 + core
    first = []
    second = []
    for d in range(1, 8):
        g = lax.rem(group + d, 8)
        first.append((g // 2) * 16 + z * 2 + lax.rem(g, 2))
        second.append(x * 16 + lax.rem(z + d, 8) * 2 + core)

    want = ref[0] - pix * (TILES * 128)

    def at_ref(parts):
        total = None
        for t, part in enumerate(parts):
            lane = lax.broadcasted_iota(jnp.int32, part.shape, 1)
            part = jnp.where(lane == want - t * 128, part, 0.0)
            total = part if total is None else total + part
        return jnp.sum(total, axis=1, keepdims=True)

    def arrived(ref, sem):
        pltpu.make_async_copy(ref, ref, sem).wait()

    def start(src, dst, sem, devices):
        for i, device in enumerate(devices):
            remote(src, dst.at[i], sem.at[0], sem.at[1], (sec, device)).start()

    def finish(src, dst, sem, devices):
        arrived(dst, sem.at[0])
        arrived(dst, sem.at[1])

    def sum_of(own, buffers):
        total = own[...]
        for i in range(7):
            total = total + buffers[i]
        return total

    steps_n = (nmsg, nbuf1, early_sem.at[0], first), (nmsg2, nbuf2, early_sem.at[1], second)
    steps_e = (emsg, ebuf1, early_sem.at[0], first), (emsg2, ebuf2, early_sem.at[1], second)
    steps_r = (rmsg, rbuf1, r_sem, first)
    steps_b = (bmsg, bbuf, b_sem, second)

    chunks = [(0, 3), (3, GROUPS)]
    spans = [pl.ds(32 * low, min(32 * high, FLAT) - 32 * low) for low, high in chunks]
    loads = [
        pltpu.make_async_copy(slc_hbm.at[span], blocks.at[1, span], load_sem.at[i]) for i, span in enumerate(spans)
    ]
    loads.append(pltpu.make_async_copy(nbr_hbm, nbr, load_sem.at[2]))
    for load in loads:
        load.start()
    barrier = pltpu.get_barrier_semaphore()
    peers = [(sec, before), (sec, after), (sec_up, pix), (sec_down, pix)]
    peers += [(sec, x * 16 + lax.rem(z + d, 8) * 2 + core) for d in (1, 7)]
    peers += [(sec, lax.rem(x + d, 4) * 16 + z * 2 + core) for d in (1, 3)]

    def tell(sem):
        for peer in peers:
            pl.semaphore_signal(sem, inc=1, device_id=peer, device_id_type=MESH)

    def hear(sem):
        pl.semaphore_wait(sem, len(peers))

    tell(barrier)
    hear(barrier)
    tell(ready.at[0])

    def halo(i, n):
        part = blocks.at[1, spans[n]]
        return remote(part, blocks.at[2 - i, spans[n]], halo_send.at[i // 2], halo_recv.at[i // 2, n], (sec, near[i]))

    for n in range(len(chunks)):
        loads[n].wait()
        for i in (0, 2):
            pl.when(present[i])(halo(i, n).start)

    for i in range(3):
        blocks[i, FLAT:, :] = jnp.zeros((32 * GROUPS - FLAT, 128), F32)
    kre[...] = jnp.zeros_like(kre)
    kim[...] = jnp.zeros_like(kim)
    red[...] = jnp.zeros_like(red)
    cvec[...] = jnp.zeros_like(cvec)
    bvec[...] = jnp.zeros_like(bvec)
    for i in (0, 2):

        @pl.when(jnp.logical_not(present[i]))
        def _():
            blocks[i] = jnp.zeros((32 * GROUPS, 128), F32)
            vbuf[i] = jnp.zeros_like(vbuf[i])

    loads[2].wait()

    base = pix * (TILES * 128) - REACH
    for t in range(TILES):
        rel = nbr[:, t * 128 : (t + 1) * 128] - (base + t * 128)
        lanes[t, 0:NB, :] = jnp.bitwise_and(rel, 127)
        tiles[t, 0:NB, :] = jnp.right_shift(rel, 7)
        lanes[t, NB : NB + 1, :] = jnp.zeros((1, 128), jnp.int32)
        tiles[t, NB : NB + 1, :] = jnp.full((1, 128), SPAN, jnp.int32)

    def spread(i, groups=range(GROUPS)):
        for g in groups:
            for m in range(2):
                for c in range(2):
                    ext[2 * i + m, c, g * 8 : (g + 1) * 8, :] = blocks[i, pl.ds(g * 32 + m * 2 + c, 8, stride=4), :]

    spread(1)
    for t in range(TILES):
        for c in range(2):
            total = None
            for g in range(GROUPS):
                own = ext[2 + t, c, g * 8 : (g + 1) * 8, :]
                zs[t, 0, c, g * 8 : (g + 1) * 8, :] = own
                total = own if total is None else total + own
            xsum[t, c : c + 1, :] = column_sum(total)

    def gather(t, offsets, begin, groups=range(GROUPS), halves=None):
        def some(half):
            for i in range(NB // 2):
                k = 1 + half * (NB // 2) + i
                lane = bcast(lanes[t, pl.ds(k, 1), :])
                tile = bcast(tiles[t, pl.ds(k, 1), :])
                for g in groups:
                    rows = slice(g * 8, (g + 1) * 8)
                    for c in range(2):
                        out = None if begin else zs[t, k, c, rows, :]
                        for m in offsets:
                            got = take(ext[t + m, c, rows, :], lane)
                            out = got if out is None else jnp.where(tile == m, got, out)
                        zs[t, k, c, rows, :] = out

        if halves is None:
            pl.loop(0, 2)(some)
        else:
            for half in halves:
                some(half)

    for t in range(TILES):
        gather(t, (2 - t, 3 - t), True)

    def side(s, groups, halves=None):
        spread(2 * s, groups)
        close, distant = 1 + 3 * s, 5 * s
        gather(s, (close - s, distant - s), False, groups, halves)
        gather(1 - s, (close - (1 - s),), False, groups, halves)

    def both(soon):
        late = 1 - soon
        for n in range(len(chunks)):
            arrived(blocks.at[2 * soon, spans[n]], halo_recv.at[1 - soon, n])
        side(soon, range(GROUPS))
        hear(ready.at[0])
        tell(ready.at[1])
        for n, (low, high) in enumerate(chunks):
            pl.when(inner)(lambda n=n: arrived(blocks.at[2 * late, spans[n]], halo_recv.at[1 - late, n]))
            side(late, range(low, high), range(2))

    pl.when(core == 0)(lambda: both(1))
    pl.when(core == 1)(lambda: both(0))

    @pl.when(sec >= 2)
    def _():
        hear(ready.at[1])
        tell(ready.at[2])

    @pl.when(sec == 2)
    def _():
        column = at_ref([nbr[:, t * 128 : (t + 1) * 128].astype(F32) for t in range(TILES)])
        nmsg[...] = to_row(column)
        start(*steps_n[0])

    @pl.loop(0, TILES)
    def _(t):
        for g in range(GROUPS):
            rows = slice(g * 8, (g + 1) * 8)
            power = None
            for k in range(NB):
                re, im = zs[t, k, 0, rows, :], zs[t, k, 1, rows, :]
                zs[t, k, 2, rows, :] = re - im
                term = re * re + im * im
                power = term if power is None else power + term
            wbuf[t, rows, :] = lax.rsqrt(jnp.maximum(power, 1.0))

        def fold(slot, parts):
            for i, part in enumerate(parts):
                red[slot, i * 8 : (i + 1) * 8, :] = part
            total = None
            for i in range(8):
                row = red[slot, pl.ds(i, 8, stride=8), :]
                total = row if total is None else total + row
            return total

        slot = 0
        for l in range(NB + 1):
            for kg in range(2):
                low, high = 8 * kg, min(8 * kg + 8, l + 1, NB)
                if high <= low:
                    continue
                count = high - low
                p, q, r = [None] * count, [None] * count, [None] * count
                cr, ci = [None] * count, [None] * count

                def put(box, i, value):
                    box[i] = value if box[i] is None else box[i] + value

                for g in range(GROUPS):
                    rows = slice(g * 8, (g + 1) * 8)
                    w = wbuf[t, rows, :]
                    if l < NB:
                        w2 = w * w
                        lr, li = zs[t, l, 0, rows, :] * w2, zs[t, l, 1, rows, :] * w2
                    else:
                        lr, li = zs[t, 0, 0, rows, :] * w, zs[t, 0, 1, rows, :] * w
                    le = lr + li
                    for i in range(count):
                        k = low + i
                        kr, ki = zs[t, k, 0, rows, :], zs[t, k, 1, rows, :]
                        put(p, i, kr * lr)
                        put(q, i, ki * li)
                        if k != l:
                            put(r, i, zs[t, k, 2, rows, :] * le)
                        if l == NB:
                            put(cr, i, kr * w)
                            put(ci, i, ki * w)
                re = fold(4 * kg + slot, [a + b for a, b in zip(p, q)])
                im = fold(4 * kg + slot + 1, [jnp.zeros((8, 128), F32) if c is None else c + (b - a) for a, b, c in zip(p, q, r)])
                rows = slice(low, low + 8)
                if l < NB:
                    kre[t, l, rows, :] = re
                    kim[t, l, rows, :] = im
                    for i in range(count):
                        k = low + i
                        if k != l:
                            kre[t, k, l : l + 1, :] = re[i : i + 1, :]
                            kim[t, k, l : l + 1, :] = -im[i : i + 1, :]
                else:
                    bvec[t, 0, rows, :] = re
                    bvec[t, 1, rows, :] = im
                    slot = 2 - slot
                    cvec[t, 0, rows, :] = START * fold(4 * kg + slot, cr)
                    cvec[t, 1, rows, :] = -START * fold(4 * kg + slot + 1, ci)
                slot = 2 - slot
        ksum[t] = kre[t] + kim[t]

    def pieces(count):
        return [(t, c, kg) for t in range(count) for c in range(2) for kg in range(2)]

    def load(ref, count):
        return [ref[t, c, 8 * kg : 8 * kg + 8, :] for t, c, kg in pieces(count)]

    def save(ref, value):
        for (t, c, kg), part in zip(pieces(len(value) // 4), value):
            ref[t, c, 8 * kg : 8 * kg + 8, :] = part

    def plus(*values):
        return [sum(parts[1:], parts[0]) for parts in zip(*values)]

    def times(factor, value):
        return [factor * part for part in value]

    def product(m, box, value):
        for t in range(len(value) // 4):
            for kg in range(2):
                re, im = value[4 * t + kg], value[4 * t + 2 + kg]
                for c, part in enumerate((re, im, re + im)):
                    box[t, c, 8 * kg : 8 * kg + 8, :] = part
        out = []
        for t in range(len(value) // 4):
            y = [[None, None] for _ in range(3)]
            for l in range(NB):
                for c in range(3):
                    row = bcast(box[t, c, l : l + 1, :])
                    for kg in range(2):
                        part = m[c][t, l, 8 * kg : 8 * kg + 8, :] * row
                        y[c][kg] = part if l == 0 else y[c][kg] + part
            out += [y[0][kg] - y[1][kg] for kg in range(2)]
            out += [y[2][kg] - (y[0][kg] + y[1][kg]) for kg in range(2)]
        return out

    def prepare(m3, s3, cv, qv, box, count):
        mr, mi, _ = m3
        sr, si, _ = s3
        for t in range(count):

            @pl.loop(0, NB)
            def _(l):
                for kg in range(2):
                    rows = slice(8 * kg, 8 * kg + 8)
                    re, im = 2.0 * mr[t, l, rows, :], 2.0 * mi[t, l, rows, :]
                    for m in range(NB):
                        lr = bcast(mr[t, l, m : m + 1, :])
                        li = bcast(mi[t, l, m : m + 1, :])
                        ar, ai = mr[t, m, rows, :], mi[t, m, rows, :]
                        re = re + (ar * lr - ai * li)
                        im = im + (ar * li + ai * lr)
                    sr[t, l, rows, :] = re
                    si[t, l, rows, :] = im

        save(qv, product(m3, box, load(cv, count)))

    def joined(z, value):
        out = []
        for t in range(len(value) // 4):
            zr, zi = z[4 * t : 4 * t + 2], z[4 * t + 2 : 4 * t + 4]
            vr, vi = value[4 * t : 4 * t + 2], value[4 * t + 2 : 4 * t + 4]
            ar = column_sum(zr[0] * vr[0] - zi[0] * vi[0] + (zr[1] * vr[1] - zi[1] * vi[1]))
            ai = column_sum(zr[0] * vi[0] + zi[0] * vr[0] + (zr[1] * vi[1] + zi[1] * vr[1]))
            out += [zr[i] * ar + zi[i] * ai for i in range(2)] + [zr[i] * ai - zi[i] * ar for i in range(2)]
        return out

    def conj(value):
        return [part if (i // 2) % 2 == 0 else -part for i, part in enumerate(value)]

    def norms_of(value, image, start):
        out = []
        for t in range(len(value) // 4):
            total = None
            for i in range(4 * t, 4 * t + 4):
                term = value[i] * (image[i] + (2.0 * SCALE) * start[i])
                total = term if total is None else total + term
            out.append(lax.rsqrt(column_sum(total) + SCALE * SCALE))
        return out

    def solve(m3, cv, box, count):
        def turn(_, value):
            return tuple(plus(value, product(m3, box, value), load(cv, count)))

        value = lax.fori_loop(0, ITERS - 1, turn, tuple(load(cv, count)))
        value = times(SCALE, value)
        return value, norms_of(value, product(m3, box, value), load(cv, count))

    def solve_joined(m3, s3, cv, qv, zv, box, gbox, count):
        z = load(zv, count)
        r = conj(z)
        kr = product(m3, box, r)
        c = plus(load(cv, count), times(START, r))
        g = plus(r, kr)
        for t in range(count):
            squares = [z[4 * t + i] * z[4 * t + i] for i in range(4)]
            half = 0.5 * column_sum(squares[0] + squares[1] + (squares[2] + squares[3]))
            for i in range(4 * t, 4 * t + 4):
                g[i] = g[i] + half * r[i]
        save(gbox, g)
        sr, si, both = s3
        for t in range(count):
            for l in range(NB):
                zr, zi = bcast(zv[t, 0, l : l + 1, :]), bcast(zv[t, 1, l : l + 1, :])
                gr, gi = bcast(gbox[t, 0, l : l + 1, :]), bcast(gbox[t, 1, l : l + 1, :])
                for kg in range(2):
                    rows = slice(8 * kg, 8 * kg + 8)
                    hr, hi = g[4 * t + kg], g[4 * t + 2 + kg]
                    xr, xi = z[4 * t + kg], z[4 * t + 2 + kg]
                    re = sr[t, l, rows, :] + (hr * zr - hi * zi + (xr * gr - xi * gi))
                    im = si[t, l, rows, :] + (hr * zi + hi * zr - (xr * gi + xi * gr))
                    sr[t, l, rows, :] = re
                    si[t, l, rows, :] = im
                    both[t, l, rows, :] = re + im

        def square(value):
            return plus(value, product(s3, box, value))

        value = plus(c, c, load(qv, count), times(START, kr), joined(z, c))
        value = plus(value, square(value))
        value = plus(value, square(square(value)))

        last = lax.fori_loop(0, 4, lambda _, v: tuple(square(v)), tuple(value))
        value = times(SCALE, plus(value, last))
        image = plus(product(m3, box, value), joined(z, value))
        return value, norms_of(value, image, c)

    @pl.when(sec == 1)
    def _():
        hear(ready.at[1])
        tell(ready.at[2])

    def prepare_own():
        prepare((kre, kim, ksum), (kre2, kim2, ksum2), cvec, qvec, sbuf, TILES)

    pl.when(jnp.logical_or(sec == 1, sec == 2))(prepare_own)

    @pl.when(sec == 2)
    def _():
        finish(*steps_n[0])
        hear(ready.at[2])
        tell(ready.at[3])
        nmsg2[...] = sum_of(nmsg, nbuf1)
        start(*steps_n[1])

    def expand():
        for l in range(NB):
            kref[0, l] = jnp.broadcast_to(eall[0:16, l : l + 1], (16, 128))
            kimf[0, l] = jnp.broadcast_to(eall[0:16, 16 + l : 17 + l], (16, 128))
        for c in range(2):
            cref[0, c] = jnp.broadcast_to(eall[0:16, 32 + c : 33 + c], (16, 128))
        ksumf[...] = kref[...] + kimf[...]
        prepare((kref, kimf, ksumf), (kref2, kimf2, ksumf2), cref, qref, sref, 1)

    @pl.when(sec == SECTIONS - 1)
    def _():
        lane = lax.broadcasted_iota(jnp.int32, (16, 128), 1)
        emsg[16:32, :] = jnp.zeros((16, 128), F32)
        acc = jnp.zeros((16, 128), F32)
        for c in range(2):
            acc = jnp.where(lane == 32 + c, at_ref([cvec[t, c] for t in range(TILES)]), acc)
        emsg[0:16, :] = acc

        @pl.loop(0, NB)
        def _(k):
            acc = emsg[0:16, :]
            acc = jnp.where(lane == k, at_ref([kre[t, k] for t in range(TILES)]), acc)
            emsg[0:16, :] = jnp.where(lane == 16 + k, at_ref([kim[t, k] for t in range(TILES)]), acc)
            parts = [at_ref([zs[t, k, c] * wbuf[t] for t in range(TILES)]) for c in range(2)]
            emsg[pl.ds(16 + k, 1), :] = to_row(parts[0]) + to_row(parts[1], 64)

        start(*steps_e[0])
        prepare_own()
        finish(*steps_e[0])
        hear(ready.at[2])
        tell(ready.at[3])
        emsg2[...] = sum_of(emsg, ebuf1)
        start(*steps_e[1])
        finish(*steps_e[1])
        eall[...] = sum_of(emsg2, ebuf2)
        for j in range(SECTIONS - 1):
            remote(eall.at[pl.ds(0, 16)], eall.at[pl.ds(0, 16)], y_send, y_recv, (j, pix)).start()
        expand()

    @pl.when(sec == 2)
    def _():
        finish(*steps_n[1])
        column = to_column(sum_of(nmsg2, nbuf2), 16)
        row = lax.broadcasted_iota(jnp.int32, (16, 128), 0)
        ncol[...] = jnp.where(row == NB, ref[0].astype(F32), column) - (pix * (TILES * 128)).astype(F32)

    def step_one():
        @pl.when(sec == 2)
        def _():
            arrived(gbuf.at[1:8], g_recv)

        @pl.when(sec != 2)
        def _():
            arrived(gbuf.at[0:8], g_recv)

        total = gbuf[0]
        for d in range(1, 8):
            total = total + gbuf[d]
        bmsg[2:4, :] = total
        bmsg[0:2, :] = jnp.zeros((2, 128), F32)

        @pl.when(sec < SECTIONS - 1)
        def _():
            finish(*steps_r)
            bmsg[0:2, :] = sum_of(rmsg, rbuf1)

        start(*steps_b)

    pl.when(sec == SECTIONS - 1)(step_one)

    def keep(solved):
        value, norms = solved
        save(result, value)
        for t, norm in enumerate(norms):
            inverse[t] = norm

    @pl.when(sec == 0)
    def _():
        zbuf[...] = jnp.zeros_like(zbuf)
        keep(solve((kre, kim, ksum), cvec, sbuf, TILES))

    @pl.when(sec > 0)
    def _():
        pl.when(inner)(lambda: arrived(vbuf, v_recv))
        pl.when(jnp.logical_not(inner))(lambda: arrived(vbuf.at[0:2], v_recv))
        for t in range(TILES):
            z0 = []
            for kg in range(2):
                rows = slice(8 * kg, 8 * kg + 8)
                lane = lanes[t, rows, :]
                tile = tiles[t, rows, :]
                pair = []
                for c in range(2):
                    src = []
                    for m in range(SPAN):
                        at = t + m
                        src.append(bcast(vbuf[at // 2, c : c + 1, (at % 2) * 128 : (at % 2) * 128 + 128]))
                    pair.append(pick(src, lane, tile))
                z0.append(pair)
            power = column_sum(z0[0][0] * z0[0][0] + z0[0][1] * z0[0][1] + (z0[1][0] * z0[1][0] + z0[1][1] * z0[1][1]))
            w = lax.rsqrt(jnp.maximum(power, 1.0))
            vr = vbuf[1, 0:1, t * 128 : (t + 1) * 128]
            vi = vbuf[1, 1:2, t * 128 : (t + 1) * 128]
            xsum[t, 0:1, :] = xsum[t, 0:1, :] + vr
            xsum[t, 1:2, :] = xsum[t, 1:2, :] + vi
            for kg in range(2):
                rows = slice(8 * kg, 8 * kg + 8)
                zr, zi = z0[kg][0] * w, z0[kg][1] * w
                zbuf[t, 0, rows, :] = zr
                zbuf[t, 1, rows, :] = zi
                bvec[t, 0, rows, :] = bvec[t, 0, rows, :] + (zr * vr + zi * vi)
                bvec[t, 1, rows, :] = bvec[t, 1, rows, :] + (zr * vi - zi * vr)
        keep(solve_joined((kre, kim, ksum), (kre2, kim2, ksum2), cvec, qvec, zbuf, sbuf, gvec, TILES))

    state = load(result, TILES)
    norms = [inverse[t] for t in range(TILES)]
    for t in range(TILES):
        s = state[4 * t : 4 * t + 4]
        norm = norms[t]
        cr = ci = fr = fi = None
        for kg in range(2):
            rows = slice(8 * kg, 8 * kg + 8)
            sr, si = s[kg], s[2 + kg]
            br, bi = bvec[t, 0, rows, :], bvec[t, 1, rows, :]
            zr, zi = zbuf[t, 0, rows, :], zbuf[t, 1, rows, :]
            a, b = sr * br + si * bi, sr * bi - si * br
            e, f = zr * sr - zi * si, zr * si + zi * sr
            cr = a if kg == 0 else column_sum(cr + a)
            ci = b if kg == 0 else column_sum(ci + b)
            fr = e if kg == 0 else column_sum(fr + e)
            fi = f if kg == 0 else column_sum(fi + f)
        cols = slice(t * 128, (t + 1) * 128)
        msg[0:1, cols] = (cr + (SCALE * START) * xsum[t, 0:1, :]) * norm
        msg[1:2, cols] = (ci + (SCALE * START) * xsum[t, 1:2, :]) * norm
        fr, fi = unit((fr + SCALE * START) * norm, fi * norm)
        fmsg[0:1, cols] = fr
        fmsg[1:2, cols] = fi

    steps_g = [
        remote(gmsg, gbuf.at[d], g_send, g_recv, (s, pix if d == 0 else first[d - 1]))
        for s in range(SECTIONS)
        for d in range(8)
        if (s, d) != (2, 0)
    ]

    @pl.when(sec == 2)
    def _():
        hear(ready.at[3])
        lane = lax.broadcasted_iota(jnp.int32, (16, 128), 1).astype(F32)
        row = lax.broadcasted_iota(jnp.int32, (16, 128), 0)
        for c in range(2):
            total = None
            for t in range(TILES):
                cols = slice(t * 128, (t + 1) * 128)
                value = jnp.where(
                    row == NB,
                    jnp.broadcast_to(fmsg[c : c + 1, cols], (16, 128)),
                    jnp.broadcast_to(msg[c : c + 1, cols], (16, 128)),
                )
                value = jnp.where(ncol[...] - t * 128.0 == lane, value, 0.0)
                total = value if total is None else total + value
            gmsg[c : c + 1, :] = to_row(jnp.sum(total, axis=1, keepdims=True))
        for copy in steps_g:
            copy.start()
        gbuf[0] = gmsg[...]

    @pl.when(sec < SECTIONS - 1)
    def _():
        for i in range(3):
            pl.when(present[i])(remote(msg, vbuf.at[2 - i], v_send, v_recv, (sec_up, near[i])).start)

    for s in range(1, SECTIONS):

        @pl.when(sec == s)
        def _():
            for j in range(s):
                remote(fmsg, fbuf.at[s - 1], f_send, f_recv.at[s - 1], (j, pix)).start()

    @pl.when(sec == 0)
    def _():
        hear(ready.at[1])
        tell(ready.at[2])

    @pl.when(sec < 2)
    def _():
        hear(ready.at[2])
        tell(ready.at[3])

    pl.when(sec != 2)(lambda: hear(ready.at[3]))
    comp[0, 0:1, :] = msg[0:1, :]
    comp[1, 0:1, :] = msg[1:2, :]

    def vector():
        for i, (t, c, kg) in enumerate((t, c, kg) for t in range(TILES) for c in range(2) for kg in range(2)):
            sbuf[t, c, 8 * kg : 8 * kg + 8, :] = result[t, c, 8 * kg : 8 * kg + 8, :] * inverse[t]
        for t in range(TILES):

            @pl.loop(0, GROUPS)
            def _(g):
                rows = pl.ds(pl.multiple_of(g * 8, 8), 8)
                re = im = None
                for k in range(NB):
                    sr = bcast(sbuf[t, 0, k : k + 1, :])
                    si = bcast(sbuf[t, 1, k : k + 1, :])
                    zr, zi = zs[t, k, 0, rows, :], zs[t, k, 1, rows, :]
                    a, b = zr * sr - zi * si, zr * si + zi * sr
                    re = a if re is None else re + a
                    im = b if im is None else im + b
                w = wbuf[t, rows, :]
                series[t, 0, rows, :] = bcast((SCALE * START) * inverse[t]) + w * re
                series[t, 1, rows, :] = w * im

    pl.when(sec < SECTIONS - 1)(vector)

    def take_f(j):
        arrived(fbuf.at[j - 1], f_recv.at[j - 1])

    @pl.when(sec == 0)
    def _():
        take_f(1)
        for t in range(TILES):
            fr = fbuf[0, 0:1, t * 128 : (t + 1) * 128]
            fi = fbuf[0, 1:2, t * 128 : (t + 1) * 128]
            re, im = series[t, 0], series[t, 1]
            series[t, 0] = re * fr - im * fi
            series[t, 1] = re * fi + im * fr

    @pl.when(sec < SECTIONS - 1)
    def _():
        for c in range(2):
            rmsg[c : c + 1, :] = to_row(at_ref([series[t, c] for t in range(TILES)]))
        start(*steps_r)

    pl.when(sec < SECTIONS - 1)(step_one)

    pl.when(sec == SECTIONS - 1)(vector)

    @pl.when(sec < SECTIONS - 1)
    def _():
        remote(eall.at[pl.ds(0, 16)], eall.at[pl.ds(0, 16)], y_send, y_recv, (SECTIONS - 1, pix)).wait_recv()
        expand()

    finish(*steps_b)
    total = sum_of(bmsg, bbuf)

    values = [to_column(total[2 + c : 3 + c, :], 16) for c in range(2)]
    f2r, f2i = values[0][NB:16], values[1][NB:16]
    row = lax.broadcasted_iota(jnp.int32, (16, 128), 0)
    zr, zi = (jnp.where(row < NB, value, 0.0) for value in values)
    w = lax.rsqrt(jnp.maximum(column_sum(zr * zr + zi * zi), 1.0))
    zr, zi = zr * w, zi * w
    zref[0, 0] = zr
    zref[0, 1] = zi
    state_ref, norm_ref = solve_joined((kref, kimf, ksumf), (kref2, kimf2, ksumf2), cref, qref, zref, sref, gref, 1)
    sr = jnp.concatenate(state_ref[0:2], axis=0)
    si = jnp.concatenate(state_ref[2:4], axis=0)
    norm = norm_ref[0]
    f3r = column_sum(zr * sr - zi * si)
    f3i = column_sum(zr * si + zi * sr)
    f3r, f3i = unit((f3r + SCALE * START) * norm, f3i * norm)
    fr = jnp.where(sec < 2, f3r * f2r - f3i * f2i, f3r)
    fi = jnp.where(sec < 2, f3r * f2i + f3i * f2r, f3i)
    vr, vi = total[0:1, :], total[1:2, :]
    rmsg[0:1, :] = vr * fr - vi * fi
    rmsg[1:2, :] = vr * fi + vi * fr

    @pl.when(sec == SECTIONS - 1)
    def _():
        z = eall[16:32, :]
        a = bcast(column_sum(z * sr))
        b = bcast(column_sum(z * si))
        re = a - pltpu.roll(b, 64, 1)
        im = b + pltpu.roll(a, 64, 1)
        rmsg[0:1, :] = (re[0:1] + SCALE * START) * norm
        rmsg[1:2, :] = im[0:1] * norm

    ur, ui = unit(rmsg[0:1, :], rmsg[1:2, :])
    ur, ui = GAIN * to_column(ur, PAD), GAIN * to_column(ui, PAD)

    datum[0:1, :] = jnp.ones((1, TILES * 128), F32)
    datum[1:2, :] = jnp.zeros((1, TILES * 128), F32)

    @pl.when(sec < SECTIONS - 1)
    def _():
        take_f(3)
        datum[...] = fbuf[2]

    @pl.when(sec < 2)
    def _():
        take_f(2)
        dr, di = datum[0:1, :], datum[1:2, :]
        fr, fi = fbuf[1, 0:1, :], fbuf[1, 1:2, :]
        datum[0:1, :] = dr * fr - di * fi
        datum[1:2, :] = dr * fi + di * fr

    for t in range(TILES):
        dr, di = datum[0:1, t * 128 : (t + 1) * 128], datum[1:2, t * 128 : (t + 1) * 128]
        re, im = series[t, 0], series[t, 1]
        re, im = re * dr - im * di, re * di + im * dr
        for c, part in enumerate((re * ur + im * ui, im * ur - re * ui)):
            for g in range(GROUPS):
                count = min(8, ROWS - g * 8)
                phases[pl.ds(g * 32 + t * 2 + c, count, stride=4), :] = part[g * 8 : g * 8 + count]

    for i in (0, 2):
        pl.when(present[i])(lambda i=i: arrived(blocks.at[1, pl.ds(0, FLAT)], halo_send.at[i // 2]))
    @pl.when(sec == 2)
    def _():
        arrived(gbuf, g_send)

    @pl.when(sec == SECTIONS - 1)
    def _():
        arrived(ebuf1.at[0:3, 0:16], y_send)

    @pl.when(sec < SECTIONS - 1)
    def _():
        pl.when(inner)(lambda: arrived(vbuf, v_send))
        pl.when(jnp.logical_not(inner))(lambda: arrived(vbuf.at[0:2], v_send))

    for s in range(1, SECTIONS):

        @pl.when(sec == s)
        def _():
            arrived(fbuf.at[0:s], f_send)


def hand_out(phases_in, comp_in, phases, comp, sem):
    copies = [
        pltpu.make_async_copy(phases_in, phases, sem.at[0]),
        pltpu.make_async_copy(comp_in, comp, sem.at[1]),
    ]
    for copy in copies:
        copy.start()
    for copy in copies:
        copy.wait()


def on_device(slc, neighbours, reference_pixel):
    vmem = pl.BlockSpec(memory_space=pltpu.VMEM)
    hbm = pl.BlockSpec(memory_space=pltpu.HBM)
    pixels = slc.shape[2]
    dma = pltpu.SemaphoreType.DMA
    flat = slc.reshape(2, ROWS, TILES, 128).transpose(1, 2, 0, 3).reshape(FLAT, 128)
    phases, comp = pl.pallas_call(
        kernel,
        out_shape=(
            jax.ShapeDtypeStruct((FLAT, 128), F32),
            jax.ShapeDtypeStruct((2, 1, pixels), F32),
        ),
        in_specs=[hbm, hbm, pl.BlockSpec(memory_space=pltpu.SMEM)],
        out_specs=(vmem, vmem),
        scratch_shapes=[
            pltpu.VMEM((NB, pixels), jnp.int32),
            pltpu.VMEM((3, 32 * GROUPS, 128), F32),
            pltpu.VMEM((6, 2, PAD, 128), F32),
            pltpu.VMEM((TILES, 16, 128), jnp.int32),
            pltpu.VMEM((TILES, 16, 128), jnp.int32),
            pltpu.VMEM((TILES, NB, 3, PAD, 128), F32),
            pltpu.VMEM((TILES, PAD, 128), F32),
            pltpu.VMEM((8, 64, 128), F32),
            pltpu.VMEM((TILES, 16, 16, 128), F32),
            pltpu.VMEM((TILES, 16, 16, 128), F32),
            pltpu.VMEM((TILES, 2, 16, 128), F32),
            pltpu.VMEM((TILES, 2, 16, 128), F32),
            pltpu.VMEM((TILES, 2, 128), F32),
            pltpu.VMEM((TILES, 2, 16, 128), F32),
            pltpu.VMEM((TILES, 3, 16, 128), F32),
            pltpu.VMEM((3, 2, pixels), F32),
            pltpu.VMEM((2, pixels), F32),
            pltpu.VMEM((2, pixels), F32),
            pltpu.VMEM((3, 2, pixels), F32),
            pltpu.VMEM((TILES, 2, PAD, 128), F32),
            pltpu.VMEM((2, pixels), F32),
            pltpu.VMEM((1, 128), F32),
            pltpu.VMEM((7, 1, 128), F32),
            pltpu.VMEM((1, 128), F32),
            pltpu.VMEM((7, 1, 128), F32),
            pltpu.VMEM((16, 128), F32),
            pltpu.VMEM((32, 128), F32),
            pltpu.VMEM((7, 32, 128), F32),
            pltpu.VMEM((32, 128), F32),
            pltpu.VMEM((7, 32, 128), F32),
            pltpu.VMEM((32, 128), F32),
            pltpu.VMEM((2, 128), F32),
            pltpu.VMEM((31, 2, 128), F32),
            pltpu.VMEM((2, 128), F32),
            pltpu.VMEM((7, 2, 128), F32),
            pltpu.VMEM((4, 128), F32),
            pltpu.VMEM((7, 4, 128), F32),
            pltpu.VMEM((1, 16, 16, 128), F32),
            pltpu.VMEM((1, 16, 16, 128), F32),
            pltpu.VMEM((1, 2, 16, 128), F32),
            pltpu.VMEM((1, 2, 16, 128), F32),
            pltpu.VMEM((1, 3, 16, 128), F32),
            pltpu.VMEM((TILES, 16, 16, 128), F32),
            pltpu.VMEM((TILES, 16, 16, 128), F32),
            pltpu.VMEM((TILES, 2, 16, 128), F32),
            pltpu.VMEM((TILES, 2, 16, 128), F32),
            pltpu.VMEM((TILES, 2, 16, 128), F32),
            pltpu.VMEM((TILES, 1, 128), F32),
            pltpu.VMEM((1, 16, 16, 128), F32),
            pltpu.VMEM((1, 16, 16, 128), F32),
            pltpu.VMEM((1, 2, 16, 128), F32),
            pltpu.VMEM((1, 2, 16, 128), F32),
            pltpu.VMEM((TILES, 16, 16, 128), F32),
            pltpu.VMEM((TILES, 16, 16, 128), F32),
            pltpu.VMEM((1, 16, 16, 128), F32),
            pltpu.VMEM((1, 16, 16, 128), F32),
            dma((3,)),
            dma((2,)),
            dma((2, 2)),
            dma(()),
            dma(()),
            dma(()),
            dma((3,)),
            dma((2, 2)),
            dma(()),
            dma(()),
            dma(()),
            dma(()),
            dma((2,)),
            dma((2,)),
            pltpu.SemaphoreType.REGULAR((4,)),
        ],
        compiler_params=pltpu.CompilerParams(
            collective_id=0, has_side_effects=True, vmem_limit_bytes=16 * 2**20
        ),
        cost_estimate=pl.CostEstimate(flops=100_000_000, bytes_accessed=1_000_000, transcendentals=0),
    )(*(pltpu.with_memory_space_constraint(a, pltpu.HBM) for a in (flat, neighbours)), reference_pixel)
    phases, comp = pl.pallas_call(
        hand_out,
        out_shape=(
            jax.ShapeDtypeStruct((FLAT, 128), F32),
            jax.ShapeDtypeStruct((2, 1, pixels), F32),
        ),
        in_specs=[pl.BlockSpec(memory_space=pl.ANY)] * 2,
        out_specs=(hbm, hbm),
        scratch_shapes=[dma((2,))],
        compiler_params=pltpu.CompilerParams(vmem_limit_bytes=2**20),
    )(phases, comp)
    return phases.reshape(ROWS, TILES, 2, 128).transpose(2, 0, 1, 3).reshape(2, ROWS, pixels), comp


def solution(mesh):
    return jax.shard_map(
        on_device,
        mesh=mesh,
        in_specs=(P(None, "section", "pix"), P(None, "pix"), P()),
        out_specs=(P(None, "section", "pix"), P(None, "section", "pix")),
        check_vma=False,
    )
```

```python
import math

import jax
import jax.numpy as jnp
from jax import lax
from jax.experimental import pallas as pl
from jax.experimental.pallas import tpu as pltpu
from jax.sharding import PartitionSpec as P

ITERS = 16
FLOOR = 0.05
REACH = 256
NB = 15
ROWS = 50
PAD = 56
GROUPS = PAD // 8
FLAT = 4 * ROWS
TILES = 2
SPAN = 5
SCALE = 2.0**-45
START = 1.0 / math.sqrt(ROWS + 1)
GAIN = math.sqrt(ROWS + 1)
SECTIONS = 4
PIX = 64
MESH = pl.DeviceIdType.MESH
F32 = jnp.float32


def bcast(row):
    return jnp.broadcast_to(row, (8, 128))


def pick(sources, lane, tile):
    out = jnp.zeros((8, 128), F32)
    for m, source in enumerate(sources):
        out = jnp.where(tile == m, take(source, lane), out)
    return out


def take(source, lane):
    return jnp.take_along_axis(source, lane, axis=1, mode="promise_in_bounds")


def column_sum(x):
    return jnp.sum(x, axis=0, keepdims=True)


def eye(count, shift=0):
    lane = lax.broadcasted_iota(jnp.int32, (count, 128), 1)
    return lane == lax.broadcasted_iota(jnp.int32, (count, 128), 0) + shift


def to_row(column, shift=0):
    return column_sum(jnp.where(eye(column.shape[0], shift), column, 0.0))


def to_column(row, count):
    spread = jnp.broadcast_to(row, (count, 128))
    return jnp.sum(jnp.where(eye(count), spread, 0.0), axis=1, keepdims=True)


def unit(re, im):
    scale = 1.0 / jnp.maximum(jnp.sqrt(re * re + im * im), FLOOR)
    return re * scale, im * scale


def remote(src, dst, send, recv, device):
    return pltpu.make_async_remote_copy(
        src_ref=src, dst_ref=dst, send_sem=send, recv_sem=recv, device_id=device, device_id_type=MESH
    )


def kernel(
    slc_hbm, nbr_hbm, ref, phases, comp,
    nbr, blocks, ext, lanes, tiles, zs, wbuf, red, kre, kim, cvec, bvec, xsum, zbuf, sbuf,
    vbuf, msg, fmsg, fbuf, series, datum,
    nmsg, nbuf1, nmsg2, nbuf2, ncol, emsg, ebuf1, emsg2, ebuf2, eall, gmsg, gbuf, rmsg, rbuf1, bmsg, bbuf,
    kref, kimf, cref, zref, sref, kre2, kim2, qvec, gvec, result, inverse, kref2, kimf2, qref, gref,
    ksum, ksum2, ksumf, ksumf2,
    load_sem, halo_send, halo_recv, v_send, v_recv, f_send, f_recv, early_sem,
    y_send, y_recv, g_send, g_recv, r_sem, b_sem, ready,
):
    sec = lax.axis_index("section")
    pix = lax.axis_index("pix")
    before = lax.rem(pix + (PIX - 1), PIX)
    after = lax.rem(pix + 1, PIX)
    near = (before, pix, after)
    present = (pix > 0, pix >= 0, pix < PIX - 1)
    inner = jnp.logical_and(present[0], present[2])
    sec_up = lax.rem(sec + 1, SECTIONS)
    sec_down = lax.rem(sec + (SECTIONS - 1), SECTIONS)
    x = pix // 16
    z = lax.rem(pix // 2, 8)
    core = lax.rem(pix, 2)
    group = x * 2 + core
    first = []
    second = []
    for d in range(1, 8):
        g = lax.rem(group + d, 8)
        first.append((g // 2) * 16 + z * 2 + lax.rem(g, 2))
        second.append(x * 16 + lax.rem(z + d, 8) * 2 + core)

    want = ref[0] - pix * (TILES * 128)

    def at_ref(parts):
        total = None
        for t, part in enumerate(parts):
            lane = lax.broadcasted_iota(jnp.int32, part.shape, 1)
            part = jnp.where(lane == want - t * 128, part, 0.0)
            total = part if total is None else total + part
        return jnp.sum(total, axis=1, keepdims=True)

    def arrived(ref, sem):
        pltpu.make_async_copy(ref, ref, sem).wait()

    def start(src, dst, sem, devices):
        for i, device in enumerate(devices):
            remote(src, dst.at[i], sem.at[0], sem.at[1], (sec, device)).start()

    def finish(src, dst, sem, devices):
        arrived(dst, sem.at[0])
        arrived(dst, sem.at[1])

    def sum_of(own, buffers):
        total = own[...]
        for i in range(7):
            total = total + buffers[i]
        return total

    steps_n = (nmsg, nbuf1, early_sem.at[0], first), (nmsg2, nbuf2, early_sem.at[1], second)
    steps_e = (emsg, ebuf1, early_sem.at[0], first), (emsg2, ebuf2, early_sem.at[1], second)
    steps_r = (rmsg, rbuf1, r_sem, first)
    steps_b = (bmsg, bbuf, b_sem, second)

    chunks = [(0, 3), (3, GROUPS)]
    spans = [pl.ds(32 * low, min(32 * high, FLAT) - 32 * low) for low, high in chunks]
    loads = [
        pltpu.make_async_copy(slc_hbm.at[span], blocks.at[1, span], load_sem.at[i]) for i, span in enumerate(spans)
    ]
    loads.append(pltpu.make_async_copy(nbr_hbm, nbr, load_sem.at[2]))
    for load in loads:
        load.start()
    barrier = pltpu.get_barrier_semaphore()
    line = [(sec, before), (sec, after)]
    aside = [(sec_up, pix), (sec_down, pix)]
    plane = [(sec, x * 16 + lax.rem(z + d, 8) * 2 + core) for d in (1, 7)]
    plane += [(sec, lax.rem(x + d, 4) * 16 + z * 2 + core) for d in (1, 3)]
    leads = sec == 0
    follows = sec > 0

    def signal(sem, devices):
        for device in devices:
            pl.semaphore_signal(sem, inc=1, device_id=device, device_id_type=MESH)

    def tell(sem):
        signal(sem, line + aside)
        pl.when(follows)(lambda: signal(sem, plane))

    def hear(sem):
        pl.when(leads)(lambda: pl.semaphore_wait(sem, 4))
        pl.when(follows)(lambda: pl.semaphore_wait(sem, 8))

    signal(barrier, line)
    pl.when(sec != SECTIONS - 1)(lambda: signal(barrier, aside[:1]))
    pl.when(sec != 1)(lambda: signal(barrier, aside[1:]))
    pl.when(follows)(lambda: signal(barrier, plane))
    pl.when(leads)(lambda: pl.semaphore_wait(barrier, 2))
    pl.when(follows)(lambda: pl.semaphore_wait(barrier, 8))
    signal(ready.at[0], line)
    pl.when(follows)(lambda: signal(ready.at[0], aside + plane))

    def halo(i, n):
        part = blocks.at[1, spans[n]]
        return remote(part, blocks.at[2 - i, spans[n]], halo_send.at[i // 2], halo_recv.at[i // 2, n], (sec, near[i]))

    for n in range(len(chunks)):
        loads[n].wait()
        pl.when(jnp.logical_and(present[0], core == 0))(halo(0, n).start)
        pl.when(present[2])(halo(2, n).start)
        pl.when(jnp.logical_and(present[0], core == 1))(halo(0, n).start)

    for i in range(3):
        blocks[i, FLAT:, :] = jnp.zeros((32 * GROUPS - FLAT, 128), F32)
    kre[...] = jnp.zeros_like(kre)
    kim[...] = jnp.zeros_like(kim)
    red[...] = jnp.zeros_like(red)
    cvec[...] = jnp.zeros_like(cvec)
    bvec[...] = jnp.zeros_like(bvec)
    for i in (0, 2):

        @pl.when(jnp.logical_not(present[i]))
        def _():
            blocks[i] = jnp.zeros((32 * GROUPS, 128), F32)
            vbuf[i] = jnp.zeros_like(vbuf[i])

    loads[2].wait()

    base = pix * (TILES * 128) - REACH
    for t in range(TILES):
        rel = nbr[:, t * 128 : (t + 1) * 128] - (base + t * 128)
        lanes[t, 0:NB, :] = jnp.bitwise_and(rel, 127)
        tiles[t, 0:NB, :] = jnp.right_shift(rel, 7)
        lanes[t, NB : NB + 1, :] = jnp.zeros((1, 128), jnp.int32)
        tiles[t, NB : NB + 1, :] = jnp.full((1, 128), SPAN, jnp.int32)

    def spread(i, groups=range(GROUPS)):
        for g in groups:
            for m in range(2):
                for c in range(2):
                    ext[2 * i + m, c, g * 8 : (g + 1) * 8, :] = blocks[i, pl.ds(g * 32 + m * 2 + c, 8, stride=4), :]

    spread(1)
    for t in range(TILES):
        for c in range(2):
            total = None
            for g in range(GROUPS):
                own = ext[2 + t, c, g * 8 : (g + 1) * 8, :]
                zs[t, 0, c, g * 8 : (g + 1) * 8, :] = own
                total = own if total is None else total + own
            xsum[t, c : c + 1, :] = column_sum(total)

    def gather(t, offsets, begin, groups=range(GROUPS), halves=None):
        def some(half):
            for i in range(NB // 2):
                k = 1 + half * (NB // 2) + i
                lane = bcast(lanes[t, pl.ds(k, 1), :])
                tile = bcast(tiles[t, pl.ds(k, 1), :])
                for g in groups:
                    rows = slice(g * 8, (g + 1) * 8)
                    for c in range(2):
                        out = None if begin else zs[t, k, c, rows, :]
                        for m in offsets:
                            got = take(ext[t + m, c, rows, :], lane)
                            out = got if out is None else jnp.where(tile == m, got, out)
                        zs[t, k, c, rows, :] = out

        if halves is None:
            pl.loop(0, 2)(some)
        else:
            for half in halves:
                some(half)

    for t in range(TILES):
        gather(t, (2 - t, 3 - t), True)

    def side(s, groups, halves=None):
        spread(2 * s, groups)
        close, distant = 1 + 3 * s, 5 * s
        gather(s, (close - s, distant - s), False, groups, halves)
        gather(1 - s, (close - (1 - s),), False, groups, halves)

    def both(soon):
        late = 1 - soon
        for n in range(len(chunks)):
            arrived(blocks.at[2 * soon, spans[n]], halo_recv.at[1 - soon, n])
        side(soon, range(GROUPS))
        hear(ready.at[0])
        pl.when(leads)(lambda: signal(ready.at[0], aside))
        tell(ready.at[1])
        for n, (low, high) in enumerate(chunks):
            pl.when(inner)(lambda n=n: arrived(blocks.at[2 * late, spans[n]], halo_recv.at[1 - late, n]))
            side(late, range(low, high), range(2))

    pl.when(core == 0)(lambda: both(1))
    pl.when(core == 1)(lambda: both(0))

    @pl.when(sec >= 2)
    def _():
        hear(ready.at[1])
        tell(ready.at[2])

    @pl.when(sec == 2)
    def _():
        column = at_ref([nbr[:, t * 128 : (t + 1) * 128].astype(F32) for t in range(TILES)])
        nmsg[...] = to_row(column)
        start(*steps_n[0])

    @pl.loop(0, TILES)
    def _(t):
        for g in range(GROUPS):
            rows = slice(g * 8, (g + 1) * 8)
            power = None
            for k in range(NB):
                re, im = zs[t, k, 0, rows, :], zs[t, k, 1, rows, :]
                zs[t, k, 2, rows, :] = re - im
                term = re * re + im * im
                power = term if power is None else power + term
            wbuf[t, rows, :] = lax.rsqrt(jnp.maximum(power, 1.0))

        def fold(slot, parts):
            for i, part in enumerate(parts):
                red[slot, i * 8 : (i + 1) * 8, :] = part
            total = None
            for i in range(8):
                row = red[slot, pl.ds(i, 8, stride=8), :]
                total = row if total is None else total + row
            return total

        slot = 0
        for l in range(NB + 1):
            for kg in range(2):
                low, high = 8 * kg, min(8 * kg + 8, l + 1, NB)
                if high <= low:
                    continue
                count = high - low
                p, q, r = [None] * count, [None] * count, [None] * count
                cr, ci = [None] * count, [None] * count

                def put(box, i, value):
                    box[i] = value if box[i] is None else box[i] + value

                for g in range(GROUPS):
                    rows = slice(g * 8, (g + 1) * 8)
                    w = wbuf[t, rows, :]
                    if l < NB:
                        w2 = w * w
                        lr, li = zs[t, l, 0, rows, :] * w2, zs[t, l, 1, rows, :] * w2
                    else:
                        lr, li = zs[t, 0, 0, rows, :] * w, zs[t, 0, 1, rows, :] * w
                    le = lr + li
                    for i in range(count):
                        k = low + i
                        kr, ki = zs[t, k, 0, rows, :], zs[t, k, 1, rows, :]
                        put(p, i, kr * lr)
                        put(q, i, ki * li)
                        if k != l:
                            put(r, i, zs[t, k, 2, rows, :] * le)
                        if l == NB:
                            put(cr, i, kr * w)
                            put(ci, i, ki * w)
                re = fold(4 * kg + slot, [a + b for a, b in zip(p, q)])
                im = fold(4 * kg + slot + 1, [jnp.zeros((8, 128), F32) if c is None else c + (b - a) for a, b, c in zip(p, q, r)])
                rows = slice(low, low + 8)
                if l < NB:
                    kre[t, l, rows, :] = re
                    kim[t, l, rows, :] = im
                    for i in range(count):
                        k = low + i
                        if k != l:
                            kre[t, k, l : l + 1, :] = re[i : i + 1, :]
                            kim[t, k, l : l + 1, :] = -im[i : i + 1, :]
                else:
                    bvec[t, 0, rows, :] = re
                    bvec[t, 1, rows, :] = im
                    slot = 2 - slot
                    cvec[t, 0, rows, :] = START * fold(4 * kg + slot, cr)
                    cvec[t, 1, rows, :] = -START * fold(4 * kg + slot + 1, ci)
                slot = 2 - slot
        ksum[t] = kre[t] + kim[t]

    def pieces(count):
        return [(t, c, kg) for t in range(count) for c in range(2) for kg in range(2)]

    def load(ref, count):
        return [ref[t, c, 8 * kg : 8 * kg + 8, :] for t, c, kg in pieces(count)]

    def save(ref, value):
        for (t, c, kg), part in zip(pieces(len(value) // 4), value):
            ref[t, c, 8 * kg : 8 * kg + 8, :] = part

    def plus(*values):
        return [sum(parts[1:], parts[0]) for parts in zip(*values)]

    def times(factor, value):
        return [factor * part for part in value]

    def product(m, box, value):
        for t in range(len(value) // 4):
            for kg in range(2):
                re, im = value[4 * t + kg], value[4 * t + 2 + kg]
                for c, part in enumerate((re, im, re + im)):
                    box[t, c, 8 * kg : 8 * kg + 8, :] = part
        out = []
        for t in range(len(value) // 4):
            y = [[None, None] for _ in range(3)]
            for l in range(NB):
                for c in range(3):
                    row = bcast(box[t, c, l : l + 1, :])
                    for kg in range(2):
                        part = m[c][t, l, 8 * kg : 8 * kg + 8, :] * row
                        y[c][kg] = part if l == 0 else y[c][kg] + part
            out += [y[0][kg] - y[1][kg] for kg in range(2)]
            out += [y[2][kg] - (y[0][kg] + y[1][kg]) for kg in range(2)]
        return out

    def prepare(m3, s3, cv, qv, box, count):
        mr, mi, _ = m3
        sr, si, _ = s3
        for t in range(count):

            @pl.loop(0, NB)
            def _(l):
                for kg in range(2):
                    rows = slice(8 * kg, 8 * kg + 8)
                    re, im = 2.0 * mr[t, l, rows, :], 2.0 * mi[t, l, rows, :]
                    for m in range(NB):
                        lr = bcast(mr[t, l, m : m + 1, :])
                        li = bcast(mi[t, l, m : m + 1, :])
                        ar, ai = mr[t, m, rows, :], mi[t, m, rows, :]
                        re = re + (ar * lr - ai * li)
                        im = im + (ar * li + ai * lr)
                    sr[t, l, rows, :] = re
                    si[t, l, rows, :] = im

        save(qv, product(m3, box, load(cv, count)))

    def joined(z, value):
        out = []
        for t in range(len(value) // 4):
            zr, zi = z[4 * t : 4 * t + 2], z[4 * t + 2 : 4 * t + 4]
            vr, vi = value[4 * t : 4 * t + 2], value[4 * t + 2 : 4 * t + 4]
            ar = column_sum(zr[0] * vr[0] - zi[0] * vi[0] + (zr[1] * vr[1] - zi[1] * vi[1]))
            ai = column_sum(zr[0] * vi[0] + zi[0] * vr[0] + (zr[1] * vi[1] + zi[1] * vr[1]))
            out += [zr[i] * ar + zi[i] * ai for i in range(2)] + [zr[i] * ai - zi[i] * ar for i in range(2)]
        return out

    def conj(value):
        return [part if (i // 2) % 2 == 0 else -part for i, part in enumerate(value)]

    def norms_of(value, image, start):
        out = []
        for t in range(len(value) // 4):
            total = None
            for i in range(4 * t, 4 * t + 4):
                term = value[i] * (image[i] + (2.0 * SCALE) * start[i])
                total = term if total is None else total + term
            out.append(lax.rsqrt(column_sum(total) + SCALE * SCALE))
        return out

    def solve(m3, cv, box, count):
        def turn(_, value):
            return tuple(plus(value, product(m3, box, value), load(cv, count)))

        value = lax.fori_loop(0, ITERS - 1, turn, tuple(load(cv, count)))
        value = times(SCALE, value)
        return value, norms_of(value, product(m3, box, value), load(cv, count))

    def solve_joined(m3, s3, cv, qv, zv, box, gbox, count):
        z = load(zv, count)
        r = conj(z)
        kr = product(m3, box, r)
        c = plus(load(cv, count), times(START, r))
        g = plus(r, kr)
        for t in range(count):
            squares = [z[4 * t + i] * z[4 * t + i] for i in range(4)]
            half = 0.5 * column_sum(squares[0] + squares[1] + (squares[2] + squares[3]))
            for i in range(4 * t, 4 * t + 4):
                g[i] = g[i] + half * r[i]
        save(gbox, g)
        sr, si, both = s3
        for t in range(count):
            for l in range(NB):
                zr, zi = bcast(zv[t, 0, l : l + 1, :]), bcast(zv[t, 1, l : l + 1, :])
                gr, gi = bcast(gbox[t, 0, l : l + 1, :]), bcast(gbox[t, 1, l : l + 1, :])
                for kg in range(2):
                    rows = slice(8 * kg, 8 * kg + 8)
                    hr, hi = g[4 * t + kg], g[4 * t + 2 + kg]
                    xr, xi = z[4 * t + kg], z[4 * t + 2 + kg]
                    re = sr[t, l, rows, :] + (hr * zr - hi * zi + (xr * gr - xi * gi))
                    im = si[t, l, rows, :] + (hr * zi + hi * zr - (xr * gi + xi * gr))
                    sr[t, l, rows, :] = re
                    si[t, l, rows, :] = im
                    both[t, l, rows, :] = re + im

        def square(value):
            return plus(value, product(s3, box, value))

        value = plus(c, c, load(qv, count), times(START, kr), joined(z, c))
        value = plus(value, square(value))
        value = plus(value, square(square(value)))

        last = lax.fori_loop(0, 4, lambda _, v: tuple(square(v)), tuple(value))
        value = times(SCALE, plus(value, last))
        image = plus(product(m3, box, value), joined(z, value))
        return value, norms_of(value, image, c)

    def step_one():
        @pl.when(sec == 2)
        def _():
            arrived(gbuf.at[1:8], g_recv)

        @pl.when(sec != 2)
        def _():
            arrived(gbuf.at[0:8], g_recv)

        total = gbuf[0]
        for d in range(1, 8):
            total = total + gbuf[d]
        bmsg[2:4, :] = total
        bmsg[0:2, :] = jnp.zeros((2, 128), F32)

        @pl.when(sec < SECTIONS - 1)
        def _():
            finish(*steps_r)
            bmsg[0:2, :] = sum_of(rmsg, rbuf1)

        pl.when(leads)(lambda: pl.semaphore_wait(ready.at[4], 4))
        start(*steps_b)

    @pl.when(sec == 1)
    def _():
        hear(ready.at[1])
        tell(ready.at[2])

    def prepare_own():
        prepare((kre, kim, ksum), (kre2, kim2, ksum2), cvec, qvec, sbuf, TILES)

    pl.when(jnp.logical_or(sec == 1, sec == 2))(prepare_own)

    @pl.when(sec == 2)
    def _():
        finish(*steps_n[0])
        hear(ready.at[2])
        tell(ready.at[3])
        nmsg2[...] = sum_of(nmsg, nbuf1)
        start(*steps_n[1])

    def expand():
        for l in range(NB):
            kref[0, l] = jnp.broadcast_to(eall[0:16, l : l + 1], (16, 128))
            kimf[0, l] = jnp.broadcast_to(eall[0:16, 16 + l : 17 + l], (16, 128))
        for c in range(2):
            cref[0, c] = jnp.broadcast_to(eall[0:16, 32 + c : 33 + c], (16, 128))
        ksumf[...] = kref[...] + kimf[...]
        prepare((kref, kimf, ksumf), (kref2, kimf2, ksumf2), cref, qref, sref, 1)

    @pl.when(sec == SECTIONS - 1)
    def _():
        lane = lax.broadcasted_iota(jnp.int32, (16, 128), 1)
        emsg[16:32, :] = jnp.zeros((16, 128), F32)
        acc = jnp.zeros((16, 128), F32)
        for c in range(2):
            acc = jnp.where(lane == 32 + c, at_ref([cvec[t, c] for t in range(TILES)]), acc)
        emsg[0:16, :] = acc

        @pl.loop(0, NB)
        def _(k):
            acc = emsg[0:16, :]
            acc = jnp.where(lane == k, at_ref([kre[t, k] for t in range(TILES)]), acc)
            emsg[0:16, :] = jnp.where(lane == 16 + k, at_ref([kim[t, k] for t in range(TILES)]), acc)
            parts = [at_ref([zs[t, k, c] * wbuf[t] for t in range(TILES)]) for c in range(2)]
            emsg[pl.ds(16 + k, 1), :] = to_row(parts[0]) + to_row(parts[1], 64)

        start(*steps_e[0])
        prepare_own()
        finish(*steps_e[0])
        hear(ready.at[2])
        tell(ready.at[3])
        emsg2[...] = sum_of(emsg, ebuf1)
        start(*steps_e[1])
        hear(ready.at[3])
        tell(ready.at[4])
        step_one()
        finish(*steps_e[1])
        eall[...] = sum_of(emsg2, ebuf2)
        for j in range(SECTIONS - 1):
            remote(eall.at[pl.ds(0, 16)], eall.at[pl.ds(0, 16)], y_send, y_recv, (j, pix)).start()
        expand()

    @pl.when(sec == 2)
    def _():
        finish(*steps_n[1])
        column = to_column(sum_of(nmsg2, nbuf2), 16)
        row = lax.broadcasted_iota(jnp.int32, (16, 128), 0)
        ncol[...] = jnp.where(row == NB, ref[0].astype(F32), column) - (pix * (TILES * 128)).astype(F32)

    def keep(solved):
        value, norms = solved
        save(result, value)
        for t, norm in enumerate(norms):
            inverse[t] = norm

    @pl.when(sec == 0)
    def _():
        zbuf[...] = jnp.zeros_like(zbuf)
        keep(solve((kre, kim, ksum), cvec, sbuf, TILES))

    @pl.when(sec > 0)
    def _():
        pl.when(inner)(lambda: arrived(vbuf, v_recv))
        pl.when(jnp.logical_not(inner))(lambda: arrived(vbuf.at[0:2], v_recv))
        for t in range(TILES):
            z0 = []
            for kg in range(2):
                rows = slice(8 * kg, 8 * kg + 8)
                lane = lanes[t, rows, :]
                tile = tiles[t, rows, :]
                pair = []
                for c in range(2):
                    src = []
                    for m in range(SPAN):
                        at = t + m
                        src.append(bcast(vbuf[at // 2, c : c + 1, (at % 2) * 128 : (at % 2) * 128 + 128]))
                    pair.append(pick(src, lane, tile))
                z0.append(pair)
            power = column_sum(z0[0][0] * z0[0][0] + z0[0][1] * z0[0][1] + (z0[1][0] * z0[1][0] + z0[1][1] * z0[1][1]))
            w = lax.rsqrt(jnp.maximum(power, 1.0))
            vr = vbuf[1, 0:1, t * 128 : (t + 1) * 128]
            vi = vbuf[1, 1:2, t * 128 : (t + 1) * 128]
            xsum[t, 0:1, :] = xsum[t, 0:1, :] + vr
            xsum[t, 1:2, :] = xsum[t, 1:2, :] + vi
            for kg in range(2):
                rows = slice(8 * kg, 8 * kg + 8)
                zr, zi = z0[kg][0] * w, z0[kg][1] * w
                zbuf[t, 0, rows, :] = zr
                zbuf[t, 1, rows, :] = zi
                bvec[t, 0, rows, :] = bvec[t, 0, rows, :] + (zr * vr + zi * vi)
                bvec[t, 1, rows, :] = bvec[t, 1, rows, :] + (zr * vi - zi * vr)
        keep(solve_joined((kre, kim, ksum), (kre2, kim2, ksum2), cvec, qvec, zbuf, sbuf, gvec, TILES))

    state = load(result, TILES)
    norms = [inverse[t] for t in range(TILES)]
    for t in range(TILES):
        s = state[4 * t : 4 * t + 4]
        norm = norms[t]
        cr = ci = fr = fi = None
        for kg in range(2):
            rows = slice(8 * kg, 8 * kg + 8)
            sr, si = s[kg], s[2 + kg]
            br, bi = bvec[t, 0, rows, :], bvec[t, 1, rows, :]
            zr, zi = zbuf[t, 0, rows, :], zbuf[t, 1, rows, :]
            a, b = sr * br + si * bi, sr * bi - si * br
            e, f = zr * sr - zi * si, zr * si + zi * sr
            cr = a if kg == 0 else column_sum(cr + a)
            ci = b if kg == 0 else column_sum(ci + b)
            fr = e if kg == 0 else column_sum(fr + e)
            fi = f if kg == 0 else column_sum(fi + f)
        cols = slice(t * 128, (t + 1) * 128)
        msg[0:1, cols] = (cr + (SCALE * START) * xsum[t, 0:1, :]) * norm
        msg[1:2, cols] = (ci + (SCALE * START) * xsum[t, 1:2, :]) * norm
        fr, fi = unit((fr + SCALE * START) * norm, fi * norm)
        fmsg[0:1, cols] = fr
        fmsg[1:2, cols] = fi

    steps_g = [
        remote(gmsg, gbuf.at[d], g_send, g_recv, (s, pix if d == 0 else first[d - 1]))
        for s in range(SECTIONS)
        for d in range(8)
        if (s, d) != (2, 0)
    ]

    @pl.when(sec == 2)
    def _():
        hear(ready.at[3])
        lane = lax.broadcasted_iota(jnp.int32, (16, 128), 1).astype(F32)
        row = lax.broadcasted_iota(jnp.int32, (16, 128), 0)
        for c in range(2):
            total = None
            for t in range(TILES):
                cols = slice(t * 128, (t + 1) * 128)
                value = jnp.where(
                    row == NB,
                    jnp.broadcast_to(fmsg[c : c + 1, cols], (16, 128)),
                    jnp.broadcast_to(msg[c : c + 1, cols], (16, 128)),
                )
                value = jnp.where(ncol[...] - t * 128.0 == lane, value, 0.0)
                total = value if total is None else total + value
            gmsg[c : c + 1, :] = to_row(jnp.sum(total, axis=1, keepdims=True))
        for copy in steps_g:
            copy.start()
        gbuf[0] = gmsg[...]
        tell(ready.at[4])

    @pl.when(sec < SECTIONS - 1)
    def _():
        for i in range(3):
            pl.when(present[i])(remote(msg, vbuf.at[2 - i], v_send, v_recv, (sec_up, near[i])).start)

    for s in range(1, SECTIONS):

        @pl.when(sec == s)
        def _():
            for j in range(s):
                remote(fmsg, fbuf.at[s - 1], f_send, f_recv.at[s - 1], (j, pix)).start()

    @pl.when(sec == 0)
    def _():
        hear(ready.at[1])
        tell(ready.at[2])

    @pl.when(sec < 2)
    def _():
        hear(ready.at[2])
        tell(ready.at[3])
        hear(ready.at[3])
        tell(ready.at[4])

    comp[0, 0:1, :] = msg[0:1, :]
    comp[1, 0:1, :] = msg[1:2, :]

    def vector():
        for i, (t, c, kg) in enumerate((t, c, kg) for t in range(TILES) for c in range(2) for kg in range(2)):
            sbuf[t, c, 8 * kg : 8 * kg + 8, :] = result[t, c, 8 * kg : 8 * kg + 8, :] * inverse[t]
        for t in range(TILES):

            @pl.loop(0, GROUPS)
            def _(g):
                rows = pl.ds(pl.multiple_of(g * 8, 8), 8)
                re = im = None
                for k in range(NB):
                    sr = bcast(sbuf[t, 0, k : k + 1, :])
                    si = bcast(sbuf[t, 1, k : k + 1, :])
                    zr, zi = zs[t, k, 0, rows, :], zs[t, k, 1, rows, :]
                    a, b = zr * sr - zi * si, zr * si + zi * sr
                    re = a if re is None else re + a
                    im = b if im is None else im + b
                w = wbuf[t, rows, :]
                series[t, 0, rows, :] = bcast((SCALE * START) * inverse[t]) + w * re
                series[t, 1, rows, :] = w * im

    pl.when(sec < SECTIONS - 1)(vector)

    def take_f(j):
        arrived(fbuf.at[j - 1], f_recv.at[j - 1])

    @pl.when(sec == 0)
    def _():
        take_f(1)
        for t in range(TILES):
            fr = fbuf[0, 0:1, t * 128 : (t + 1) * 128]
            fi = fbuf[0, 1:2, t * 128 : (t + 1) * 128]
            re, im = series[t, 0], series[t, 1]
            series[t, 0] = re * fr - im * fi
            series[t, 1] = re * fi + im * fr

    @pl.when(sec < SECTIONS - 1)
    def _():
        for c in range(2):
            rmsg[c : c + 1, :] = to_row(at_ref([series[t, c] for t in range(TILES)]))
        start(*steps_r)

    pl.when(sec < SECTIONS - 1)(step_one)

    pl.when(sec == SECTIONS - 1)(vector)

    @pl.when(sec < SECTIONS - 1)
    def _():
        remote(eall.at[pl.ds(0, 16)], eall.at[pl.ds(0, 16)], y_send, y_recv, (SECTIONS - 1, pix)).wait_recv()
        expand()

    finish(*steps_b)
    total = sum_of(bmsg, bbuf)

    values = [to_column(total[2 + c : 3 + c, :], 16) for c in range(2)]
    f2r, f2i = values[0][NB:16], values[1][NB:16]
    row = lax.broadcasted_iota(jnp.int32, (16, 128), 0)
    zr, zi = (jnp.where(row < NB, value, 0.0) for value in values)
    w = lax.rsqrt(jnp.maximum(column_sum(zr * zr + zi * zi), 1.0))
    zr, zi = zr * w, zi * w
    zref[0, 0] = zr
    zref[0, 1] = zi
    state_ref, norm_ref = solve_joined((kref, kimf, ksumf), (kref2, kimf2, ksumf2), cref, qref, zref, sref, gref, 1)
    sr = jnp.concatenate(state_ref[0:2], axis=0)
    si = jnp.concatenate(state_ref[2:4], axis=0)
    norm = norm_ref[0]
    f3r = column_sum(zr * sr - zi * si)
    f3i = column_sum(zr * si + zi * sr)
    f3r, f3i = unit((f3r + SCALE * START) * norm, f3i * norm)
    fr = jnp.where(sec < 2, f3r * f2r - f3i * f2i, f3r)
    fi = jnp.where(sec < 2, f3r * f2i + f3i * f2r, f3i)
    vr, vi = total[0:1, :], total[1:2, :]
    rmsg[0:1, :] = vr * fr - vi * fi
    rmsg[1:2, :] = vr * fi + vi * fr

    @pl.when(sec == SECTIONS - 1)
    def _():
        z = eall[16:32, :]
        a = bcast(column_sum(z * sr))
        b = bcast(column_sum(z * si))
        re = a - pltpu.roll(b, 64, 1)
        im = b + pltpu.roll(a, 64, 1)
        rmsg[0:1, :] = (re[0:1] + SCALE * START) * norm
        rmsg[1:2, :] = im[0:1] * norm

    ur, ui = unit(rmsg[0:1, :], rmsg[1:2, :])
    ur, ui = GAIN * to_column(ur, PAD), GAIN * to_column(ui, PAD)

    datum[0:1, :] = jnp.ones((1, TILES * 128), F32)
    datum[1:2, :] = jnp.zeros((1, TILES * 128), F32)

    @pl.when(sec < SECTIONS - 1)
    def _():
        take_f(3)
        datum[...] = fbuf[2]

    @pl.when(sec < 2)
    def _():
        take_f(2)
        dr, di = datum[0:1, :], datum[1:2, :]
        fr, fi = fbuf[1, 0:1, :], fbuf[1, 1:2, :]
        datum[0:1, :] = dr * fr - di * fi
        datum[1:2, :] = dr * fi + di * fr

    for t in range(TILES):
        dr, di = datum[0:1, t * 128 : (t + 1) * 128], datum[1:2, t * 128 : (t + 1) * 128]
        re, im = series[t, 0], series[t, 1]
        re, im = re * dr - im * di, re * di + im * dr
        for c, part in enumerate((re * ur + im * ui, im * ur - re * ui)):
            for g in range(GROUPS):
                count = min(8, ROWS - g * 8)
                phases[pl.ds(g * 32 + t * 2 + c, count, stride=4), :] = part[g * 8 : g * 8 + count]

    pl.when(follows)(lambda: pl.semaphore_wait(ready.at[4], 8))
    for i in (0, 2):
        pl.when(present[i])(lambda i=i: arrived(blocks.at[1, pl.ds(0, FLAT)], halo_send.at[i // 2]))
    @pl.when(sec == 2)
    def _():
        arrived(gbuf, g_send)

    @pl.when(sec == SECTIONS - 1)
    def _():
        arrived(ebuf1.at[0:3, 0:16], y_send)

    @pl.when(sec < SECTIONS - 1)
    def _():
        pl.when(inner)(lambda: arrived(vbuf, v_send))
        pl.when(jnp.logical_not(inner))(lambda: arrived(vbuf.at[0:2], v_send))

    for s in range(1, SECTIONS):

        @pl.when(sec == s)
        def _():
            arrived(fbuf.at[0:s], f_send)


def hand_out(phases_in, comp_in, phases, comp, sem):
    copies = [
        pltpu.make_async_copy(phases_in, phases, sem.at[0]),
        pltpu.make_async_copy(comp_in, comp, sem.at[1]),
    ]
    for copy in copies:
        copy.start()
    for copy in copies:
        copy.wait()


def on_device(slc, neighbours, reference_pixel):
    vmem = pl.BlockSpec(memory_space=pltpu.VMEM)
    hbm = pl.BlockSpec(memory_space=pltpu.HBM)
    pixels = slc.shape[2]
    dma = pltpu.SemaphoreType.DMA
    flat = slc.reshape(2, ROWS, TILES, 128).transpose(1, 2, 0, 3).reshape(FLAT, 128)
    phases, comp = pl.pallas_call(
        kernel,
        out_shape=(
            jax.ShapeDtypeStruct((FLAT, 128), F32),
            jax.ShapeDtypeStruct((2, 1, pixels), F32),
        ),
        in_specs=[hbm, hbm, pl.BlockSpec(memory_space=pltpu.SMEM)],
        out_specs=(vmem, vmem),
        scratch_shapes=[
            pltpu.VMEM((NB, pixels), jnp.int32),
            pltpu.VMEM((3, 32 * GROUPS, 128), F32),
            pltpu.VMEM((6, 2, PAD, 128), F32),
            pltpu.VMEM((TILES, 16, 128), jnp.int32),
            pltpu.VMEM((TILES, 16, 128), jnp.int32),
            pltpu.VMEM((TILES, NB, 3, PAD, 128), F32),
            pltpu.VMEM((TILES, PAD, 128), F32),
            pltpu.VMEM((8, 64, 128), F32),
            pltpu.VMEM((TILES, 16, 16, 128), F32),
            pltpu.VMEM((TILES, 16, 16, 128), F32),
            pltpu.VMEM((TILES, 2, 16, 128), F32),
            pltpu.VMEM((TILES, 2, 16, 128), F32),
            pltpu.VMEM((TILES, 2, 128), F32),
            pltpu.VMEM((TILES, 2, 16, 128), F32),
            pltpu.VMEM((TILES, 3, 16, 128), F32),
            pltpu.VMEM((3, 2, pixels), F32),
            pltpu.VMEM((2, pixels), F32),
            pltpu.VMEM((2, pixels), F32),
            pltpu.VMEM((3, 2, pixels), F32),
            pltpu.VMEM((TILES, 2, PAD, 128), F32),
            pltpu.VMEM((2, pixels), F32),
            pltpu.VMEM((1, 128), F32),
            pltpu.VMEM((7, 1, 128), F32),
            pltpu.VMEM((1, 128), F32),
            pltpu.VMEM((7, 1, 128), F32),
            pltpu.VMEM((16, 128), F32),
            pltpu.VMEM((32, 128), F32),
            pltpu.VMEM((7, 32, 128), F32),
            pltpu.VMEM((32, 128), F32),
            pltpu.VMEM((7, 32, 128), F32),
            pltpu.VMEM((32, 128), F32),
            pltpu.VMEM((2, 128), F32),
            pltpu.VMEM((31, 2, 128), F32),
            pltpu.VMEM((2, 128), F32),
            pltpu.VMEM((7, 2, 128), F32),
            pltpu.VMEM((4, 128), F32),
            pltpu.VMEM((7, 4, 128), F32),
            pltpu.VMEM((1, 16, 16, 128), F32),
            pltpu.VMEM((1, 16, 16, 128), F32),
            pltpu.VMEM((1, 2, 16, 128), F32),
            pltpu.VMEM((1, 2, 16, 128), F32),
            pltpu.VMEM((1, 3, 16, 128), F32),
            pltpu.VMEM((TILES, 16, 16, 128), F32),
            pltpu.VMEM((TILES, 16, 16, 128), F32),
            pltpu.VMEM((TILES, 2, 16, 128), F32),
            pltpu.VMEM((TILES, 2, 16, 128), F32),
            pltpu.VMEM((TILES, 2, 16, 128), F32),
            pltpu.VMEM((TILES, 1, 128), F32),
            pltpu.VMEM((1, 16, 16, 128), F32),
            pltpu.VMEM((1, 16, 16, 128), F32),
            pltpu.VMEM((1, 2, 16, 128), F32),
            pltpu.VMEM((1, 2, 16, 128), F32),
            pltpu.VMEM((TILES, 16, 16, 128), F32),
            pltpu.VMEM((TILES, 16, 16, 128), F32),
            pltpu.VMEM((1, 16, 16, 128), F32),
            pltpu.VMEM((1, 16, 16, 128), F32),
            dma((3,)),
            dma((2,)),
            dma((2, 2)),
            dma(()),
            dma(()),
            dma(()),
            dma((3,)),
            dma((2, 2)),
            dma(()),
            dma(()),
            dma(()),
            dma(()),
            dma((2,)),
            dma((2,)),
            pltpu.SemaphoreType.REGULAR((5,)),
        ],
        compiler_params=pltpu.CompilerParams(
            collective_id=0, has_side_effects=True, vmem_limit_bytes=16 * 2**20
        ),
        cost_estimate=pl.CostEstimate(flops=100_000_000, bytes_accessed=1_000_000, transcendentals=0),
    )(*(pltpu.with_memory_space_constraint(a, pltpu.HBM) for a in (flat, neighbours)), reference_pixel)
    phases, comp = pl.pallas_call(
        hand_out,
        out_shape=(
            jax.ShapeDtypeStruct((FLAT, 128), F32),
            jax.ShapeDtypeStruct((2, 1, pixels), F32),
        ),
        in_specs=[pl.BlockSpec(memory_space=pl.ANY)] * 2,
        out_specs=(hbm, hbm),
        scratch_shapes=[dma((2,))],
        compiler_params=pltpu.CompilerParams(vmem_limit_bytes=2**20),
    )(phases, comp)
    return phases.reshape(ROWS, TILES, 2, 128).transpose(2, 0, 1, 3).reshape(2, ROWS, pixels), comp


def solution(mesh):
    return jax.shard_map(
        on_device,
        mesh=mesh,
        in_specs=(P(None, "section", "pix"), P(None, "pix"), P()),
        out_specs=(P(None, "section", "pix"), P(None, "section", "pix")),
        check_vma=False,
    )
```

```python
import math

import jax
import jax.numpy as jnp
from jax import lax
from jax.experimental import pallas as pl
from jax.experimental.pallas import tpu as pltpu
from jax.sharding import PartitionSpec as P

ITERS = 16
FLOOR = 0.05
REACH = 256
NB = 15
ROWS = 50
PAD = 56
GROUPS = PAD // 8
FLAT = 4 * ROWS
TILES = 2
SPAN = 5
SCALE = 2.0**-45
START = 1.0 / math.sqrt(ROWS + 1)
GAIN = math.sqrt(ROWS + 1)
SECTIONS = 4
PIX = 64
MESH = pl.DeviceIdType.MESH
F32 = jnp.float32


def bcast(row):
    return jnp.broadcast_to(row, (8, 128))


def pick(sources, lane, tile):
    out = jnp.zeros((8, 128), F32)
    for m, source in enumerate(sources):
        out = jnp.where(tile == m, take(source, lane), out)
    return out


def take(source, lane):
    return jnp.take_along_axis(source, lane, axis=1, mode="promise_in_bounds")


def column_sum(x):
    return jnp.sum(x, axis=0, keepdims=True)


def eye(count, shift=0):
    lane = lax.broadcasted_iota(jnp.int32, (count, 128), 1)
    return lane == lax.broadcasted_iota(jnp.int32, (count, 128), 0) + shift


def to_row(column, shift=0):
    return column_sum(jnp.where(eye(column.shape[0], shift), column, 0.0))


def to_column(row, count):
    spread = jnp.broadcast_to(row, (count, 128))
    return jnp.sum(jnp.where(eye(count), spread, 0.0), axis=1, keepdims=True)


def unit(re, im):
    scale = 1.0 / jnp.maximum(jnp.sqrt(re * re + im * im), FLOOR)
    return re * scale, im * scale


def remote(src, dst, send, recv, device):
    return pltpu.make_async_remote_copy(
        src_ref=src, dst_ref=dst, send_sem=send, recv_sem=recv, device_id=device, device_id_type=MESH
    )


def kernel(
    slc_hbm, nbr_hbm, ref, phases, comp,
    nbr, blocks, ext, lanes, tiles, zs, wbuf, red, kre, kim, cvec, bvec, xsum, zbuf, sbuf,
    vbuf, msg, fmsg, fbuf, series, datum,
    nmsg, nbuf1, nmsg2, nbuf2, ncol, emsg, ebuf1, emsg2, ebuf2, eall, gmsg, gbuf, rmsg, rbuf1, bmsg, bbuf,
    kref, kimf, cref, zref, sref, kre2, kim2, qvec, gvec, result, inverse, kref2, kimf2, qref, gref,
    ksum, ksum2, ksumf, ksumf2,
    load_sem, halo_send, halo_recv, v_send, v_recv, f_send, f_recv, early_sem,
    y_send, y_recv, g_send, g_recv, r_sem, b_sem, ready,
):
    sec = lax.axis_index("section")
    pix = lax.axis_index("pix")
    before = lax.rem(pix + (PIX - 1), PIX)
    after = lax.rem(pix + 1, PIX)
    near = (before, pix, after)
    present = (pix > 0, pix >= 0, pix < PIX - 1)
    inner = jnp.logical_and(present[0], present[2])
    sec_up = lax.rem(sec + 1, SECTIONS)
    sec_down = lax.rem(sec + (SECTIONS - 1), SECTIONS)
    x = pix // 16
    z = lax.rem(pix // 2, 8)
    core = lax.rem(pix, 2)
    group = x * 2 + core
    first = []
    second = []
    for d in range(1, 8):
        g = lax.rem(group + d, 8)
        first.append((g // 2) * 16 + z * 2 + lax.rem(g, 2))
        second.append(x * 16 + lax.rem(z + d, 8) * 2 + core)

    want = ref[0] - pix * (TILES * 128)

    def at_ref(parts):
        total = None
        for t, part in enumerate(parts):
            lane = lax.broadcasted_iota(jnp.int32, part.shape, 1)
            part = jnp.where(lane == want - t * 128, part, 0.0)
            total = part if total is None else total + part
        return jnp.sum(total, axis=1, keepdims=True)

    def arrived(ref, sem):
        pltpu.make_async_copy(ref, ref, sem).wait()

    def start(src, dst, sem, devices):
        for i, device in enumerate(devices):
            remote(src, dst.at[i], sem.at[0], sem.at[1], (sec, device)).start()

    def finish(src, dst, sem, devices):
        arrived(dst, sem.at[0])
        arrived(dst, sem.at[1])

    def sum_of(own, buffers):
        total = own[...]
        for i in range(7):
            total = total + buffers[i]
        return total

    steps_n = (nmsg, nbuf1, early_sem.at[0], first), (nmsg2, nbuf2, early_sem.at[1], second)
    steps_e = (emsg, ebuf1, early_sem.at[0], first), (emsg2, ebuf2, early_sem.at[1], second)
    steps_r = (rmsg, rbuf1, r_sem, first)
    steps_b = (bmsg, bbuf, b_sem, second)

    chunks = [(0, 3), (3, GROUPS)]
    spans = [pl.ds(32 * low, min(32 * high, FLAT) - 32 * low) for low, high in chunks]
    loads = [
        pltpu.make_async_copy(slc_hbm.at[span], blocks.at[1, span], load_sem.at[i]) for i, span in enumerate(spans)
    ]
    loads.append(pltpu.make_async_copy(nbr_hbm, nbr, load_sem.at[2]))
    for load in loads:
        load.start()
    barrier = pltpu.get_barrier_semaphore()
    aside = [(sec_up, pix), (sec_down, pix)]
    plane = [(sec, x * 16 + lax.rem(z + d, 8) * 2 + core) for d in (1, 7)]
    plane += [(sec, lax.rem(x + d, 4) * 16 + z * 2 + core) for d in (1, 3)]
    leads = sec == 0
    follows = sec > 0

    def signal(sem, devices):
        for device in devices:
            pl.semaphore_signal(sem, inc=1, device_id=device, device_id_type=MESH)

    def greet(sem):
        for i in (0, 2):
            pl.when(present[i])(lambda i=i: signal(sem, [(sec, near[i])]))

    def tell(sem):
        greet(sem)
        signal(sem, aside)
        pl.when(follows)(lambda: signal(sem, plane))

    def receive(sem, lead, follow):
        for first_one, wanted in ((leads, lead), (follows, follow)):
            pl.when(jnp.logical_and(first_one, inner))(lambda wanted=wanted: pl.semaphore_wait(sem, wanted))
            pl.when(jnp.logical_and(first_one, jnp.logical_not(inner)))(
                lambda wanted=wanted: pl.semaphore_wait(sem, wanted - 1)
            )

    def hear(sem):
        receive(sem, 4, 8)

    greet(barrier)
    pl.when(sec != SECTIONS - 1)(lambda: signal(barrier, aside[:1]))
    pl.when(sec != 1)(lambda: signal(barrier, aside[1:]))
    pl.when(follows)(lambda: signal(barrier, plane))
    receive(barrier, 2, 8)
    greet(ready.at[0])
    pl.when(follows)(lambda: signal(ready.at[0], aside + plane))

    def halo(i, n):
        part = blocks.at[1, spans[n]]
        return remote(part, blocks.at[2 - i, spans[n]], halo_send.at[i // 2], halo_recv.at[i // 2, n], (sec, near[i]))

    for n in range(len(chunks)):
        loads[n].wait()
        pl.when(jnp.logical_and(present[0], core == 0))(halo(0, n).start)
        pl.when(present[2])(halo(2, n).start)
        pl.when(jnp.logical_and(present[0], core == 1))(halo(0, n).start)

    for i in range(3):
        blocks[i, FLAT:, :] = jnp.zeros((32 * GROUPS - FLAT, 128), F32)
    kre[...] = jnp.zeros_like(kre)
    kim[...] = jnp.zeros_like(kim)
    red[...] = jnp.zeros_like(red)
    cvec[...] = jnp.zeros_like(cvec)
    bvec[...] = jnp.zeros_like(bvec)
    for i in (0, 2):

        @pl.when(jnp.logical_not(present[i]))
        def _():
            blocks[i] = jnp.zeros((32 * GROUPS, 128), F32)
            vbuf[i] = jnp.zeros_like(vbuf[i])

    loads[2].wait()

    base = pix * (TILES * 128) - REACH
    for t in range(TILES):
        rel = nbr[:, t * 128 : (t + 1) * 128] - (base + t * 128)
        lanes[t, 0:NB, :] = jnp.bitwise_and(rel, 127)
        tiles[t, 0:NB, :] = jnp.right_shift(rel, 7)
        lanes[t, NB : NB + 1, :] = jnp.zeros((1, 128), jnp.int32)
        tiles[t, NB : NB + 1, :] = jnp.full((1, 128), SPAN, jnp.int32)

    def spread(i, groups=range(GROUPS)):
        for g in groups:
            for m in range(2):
                for c in range(2):
                    ext[2 * i + m, c, g * 8 : (g + 1) * 8, :] = blocks[i, pl.ds(g * 32 + m * 2 + c, 8, stride=4), :]

    spread(1)
    for t in range(TILES):
        for c in range(2):
            total = None
            for g in range(GROUPS):
                own = ext[2 + t, c, g * 8 : (g + 1) * 8, :]
                zs[t, 0, c, g * 8 : (g + 1) * 8, :] = own
                total = own if total is None else total + own
            xsum[t, c : c + 1, :] = column_sum(total)

    def gather(t, offsets, begin, groups=range(GROUPS), halves=None):
        def some(half):
            for i in range(NB // 2):
                k = 1 + half * (NB // 2) + i
                lane = bcast(lanes[t, pl.ds(k, 1), :])
                tile = bcast(tiles[t, pl.ds(k, 1), :])
                for g in groups:
                    rows = slice(g * 8, (g + 1) * 8)
                    for c in range(2):
                        out = None if begin else zs[t, k, c, rows, :]
                        for m in offsets:
                            got = take(ext[t + m, c, rows, :], lane)
                            out = got if out is None else jnp.where(tile == m, got, out)
                        zs[t, k, c, rows, :] = out

        if halves is None:
            pl.loop(0, 2)(some)
        else:
            for half in halves:
                some(half)

    for t in range(TILES):
        gather(t, (2 - t, 3 - t), True)

    def side(s, groups, halves=None):
        spread(2 * s, groups)
        close, distant = 1 + 3 * s, 5 * s
        gather(s, (close - s, distant - s), False, groups, halves)
        gather(1 - s, (close - (1 - s),), False, groups, halves)

    def both(soon):
        late = 1 - soon
        for n in range(len(chunks)):
            arrived(blocks.at[2 * soon, spans[n]], halo_recv.at[1 - soon, n])
        side(soon, range(GROUPS))
        hear(ready.at[0])
        pl.when(leads)(lambda: signal(ready.at[0], aside))
        tell(ready.at[1])
        for n, (low, high) in enumerate(chunks):
            pl.when(inner)(lambda n=n: arrived(blocks.at[2 * late, spans[n]], halo_recv.at[1 - late, n]))
            side(late, range(low, high), range(2))

    pl.when(core == 0)(lambda: both(1))
    pl.when(core == 1)(lambda: both(0))

    @pl.when(sec >= 2)
    def _():
        hear(ready.at[1])
        tell(ready.at[2])

    @pl.when(sec == 2)
    def _():
        column = at_ref([nbr[:, t * 128 : (t + 1) * 128].astype(F32) for t in range(TILES)])
        nmsg[...] = to_row(column)
        start(*steps_n[0])

    @pl.loop(0, TILES)
    def _(t):
        for g in range(GROUPS):
            rows = slice(g * 8, (g + 1) * 8)
            power = None
            for k in range(NB):
                re, im = zs[t, k, 0, rows, :], zs[t, k, 1, rows, :]
                zs[t, k, 2, rows, :] = re - im
                term = re * re + im * im
                power = term if power is None else power + term
            wbuf[t, rows, :] = lax.rsqrt(jnp.maximum(power, 1.0))

        def fold(slot, parts):
            for i, part in enumerate(parts):
                red[slot, i * 8 : (i + 1) * 8, :] = part
            total = None
            for i in range(8):
                row = red[slot, pl.ds(i, 8, stride=8), :]
                total = row if total is None else total + row
            return total

        slot = 0
        for l in range(NB + 1):
            for kg in range(2):
                low, high = 8 * kg, min(8 * kg + 8, l + 1, NB)
                if high <= low:
                    continue
                count = high - low
                p, q, r = [None] * count, [None] * count, [None] * count
                cr, ci = [None] * count, [None] * count

                def put(box, i, value):
                    box[i] = value if box[i] is None else box[i] + value

                for g in range(GROUPS):
                    rows = slice(g * 8, (g + 1) * 8)
                    w = wbuf[t, rows, :]
                    if l < NB:
                        w2 = w * w
                        lr, li = zs[t, l, 0, rows, :] * w2, zs[t, l, 1, rows, :] * w2
                    else:
                        lr, li = zs[t, 0, 0, rows, :] * w, zs[t, 0, 1, rows, :] * w
                    le = lr + li
                    for i in range(count):
                        k = low + i
                        kr, ki = zs[t, k, 0, rows, :], zs[t, k, 1, rows, :]
                        put(p, i, kr * lr)
                        put(q, i, ki * li)
                        if k != l:
                            put(r, i, zs[t, k, 2, rows, :] * le)
                        if l == NB:
                            put(cr, i, kr * w)
                            put(ci, i, ki * w)
                re = fold(4 * kg + slot, [a + b for a, b in zip(p, q)])
                im = fold(4 * kg + slot + 1, [jnp.zeros((8, 128), F32) if c is None else c + (b - a) for a, b, c in zip(p, q, r)])
                rows = slice(low, low + 8)
                if l < NB:
                    kre[t, l, rows, :] = re
                    kim[t, l, rows, :] = im
                    for i in range(count):
                        k = low + i
                        if k != l:
                            kre[t, k, l : l + 1, :] = re[i : i + 1, :]
                            kim[t, k, l : l + 1, :] = -im[i : i + 1, :]
                else:
                    bvec[t, 0, rows, :] = re
                    bvec[t, 1, rows, :] = im
                    slot = 2 - slot
                    cvec[t, 0, rows, :] = START * fold(4 * kg + slot, cr)
                    cvec[t, 1, rows, :] = -START * fold(4 * kg + slot + 1, ci)
                slot = 2 - slot
        ksum[t] = kre[t] + kim[t]

    def pieces(count):
        return [(t, c, kg) for t in range(count) for c in range(2) for kg in range(2)]

    def load(ref, count):
        return [ref[t, c, 8 * kg : 8 * kg + 8, :] for t, c, kg in pieces(count)]

    def save(ref, value):
        for (t, c, kg), part in zip(pieces(len(value) // 4), value):
            ref[t, c, 8 * kg : 8 * kg + 8, :] = part

    def plus(*values):
        return [sum(parts[1:], parts[0]) for parts in zip(*values)]

    def times(factor, value):
        return [factor * part for part in value]

    def product(m, box, value):
        for t in range(len(value) // 4):
            for kg in range(2):
                re, im = value[4 * t + kg], value[4 * t + 2 + kg]
                for c, part in enumerate((re, im, re + im)):
                    box[t, c, 8 * kg : 8 * kg + 8, :] = part
        out = []
        for t in range(len(value) // 4):
            y = [[None, None] for _ in range(3)]
            for l in range(NB):
                for c in range(3):
                    row = bcast(box[t, c, l : l + 1, :])
                    for kg in range(2):
                        part = m[c][t, l, 8 * kg : 8 * kg + 8, :] * row
                        y[c][kg] = part if l == 0 else y[c][kg] + part
            out += [y[0][kg] - y[1][kg] for kg in range(2)]
            out += [y[2][kg] - (y[0][kg] + y[1][kg]) for kg in range(2)]
        return out

    def prepare(m3, s3, cv, qv, box, count):
        mr, mi, _ = m3
        sr, si, _ = s3
        for t in range(count):

            @pl.loop(0, NB)
            def _(l):
                for kg in range(2):
                    rows = slice(8 * kg, 8 * kg + 8)
                    re, im = 2.0 * mr[t, l, rows, :], 2.0 * mi[t, l, rows, :]
                    for m in range(NB):
                        lr = bcast(mr[t, l, m : m + 1, :])
                        li = bcast(mi[t, l, m : m + 1, :])
                        ar, ai = mr[t, m, rows, :], mi[t, m, rows, :]
                        re = re + (ar * lr - ai * li)
                        im = im + (ar * li + ai * lr)
                    sr[t, l, rows, :] = re
                    si[t, l, rows, :] = im

        save(qv, product(m3, box, load(cv, count)))

    def joined(z, value):
        out = []
        for t in range(len(value) // 4):
            zr, zi = z[4 * t : 4 * t + 2], z[4 * t + 2 : 4 * t + 4]
            vr, vi = value[4 * t : 4 * t + 2], value[4 * t + 2 : 4 * t + 4]
            ar = column_sum(zr[0] * vr[0] - zi[0] * vi[0] + (zr[1] * vr[1] - zi[1] * vi[1]))
            ai = column_sum(zr[0] * vi[0] + zi[0] * vr[0] + (zr[1] * vi[1] + zi[1] * vr[1]))
            out += [zr[i] * ar + zi[i] * ai for i in range(2)] + [zr[i] * ai - zi[i] * ar for i in range(2)]
        return out

    def conj(value):
        return [part if (i // 2) % 2 == 0 else -part for i, part in enumerate(value)]

    def norms_of(value, image, start):
        out = []
        for t in range(len(value) // 4):
            total = None
            for i in range(4 * t, 4 * t + 4):
                term = value[i] * (image[i] + (2.0 * SCALE) * start[i])
                total = term if total is None else total + term
            out.append(lax.rsqrt(column_sum(total) + SCALE * SCALE))
        return out

    def solve(m3, cv, box, count):
        def turn(_, value):
            return tuple(plus(value, product(m3, box, value), load(cv, count)))

        value = lax.fori_loop(0, ITERS - 1, turn, tuple(load(cv, count)))
        value = times(SCALE, value)
        return value, norms_of(value, product(m3, box, value), load(cv, count))

    def solve_joined(m3, s3, cv, qv, zv, box, gbox, count):
        z = load(zv, count)
        r = conj(z)
        kr = product(m3, box, r)
        c = plus(load(cv, count), times(START, r))
        g = plus(r, kr)
        for t in range(count):
            squares = [z[4 * t + i] * z[4 * t + i] for i in range(4)]
            half = 0.5 * column_sum(squares[0] + squares[1] + (squares[2] + squares[3]))
            for i in range(4 * t, 4 * t + 4):
                g[i] = g[i] + half * r[i]
        save(gbox, g)
        sr, si, both = s3
        for t in range(count):
            for l in range(NB):
                zr, zi = bcast(zv[t, 0, l : l + 1, :]), bcast(zv[t, 1, l : l + 1, :])
                gr, gi = bcast(gbox[t, 0, l : l + 1, :]), bcast(gbox[t, 1, l : l + 1, :])
                for kg in range(2):
                    rows = slice(8 * kg, 8 * kg + 8)
                    hr, hi = g[4 * t + kg], g[4 * t + 2 + kg]
                    xr, xi = z[4 * t + kg], z[4 * t + 2 + kg]
                    re = sr[t, l, rows, :] + (hr * zr - hi * zi + (xr * gr - xi * gi))
                    im = si[t, l, rows, :] + (hr * zi + hi * zr - (xr * gi + xi * gr))
                    sr[t, l, rows, :] = re
                    si[t, l, rows, :] = im
                    both[t, l, rows, :] = re + im

        def square(value):
            return plus(value, product(s3, box, value))

        value = plus(c, c, load(qv, count), times(START, kr), joined(z, c))
        value = plus(value, square(value))
        value = plus(value, square(square(value)))

        last = lax.fori_loop(0, 4, lambda _, v: tuple(square(v)), tuple(value))
        value = times(SCALE, plus(value, last))
        image = plus(product(m3, box, value), joined(z, value))
        return value, norms_of(value, image, c)

    def step_one():
        @pl.when(sec == 2)
        def _():
            arrived(gbuf.at[1:8], g_recv)

        @pl.when(sec != 2)
        def _():
            arrived(gbuf.at[0:8], g_recv)

        total = gbuf[0]
        for d in range(1, 8):
            total = total + gbuf[d]
        bmsg[2:4, :] = total
        bmsg[0:2, :] = jnp.zeros((2, 128), F32)

        @pl.when(sec < SECTIONS - 1)
        def _():
            finish(*steps_r)
            bmsg[0:2, :] = sum_of(rmsg, rbuf1)

        pl.when(leads)(lambda: hear(ready.at[4]))
        start(*steps_b)

    @pl.when(sec == 1)
    def _():
        hear(ready.at[1])
        tell(ready.at[2])

    def prepare_own():
        prepare((kre, kim, ksum), (kre2, kim2, ksum2), cvec, qvec, sbuf, TILES)

    pl.when(jnp.logical_or(sec == 1, sec == 2))(prepare_own)

    @pl.when(sec == 2)
    def _():
        finish(*steps_n[0])
        hear(ready.at[2])
        tell(ready.at[3])
        nmsg2[...] = sum_of(nmsg, nbuf1)
        start(*steps_n[1])

    def expand():
        for l in range(NB):
            kref[0, l] = jnp.broadcast_to(eall[0:16, l : l + 1], (16, 128))
            kimf[0, l] = jnp.broadcast_to(eall[0:16, 16 + l : 17 + l], (16, 128))
        for c in range(2):
            cref[0, c] = jnp.broadcast_to(eall[0:16, 32 + c : 33 + c], (16, 128))
        ksumf[...] = kref[...] + kimf[...]
        prepare((kref, kimf, ksumf), (kref2, kimf2, ksumf2), cref, qref, sref, 1)

    @pl.when(sec == SECTIONS - 1)
    def _():
        lane = lax.broadcasted_iota(jnp.int32, (16, 128), 1)
        emsg[16:32, :] = jnp.zeros((16, 128), F32)
        acc = jnp.zeros((16, 128), F32)
        for c in range(2):
            acc = jnp.where(lane == 32 + c, at_ref([cvec[t, c] for t in range(TILES)]), acc)
        emsg[0:16, :] = acc

        @pl.loop(0, NB)
        def _(k):
            acc = emsg[0:16, :]
            acc = jnp.where(lane == k, at_ref([kre[t, k] for t in range(TILES)]), acc)
            emsg[0:16, :] = jnp.where(lane == 16 + k, at_ref([kim[t, k] for t in range(TILES)]), acc)
            parts = [at_ref([zs[t, k, c] * wbuf[t] for t in range(TILES)]) for c in range(2)]
            emsg[pl.ds(16 + k, 1), :] = to_row(parts[0]) + to_row(parts[1], 64)

        start(*steps_e[0])
        prepare_own()
        finish(*steps_e[0])
        hear(ready.at[2])
        tell(ready.at[3])
        emsg2[...] = sum_of(emsg, ebuf1)
        start(*steps_e[1])
        hear(ready.at[3])
        tell(ready.at[4])
        step_one()
        finish(*steps_e[1])
        eall[...] = sum_of(emsg2, ebuf2)
        for j in range(SECTIONS - 1):
            remote(eall.at[pl.ds(0, 16)], eall.at[pl.ds(0, 16)], y_send, y_recv, (j, pix)).start()
        expand()

    @pl.when(sec == 2)
    def _():
        finish(*steps_n[1])
        column = to_column(sum_of(nmsg2, nbuf2), 16)
        row = lax.broadcasted_iota(jnp.int32, (16, 128), 0)
        ncol[...] = jnp.where(row == NB, ref[0].astype(F32), column) - (pix * (TILES * 128)).astype(F32)

    def keep(solved):
        value, norms = solved
        save(result, value)
        for t, norm in enumerate(norms):
            inverse[t] = norm

    @pl.when(sec == 0)
    def _():
        zbuf[...] = jnp.zeros_like(zbuf)
        keep(solve((kre, kim, ksum), cvec, sbuf, TILES))

    @pl.when(sec > 0)
    def _():
        pl.when(inner)(lambda: arrived(vbuf, v_recv))
        pl.when(jnp.logical_not(inner))(lambda: arrived(vbuf.at[0:2], v_recv))
        for t in range(TILES):
            z0 = []
            for kg in range(2):
                rows = slice(8 * kg, 8 * kg + 8)
                lane = lanes[t, rows, :]
                tile = tiles[t, rows, :]
                pair = []
                for c in range(2):
                    src = []
                    for m in range(SPAN):
                        at = t + m
                        src.append(bcast(vbuf[at // 2, c : c + 1, (at % 2) * 128 : (at % 2) * 128 + 128]))
                    pair.append(pick(src, lane, tile))
                z0.append(pair)
            power = column_sum(z0[0][0] * z0[0][0] + z0[0][1] * z0[0][1] + (z0[1][0] * z0[1][0] + z0[1][1] * z0[1][1]))
            w = lax.rsqrt(jnp.maximum(power, 1.0))
            vr = vbuf[1, 0:1, t * 128 : (t + 1) * 128]
            vi = vbuf[1, 1:2, t * 128 : (t + 1) * 128]
            xsum[t, 0:1, :] = xsum[t, 0:1, :] + vr
            xsum[t, 1:2, :] = xsum[t, 1:2, :] + vi
            for kg in range(2):
                rows = slice(8 * kg, 8 * kg + 8)
                zr, zi = z0[kg][0] * w, z0[kg][1] * w
                zbuf[t, 0, rows, :] = zr
                zbuf[t, 1, rows, :] = zi
                bvec[t, 0, rows, :] = bvec[t, 0, rows, :] + (zr * vr + zi * vi)
                bvec[t, 1, rows, :] = bvec[t, 1, rows, :] + (zr * vi - zi * vr)
        keep(solve_joined((kre, kim, ksum), (kre2, kim2, ksum2), cvec, qvec, zbuf, sbuf, gvec, TILES))

    state = load(result, TILES)
    norms = [inverse[t] for t in range(TILES)]
    for t in range(TILES):
        s = state[4 * t : 4 * t + 4]
        cr = ci = None
        for kg in range(2):
            rows = slice(8 * kg, 8 * kg + 8)
            sr, si = s[kg], s[2 + kg]
            br, bi = bvec[t, 0, rows, :], bvec[t, 1, rows, :]
            a, b = sr * br + si * bi, sr * bi - si * br
            cr = a if kg == 0 else column_sum(cr + a)
            ci = b if kg == 0 else column_sum(ci + b)
        cols = slice(t * 128, (t + 1) * 128)
        msg[0:1, cols] = (cr + (SCALE * START) * xsum[t, 0:1, :]) * norms[t]
        msg[1:2, cols] = (ci + (SCALE * START) * xsum[t, 1:2, :]) * norms[t]

    def send_virtual():
        for i in range(3):
            pl.when(present[i])(remote(msg, vbuf.at[2 - i], v_send, v_recv, (sec_up, near[i])).start)

    pl.when(sec < 2)(send_virtual)
    for t in range(TILES):
        s = state[4 * t : 4 * t + 4]
        fr = fi = None
        for kg in range(2):
            rows = slice(8 * kg, 8 * kg + 8)
            sr, si = s[kg], s[2 + kg]
            zr, zi = zbuf[t, 0, rows, :], zbuf[t, 1, rows, :]
            e, f = zr * sr - zi * si, zr * si + zi * sr
            fr = e if kg == 0 else column_sum(fr + e)
            fi = f if kg == 0 else column_sum(fi + f)
        cols = slice(t * 128, (t + 1) * 128)
        fr, fi = unit((fr + SCALE * START) * norms[t], fi * norms[t])
        fmsg[0:1, cols] = fr
        fmsg[1:2, cols] = fi

    steps_g = [
        remote(gmsg, gbuf.at[d], g_send, g_recv, (s, pix if d == 0 else first[d - 1]))
        for s in range(SECTIONS)
        for d in range(8)
        if (s, d) != (2, 0)
    ]

    @pl.when(sec == 2)
    def _():
        hear(ready.at[3])
        lane = lax.broadcasted_iota(jnp.int32, (16, 128), 1).astype(F32)
        row = lax.broadcasted_iota(jnp.int32, (16, 128), 0)
        for c in range(2):
            total = None
            for t in range(TILES):
                cols = slice(t * 128, (t + 1) * 128)
                value = jnp.where(
                    row == NB,
                    jnp.broadcast_to(fmsg[c : c + 1, cols], (16, 128)),
                    jnp.broadcast_to(msg[c : c + 1, cols], (16, 128)),
                )
                value = jnp.where(ncol[...] - t * 128.0 == lane, value, 0.0)
                total = value if total is None else total + value
            gmsg[c : c + 1, :] = to_row(jnp.sum(total, axis=1, keepdims=True))
        for copy in steps_g:
            copy.start()
        gbuf[0] = gmsg[...]
        tell(ready.at[4])

    pl.when(sec == 2)(send_virtual)

    for s in range(1, SECTIONS):

        @pl.when(sec == s)
        def _():
            for j in range(s):
                remote(fmsg, fbuf.at[s - 1], f_send, f_recv.at[s - 1], (j, pix)).start()

    @pl.when(sec == 0)
    def _():
        hear(ready.at[1])
        tell(ready.at[2])

    @pl.when(sec < 2)
    def _():
        hear(ready.at[2])
        tell(ready.at[3])
        hear(ready.at[3])
        tell(ready.at[4])

    comp[0, 0:1, :] = msg[0:1, :]
    comp[1, 0:1, :] = msg[1:2, :]

    def vector():
        for i, (t, c, kg) in enumerate((t, c, kg) for t in range(TILES) for c in range(2) for kg in range(2)):
            sbuf[t, c, 8 * kg : 8 * kg + 8, :] = result[t, c, 8 * kg : 8 * kg + 8, :] * inverse[t]
        for t in range(TILES):

            @pl.loop(0, GROUPS)
            def _(g):
                rows = pl.ds(pl.multiple_of(g * 8, 8), 8)
                re = im = None
                for k in range(NB):
                    sr = bcast(sbuf[t, 0, k : k + 1, :])
                    si = bcast(sbuf[t, 1, k : k + 1, :])
                    zr, zi = zs[t, k, 0, rows, :], zs[t, k, 1, rows, :]
                    a, b = zr * sr - zi * si, zr * si + zi * sr
                    re = a if re is None else re + a
                    im = b if im is None else im + b
                w = wbuf[t, rows, :]
                series[t, 0, rows, :] = bcast((SCALE * START) * inverse[t]) + w * re
                series[t, 1, rows, :] = w * im

    pl.when(sec < SECTIONS - 1)(vector)

    def take_f(j):
        arrived(fbuf.at[j - 1], f_recv.at[j - 1])

    @pl.when(sec == 0)
    def _():
        take_f(1)
        for t in range(TILES):
            fr = fbuf[0, 0:1, t * 128 : (t + 1) * 128]
            fi = fbuf[0, 1:2, t * 128 : (t + 1) * 128]
            re, im = series[t, 0], series[t, 1]
            series[t, 0] = re * fr - im * fi
            series[t, 1] = re * fi + im * fr

    @pl.when(sec < SECTIONS - 1)
    def _():
        for c in range(2):
            rmsg[c : c + 1, :] = to_row(at_ref([series[t, c] for t in range(TILES)]))
        start(*steps_r)

    pl.when(sec < SECTIONS - 1)(step_one)

    pl.when(sec == SECTIONS - 1)(vector)

    @pl.when(sec < SECTIONS - 1)
    def _():
        remote(eall.at[pl.ds(0, 16)], eall.at[pl.ds(0, 16)], y_send, y_recv, (SECTIONS - 1, pix)).wait_recv()
        expand()

    finish(*steps_b)
    total = sum_of(bmsg, bbuf)

    values = [to_column(total[2 + c : 3 + c, :], 16) for c in range(2)]
    f2r, f2i = values[0][NB:16], values[1][NB:16]
    row = lax.broadcasted_iota(jnp.int32, (16, 128), 0)
    zr, zi = (jnp.where(row < NB, value, 0.0) for value in values)
    w = lax.rsqrt(jnp.maximum(column_sum(zr * zr + zi * zi), 1.0))
    zr, zi = zr * w, zi * w
    zref[0, 0] = zr
    zref[0, 1] = zi
    state_ref, norm_ref = solve_joined((kref, kimf, ksumf), (kref2, kimf2, ksumf2), cref, qref, zref, sref, gref, 1)
    sr = jnp.concatenate(state_ref[0:2], axis=0)
    si = jnp.concatenate(state_ref[2:4], axis=0)
    norm = norm_ref[0]
    f3r = column_sum(zr * sr - zi * si)
    f3i = column_sum(zr * si + zi * sr)
    f3r, f3i = unit((f3r + SCALE * START) * norm, f3i * norm)
    fr = jnp.where(sec < 2, f3r * f2r - f3i * f2i, f3r)
    fi = jnp.where(sec < 2, f3r * f2i + f3i * f2r, f3i)
    vr, vi = total[0:1, :], total[1:2, :]
    rmsg[0:1, :] = vr * fr - vi * fi
    rmsg[1:2, :] = vr * fi + vi * fr

    @pl.when(sec == SECTIONS - 1)
    def _():
        z = eall[16:32, :]
        a = bcast(column_sum(z * sr))
        b = bcast(column_sum(z * si))
        re = a - pltpu.roll(b, 64, 1)
        im = b + pltpu.roll(a, 64, 1)
        rmsg[0:1, :] = (re[0:1] + SCALE * START) * norm
        rmsg[1:2, :] = im[0:1] * norm

    ur, ui = unit(rmsg[0:1, :], rmsg[1:2, :])
    ur, ui = GAIN * to_column(ur, PAD), GAIN * to_column(ui, PAD)

    datum[0:1, :] = jnp.ones((1, TILES * 128), F32)
    datum[1:2, :] = jnp.zeros((1, TILES * 128), F32)

    @pl.when(sec < SECTIONS - 1)
    def _():
        take_f(3)
        datum[...] = fbuf[2]

    @pl.when(sec < 2)
    def _():
        take_f(2)
        dr, di = datum[0:1, :], datum[1:2, :]
        fr, fi = fbuf[1, 0:1, :], fbuf[1, 1:2, :]
        datum[0:1, :] = dr * fr - di * fi
        datum[1:2, :] = dr * fi + di * fr

    for t in range(TILES):
        dr, di = datum[0:1, t * 128 : (t + 1) * 128], datum[1:2, t * 128 : (t + 1) * 128]
        re, im = series[t, 0], series[t, 1]
        re, im = re * dr - im * di, re * di + im * dr
        for c, part in enumerate((re * ur + im * ui, im * ur - re * ui)):
            for g in range(GROUPS):
                count = min(8, ROWS - g * 8)
                phases[pl.ds(g * 32 + t * 2 + c, count, stride=4), :] = part[g * 8 : g * 8 + count]

    pl.when(follows)(lambda: hear(ready.at[4]))
    for i in (0, 2):
        pl.when(present[i])(lambda i=i: arrived(blocks.at[1, pl.ds(0, FLAT)], halo_send.at[i // 2]))
    @pl.when(sec == 2)
    def _():
        arrived(gbuf, g_send)

    @pl.when(sec == SECTIONS - 1)
    def _():
        arrived(ebuf1.at[0:3, 0:16], y_send)

    @pl.when(sec < SECTIONS - 1)
    def _():
        pl.when(inner)(lambda: arrived(vbuf, v_send))
        pl.when(jnp.logical_not(inner))(lambda: arrived(vbuf.at[0:2], v_send))

    for s in range(1, SECTIONS):

        @pl.when(sec == s)
        def _():
            arrived(fbuf.at[0:s], f_send)


def hand_out(phases_in, comp_in, phases, comp, sem):
    copies = [
        pltpu.make_async_copy(phases_in, phases, sem.at[0]),
        pltpu.make_async_copy(comp_in, comp, sem.at[1]),
    ]
    for copy in copies:
        copy.start()
    for copy in copies:
        copy.wait()


def on_device(slc, neighbours, reference_pixel):
    vmem = pl.BlockSpec(memory_space=pltpu.VMEM)
    hbm = pl.BlockSpec(memory_space=pltpu.HBM)
    pixels = slc.shape[2]
    dma = pltpu.SemaphoreType.DMA
    flat = slc.reshape(2, ROWS, TILES, 128).transpose(1, 2, 0, 3).reshape(FLAT, 128)
    phases, comp = pl.pallas_call(
        kernel,
        out_shape=(
            jax.ShapeDtypeStruct((FLAT, 128), F32),
            jax.ShapeDtypeStruct((2, 1, pixels), F32),
        ),
        in_specs=[hbm, hbm, pl.BlockSpec(memory_space=pltpu.SMEM)],
        out_specs=(vmem, vmem),
        scratch_shapes=[
            pltpu.VMEM((NB, pixels), jnp.int32),
            pltpu.VMEM((3, 32 * GROUPS, 128), F32),
            pltpu.VMEM((6, 2, PAD, 128), F32),
            pltpu.VMEM((TILES, 16, 128), jnp.int32),
            pltpu.VMEM((TILES, 16, 128), jnp.int32),
            pltpu.VMEM((TILES, NB, 3, PAD, 128), F32),
            pltpu.VMEM((TILES, PAD, 128), F32),
            pltpu.VMEM((8, 64, 128), F32),
            pltpu.VMEM((TILES, 16, 16, 128), F32),
            pltpu.VMEM((TILES, 16, 16, 128), F32),
            pltpu.VMEM((TILES, 2, 16, 128), F32),
            pltpu.VMEM((TILES, 2, 16, 128), F32),
            pltpu.VMEM((TILES, 2, 128), F32),
            pltpu.VMEM((TILES, 2, 16, 128), F32),
            pltpu.VMEM((TILES, 3, 16, 128), F32),
            pltpu.VMEM((3, 2, pixels), F32),
            pltpu.VMEM((2, pixels), F32),
            pltpu.VMEM((2, pixels), F32),
            pltpu.VMEM((3, 2, pixels), F32),
            pltpu.VMEM((TILES, 2, PAD, 128), F32),
            pltpu.VMEM((2, pixels), F32),
            pltpu.VMEM((1, 128), F32),
            pltpu.VMEM((7, 1, 128), F32),
            pltpu.VMEM((1, 128), F32),
            pltpu.VMEM((7, 1, 128), F32),
            pltpu.VMEM((16, 128), F32),
            pltpu.VMEM((32, 128), F32),
            pltpu.VMEM((7, 32, 128), F32),
            pltpu.VMEM((32, 128), F32),
            pltpu.VMEM((7, 32, 128), F32),
            pltpu.VMEM((32, 128), F32),
            pltpu.VMEM((2, 128), F32),
            pltpu.VMEM((31, 2, 128), F32),
            pltpu.VMEM((2, 128), F32),
            pltpu.VMEM((7, 2, 128), F32),
            pltpu.VMEM((4, 128), F32),
            pltpu.VMEM((7, 4, 128), F32),
            pltpu.VMEM((1, 16, 16, 128), F32),
            pltpu.VMEM((1, 16, 16, 128), F32),
            pltpu.VMEM((1, 2, 16, 128), F32),
            pltpu.VMEM((1, 2, 16, 128), F32),
            pltpu.VMEM((1, 3, 16, 128), F32),
            pltpu.VMEM((TILES, 16, 16, 128), F32),
            pltpu.VMEM((TILES, 16, 16, 128), F32),
            pltpu.VMEM((TILES, 2, 16, 128), F32),
            pltpu.VMEM((TILES, 2, 16, 128), F32),
            pltpu.VMEM((TILES, 2, 16, 128), F32),
            pltpu.VMEM((TILES, 1, 128), F32),
            pltpu.VMEM((1, 16, 16, 128), F32),
            pltpu.VMEM((1, 16, 16, 128), F32),
            pltpu.VMEM((1, 2, 16, 128), F32),
            pltpu.VMEM((1, 2, 16, 128), F32),
            pltpu.VMEM((TILES, 16, 16, 128), F32),
            pltpu.VMEM((TILES, 16, 16, 128), F32),
            pltpu.VMEM((1, 16, 16, 128), F32),
            pltpu.VMEM((1, 16, 16, 128), F32),
            dma((3,)),
            dma((2,)),
            dma((2, 2)),
            dma(()),
            dma(()),
            dma(()),
            dma((3,)),
            dma((2, 2)),
            dma(()),
            dma(()),
            dma(()),
            dma(()),
            dma((2,)),
            dma((2,)),
            pltpu.SemaphoreType.REGULAR((5,)),
        ],
        compiler_params=pltpu.CompilerParams(
            collective_id=0, has_side_effects=True, vmem_limit_bytes=16 * 2**20
        ),
        cost_estimate=pl.CostEstimate(flops=100_000_000, bytes_accessed=1_000_000, transcendentals=0),
    )(*(pltpu.with_memory_space_constraint(a, pltpu.HBM) for a in (flat, neighbours)), reference_pixel)
    phases, comp = pl.pallas_call(
        hand_out,
        out_shape=(
            jax.ShapeDtypeStruct((FLAT, 128), F32),
            jax.ShapeDtypeStruct((2, 1, pixels), F32),
        ),
        in_specs=[pl.BlockSpec(memory_space=pl.ANY)] * 2,
        out_specs=(hbm, hbm),
        scratch_shapes=[dma((2,))],
        compiler_params=pltpu.CompilerParams(vmem_limit_bytes=2**20),
    )(phases, comp)
    return phases.reshape(ROWS, TILES, 2, 128).transpose(2, 0, 1, 3).reshape(2, ROWS, pixels), comp


def solution(mesh):
    return jax.shard_map(
        on_device,
        mesh=mesh,
        in_specs=(P(None, "section", "pix"), P(None, "pix"), P()),
        out_specs=(P(None, "section", "pix"), P(None, "section", "pix")),
        check_vma=False,
    )
```

```python
import math

import jax
import jax.numpy as jnp
from jax import lax
from jax.experimental import pallas as pl
from jax.experimental.pallas import tpu as pltpu
from jax.sharding import PartitionSpec as P

ITERS = 16
FLOOR = 0.05
REACH = 256
NB = 15
ROWS = 50
PAD = 56
GROUPS = PAD // 8
FLAT = 4 * ROWS
TILES = 2
SPAN = 5
SCALE = 2.0**-45
START = 1.0 / math.sqrt(ROWS + 1)
GAIN = math.sqrt(ROWS + 1)
SECTIONS = 4
PIX = 64
MESH = pl.DeviceIdType.MESH
F32 = jnp.float32


def bcast(row):
    return jnp.broadcast_to(row, (8, 128))


def pick(sources, lane, tile):
    out = jnp.zeros((8, 128), F32)
    for m, source in enumerate(sources):
        out = jnp.where(tile == m, take(source, lane), out)
    return out


def take(source, lane):
    return jnp.take_along_axis(source, lane, axis=1, mode="promise_in_bounds")


def column_sum(x):
    return jnp.sum(x, axis=0, keepdims=True)


def eye(count, shift=0):
    lane = lax.broadcasted_iota(jnp.int32, (count, 128), 1)
    return lane == lax.broadcasted_iota(jnp.int32, (count, 128), 0) + shift


def to_row(column, shift=0):
    return column_sum(jnp.where(eye(column.shape[0], shift), column, 0.0))


def to_column(row, count):
    spread = jnp.broadcast_to(row, (count, 128))
    return jnp.sum(jnp.where(eye(count), spread, 0.0), axis=1, keepdims=True)


def unit(re, im):
    scale = 1.0 / jnp.maximum(jnp.sqrt(re * re + im * im), FLOOR)
    return re * scale, im * scale


def remote(src, dst, send, recv, device):
    return pltpu.make_async_remote_copy(
        src_ref=src, dst_ref=dst, send_sem=send, recv_sem=recv, device_id=device, device_id_type=MESH
    )


def kernel(
    slc_hbm, nbr_hbm, ref, phases, comp,
    nbr, blocks, ext, lanes, tiles, zs, wbuf, red, kre, kim, cvec, bvec, xsum, zbuf, sbuf,
    vbuf, msg, fmsg, fbuf, series, datum,
    nmsg, nbuf1, nmsg2, nbuf2, ncol, emsg, ebuf1, emsg2, ebuf2, eall, gmsg, gbuf, rmsg, rbuf1, bmsg, bbuf,
    kref, kimf, cref, zref, sref, kre2, kim2, qvec, gvec, result, inverse, kref2, kimf2, qref, gref,
    ksum, ksum2, ksumf, ksumf2,
    load_sem, halo_send, halo_recv, v_send, v_recv, f_send, f_recv, early_sem,
    y_send, y_recv, g_send, g_recv, r_sem, b_sem, ready,
):
    sec = lax.axis_index("section")
    pix = lax.axis_index("pix")
    before = lax.rem(pix + (PIX - 1), PIX)
    after = lax.rem(pix + 1, PIX)
    near = (before, pix, after)
    present = (pix > 0, pix >= 0, pix < PIX - 1)
    inner = jnp.logical_and(present[0], present[2])
    sec_up = lax.rem(sec + 1, SECTIONS)
    sec_down = lax.rem(sec + (SECTIONS - 1), SECTIONS)
    x = pix // 16
    z = lax.rem(pix // 2, 8)
    core = lax.rem(pix, 2)
    group = x * 2 + core
    first = []
    second = []
    for d in range(1, 8):
        g = lax.rem(group + d, 8)
        first.append((g // 2) * 16 + z * 2 + lax.rem(g, 2))
        second.append(x * 16 + lax.rem(z + d, 8) * 2 + core)

    want = ref[0] - pix * (TILES * 128)

    def at_ref(parts):
        total = None
        for t, part in enumerate(parts):
            lane = lax.broadcasted_iota(jnp.int32, part.shape, 1)
            part = jnp.where(lane == want - t * 128, part, 0.0)
            total = part if total is None else total + part
        return jnp.sum(total, axis=1, keepdims=True)

    def arrived(ref, sem):
        pltpu.make_async_copy(ref, ref, sem).wait()

    def start(src, dst, sem, devices):
        for i, device in enumerate(devices):
            remote(src, dst.at[i], sem.at[0], sem.at[1], (sec, device)).start()

    def finish(src, dst, sem, devices):
        arrived(dst, sem.at[0])
        arrived(dst, sem.at[1])

    def sum_of(own, buffers):
        total = own[...]
        for i in range(7):
            total = total + buffers[i]
        return total

    steps_n = (nmsg, nbuf1, early_sem.at[0], first), (nmsg2, nbuf2, early_sem.at[1], second)
    steps_e = (emsg, ebuf1, early_sem.at[0], first), (emsg2, ebuf2, early_sem.at[1], second)
    steps_r = (rmsg, rbuf1, r_sem, first)
    steps_b = (bmsg, bbuf, b_sem, second)

    chunks = [(0, 3), (3, GROUPS)]
    spans = [pl.ds(32 * low, min(32 * high, FLAT) - 32 * low) for low, high in chunks]
    loads = [
        pltpu.make_async_copy(slc_hbm.at[span], blocks.at[1, span], load_sem.at[i]) for i, span in enumerate(spans)
    ]
    loads.append(pltpu.make_async_copy(nbr_hbm, nbr, load_sem.at[2]))
    for load in loads:
        load.start()
    barrier = pltpu.get_barrier_semaphore()
    aside = [(sec_up, pix), (sec_down, pix)]
    plane = [(sec, x * 16 + lax.rem(z + d, 8) * 2 + core) for d in (1, 7)]
    plane += [(sec, lax.rem(x + d, 4) * 16 + z * 2 + core) for d in (1, 3)]
    leads = sec == 0
    follows = sec > 0

    def signal(sem, devices):
        for device in devices:
            pl.semaphore_signal(sem, inc=1, device_id=device, device_id_type=MESH)

    def greet(sem):
        for i in (0, 2):
            pl.when(present[i])(lambda i=i: signal(sem, [(sec, near[i])]))

    def tell(sem):
        greet(sem)
        signal(sem, aside)
        pl.when(follows)(lambda: signal(sem, plane))

    def receive(sem, lead, follow):
        for first_one, wanted in ((leads, lead), (follows, follow)):
            pl.when(jnp.logical_and(first_one, inner))(lambda wanted=wanted: pl.semaphore_wait(sem, wanted))
            pl.when(jnp.logical_and(first_one, jnp.logical_not(inner)))(
                lambda wanted=wanted: pl.semaphore_wait(sem, wanted - 1)
            )

    def hear(sem):
        receive(sem, 4, 8)

    greet(barrier)
    pl.when(sec != SECTIONS - 1)(lambda: signal(barrier, aside[:1]))
    pl.when(sec != 1)(lambda: signal(barrier, aside[1:]))
    pl.when(follows)(lambda: signal(barrier, plane))
    receive(barrier, 2, 8)
    greet(ready.at[0])
    pl.when(follows)(lambda: signal(ready.at[0], aside + plane))

    def halo(i, n):
        part = blocks.at[1, spans[n]]
        return remote(part, blocks.at[2 - i, spans[n]], halo_send.at[i // 2], halo_recv.at[i // 2, n], (sec, near[i]))

    for n in range(len(chunks)):
        loads[n].wait()
        pl.when(jnp.logical_and(present[0], core == 0))(halo(0, n).start)
        pl.when(present[2])(halo(2, n).start)
        pl.when(jnp.logical_and(present[0], core == 1))(halo(0, n).start)

    for i in range(3):
        blocks[i, FLAT:, :] = jnp.zeros((32 * GROUPS - FLAT, 128), F32)
    kre[...] = jnp.zeros_like(kre)
    kim[...] = jnp.zeros_like(kim)
    red[...] = jnp.zeros_like(red)
    cvec[...] = jnp.zeros_like(cvec)
    bvec[...] = jnp.zeros_like(bvec)
    for i in (0, 2):

        @pl.when(jnp.logical_not(present[i]))
        def _():
            blocks[i] = jnp.zeros((32 * GROUPS, 128), F32)
            vbuf[i] = jnp.zeros_like(vbuf[i])

    loads[2].wait()

    base = pix * (TILES * 128) - REACH
    for t in range(TILES):
        rel = nbr[:, t * 128 : (t + 1) * 128] - (base + t * 128)
        lanes[t, 0:NB, :] = jnp.bitwise_and(rel, 127)
        tiles[t, 0:NB, :] = jnp.right_shift(rel, 7)
        lanes[t, NB : NB + 1, :] = jnp.zeros((1, 128), jnp.int32)
        tiles[t, NB : NB + 1, :] = jnp.full((1, 128), SPAN, jnp.int32)

    def spread(i, groups=range(GROUPS)):
        for g in groups:
            for m in range(2):
                for c in range(2):
                    ext[2 * i + m, c, g * 8 : (g + 1) * 8, :] = blocks[i, pl.ds(g * 32 + m * 2 + c, 8, stride=4), :]

    spread(1)
    for t in range(TILES):
        for c in range(2):
            total = None
            for g in range(GROUPS):
                own = ext[2 + t, c, g * 8 : (g + 1) * 8, :]
                zs[t, 0, c, g * 8 : (g + 1) * 8, :] = own
                total = own if total is None else total + own
            xsum[t, c : c + 1, :] = column_sum(total)

    def gather(t, offsets, begin, groups=range(GROUPS), halves=None):
        def some(half):
            for i in range(NB // 2):
                k = 1 + half * (NB // 2) + i
                lane = bcast(lanes[t, pl.ds(k, 1), :])
                tile = bcast(tiles[t, pl.ds(k, 1), :])
                for g in groups:
                    rows = slice(g * 8, (g + 1) * 8)
                    for c in range(2):
                        out = None if begin else zs[t, k, c, rows, :]
                        for m in offsets:
                            got = take(ext[t + m, c, rows, :], lane)
                            out = got if out is None else jnp.where(tile == m, got, out)
                        zs[t, k, c, rows, :] = out

        if halves is None:
            pl.loop(0, 2)(some)
        else:
            for half in halves:
                some(half)

    for t in range(TILES):
        gather(t, (2 - t, 3 - t), True)

    def side(s, groups, halves=None):
        spread(2 * s, groups)
        close, distant = 1 + 3 * s, 5 * s
        gather(s, (close - s, distant - s), False, groups, halves)
        gather(1 - s, (close - (1 - s),), False, groups, halves)

    def both(soon):
        late = 1 - soon
        for n in range(len(chunks)):
            arrived(blocks.at[2 * soon, spans[n]], halo_recv.at[1 - soon, n])
        side(soon, range(GROUPS))
        hear(ready.at[0])
        pl.when(leads)(lambda: signal(ready.at[0], aside))
        tell(ready.at[1])
        for n, (low, high) in enumerate(chunks):
            pl.when(inner)(lambda n=n: arrived(blocks.at[2 * late, spans[n]], halo_recv.at[1 - late, n]))
            side(late, range(low, high), range(2))

    pl.when(core == 0)(lambda: both(1))
    pl.when(core == 1)(lambda: both(0))

    @pl.when(sec >= 2)
    def _():
        hear(ready.at[1])
        tell(ready.at[2])

    @pl.when(sec == 2)
    def _():
        column = at_ref([nbr[:, t * 128 : (t + 1) * 128].astype(F32) for t in range(TILES)])
        nmsg[...] = to_row(column)
        start(*steps_n[0])

    @pl.loop(0, TILES)
    def _(t):
        for g in range(GROUPS):
            rows = slice(g * 8, (g + 1) * 8)
            power = None
            for k in range(NB):
                re, im = zs[t, k, 0, rows, :], zs[t, k, 1, rows, :]
                zs[t, k, 2, rows, :] = re - im
                term = re * re + im * im
                power = term if power is None else power + term
            wbuf[t, rows, :] = lax.rsqrt(jnp.maximum(power, 1.0))

        def fold(slot, parts):
            for i, part in enumerate(parts):
                red[slot, i * 8 : (i + 1) * 8, :] = part
            total = None
            for i in range(8):
                row = red[slot, pl.ds(i, 8, stride=8), :]
                total = row if total is None else total + row
            return total

        slot = 0
        for l in range(NB + 1):
            for kg in range(2):
                low, high = 8 * kg, min(8 * kg + 8, l + 1, NB)
                if high <= low:
                    continue
                count = high - low
                p, q, r = [None] * count, [None] * count, [None] * count
                cr, ci = [None] * count, [None] * count

                def put(box, i, value):
                    box[i] = value if box[i] is None else box[i] + value

                for g in range(GROUPS):
                    rows = slice(g * 8, (g + 1) * 8)
                    w = wbuf[t, rows, :]
                    if l < NB:
                        w2 = w * w
                        lr, li = zs[t, l, 0, rows, :] * w2, zs[t, l, 1, rows, :] * w2
                    else:
                        lr, li = zs[t, 0, 0, rows, :] * w, zs[t, 0, 1, rows, :] * w
                    le = lr + li
                    for i in range(count):
                        k = low + i
                        kr, ki = zs[t, k, 0, rows, :], zs[t, k, 1, rows, :]
                        put(p, i, kr * lr)
                        put(q, i, ki * li)
                        if k != l:
                            put(r, i, zs[t, k, 2, rows, :] * le)
                        if l == NB:
                            put(cr, i, kr * w)
                            put(ci, i, ki * w)
                re = fold(4 * kg + slot, [a + b for a, b in zip(p, q)])
                im = fold(4 * kg + slot + 1, [jnp.zeros((8, 128), F32) if c is None else c + (b - a) for a, b, c in zip(p, q, r)])
                rows = slice(low, low + 8)
                if l < NB:
                    kre[t, l, rows, :] = re
                    kim[t, l, rows, :] = im
                    for i in range(count):
                        k = low + i
                        if k != l:
                            kre[t, k, l : l + 1, :] = re[i : i + 1, :]
                            kim[t, k, l : l + 1, :] = -im[i : i + 1, :]
                else:
                    bvec[t, 0, rows, :] = re
                    bvec[t, 1, rows, :] = im
                    slot = 2 - slot
                    cvec[t, 0, rows, :] = START * fold(4 * kg + slot, cr)
                    cvec[t, 1, rows, :] = -START * fold(4 * kg + slot + 1, ci)
                slot = 2 - slot
        ksum[t] = kre[t] + kim[t]

    def pieces(count):
        return [(t, c, kg) for t in range(count) for c in range(2) for kg in range(2)]

    def load(ref, count):
        return [ref[t, c, 8 * kg : 8 * kg + 8, :] for t, c, kg in pieces(count)]

    def save(ref, value):
        for (t, c, kg), part in zip(pieces(len(value) // 4), value):
            ref[t, c, 8 * kg : 8 * kg + 8, :] = part

    def plus(*values):
        return [sum(parts[1:], parts[0]) for parts in zip(*values)]

    def times(factor, value):
        return [factor * part for part in value]

    def product(m, box, value):
        for t in range(len(value) // 4):
            for kg in range(2):
                re, im = value[4 * t + kg], value[4 * t + 2 + kg]
                for c, part in enumerate((re, im, re + im)):
                    box[t, c, 8 * kg : 8 * kg + 8, :] = part
        out = []
        for t in range(len(value) // 4):
            y = [[None, None] for _ in range(3)]
            for l in range(NB):
                for c in range(3):
                    row = bcast(box[t, c, l : l + 1, :])
                    for kg in range(2):
                        part = m[c][t, l, 8 * kg : 8 * kg + 8, :] * row
                        y[c][kg] = part if l == 0 else y[c][kg] + part
            out += [y[0][kg] - y[1][kg] for kg in range(2)]
            out += [y[2][kg] - (y[0][kg] + y[1][kg]) for kg in range(2)]
        return out

    def prepare(m3, s3, cv, qv, box, count):
        mr, mi, _ = m3
        sr, si, _ = s3
        for t in range(count):

            @pl.loop(0, NB)
            def _(l):
                for kg in range(2):
                    rows = slice(8 * kg, 8 * kg + 8)
                    re, im = 2.0 * mr[t, l, rows, :], 2.0 * mi[t, l, rows, :]
                    for m in range(NB):
                        lr = bcast(mr[t, l, m : m + 1, :])
                        li = bcast(mi[t, l, m : m + 1, :])
                        ar, ai = mr[t, m, rows, :], mi[t, m, rows, :]
                        re = re + (ar * lr - ai * li)
                        im = im + (ar * li + ai * lr)
                    sr[t, l, rows, :] = re
                    si[t, l, rows, :] = im

        save(qv, product(m3, box, load(cv, count)))

    def joined(z, value):
        out = []
        for t in range(len(value) // 4):
            zr, zi = z[4 * t : 4 * t + 2], z[4 * t + 2 : 4 * t + 4]
            vr, vi = value[4 * t : 4 * t + 2], value[4 * t + 2 : 4 * t + 4]
            ar = column_sum(zr[0] * vr[0] - zi[0] * vi[0] + (zr[1] * vr[1] - zi[1] * vi[1]))
            ai = column_sum(zr[0] * vi[0] + zi[0] * vr[0] + (zr[1] * vi[1] + zi[1] * vr[1]))
            out += [zr[i] * ar + zi[i] * ai for i in range(2)] + [zr[i] * ai - zi[i] * ar for i in range(2)]
        return out

    def conj(value):
        return [part if (i // 2) % 2 == 0 else -part for i, part in enumerate(value)]

    def norms_of(value, image, start):
        out = []
        for t in range(len(value) // 4):
            total = None
            for i in range(4 * t, 4 * t + 4):
                term = value[i] * (image[i] + (2.0 * SCALE) * start[i])
                total = term if total is None else total + term
            out.append(lax.rsqrt(column_sum(total) + SCALE * SCALE))
        return out

    def solve(m3, cv, box, count):
        def turn(_, value):
            return tuple(plus(value, product(m3, box, value), load(cv, count)))

        value = lax.fori_loop(0, ITERS - 1, turn, tuple(load(cv, count)))
        value = times(SCALE, value)
        return value, norms_of(value, product(m3, box, value), load(cv, count))

    def solve_joined(m3, s3, cv, qv, zv, box, gbox, count):
        z = load(zv, count)
        r = conj(z)
        kr = product(m3, box, r)
        c = plus(load(cv, count), times(START, r))
        g = plus(r, kr)
        for t in range(count):
            squares = [z[4 * t + i] * z[4 * t + i] for i in range(4)]
            half = 0.5 * column_sum(squares[0] + squares[1] + (squares[2] + squares[3]))
            for i in range(4 * t, 4 * t + 4):
                g[i] = g[i] + half * r[i]
        save(gbox, g)
        sr, si, both = s3
        for t in range(count):
            for l in range(NB):
                zr, zi = bcast(zv[t, 0, l : l + 1, :]), bcast(zv[t, 1, l : l + 1, :])
                gr, gi = bcast(gbox[t, 0, l : l + 1, :]), bcast(gbox[t, 1, l : l + 1, :])
                for kg in range(2):
                    rows = slice(8 * kg, 8 * kg + 8)
                    hr, hi = g[4 * t + kg], g[4 * t + 2 + kg]
                    xr, xi = z[4 * t + kg], z[4 * t + 2 + kg]
                    re = sr[t, l, rows, :] + (hr * zr - hi * zi + (xr * gr - xi * gi))
                    im = si[t, l, rows, :] + (hr * zi + hi * zr - (xr * gi + xi * gr))
                    sr[t, l, rows, :] = re
                    si[t, l, rows, :] = im
                    both[t, l, rows, :] = re + im

        def square(value):
            return plus(value, product(s3, box, value))

        value = plus(c, c, load(qv, count), times(START, kr), joined(z, c))
        value = plus(value, square(value))
        value = plus(value, square(square(value)))

        last = lax.fori_loop(0, 4, lambda _, v: tuple(square(v)), tuple(value))
        value = times(SCALE, plus(value, last))
        image = plus(product(m3, box, value), joined(z, value))
        return value, norms_of(value, image, c)

    def step_one():
        @pl.when(sec == 2)
        def _():
            arrived(gbuf.at[1:8], g_recv)

        @pl.when(sec != 2)
        def _():
            arrived(gbuf.at[0:8], g_recv)

        total = gbuf[0]
        for d in range(1, 8):
            total = total + gbuf[d]
        bmsg[2:4, :] = total
        bmsg[0:2, :] = jnp.zeros((2, 128), F32)

        @pl.when(sec < SECTIONS - 1)
        def _():
            finish(*steps_r)
            bmsg[0:2, :] = sum_of(rmsg, rbuf1)

        pl.when(leads)(lambda: hear(ready.at[4]))
        start(*steps_b)

    @pl.when(sec < 2)
    def _():
        hear(ready.at[1])
        tell(ready.at[2])

    def prepare_own():
        prepare((kre, kim, ksum), (kre2, kim2, ksum2), cvec, qvec, sbuf, TILES)

    pl.when(jnp.logical_or(sec == 1, sec == 2))(prepare_own)

    @pl.when(sec == 1)
    def _():
        hear(ready.at[2])
        tell(ready.at[3])

    @pl.when(sec == 2)
    def _():
        finish(*steps_n[0])
        hear(ready.at[2])
        tell(ready.at[3])
        nmsg2[...] = sum_of(nmsg, nbuf1)
        start(*steps_n[1])

    def expand():
        for l in range(NB):
            kref[0, l] = jnp.broadcast_to(eall[0:16, l : l + 1], (16, 128))
            kimf[0, l] = jnp.broadcast_to(eall[0:16, 16 + l : 17 + l], (16, 128))
        for c in range(2):
            cref[0, c] = jnp.broadcast_to(eall[0:16, 32 + c : 33 + c], (16, 128))
        ksumf[...] = kref[...] + kimf[...]
        prepare((kref, kimf, ksumf), (kref2, kimf2, ksumf2), cref, qref, sref, 1)

    @pl.when(sec == SECTIONS - 1)
    def _():
        lane = lax.broadcasted_iota(jnp.int32, (16, 128), 1)
        emsg[16:32, :] = jnp.zeros((16, 128), F32)
        acc = jnp.zeros((16, 128), F32)
        for c in range(2):
            acc = jnp.where(lane == 32 + c, at_ref([cvec[t, c] for t in range(TILES)]), acc)
        emsg[0:16, :] = acc

        @pl.loop(0, NB)
        def _(k):
            acc = emsg[0:16, :]
            acc = jnp.where(lane == k, at_ref([kre[t, k] for t in range(TILES)]), acc)
            emsg[0:16, :] = jnp.where(lane == 16 + k, at_ref([kim[t, k] for t in range(TILES)]), acc)
            parts = [at_ref([zs[t, k, c] * wbuf[t] for t in range(TILES)]) for c in range(2)]
            emsg[pl.ds(16 + k, 1), :] = to_row(parts[0]) + to_row(parts[1], 64)

        start(*steps_e[0])
        prepare_own()
        finish(*steps_e[0])
        hear(ready.at[2])
        tell(ready.at[3])
        emsg2[...] = sum_of(emsg, ebuf1)
        start(*steps_e[1])
        hear(ready.at[3])
        tell(ready.at[4])
        step_one()
        finish(*steps_e[1])
        eall[...] = sum_of(emsg2, ebuf2)
        for j in range(SECTIONS - 1):
            remote(eall.at[pl.ds(0, 16)], eall.at[pl.ds(0, 16)], y_send, y_recv, (j, pix)).start()
        expand()

    @pl.when(sec == 2)
    def _():
        finish(*steps_n[1])
        column = to_column(sum_of(nmsg2, nbuf2), 16)
        row = lax.broadcasted_iota(jnp.int32, (16, 128), 0)
        ncol[...] = jnp.where(row == NB, ref[0].astype(F32), column) - (pix * (TILES * 128)).astype(F32)

    def keep(solved):
        value, norms = solved
        save(result, value)
        for t, norm in enumerate(norms):
            inverse[t] = norm

    @pl.when(sec == 0)
    def _():
        zbuf[...] = jnp.zeros_like(zbuf)
        keep(solve((kre, kim, ksum), cvec, sbuf, TILES))

    @pl.when(sec > 0)
    def _():
        pl.when(inner)(lambda: arrived(vbuf, v_recv))
        pl.when(jnp.logical_not(inner))(lambda: arrived(vbuf.at[0:2], v_recv))
        for t in range(TILES):
            z0 = []
            for kg in range(2):
                rows = slice(8 * kg, 8 * kg + 8)
                lane = lanes[t, rows, :]
                tile = tiles[t, rows, :]
                pair = []
                for c in range(2):
                    src = []
                    for m in range(SPAN):
                        at = t + m
                        src.append(bcast(vbuf[at // 2, c : c + 1, (at % 2) * 128 : (at % 2) * 128 + 128]))
                    pair.append(pick(src, lane, tile))
                z0.append(pair)
            power = column_sum(z0[0][0] * z0[0][0] + z0[0][1] * z0[0][1] + (z0[1][0] * z0[1][0] + z0[1][1] * z0[1][1]))
            w = lax.rsqrt(jnp.maximum(power, 1.0))
            vr = vbuf[1, 0:1, t * 128 : (t + 1) * 128]
            vi = vbuf[1, 1:2, t * 128 : (t + 1) * 128]
            xsum[t, 0:1, :] = xsum[t, 0:1, :] + vr
            xsum[t, 1:2, :] = xsum[t, 1:2, :] + vi
            for kg in range(2):
                rows = slice(8 * kg, 8 * kg + 8)
                zr, zi = z0[kg][0] * w, z0[kg][1] * w
                zbuf[t, 0, rows, :] = zr
                zbuf[t, 1, rows, :] = zi
                bvec[t, 0, rows, :] = bvec[t, 0, rows, :] + (zr * vr + zi * vi)
                bvec[t, 1, rows, :] = bvec[t, 1, rows, :] + (zr * vi - zi * vr)
        keep(solve_joined((kre, kim, ksum), (kre2, kim2, ksum2), cvec, qvec, zbuf, sbuf, gvec, TILES))

    state = load(result, TILES)
    norms = [inverse[t] for t in range(TILES)]
    for t in range(TILES):
        s = state[4 * t : 4 * t + 4]
        cr = ci = None
        for kg in range(2):
            rows = slice(8 * kg, 8 * kg + 8)
            sr, si = s[kg], s[2 + kg]
            br, bi = bvec[t, 0, rows, :], bvec[t, 1, rows, :]
            a, b = sr * br + si * bi, sr * bi - si * br
            cr = a if kg == 0 else column_sum(cr + a)
            ci = b if kg == 0 else column_sum(ci + b)
        cols = slice(t * 128, (t + 1) * 128)
        msg[0:1, cols] = (cr + (SCALE * START) * xsum[t, 0:1, :]) * norms[t]
        msg[1:2, cols] = (ci + (SCALE * START) * xsum[t, 1:2, :]) * norms[t]

    def send_virtual():
        for i in range(3):
            pl.when(present[i])(remote(msg, vbuf.at[2 - i], v_send, v_recv, (sec_up, near[i])).start)

    pl.when(sec < 2)(send_virtual)
    for t in range(TILES):
        s = state[4 * t : 4 * t + 4]
        fr = fi = None
        for kg in range(2):
            rows = slice(8 * kg, 8 * kg + 8)
            sr, si = s[kg], s[2 + kg]
            zr, zi = zbuf[t, 0, rows, :], zbuf[t, 1, rows, :]
            e, f = zr * sr - zi * si, zr * si + zi * sr
            fr = e if kg == 0 else column_sum(fr + e)
            fi = f if kg == 0 else column_sum(fi + f)
        cols = slice(t * 128, (t + 1) * 128)
        fr, fi = unit((fr + SCALE * START) * norms[t], fi * norms[t])
        fmsg[0:1, cols] = fr
        fmsg[1:2, cols] = fi

    steps_g = [
        remote(gmsg, gbuf.at[d], g_send, g_recv, (s, pix if d == 0 else first[d - 1]))
        for s in range(SECTIONS)
        for d in range(8)
        if (s, d) != (2, 0)
    ]

    @pl.when(sec == 2)
    def _():
        hear(ready.at[3])
        lane = lax.broadcasted_iota(jnp.int32, (16, 128), 1).astype(F32)
        row = lax.broadcasted_iota(jnp.int32, (16, 128), 0)
        for c in range(2):
            total = None
            for t in range(TILES):
                cols = slice(t * 128, (t + 1) * 128)
                value = jnp.where(
                    row == NB,
                    jnp.broadcast_to(fmsg[c : c + 1, cols], (16, 128)),
                    jnp.broadcast_to(msg[c : c + 1, cols], (16, 128)),
                )
                value = jnp.where(ncol[...] - t * 128.0 == lane, value, 0.0)
                total = value if total is None else total + value
            gmsg[c : c + 1, :] = to_row(jnp.sum(total, axis=1, keepdims=True))
        for copy in steps_g:
            copy.start()
        gbuf[0] = gmsg[...]
        tell(ready.at[4])

    pl.when(sec == 2)(send_virtual)

    for s in range(1, SECTIONS):

        @pl.when(sec == s)
        def _():
            for j in range(s):
                remote(fmsg, fbuf.at[s - 1], f_send, f_recv.at[s - 1], (j, pix)).start()

    @pl.when(sec == 0)
    def _():
        hear(ready.at[2])
        tell(ready.at[3])

    @pl.when(sec < 2)
    def _():
        hear(ready.at[3])
        tell(ready.at[4])

    comp[0, 0:1, :] = msg[0:1, :]
    comp[1, 0:1, :] = msg[1:2, :]

    def vector():
        for i, (t, c, kg) in enumerate((t, c, kg) for t in range(TILES) for c in range(2) for kg in range(2)):
            sbuf[t, c, 8 * kg : 8 * kg + 8, :] = result[t, c, 8 * kg : 8 * kg + 8, :] * inverse[t]
        for t in range(TILES):

            @pl.loop(0, GROUPS)
            def _(g):
                rows = pl.ds(pl.multiple_of(g * 8, 8), 8)
                re = im = None
                for k in range(NB):
                    sr = bcast(sbuf[t, 0, k : k + 1, :])
                    si = bcast(sbuf[t, 1, k : k + 1, :])
                    zr, zi = zs[t, k, 0, rows, :], zs[t, k, 1, rows, :]
                    a, b = zr * sr - zi * si, zr * si + zi * sr
                    re = a if re is None else re + a
                    im = b if im is None else im + b
                w = wbuf[t, rows, :]
                series[t, 0, rows, :] = bcast((SCALE * START) * inverse[t]) + w * re
                series[t, 1, rows, :] = w * im

    pl.when(sec < SECTIONS - 1)(vector)

    def take_f(j):
        arrived(fbuf.at[j - 1], f_recv.at[j - 1])

    @pl.when(sec == 0)
    def _():
        take_f(1)
        for t in range(TILES):
            fr = fbuf[0, 0:1, t * 128 : (t + 1) * 128]
            fi = fbuf[0, 1:2, t * 128 : (t + 1) * 128]
            re, im = series[t, 0], series[t, 1]
            series[t, 0] = re * fr - im * fi
            series[t, 1] = re * fi + im * fr

    @pl.when(sec < SECTIONS - 1)
    def _():
        for c in range(2):
            rmsg[c : c + 1, :] = to_row(at_ref([series[t, c] for t in range(TILES)]))
        start(*steps_r)

    pl.when(sec < SECTIONS - 1)(step_one)

    pl.when(sec == SECTIONS - 1)(vector)

    @pl.when(sec < SECTIONS - 1)
    def _():
        remote(eall.at[pl.ds(0, 16)], eall.at[pl.ds(0, 16)], y_send, y_recv, (SECTIONS - 1, pix)).wait_recv()
        expand()

    finish(*steps_b)
    total = sum_of(bmsg, bbuf)

    values = [to_column(total[2 + c : 3 + c, :], 16) for c in range(2)]
    f2r, f2i = values[0][NB:16], values[1][NB:16]
    row = lax.broadcasted_iota(jnp.int32, (16, 128), 0)
    zr, zi = (jnp.where(row < NB, value, 0.0) for value in values)
    w = lax.rsqrt(jnp.maximum(column_sum(zr * zr + zi * zi), 1.0))
    zr, zi = zr * w, zi * w
    zref[0, 0] = zr
    zref[0, 1] = zi
    state_ref, norm_ref = solve_joined((kref, kimf, ksumf), (kref2, kimf2, ksumf2), cref, qref, zref, sref, gref, 1)
    sr = jnp.concatenate(state_ref[0:2], axis=0)
    si = jnp.concatenate(state_ref[2:4], axis=0)
    norm = norm_ref[0]
    f3r = column_sum(zr * sr - zi * si)
    f3i = column_sum(zr * si + zi * sr)
    f3r, f3i = unit((f3r + SCALE * START) * norm, f3i * norm)
    fr = jnp.where(sec < 2, f3r * f2r - f3i * f2i, f3r)
    fi = jnp.where(sec < 2, f3r * f2i + f3i * f2r, f3i)
    vr, vi = total[0:1, :], total[1:2, :]
    rmsg[0:1, :] = vr * fr - vi * fi
    rmsg[1:2, :] = vr * fi + vi * fr

    @pl.when(sec == SECTIONS - 1)
    def _():
        z = eall[16:32, :]
        a = bcast(column_sum(z * sr))
        b = bcast(column_sum(z * si))
        re = a - pltpu.roll(b, 64, 1)
        im = b + pltpu.roll(a, 64, 1)
        rmsg[0:1, :] = (re[0:1] + SCALE * START) * norm
        rmsg[1:2, :] = im[0:1] * norm

    ur, ui = unit(rmsg[0:1, :], rmsg[1:2, :])
    ur, ui = GAIN * to_column(ur, PAD), GAIN * to_column(ui, PAD)

    datum[0:1, :] = jnp.ones((1, TILES * 128), F32)
    datum[1:2, :] = jnp.zeros((1, TILES * 128), F32)

    @pl.when(sec < SECTIONS - 1)
    def _():
        take_f(3)
        datum[...] = fbuf[2]

    @pl.when(sec < 2)
    def _():
        take_f(2)
        dr, di = datum[0:1, :], datum[1:2, :]
        fr, fi = fbuf[1, 0:1, :], fbuf[1, 1:2, :]
        datum[0:1, :] = dr * fr - di * fi
        datum[1:2, :] = dr * fi + di * fr

    for t in range(TILES):
        dr, di = datum[0:1, t * 128 : (t + 1) * 128], datum[1:2, t * 128 : (t + 1) * 128]
        re, im = series[t, 0], series[t, 1]
        re, im = re * dr - im * di, re * di + im * dr
        for c, part in enumerate((re * ur + im * ui, im * ur - re * ui)):
            for g in range(GROUPS):
                count = min(8, ROWS - g * 8)
                phases[pl.ds(g * 32 + t * 2 + c, count, stride=4), :] = part[g * 8 : g * 8 + count]

    pl.when(follows)(lambda: hear(ready.at[4]))
    for i in (0, 2):
        pl.when(present[i])(lambda i=i: arrived(blocks.at[1, pl.ds(0, FLAT)], halo_send.at[i // 2]))
    @pl.when(sec == 2)
    def _():
        arrived(gbuf, g_send)

    @pl.when(sec == SECTIONS - 1)
    def _():
        arrived(ebuf1.at[0:3, 0:16], y_send)

    @pl.when(sec < SECTIONS - 1)
    def _():
        pl.when(inner)(lambda: arrived(vbuf, v_send))
        pl.when(jnp.logical_not(inner))(lambda: arrived(vbuf.at[0:2], v_send))

    for s in range(1, SECTIONS):

        @pl.when(sec == s)
        def _():
            arrived(fbuf.at[0:s], f_send)


def hand_out(phases_in, comp_in, phases, comp, sem):
    copies = [
        pltpu.make_async_copy(phases_in, phases, sem.at[0]),
        pltpu.make_async_copy(comp_in, comp, sem.at[1]),
    ]
    for copy in copies:
        copy.start()
    for copy in copies:
        copy.wait()


def on_device(slc, neighbours, reference_pixel):
    vmem = pl.BlockSpec(memory_space=pltpu.VMEM)
    hbm = pl.BlockSpec(memory_space=pltpu.HBM)
    pixels = slc.shape[2]
    dma = pltpu.SemaphoreType.DMA
    flat = slc.reshape(2, ROWS, TILES, 128).transpose(1, 2, 0, 3).reshape(FLAT, 128)
    phases, comp = pl.pallas_call(
        kernel,
        out_shape=(
            jax.ShapeDtypeStruct((FLAT, 128), F32),
            jax.ShapeDtypeStruct((2, 1, pixels), F32),
        ),
        in_specs=[hbm, hbm, pl.BlockSpec(memory_space=pltpu.SMEM)],
        out_specs=(vmem, vmem),
        scratch_shapes=[
            pltpu.VMEM((NB, pixels), jnp.int32),
            pltpu.VMEM((3, 32 * GROUPS, 128), F32),
            pltpu.VMEM((6, 2, PAD, 128), F32),
            pltpu.VMEM((TILES, 16, 128), jnp.int32),
            pltpu.VMEM((TILES, 16, 128), jnp.int32),
            pltpu.VMEM((TILES, NB, 3, PAD, 128), F32),
            pltpu.VMEM((TILES, PAD, 128), F32),
            pltpu.VMEM((8, 64, 128), F32),
            pltpu.VMEM((TILES, 16, 16, 128), F32),
            pltpu.VMEM((TILES, 16, 16, 128), F32),
            pltpu.VMEM((TILES, 2, 16, 128), F32),
            pltpu.VMEM((TILES, 2, 16, 128), F32),
            pltpu.VMEM((TILES, 2, 128), F32),
            pltpu.VMEM((TILES, 2, 16, 128), F32),
            pltpu.VMEM((TILES, 3, 16, 128), F32),
            pltpu.VMEM((3, 2, pixels), F32),
            pltpu.VMEM((2, pixels), F32),
            pltpu.VMEM((2, pixels), F32),
            pltpu.VMEM((3, 2, pixels), F32),
            pltpu.VMEM((TILES, 2, PAD, 128), F32),
            pltpu.VMEM((2, pixels), F32),
            pltpu.VMEM((1, 128), F32),
            pltpu.VMEM((7, 1, 128), F32),
            pltpu.VMEM((1, 128), F32),
            pltpu.VMEM((7, 1, 128), F32),
            pltpu.VMEM((16, 128), F32),
            pltpu.VMEM((32, 128), F32),
            pltpu.VMEM((7, 32, 128), F32),
            pltpu.VMEM((32, 128), F32),
            pltpu.VMEM((7, 32, 128), F32),
            pltpu.VMEM((32, 128), F32),
            pltpu.VMEM((2, 128), F32),
            pltpu.VMEM((31, 2, 128), F32),
            pltpu.VMEM((2, 128), F32),
            pltpu.VMEM((7, 2, 128), F32),
            pltpu.VMEM((4, 128), F32),
            pltpu.VMEM((7, 4, 128), F32),
            pltpu.VMEM((1, 16, 16, 128), F32),
            pltpu.VMEM((1, 16, 16, 128), F32),
            pltpu.VMEM((1, 2, 16, 128), F32),
            pltpu.VMEM((1, 2, 16, 128), F32),
            pltpu.VMEM((1, 3, 16, 128), F32),
            pltpu.VMEM((TILES, 16, 16, 128), F32),
            pltpu.VMEM((TILES, 16, 16, 128), F32),
            pltpu.VMEM((TILES, 2, 16, 128), F32),
            pltpu.VMEM((TILES, 2, 16, 128), F32),
            pltpu.VMEM((TILES, 2, 16, 128), F32),
            pltpu.VMEM((TILES, 1, 128), F32),
            pltpu.VMEM((1, 16, 16, 128), F32),
            pltpu.VMEM((1, 16, 16, 128), F32),
            pltpu.VMEM((1, 2, 16, 128), F32),
            pltpu.VMEM((1, 2, 16, 128), F32),
            pltpu.VMEM((TILES, 16, 16, 128), F32),
            pltpu.VMEM((TILES, 16, 16, 128), F32),
            pltpu.VMEM((1, 16, 16, 128), F32),
            pltpu.VMEM((1, 16, 16, 128), F32),
            dma((3,)),
            dma((2,)),
            dma((2, 2)),
            dma(()),
            dma(()),
            dma(()),
            dma((3,)),
            dma((2, 2)),
            dma(()),
            dma(()),
            dma(()),
            dma(()),
            dma((2,)),
            dma((2,)),
            pltpu.SemaphoreType.REGULAR((5,)),
        ],
        compiler_params=pltpu.CompilerParams(
            collective_id=0, has_side_effects=True, vmem_limit_bytes=16 * 2**20
        ),
        cost_estimate=pl.CostEstimate(flops=100_000_000, bytes_accessed=1_000_000, transcendentals=0),
    )(*(pltpu.with_memory_space_constraint(a, pltpu.HBM) for a in (flat, neighbours)), reference_pixel)
    phases, comp = pl.pallas_call(
        hand_out,
        out_shape=(
            jax.ShapeDtypeStruct((FLAT, 128), F32),
            jax.ShapeDtypeStruct((2, 1, pixels), F32),
        ),
        in_specs=[pl.BlockSpec(memory_space=pl.ANY)] * 2,
        out_specs=(hbm, hbm),
        scratch_shapes=[dma((2,))],
        compiler_params=pltpu.CompilerParams(vmem_limit_bytes=2**20),
    )(phases, comp)
    return phases.reshape(ROWS, TILES, 2, 128).transpose(2, 0, 1, 3).reshape(2, ROWS, pixels), comp


def solution(mesh):
    return jax.shard_map(
        on_device,
        mesh=mesh,
        in_specs=(P(None, "section", "pix"), P(None, "pix"), P()),
        out_specs=(P(None, "section", "pix"), P(None, "section", "pix")),
        check_vma=False,
    )
```

```python
import math

import jax
import jax.numpy as jnp
from jax import lax
from jax.experimental import pallas as pl
from jax.experimental.pallas import tpu as pltpu
from jax.sharding import PartitionSpec as P

ITERS = 16
FLOOR = 0.05
REACH = 256
NB = 15
ROWS = 50
PAD = 56
GROUPS = PAD // 8
FLAT = 4 * ROWS
TILES = 2
SPAN = 5
SCALE = 2.0**-45
START = 1.0 / math.sqrt(ROWS + 1)
GAIN = math.sqrt(ROWS + 1)
SECTIONS = 4
PIX = 64
MESH = pl.DeviceIdType.MESH
F32 = jnp.float32


def bcast(row):
    return jnp.broadcast_to(row, (8, 128))


def pick(sources, lane, tile):
    out = jnp.zeros((8, 128), F32)
    for m, source in enumerate(sources):
        out = jnp.where(tile == m, take(source, lane), out)
    return out


def take(source, lane):
    return jnp.take_along_axis(source, lane, axis=1, mode="promise_in_bounds")


def column_sum(x):
    return jnp.sum(x, axis=0, keepdims=True)


def eye(count, shift=0):
    lane = lax.broadcasted_iota(jnp.int32, (count, 128), 1)
    return lane == lax.broadcasted_iota(jnp.int32, (count, 128), 0) + shift


def to_row(column, shift=0):
    return column_sum(jnp.where(eye(column.shape[0], shift), column, 0.0))


def to_column(row, count):
    spread = jnp.broadcast_to(row, (count, 128))
    return jnp.sum(jnp.where(eye(count), spread, 0.0), axis=1, keepdims=True)


def unit(re, im):
    scale = 1.0 / jnp.maximum(jnp.sqrt(re * re + im * im), FLOOR)
    return re * scale, im * scale


def remote(src, dst, send, recv, device):
    return pltpu.make_async_remote_copy(
        src_ref=src, dst_ref=dst, send_sem=send, recv_sem=recv, device_id=device, device_id_type=MESH
    )


def kernel(
    slc_hbm, nbr_hbm, ref, phases, comp,
    nbr, blocks, ext, lanes, tiles, zs, wbuf, red, kre, kim, cvec, bvec, xsum, zbuf, sbuf,
    vbuf, msg, fmsg, fbuf, series, datum,
    nmsg, nbuf1, nmsg2, nbuf2, ncol, emsg, ebuf1, emsg2, ebuf2, eall, gmsg, gbuf, rmsg, rbuf1, bmsg, bbuf,
    kref, kimf, cref, zref, sref, kre2, kim2, qvec, gvec, result, inverse, kref2, kimf2, qref, gref,
    ksum, ksum2, ksumf, ksumf2,
    load_sem, halo_send, halo_recv, v_send, v_recv, f_send, f_recv, early_sem,
    y_send, y_recv, g_send, g_recv, r_sem, b_sem, ready,
):
    sec = lax.axis_index("section")
    pix = lax.axis_index("pix")
    before = lax.rem(pix + (PIX - 1), PIX)
    after = lax.rem(pix + 1, PIX)
    near = (before, pix, after)
    present = (pix > 0, pix >= 0, pix < PIX - 1)
    inner = jnp.logical_and(present[0], present[2])
    sec_up = lax.rem(sec + 1, SECTIONS)
    sec_down = lax.rem(sec + (SECTIONS - 1), SECTIONS)
    x = pix // 16
    z = lax.rem(pix // 2, 8)
    core = lax.rem(pix, 2)
    group = x * 2 + core
    first = []
    second = []
    for d in range(1, 8):
        g = lax.rem(group + d, 8)
        first.append((g // 2) * 16 + z * 2 + lax.rem(g, 2))
        second.append(x * 16 + lax.rem(z + d, 8) * 2 + core)

    want = ref[0] - pix * (TILES * 128)

    def at_ref(parts):
        total = None
        for t, part in enumerate(parts):
            lane = lax.broadcasted_iota(jnp.int32, part.shape, 1)
            part = jnp.where(lane == want - t * 128, part, 0.0)
            total = part if total is None else total + part
        return jnp.sum(total, axis=1, keepdims=True)

    def arrived(ref, sem):
        pltpu.make_async_copy(ref, ref, sem).wait()

    def start(src, dst, sem, devices):
        for i, device in enumerate(devices):
            remote(src, dst.at[i], sem.at[0], sem.at[1], (sec, device)).start()

    def finish(src, dst, sem, devices):
        arrived(dst, sem.at[0])
        arrived(dst, sem.at[1])

    def sum_of(own, buffers):
        total = own[...]
        for i in range(7):
            total = total + buffers[i]
        return total

    steps_n = (nmsg, nbuf1, early_sem.at[0], first), (nmsg2, nbuf2, early_sem.at[1], second)
    steps_e = (emsg, ebuf1, early_sem.at[0], first), (emsg2, ebuf2, early_sem.at[1], second)
    steps_r = (rmsg, rbuf1, r_sem, first)
    steps_b = (bmsg, bbuf, b_sem, second)

    chunks = [(0, 2), (2, 5), (5, GROUPS)]
    spans = [pl.ds(32 * low, min(32 * high, FLAT) - 32 * low) for low, high in chunks]
    loads = [
        pltpu.make_async_copy(slc_hbm.at[span], blocks.at[1, span], load_sem.at[i]) for i, span in enumerate(spans)
    ]
    loads.append(pltpu.make_async_copy(nbr_hbm, nbr, load_sem.at[len(chunks)]))
    for load in loads:
        load.start()
    barrier = pltpu.get_barrier_semaphore()
    aside = [(sec_up, pix), (sec_down, pix)]
    plane = [(sec, x * 16 + lax.rem(z + d, 8) * 2 + core) for d in (1, 7)]
    plane += [(sec, lax.rem(x + d, 4) * 16 + z * 2 + core) for d in (1, 3)]
    leads = sec == 0
    follows = sec > 0

    def signal(sem, devices):
        for device in devices:
            pl.semaphore_signal(sem, inc=1, device_id=device, device_id_type=MESH)

    def greet(sem):
        for i in (0, 2):
            pl.when(present[i])(lambda i=i: signal(sem, [(sec, near[i])]))

    def tell(sem):
        greet(sem)
        signal(sem, aside)
        pl.when(follows)(lambda: signal(sem, plane))

    def receive(sem, lead, follow):
        for first_one, wanted in ((leads, lead), (follows, follow)):
            pl.when(jnp.logical_and(first_one, inner))(lambda wanted=wanted: pl.semaphore_wait(sem, wanted))
            pl.when(jnp.logical_and(first_one, jnp.logical_not(inner)))(
                lambda wanted=wanted: pl.semaphore_wait(sem, wanted - 1)
            )

    def hear(sem):
        receive(sem, 4, 8)

    greet(barrier)
    pl.when(sec != SECTIONS - 1)(lambda: signal(barrier, aside[:1]))
    pl.when(sec != 1)(lambda: signal(barrier, aside[1:]))
    pl.when(follows)(lambda: signal(barrier, plane))
    receive(barrier, 2, 8)
    greet(ready.at[0])
    pl.when(follows)(lambda: signal(ready.at[0], aside + plane))

    def halo(i, n):
        part = blocks.at[1, spans[n]]
        return remote(part, blocks.at[2 - i, spans[n]], halo_send.at[i // 2], halo_recv.at[i // 2, n], (sec, near[i]))

    for n in range(len(chunks)):
        loads[n].wait()
        pl.when(jnp.logical_and(present[0], core == 0))(halo(0, n).start)
        pl.when(present[2])(halo(2, n).start)
        pl.when(jnp.logical_and(present[0], core == 1))(halo(0, n).start)

    for i in range(3):
        blocks[i, FLAT:, :] = jnp.zeros((32 * GROUPS - FLAT, 128), F32)
    kre[...] = jnp.zeros_like(kre)
    kim[...] = jnp.zeros_like(kim)
    red[...] = jnp.zeros_like(red)
    cvec[...] = jnp.zeros_like(cvec)
    bvec[...] = jnp.zeros_like(bvec)
    for i in (0, 2):

        @pl.when(jnp.logical_not(present[i]))
        def _():
            blocks[i] = jnp.zeros((32 * GROUPS, 128), F32)
            vbuf[i] = jnp.zeros_like(vbuf[i])

    loads[-1].wait()

    base = pix * (TILES * 128) - REACH
    for t in range(TILES):
        rel = nbr[:, t * 128 : (t + 1) * 128] - (base + t * 128)
        lanes[t, 0:NB, :] = jnp.bitwise_and(rel, 127)
        tiles[t, 0:NB, :] = jnp.right_shift(rel, 7)
        lanes[t, NB : NB + 1, :] = jnp.zeros((1, 128), jnp.int32)
        tiles[t, NB : NB + 1, :] = jnp.full((1, 128), SPAN, jnp.int32)

    def spread(i, groups=range(GROUPS)):
        for g in groups:
            for m in range(2):
                for c in range(2):
                    ext[2 * i + m, c, g * 8 : (g + 1) * 8, :] = blocks[i, pl.ds(g * 32 + m * 2 + c, 8, stride=4), :]

    spread(1)
    for t in range(TILES):
        for c in range(2):
            total = None
            for g in range(GROUPS):
                own = ext[2 + t, c, g * 8 : (g + 1) * 8, :]
                zs[t, 0, c, g * 8 : (g + 1) * 8, :] = own
                total = own if total is None else total + own
            xsum[t, c : c + 1, :] = column_sum(total)

    def gather(t, offsets, begin, groups=range(GROUPS), halves=None):
        def some(half):
            for i in range(NB // 2):
                k = 1 + half * (NB // 2) + i
                lane = bcast(lanes[t, pl.ds(k, 1), :])
                tile = bcast(tiles[t, pl.ds(k, 1), :])
                for g in groups:
                    rows = slice(g * 8, (g + 1) * 8)
                    for c in range(2):
                        out = None if begin else zs[t, k, c, rows, :]
                        for m in offsets:
                            got = take(ext[t + m, c, rows, :], lane)
                            out = got if out is None else jnp.where(tile == m, got, out)
                        zs[t, k, c, rows, :] = out

        if halves is None:
            pl.loop(0, 2)(some)
        else:
            for half in halves:
                some(half)

    for t in range(TILES):
        gather(t, (2 - t, 3 - t), True)

    def side(s, groups, halves=None):
        spread(2 * s, groups)
        close, distant = 1 + 3 * s, 5 * s
        gather(s, (close - s, distant - s), False, groups, halves)
        gather(1 - s, (close - (1 - s),), False, groups, halves)

    def both(soon):
        late = 1 - soon
        for n in range(len(chunks)):
            arrived(blocks.at[2 * soon, spans[n]], halo_recv.at[1 - soon, n])
        side(soon, range(GROUPS))
        hear(ready.at[0])
        pl.when(leads)(lambda: signal(ready.at[0], aside))
        tell(ready.at[1])
        for n, (low, high) in enumerate(chunks):
            pl.when(inner)(lambda n=n: arrived(blocks.at[2 * late, spans[n]], halo_recv.at[1 - late, n]))
            side(late, range(low, high), range(2))

    pl.when(core == 0)(lambda: both(1))
    pl.when(core == 1)(lambda: both(0))

    @pl.when(sec >= 2)
    def _():
        hear(ready.at[1])
        tell(ready.at[2])

    @pl.when(sec == 2)
    def _():
        column = at_ref([nbr[:, t * 128 : (t + 1) * 128].astype(F32) for t in range(TILES)])
        nmsg[...] = to_row(column)
        start(*steps_n[0])

    @pl.loop(0, TILES)
    def _(t):
        for g in range(GROUPS):
            rows = slice(g * 8, (g + 1) * 8)
            power = None
            for k in range(NB):
                re, im = zs[t, k, 0, rows, :], zs[t, k, 1, rows, :]
                zs[t, k, 2, rows, :] = re - im
                term = re * re + im * im
                power = term if power is None else power + term
            wbuf[t, rows, :] = lax.rsqrt(jnp.maximum(power, 1.0))

        def fold(slot, parts):
            for i, part in enumerate(parts):
                red[slot, i * 8 : (i + 1) * 8, :] = part
            total = None
            for i in range(8):
                row = red[slot, pl.ds(i, 8, stride=8), :]
                total = row if total is None else total + row
            return total

        slot = 0
        for l in range(NB + 1):
            for kg in range(2):
                low, high = 8 * kg, min(8 * kg + 8, l + 1, NB)
                if high <= low:
                    continue
                count = high - low
                p, q, r = [None] * count, [None] * count, [None] * count
                cr, ci = [None] * count, [None] * count

                def put(box, i, value):
                    box[i] = value if box[i] is None else box[i] + value

                for g in range(GROUPS):
                    rows = slice(g * 8, (g + 1) * 8)
                    w = wbuf[t, rows, :]
                    if l < NB:
                        w2 = w * w
                        lr, li = zs[t, l, 0, rows, :] * w2, zs[t, l, 1, rows, :] * w2
                    else:
                        lr, li = zs[t, 0, 0, rows, :] * w, zs[t, 0, 1, rows, :] * w
                    le = lr + li
                    for i in range(count):
                        k = low + i
                        kr, ki = zs[t, k, 0, rows, :], zs[t, k, 1, rows, :]
                        put(p, i, kr * lr)
                        put(q, i, ki * li)
                        if k != l:
                            put(r, i, zs[t, k, 2, rows, :] * le)
                        if l == NB:
                            put(cr, i, kr * w)
                            put(ci, i, ki * w)
                re = fold(4 * kg + slot, [a + b for a, b in zip(p, q)])
                im = fold(4 * kg + slot + 1, [jnp.zeros((8, 128), F32) if c is None else c + (b - a) for a, b, c in zip(p, q, r)])
                rows = slice(low, low + 8)
                if l < NB:
                    kre[t, l, rows, :] = re
                    kim[t, l, rows, :] = im
                    for i in range(count):
                        k = low + i
                        if k != l:
                            kre[t, k, l : l + 1, :] = re[i : i + 1, :]
                            kim[t, k, l : l + 1, :] = -im[i : i + 1, :]
                else:
                    bvec[t, 0, rows, :] = re
                    bvec[t, 1, rows, :] = im
                    slot = 2 - slot
                    cvec[t, 0, rows, :] = START * fold(4 * kg + slot, cr)
                    cvec[t, 1, rows, :] = -START * fold(4 * kg + slot + 1, ci)
                slot = 2 - slot
        ksum[t] = kre[t] + kim[t]

    def pieces(count):
        return [(t, c, kg) for t in range(count) for c in range(2) for kg in range(2)]

    def load(ref, count):
        return [ref[t, c, 8 * kg : 8 * kg + 8, :] for t, c, kg in pieces(count)]

    def save(ref, value):
        for (t, c, kg), part in zip(pieces(len(value) // 4), value):
            ref[t, c, 8 * kg : 8 * kg + 8, :] = part

    def plus(*values):
        return [sum(parts[1:], parts[0]) for parts in zip(*values)]

    def times(factor, value):
        return [factor * part for part in value]

    def product(m, box, value):
        for t in range(len(value) // 4):
            for kg in range(2):
                re, im = value[4 * t + kg], value[4 * t + 2 + kg]
                for c, part in enumerate((re, im, re + im)):
                    box[t, c, 8 * kg : 8 * kg + 8, :] = part
        out = []
        for t in range(len(value) // 4):
            y = [[None, None] for _ in range(3)]
            for l in range(NB):
                for c in range(3):
                    row = bcast(box[t, c, l : l + 1, :])
                    for kg in range(2):
                        part = m[c][t, l, 8 * kg : 8 * kg + 8, :] * row
                        y[c][kg] = part if l == 0 else y[c][kg] + part
            out += [y[0][kg] - y[1][kg] for kg in range(2)]
            out += [y[2][kg] - (y[0][kg] + y[1][kg]) for kg in range(2)]
        return out

    def prepare(m3, s3, cv, qv, box, count):
        mr, mi, _ = m3
        sr, si, _ = s3
        for t in range(count):

            @pl.loop(0, NB)
            def _(l):
                for kg in range(2):
                    rows = slice(8 * kg, 8 * kg + 8)
                    re, im = 2.0 * mr[t, l, rows, :], 2.0 * mi[t, l, rows, :]
                    for m in range(NB):
                        lr = bcast(mr[t, l, m : m + 1, :])
                        li = bcast(mi[t, l, m : m + 1, :])
                        ar, ai = mr[t, m, rows, :], mi[t, m, rows, :]
                        re = re + (ar * lr - ai * li)
                        im = im + (ar * li + ai * lr)
                    sr[t, l, rows, :] = re
                    si[t, l, rows, :] = im

        save(qv, product(m3, box, load(cv, count)))

    def joined(z, value):
        out = []
        for t in range(len(value) // 4):
            zr, zi = z[4 * t : 4 * t + 2], z[4 * t + 2 : 4 * t + 4]
            vr, vi = value[4 * t : 4 * t + 2], value[4 * t + 2 : 4 * t + 4]
            ar = column_sum(zr[0] * vr[0] - zi[0] * vi[0] + (zr[1] * vr[1] - zi[1] * vi[1]))
            ai = column_sum(zr[0] * vi[0] + zi[0] * vr[0] + (zr[1] * vi[1] + zi[1] * vr[1]))
            out += [zr[i] * ar + zi[i] * ai for i in range(2)] + [zr[i] * ai - zi[i] * ar for i in range(2)]
        return out

    def conj(value):
        return [part if (i // 2) % 2 == 0 else -part for i, part in enumerate(value)]

    def norms_of(value, image, start):
        out = []
        for t in range(len(value) // 4):
            total = None
            for i in range(4 * t, 4 * t + 4):
                term = value[i] * (image[i] + (2.0 * SCALE) * start[i])
                total = term if total is None else total + term
            out.append(lax.rsqrt(column_sum(total) + SCALE * SCALE))
        return out

    def solve(m3, cv, box, count):
        def turn(_, value):
            return tuple(plus(value, product(m3, box, value), load(cv, count)))

        value = lax.fori_loop(0, ITERS - 1, turn, tuple(load(cv, count)))
        value = times(SCALE, value)
        return value, norms_of(value, product(m3, box, value), load(cv, count))

    def solve_joined(m3, s3, cv, qv, zv, box, gbox, count):
        z = load(zv, count)
        r = conj(z)
        kr = product(m3, box, r)
        c = plus(load(cv, count), times(START, r))
        g = plus(r, kr)
        for t in range(count):
            squares = [z[4 * t + i] * z[4 * t + i] for i in range(4)]
            half = 0.5 * column_sum(squares[0] + squares[1] + (squares[2] + squares[3]))
            for i in range(4 * t, 4 * t + 4):
                g[i] = g[i] + half * r[i]
        save(gbox, g)
        sr, si, both = s3
        for t in range(count):
            for l in range(NB):
                zr, zi = bcast(zv[t, 0, l : l + 1, :]), bcast(zv[t, 1, l : l + 1, :])
                gr, gi = bcast(gbox[t, 0, l : l + 1, :]), bcast(gbox[t, 1, l : l + 1, :])
                for kg in range(2):
                    rows = slice(8 * kg, 8 * kg + 8)
                    hr, hi = g[4 * t + kg], g[4 * t + 2 + kg]
                    xr, xi = z[4 * t + kg], z[4 * t + 2 + kg]
                    re = sr[t, l, rows, :] + (hr * zr - hi * zi + (xr * gr - xi * gi))
                    im = si[t, l, rows, :] + (hr * zi + hi * zr - (xr * gi + xi * gr))
                    sr[t, l, rows, :] = re
                    si[t, l, rows, :] = im
                    both[t, l, rows, :] = re + im

        def square(value):
            return plus(value, product(s3, box, value))

        value = plus(c, c, load(qv, count), times(START, kr), joined(z, c))
        value = plus(value, square(value))
        value = plus(value, square(square(value)))

        last = lax.fori_loop(0, 4, lambda _, v: tuple(square(v)), tuple(value))
        value = times(SCALE, plus(value, last))
        image = plus(product(m3, box, value), joined(z, value))
        return value, norms_of(value, image, c)

    def step_one():
        @pl.when(sec == 2)
        def _():
            arrived(gbuf.at[1:8], g_recv)

        @pl.when(sec != 2)
        def _():
            arrived(gbuf.at[0:8], g_recv)

        total = gbuf[0]
        for d in range(1, 8):
            total = total + gbuf[d]
        bmsg[2:4, :] = total
        bmsg[0:2, :] = jnp.zeros((2, 128), F32)

        @pl.when(sec < SECTIONS - 1)
        def _():
            finish(*steps_r)
            bmsg[0:2, :] = sum_of(rmsg, rbuf1)

        pl.when(leads)(lambda: hear(ready.at[4]))
        start(*steps_b)

    @pl.when(sec < 2)
    def _():
        hear(ready.at[1])
        tell(ready.at[2])

    def prepare_own():
        prepare((kre, kim, ksum), (kre2, kim2, ksum2), cvec, qvec, sbuf, TILES)

    pl.when(jnp.logical_or(sec == 1, sec == 2))(prepare_own)

    @pl.when(sec == 1)
    def _():
        hear(ready.at[2])
        tell(ready.at[3])

    @pl.when(sec == 2)
    def _():
        finish(*steps_n[0])
        hear(ready.at[2])
        tell(ready.at[3])
        nmsg2[...] = sum_of(nmsg, nbuf1)
        start(*steps_n[1])

    def expand():
        for l in range(NB):
            kref[0, l] = jnp.broadcast_to(eall[0:16, l : l + 1], (16, 128))
            kimf[0, l] = jnp.broadcast_to(eall[0:16, 16 + l : 17 + l], (16, 128))
        for c in range(2):
            cref[0, c] = jnp.broadcast_to(eall[0:16, 32 + c : 33 + c], (16, 128))
        ksumf[...] = kref[...] + kimf[...]
        prepare((kref, kimf, ksumf), (kref2, kimf2, ksumf2), cref, qref, sref, 1)

    @pl.when(sec == SECTIONS - 1)
    def _():
        lane = lax.broadcasted_iota(jnp.int32, (16, 128), 1)
        emsg[16:32, :] = jnp.zeros((16, 128), F32)
        acc = jnp.zeros((16, 128), F32)
        for c in range(2):
            acc = jnp.where(lane == 32 + c, at_ref([cvec[t, c] for t in range(TILES)]), acc)
        emsg[0:16, :] = acc

        @pl.loop(0, NB)
        def _(k):
            acc = emsg[0:16, :]
            acc = jnp.where(lane == k, at_ref([kre[t, k] for t in range(TILES)]), acc)
            emsg[0:16, :] = jnp.where(lane == 16 + k, at_ref([kim[t, k] for t in range(TILES)]), acc)
            parts = [at_ref([zs[t, k, c] * wbuf[t] for t in range(TILES)]) for c in range(2)]
            emsg[pl.ds(16 + k, 1), :] = to_row(parts[0]) + to_row(parts[1], 64)

        start(*steps_e[0])
        prepare_own()
        finish(*steps_e[0])
        hear(ready.at[2])
        tell(ready.at[3])
        emsg2[...] = sum_of(emsg, ebuf1)
        start(*steps_e[1])
        hear(ready.at[3])
        tell(ready.at[4])
        step_one()
        finish(*steps_e[1])
        eall[...] = sum_of(emsg2, ebuf2)
        for j in range(SECTIONS - 1):
            remote(eall.at[pl.ds(0, 16)], eall.at[pl.ds(0, 16)], y_send, y_recv, (j, pix)).start()
        expand()

    @pl.when(sec == 2)
    def _():
        finish(*steps_n[1])
        column = to_column(sum_of(nmsg2, nbuf2), 16)
        row = lax.broadcasted_iota(jnp.int32, (16, 128), 0)
        ncol[...] = jnp.where(row == NB, ref[0].astype(F32), column) - (pix * (TILES * 128)).astype(F32)

    def keep(solved):
        value, norms = solved
        save(result, value)
        for t, norm in enumerate(norms):
            inverse[t] = norm

    @pl.when(sec == 0)
    def _():
        zbuf[...] = jnp.zeros_like(zbuf)
        keep(solve((kre, kim, ksum), cvec, sbuf, TILES))

    @pl.when(sec > 0)
    def _():
        pl.when(inner)(lambda: arrived(vbuf, v_recv))
        pl.when(jnp.logical_not(inner))(lambda: arrived(vbuf.at[0:2], v_recv))
        for t in range(TILES):
            z0 = []
            for kg in range(2):
                rows = slice(8 * kg, 8 * kg + 8)
                lane = lanes[t, rows, :]
                tile = tiles[t, rows, :]
                pair = []
                for c in range(2):
                    src = []
                    for m in range(SPAN):
                        at = t + m
                        src.append(bcast(vbuf[at // 2, c : c + 1, (at % 2) * 128 : (at % 2) * 128 + 128]))
                    pair.append(pick(src, lane, tile))
                z0.append(pair)
            power = column_sum(z0[0][0] * z0[0][0] + z0[0][1] * z0[0][1] + (z0[1][0] * z0[1][0] + z0[1][1] * z0[1][1]))
            w = lax.rsqrt(jnp.maximum(power, 1.0))
            vr = vbuf[1, 0:1, t * 128 : (t + 1) * 128]
            vi = vbuf[1, 1:2, t * 128 : (t + 1) * 128]
            xsum[t, 0:1, :] = xsum[t, 0:1, :] + vr
            xsum[t, 1:2, :] = xsum[t, 1:2, :] + vi
            for kg in range(2):
                rows = slice(8 * kg, 8 * kg + 8)
                zr, zi = z0[kg][0] * w, z0[kg][1] * w
                zbuf[t, 0, rows, :] = zr
                zbuf[t, 1, rows, :] = zi
                bvec[t, 0, rows, :] = bvec[t, 0, rows, :] + (zr * vr + zi * vi)
                bvec[t, 1, rows, :] = bvec[t, 1, rows, :] + (zr * vi - zi * vr)
        keep(solve_joined((kre, kim, ksum), (kre2, kim2, ksum2), cvec, qvec, zbuf, sbuf, gvec, TILES))

    state = load(result, TILES)
    norms = [inverse[t] for t in range(TILES)]
    for t in range(TILES):
        s = state[4 * t : 4 * t + 4]
        cr = ci = None
        for kg in range(2):
            rows = slice(8 * kg, 8 * kg + 8)
            sr, si = s[kg], s[2 + kg]
            br, bi = bvec[t, 0, rows, :], bvec[t, 1, rows, :]
            a, b = sr * br + si * bi, sr * bi - si * br
            cr = a if kg == 0 else column_sum(cr + a)
            ci = b if kg == 0 else column_sum(ci + b)
        cols = slice(t * 128, (t + 1) * 128)
        msg[0:1, cols] = (cr + (SCALE * START) * xsum[t, 0:1, :]) * norms[t]
        msg[1:2, cols] = (ci + (SCALE * START) * xsum[t, 1:2, :]) * norms[t]

    def send_virtual():
        for i in range(3):
            pl.when(present[i])(remote(msg, vbuf.at[2 - i], v_send, v_recv, (sec_up, near[i])).start)

    pl.when(sec < 2)(send_virtual)
    for t in range(TILES):
        s = state[4 * t : 4 * t + 4]
        fr = fi = None
        for kg in range(2):
            rows = slice(8 * kg, 8 * kg + 8)
            sr, si = s[kg], s[2 + kg]
            zr, zi = zbuf[t, 0, rows, :], zbuf[t, 1, rows, :]
            e, f = zr * sr - zi * si, zr * si + zi * sr
            fr = e if kg == 0 else column_sum(fr + e)
            fi = f if kg == 0 else column_sum(fi + f)
        cols = slice(t * 128, (t + 1) * 128)
        fr, fi = unit((fr + SCALE * START) * norms[t], fi * norms[t])
        fmsg[0:1, cols] = fr
        fmsg[1:2, cols] = fi

    steps_g = [
        remote(gmsg, gbuf.at[d], g_send, g_recv, (s, pix if d == 0 else first[d - 1]))
        for s in range(SECTIONS)
        for d in range(8)
        if (s, d) != (2, 0)
    ]

    @pl.when(sec == 2)
    def _():
        hear(ready.at[3])
        lane = lax.broadcasted_iota(jnp.int32, (16, 128), 1).astype(F32)
        row = lax.broadcasted_iota(jnp.int32, (16, 128), 0)
        for c in range(2):
            total = None
            for t in range(TILES):
                cols = slice(t * 128, (t + 1) * 128)
                value = jnp.where(
                    row == NB,
                    jnp.broadcast_to(fmsg[c : c + 1, cols], (16, 128)),
                    jnp.broadcast_to(msg[c : c + 1, cols], (16, 128)),
                )
                value = jnp.where(ncol[...] - t * 128.0 == lane, value, 0.0)
                total = value if total is None else total + value
            gmsg[c : c + 1, :] = to_row(jnp.sum(total, axis=1, keepdims=True))
        for copy in steps_g:
            copy.start()
        gbuf[0] = gmsg[...]
        tell(ready.at[4])

    pl.when(sec == 2)(send_virtual)

    for s in range(1, SECTIONS):

        @pl.when(sec == s)
        def _():
            for j in range(s):
                remote(fmsg, fbuf.at[s - 1], f_send, f_recv.at[s - 1], (j, pix)).start()

    @pl.when(sec == 0)
    def _():
        hear(ready.at[2])
        tell(ready.at[3])

    @pl.when(sec < 2)
    def _():
        hear(ready.at[3])
        tell(ready.at[4])

    comp[0, 0:1, :] = msg[0:1, :]
    comp[1, 0:1, :] = msg[1:2, :]

    def vector():
        for i, (t, c, kg) in enumerate((t, c, kg) for t in range(TILES) for c in range(2) for kg in range(2)):
            sbuf[t, c, 8 * kg : 8 * kg + 8, :] = result[t, c, 8 * kg : 8 * kg + 8, :] * inverse[t]
        for t in range(TILES):

            @pl.loop(0, GROUPS)
            def _(g):
                rows = pl.ds(pl.multiple_of(g * 8, 8), 8)
                re = im = None
                for k in range(NB):
                    sr = bcast(sbuf[t, 0, k : k + 1, :])
                    si = bcast(sbuf[t, 1, k : k + 1, :])
                    zr, zi = zs[t, k, 0, rows, :], zs[t, k, 1, rows, :]
                    a, b = zr * sr - zi * si, zr * si + zi * sr
                    re = a if re is None else re + a
                    im = b if im is None else im + b
                w = wbuf[t, rows, :]
                series[t, 0, rows, :] = bcast((SCALE * START) * inverse[t]) + w * re
                series[t, 1, rows, :] = w * im

    pl.when(sec < SECTIONS - 1)(vector)

    def take_f(j):
        arrived(fbuf.at[j - 1], f_recv.at[j - 1])

    @pl.when(sec == 0)
    def _():
        take_f(1)
        for t in range(TILES):
            fr = fbuf[0, 0:1, t * 128 : (t + 1) * 128]
            fi = fbuf[0, 1:2, t * 128 : (t + 1) * 128]
            re, im = series[t, 0], series[t, 1]
            series[t, 0] = re * fr - im * fi
            series[t, 1] = re * fi + im * fr

    @pl.when(sec < SECTIONS - 1)
    def _():
        for c in range(2):
            rmsg[c : c + 1, :] = to_row(at_ref([series[t, c] for t in range(TILES)]))
        start(*steps_r)

    pl.when(sec < SECTIONS - 1)(step_one)

    pl.when(sec == SECTIONS - 1)(vector)

    @pl.when(sec < SECTIONS - 1)
    def _():
        remote(eall.at[pl.ds(0, 16)], eall.at[pl.ds(0, 16)], y_send, y_recv, (SECTIONS - 1, pix)).wait_recv()
        expand()

    finish(*steps_b)
    total = sum_of(bmsg, bbuf)

    values = [to_column(total[2 + c : 3 + c, :], 16) for c in range(2)]
    f2r, f2i = values[0][NB:16], values[1][NB:16]
    row = lax.broadcasted_iota(jnp.int32, (16, 128), 0)
    zr, zi = (jnp.where(row < NB, value, 0.0) for value in values)
    w = lax.rsqrt(jnp.maximum(column_sum(zr * zr + zi * zi), 1.0))
    zr, zi = zr * w, zi * w
    zref[0, 0] = zr
    zref[0, 1] = zi
    state_ref, norm_ref = solve_joined((kref, kimf, ksumf), (kref2, kimf2, ksumf2), cref, qref, zref, sref, gref, 1)
    sr = jnp.concatenate(state_ref[0:2], axis=0)
    si = jnp.concatenate(state_ref[2:4], axis=0)
    norm = norm_ref[0]
    f3r = column_sum(zr * sr - zi * si)
    f3i = column_sum(zr * si + zi * sr)
    f3r, f3i = unit((f3r + SCALE * START) * norm, f3i * norm)
    fr = jnp.where(sec < 2, f3r * f2r - f3i * f2i, f3r)
    fi = jnp.where(sec < 2, f3r * f2i + f3i * f2r, f3i)
    vr, vi = total[0:1, :], total[1:2, :]
    rmsg[0:1, :] = vr * fr - vi * fi
    rmsg[1:2, :] = vr * fi + vi * fr

    @pl.when(sec == SECTIONS - 1)
    def _():
        z = eall[16:32, :]
        a = bcast(column_sum(z * sr))
        b = bcast(column_sum(z * si))
        re = a - pltpu.roll(b, 64, 1)
        im = b + pltpu.roll(a, 64, 1)
        rmsg[0:1, :] = (re[0:1] + SCALE * START) * norm
        rmsg[1:2, :] = im[0:1] * norm

    ur, ui = unit(rmsg[0:1, :], rmsg[1:2, :])
    ur, ui = GAIN * to_column(ur, PAD), GAIN * to_column(ui, PAD)

    datum[0:1, :] = jnp.ones((1, TILES * 128), F32)
    datum[1:2, :] = jnp.zeros((1, TILES * 128), F32)

    @pl.when(sec < SECTIONS - 1)
    def _():
        take_f(3)
        datum[...] = fbuf[2]

    @pl.when(sec < 2)
    def _():
        take_f(2)
        dr, di = datum[0:1, :], datum[1:2, :]
        fr, fi = fbuf[1, 0:1, :], fbuf[1, 1:2, :]
        datum[0:1, :] = dr * fr - di * fi
        datum[1:2, :] = dr * fi + di * fr

    for t in range(TILES):
        dr, di = datum[0:1, t * 128 : (t + 1) * 128], datum[1:2, t * 128 : (t + 1) * 128]
        re, im = series[t, 0], series[t, 1]
        re, im = re * dr - im * di, re * di + im * dr
        for c, part in enumerate((re * ur + im * ui, im * ur - re * ui)):
            for g in range(GROUPS):
                count = min(8, ROWS - g * 8)
                phases[pl.ds(g * 32 + t * 2 + c, count, stride=4), :] = part[g * 8 : g * 8 + count]

    pl.when(follows)(lambda: hear(ready.at[4]))
    for i in (0, 2):
        pl.when(present[i])(lambda i=i: arrived(blocks.at[1, pl.ds(0, FLAT)], halo_send.at[i // 2]))
    @pl.when(sec == 2)
    def _():
        arrived(gbuf, g_send)

    @pl.when(sec == SECTIONS - 1)
    def _():
        arrived(ebuf1.at[0:3, 0:16], y_send)

    @pl.when(sec < SECTIONS - 1)
    def _():
        pl.when(inner)(lambda: arrived(vbuf, v_send))
        pl.when(jnp.logical_not(inner))(lambda: arrived(vbuf.at[0:2], v_send))

    for s in range(1, SECTIONS):

        @pl.when(sec == s)
        def _():
            arrived(fbuf.at[0:s], f_send)


def hand_out(phases_in, comp_in, phases, comp, sem):
    copies = [
        pltpu.make_async_copy(phases_in, phases, sem.at[0]),
        pltpu.make_async_copy(comp_in, comp, sem.at[1]),
    ]
    for copy in copies:
        copy.start()
    for copy in copies:
        copy.wait()


def on_device(slc, neighbours, reference_pixel):
    vmem = pl.BlockSpec(memory_space=pltpu.VMEM)
    hbm = pl.BlockSpec(memory_space=pltpu.HBM)
    pixels = slc.shape[2]
    dma = pltpu.SemaphoreType.DMA
    flat = slc.reshape(2, ROWS, TILES, 128).transpose(1, 2, 0, 3).reshape(FLAT, 128)
    phases, comp = pl.pallas_call(
        kernel,
        out_shape=(
            jax.ShapeDtypeStruct((FLAT, 128), F32),
            jax.ShapeDtypeStruct((2, 1, pixels), F32),
        ),
        in_specs=[hbm, hbm, pl.BlockSpec(memory_space=pltpu.SMEM)],
        out_specs=(vmem, vmem),
        scratch_shapes=[
            pltpu.VMEM((NB, pixels), jnp.int32),
            pltpu.VMEM((3, 32 * GROUPS, 128), F32),
            pltpu.VMEM((6, 2, PAD, 128), F32),
            pltpu.VMEM((TILES, 16, 128), jnp.int32),
            pltpu.VMEM((TILES, 16, 128), jnp.int32),
            pltpu.VMEM((TILES, NB, 3, PAD, 128), F32),
            pltpu.VMEM((TILES, PAD, 128), F32),
            pltpu.VMEM((8, 64, 128), F32),
            pltpu.VMEM((TILES, 16, 16, 128), F32),
            pltpu.VMEM((TILES, 16, 16, 128), F32),
            pltpu.VMEM((TILES, 2, 16, 128), F32),
            pltpu.VMEM((TILES, 2, 16, 128), F32),
            pltpu.VMEM((TILES, 2, 128), F32),
            pltpu.VMEM((TILES, 2, 16, 128), F32),
            pltpu.VMEM((TILES, 3, 16, 128), F32),
            pltpu.VMEM((3, 2, pixels), F32),
            pltpu.VMEM((2, pixels), F32),
            pltpu.VMEM((2, pixels), F32),
            pltpu.VMEM((3, 2, pixels), F32),
            pltpu.VMEM((TILES, 2, PAD, 128), F32),
            pltpu.VMEM((2, pixels), F32),
            pltpu.VMEM((1, 128), F32),
            pltpu.VMEM((7, 1, 128), F32),
            pltpu.VMEM((1, 128), F32),
            pltpu.VMEM((7, 1, 128), F32),
            pltpu.VMEM((16, 128), F32),
            pltpu.VMEM((32, 128), F32),
            pltpu.VMEM((7, 32, 128), F32),
            pltpu.VMEM((32, 128), F32),
            pltpu.VMEM((7, 32, 128), F32),
            pltpu.VMEM((32, 128), F32),
            pltpu.VMEM((2, 128), F32),
            pltpu.VMEM((31, 2, 128), F32),
            pltpu.VMEM((2, 128), F32),
            pltpu.VMEM((7, 2, 128), F32),
            pltpu.VMEM((4, 128), F32),
            pltpu.VMEM((7, 4, 128), F32),
            pltpu.VMEM((1, 16, 16, 128), F32),
            pltpu.VMEM((1, 16, 16, 128), F32),
            pltpu.VMEM((1, 2, 16, 128), F32),
            pltpu.VMEM((1, 2, 16, 128), F32),
            pltpu.VMEM((1, 3, 16, 128), F32),
            pltpu.VMEM((TILES, 16, 16, 128), F32),
            pltpu.VMEM((TILES, 16, 16, 128), F32),
            pltpu.VMEM((TILES, 2, 16, 128), F32),
            pltpu.VMEM((TILES, 2, 16, 128), F32),
            pltpu.VMEM((TILES, 2, 16, 128), F32),
            pltpu.VMEM((TILES, 1, 128), F32),
            pltpu.VMEM((1, 16, 16, 128), F32),
            pltpu.VMEM((1, 16, 16, 128), F32),
            pltpu.VMEM((1, 2, 16, 128), F32),
            pltpu.VMEM((1, 2, 16, 128), F32),
            pltpu.VMEM((TILES, 16, 16, 128), F32),
            pltpu.VMEM((TILES, 16, 16, 128), F32),
            pltpu.VMEM((1, 16, 16, 128), F32),
            pltpu.VMEM((1, 16, 16, 128), F32),
            dma((4,)),
            dma((2,)),
            dma((2, 3)),
            dma(()),
            dma(()),
            dma(()),
            dma((3,)),
            dma((2, 2)),
            dma(()),
            dma(()),
            dma(()),
            dma(()),
            dma((2,)),
            dma((2,)),
            pltpu.SemaphoreType.REGULAR((5,)),
        ],
        compiler_params=pltpu.CompilerParams(
            collective_id=0, has_side_effects=True, vmem_limit_bytes=16 * 2**20
        ),
        cost_estimate=pl.CostEstimate(flops=100_000_000, bytes_accessed=1_000_000, transcendentals=0),
    )(*(pltpu.with_memory_space_constraint(a, pltpu.HBM) for a in (flat, neighbours)), reference_pixel)
    phases, comp = pl.pallas_call(
        hand_out,
        out_shape=(
            jax.ShapeDtypeStruct((FLAT, 128), F32),
            jax.ShapeDtypeStruct((2, 1, pixels), F32),
        ),
        in_specs=[pl.BlockSpec(memory_space=pl.ANY)] * 2,
        out_specs=(hbm, hbm),
        scratch_shapes=[dma((2,))],
        compiler_params=pltpu.CompilerParams(vmem_limit_bytes=2**20),
    )(phases, comp)
    return phases.reshape(ROWS, TILES, 2, 128).transpose(2, 0, 1, 3).reshape(2, ROWS, pixels), comp


def solution(mesh):
    return jax.shard_map(
        on_device,
        mesh=mesh,
        in_specs=(P(None, "section", "pix"), P(None, "pix"), P()),
        out_specs=(P(None, "section", "pix"), P(None, "section", "pix")),
        check_vma=False,
    )
```
